32 devices in a mesh: fsdp: 4 (over y, x), cp: 8 (over z, core).
Axes of the slice: x: 2, y: 2, z: 4, core: 2. Of those that a mesh axis runs over, the one named last changes fastest.
Arguments:
- block_input: bfloat16 [4, 1024, 2048], P('fsdp', 'cp'), may hold values from -6 to 6
- cotangent: float32 [4, 1024, 2048], P('fsdp', 'cp'), may hold values from -6 to 6
- gain_attn: bfloat16 [2048], P(('fsdp', 'cp')), may hold values from 0.5 to 1.5
- w_query: bfloat16 [2048, 4096], P(('fsdp', 'cp')), may hold values from -0.125 to 0.125
- w_key: bfloat16 [2048, 512], P(('fsdp', 'cp')), may hold values from -0.125 to 0.125
- w_value: bfloat16 [2048, 512], P(('fsdp', 'cp')), may hold values from -0.125 to 0.125
- qk_gain: bfloat16 [2, 128], P(None, ('fsdp', 'cp')), as said below
- w_out: bfloat16 [4096, 2048], P(('fsdp', 'cp')), may hold values from -0.75 to 0.75
- gain_moe: bfloat16 [2048], P(('fsdp', 'cp')), may hold values from 0.5 to 1.5
- w_gate: bfloat16 [32, 2048, 768], P(('fsdp', 'cp')), may hold values from -0.125 to 0.125
- w_up: bfloat16 [32, 2048, 768], P(('fsdp', 'cp')), may hold values from -0.125 to 0.125
- w_down: bfloat16 [32, 768, 2048], P(('fsdp', 'cp')), may hold values from -0.4375 to 0.4375
- expert_ids: int32 [4, 1024, 8], P('fsdp', 'cp'), may hold values from 0 to 31, all different within a row; in each aligned block of 128 rows (0 to 127, 128 to 255, ..., all dimensions but the last counted through in order) at most 48 rows name the same one
- route_weight: bfloat16 [4, 1024, 8], P('fsdp', 'cp'), may hold values from 0.29882812 to 1
- pair_order: int32 [8], replicated, may hold values from 0 to 7, each once
Outputs:
- block_output: bfloat16 [4, 1024, 2048], P('fsdp', 'cp')
- grad_input: float32 [4, 1024, 2048], P('fsdp', 'cp')
- grad_gain_attn: float32 [2048], P(('fsdp', 'cp'))
- grad_w_query: float32 [2048, 4096], P(('fsdp', 'cp'))
- grad_w_key: float32 [2048, 512], P(('fsdp', 'cp'))
- grad_w_value: float32 [2048, 512], P(('fsdp', 'cp'))
- grad_qk_gain: float32 [2, 128], P(None, ('fsdp', 'cp'))
- grad_w_out: float32 [4096, 2048], P(('fsdp', 'cp'))
- grad_gain_moe: float32 [2048], P(('fsdp', 'cp'))
- grad_w_gate: float32 [32, 2048, 768], P(('fsdp', 'cp'))
- grad_w_up: float32 [32, 2048, 768], P(('fsdp', 'cp'))
- grad_w_down: float32 [32, 768, 2048], P(('fsdp', 'cp'))
The draws below stay inside these ranges and needn't reach their ends.
Inputs may be any that keep to these rules, and one draw needn't show every extreme that they name: `expert_ids`: each row names 8 different experts. The rows of one device (aligned blocks of 128 rows of the first two dimensions taken together) name no expert more than 48 times, and in every draw some device's rows name some expert exactly 48 times. `pair_order`: each value appears once. `qk_gain`: the two rows are positive gains.
All inputs are finite; a program needn't handle non-finite values.
Results may differ from the reference program's by a relative error of at most 0.022.
The reference program's roundings to bfloat16 on the way count: a program that leaves them out, or rounds other values in their place, can miss the bound.
Values may be sent and summed in bfloat16 or wider, within the bound.
A program may use at most 320 MiB of HBM per device.

```python
import math
import jax
import jax.numpy as jnp
import numpy as np
from jax import lax

D = 2048
HEADS = 32
KV_HEADS = 4
HD = 128
MOE_FF = 768
TOPK = 8
BLOCK = 64
EXPERTS = 32
BLOCKS = 16
SEQ = 1024
SEQS = 4
CAP = 48
N_FSDP = 4
N_CP = 8


def draw_qk_gain(key, part):
    values = jnp.exp(jax.random.uniform(key, (2, HD), jnp.float32, -0.4, 0.5))
    return values.astype(jnp.bfloat16)


def level_of(own_key, shape, shards, low, top_value):
    loudness, own = 1.0, jax.random.fold_in(own_key, 6)
    for position, parts in shards:
        steps = jnp.exp(jax.random.uniform(jax.random.fold_in(own, position), (parts,), jnp.float32, low / len(shards), top_value / len(shards)))
        loudness = loudness * jnp.repeat(steps, shape[position] // parts).reshape([-1 if axis == position else 1 for axis in range(len(shape))])
    return loudness


def shared_out(own_key, own, number, rows, amount, top, most, slope):
    order = jax.random.permutation(own_key, amount)
    crowded, usual = portions_of(amount, rows * top, most, slope, True), portions_of(amount, rows * top, most, slope, False)
    places = jnp.arange(amount)

    def named(lengths, turn):
        used = int((lengths > 0).sum())
        fixed = max(1, used // 4)
        shifted = fixed + (places - fixed + turn * (used - fixed)) % max(1, amount - fixed)
        return jnp.zeros((amount,), jnp.int32).at[order[jnp.where(places < fixed, places, shifted)]].set(jnp.asarray(lengths, jnp.int32))

    lengths = jnp.where(number % 4 == 0, named(crowded, number // 4), named(usual, number - number // 4 - 1))
    mixed = jax.random.permutation(jax.random.fold_in(own, 3), amount)
    giver, sink = mixed[0:amount // 2 * 2:2], mixed[1:amount // 2 * 2:2]
    room = jnp.minimum(lengths[giver] - 1, most - lengths[sink]) // 2
    room = jnp.where((giver == order[0]) | (sink == order[0]) | (lengths[sink] == 0), 0, jnp.maximum(room, 0))
    shifted = jax.random.randint(jax.random.fold_in(own, 4), (amount // 2,), 0, 1 << 20) % (room + 1)
    lengths = lengths.at[giver].add(-shifted).at[sink].add(shifted)
    items = jnp.searchsorted(jnp.cumsum(lengths), jnp.arange(rows * top), side="right").astype(jnp.int32)
    table = items.reshape(top, rows).T
    table = table[jax.random.permutation(jax.random.fold_in(own, 1), rows)]
    turn = jax.random.randint(jax.random.fold_in(own, 2), (rows, 1), 0, top)
    return jnp.take_along_axis(table, (jnp.arange(top)[None, :] + turn) % top, axis=1)


def portions_of(amount, total, reach, slope, full):
    portions = [(1 << 20) // math.isqrt(rank ** slope) + 1 for rank in range(1, amount + 1)]
    largest = reach if full else min(reach, max(-(-total // amount), total * portions[0] // sum(portions)))
    least = 1 if total - largest >= amount - 1 else 0
    given, spare = [largest] + [least] * (amount - 1), total - largest - least * (amount - 1)
    while spare > 0:
        candidates = [i for i in range(1, amount) if given[i] < largest] or [i for i in range(1, amount) if given[i] < reach]
        mass, remaining = sum([portions[i] for i in candidates]), spare
        for i in candidates:
            more = min(reach - given[i], max(1, remaining * portions[i] // mass), spare)
            given[i] = given[i] + more
            spare = spare - more
    return np.array(given)


def gaussian(rng, dims, scale, most, split=(), held_as=jnp.bfloat16):
    values = jax.random.normal(rng, dims, jnp.float32) * scale
    if len(split) > 0:
        values = level_of(rng, dims, split, -0.22, 0.18) * values
    return jnp.clip(values, min=-most, max=most).astype(held_as)


def setup_inputs(seed: int = 0) -> dict:
    seeds = jax.random.split(jax.random.key(seed), 16)
    block_input = gaussian(seeds[0], (SEQS, SEQ, D), 1.0, 6.0, ((0, 4), (1, 8)))
    cotangent = gaussian(seeds[1], (SEQS, SEQ, D), 1.0, 6.0, ((0, 4), (1, 8)), jnp.float32)
    gain_attn = jnp.clip(1.0 + 0.1 * jax.random.normal(seeds[2], (D,), jnp.float32), 0.5, 1.5).astype(jnp.bfloat16)
    w_query = gaussian(seeds[3], (D, HEADS * HD), D ** -0.5, 0.125, ((0, 32),))
    w_key = gaussian(seeds[4], (D, KV_HEADS * HD), D ** -0.5, 0.125, ((0, 32),))
    w_value = gaussian(seeds[5], (D, KV_HEADS * HD), D ** -0.5, 0.125, ((0, 32),))
    qk_gain = draw_qk_gain(jax.random.fold_in(seeds[15], 71), 0)
    w_out = gaussian(seeds[7], (HEADS * HD, D), (HEADS * HD // 64) ** -0.5, 0.75, ((0, 32),))
    gain_moe = jnp.clip(1.0 + 0.1 * jax.random.normal(seeds[8], (D,), jnp.float32), 0.5, 1.5).astype(jnp.bfloat16)
    w_gate = gaussian(seeds[9], (EXPERTS, D, MOE_FF), D ** -0.5, 0.125, ((0, 32),))
    w_up = gaussian(seeds[10], (EXPERTS, D, MOE_FF), D ** -0.5, 0.125, ((0, 32),))
    w_down = gaussian(seeds[11], (EXPERTS, MOE_FF, D), (MOE_FF // 4) ** -0.5, 0.4375, ((0, 32),))
    expert_ids_keys = jax.random.split(jax.random.fold_in(seeds[12], 1), SEQS * SEQ // (2 * BLOCK))
    expert_ids_turns = jax.random.permutation(jax.random.fold_in(seeds[12], 3), SEQS * SEQ // (2 * BLOCK))
    expert_ids = jax.vmap(lambda own, number: shared_out(jax.random.fold_in(seeds[12], 2), own, number, 2 * BLOCK, EXPERTS, TOPK, CAP, 2))(expert_ids_keys, expert_ids_turns).reshape((SEQS, SEQ, TOPK))
    route_weight = jnp.clip(0.29882812 + 0.7011719 * jax.random.uniform(seeds[13], (SEQS, SEQ, TOPK), jnp.float32) ** level_of(seeds[13], (SEQS, SEQ, TOPK), ((0, 4), (1, 8)), -0.2, 0.2), 0.29882812, 1.0).astype(jnp.bfloat16)
    pair_order = jax.random.permutation(seeds[14], BLOCKS // 2).astype(jnp.int32)
    return dict(block_input=block_input, cotangent=cotangent, gain_attn=gain_attn, w_query=w_query, w_key=w_key, w_value=w_value, qk_gain=qk_gain, w_out=w_out, gain_moe=gain_moe, w_gate=w_gate, w_up=w_up, w_down=w_down, expert_ids=expert_ids, route_weight=route_weight, pair_order=pair_order)


EPSILON = 1e-06
THETA = 1000000.0

def rms_scale(values, gain):
    return values * lax.rsqrt(lax.optimization_barrier(jnp.mean(values * values, axis=-1, keepdims=True)) + EPSILON) * gain

def rotate_half(values):
    half = values.shape[-1] // 2
    return jnp.concatenate([-values[..., half:], values[..., :half]], axis=-1)

def head_post(pre, gain, cosine, sine):
    normed = rms_scale(pre, gain)
    return normed * cosine[:, None, :] + rotate_half(normed) * sine[:, None, :]

def rope_tables(positions, head_dim):
    freqs = THETA ** (-(jnp.arange(head_dim // 2, dtype=jnp.float32) * 2.0 / head_dim))
    angles = positions.astype(jnp.float32)[:, None] * freqs[None, :]
    angles = jnp.concatenate([angles, angles], axis=-1)
    return (jnp.cos(angles), jnp.sin(angles))

def seq_positions(pair_order, block):
    blocks = 2 * pair_order.shape[0]
    rows = jnp.arange(blocks * block, dtype=jnp.int32)
    owner = rows // (2 * block)
    first = pair_order[owner]
    which = jnp.where(rows // block % 2 == 0, first, blocks - 1 - first)
    return (which * block + rows % block).astype(jnp.int32)

def route_slots(ids, experts, capacity):
    flat = ids.reshape(-1)
    onehot = (flat[:, None] == jnp.arange(experts, dtype=jnp.int32)[None, :]).astype(jnp.int32)
    before = jnp.cumsum(onehot, axis=0) - onehot
    rank = lax.optimization_barrier(jnp.sum(before * onehot, axis=1))
    return (flat * capacity + rank).astype(jnp.int32).reshape(ids.shape)

def attend_head(query, keys, values, allowed, scale):
    scores = jnp.einsum('grd,sd->grs', query.astype(jnp.float32), keys.astype(jnp.float32)) * scale
    scores = jnp.where(allowed[None], scores, -jnp.inf)
    top = lax.optimization_barrier(jnp.max(scores, axis=-1, keepdims=True))
    lse = top[..., 0] + jnp.log(lax.optimization_barrier(jnp.sum(jnp.exp(scores - top), axis=-1)))
    probs = jnp.exp(scores - lse[..., None]).astype(jnp.bfloat16)
    output = jnp.einsum('grs,sd->grd', probs.astype(jnp.float32), values.astype(jnp.float32))
    return (output.astype(jnp.bfloat16), lse)

def attend_back(query, keys, values, output, grad_out, lse, allowed, scale):
    scores = jnp.einsum('grd,sd->grs', query.astype(jnp.float32), keys.astype(jnp.float32)) * scale
    scores = jnp.where(allowed[None], scores, -jnp.inf)
    probs = jnp.exp(scores - lse[..., None])
    grad_out32 = grad_out.astype(jnp.float32)
    grad_values = jnp.einsum('grs,grd->sd', probs.astype(jnp.bfloat16).astype(jnp.float32), grad_out32)
    grad_probs = jnp.einsum('grd,sd->grs', grad_out32, values.astype(jnp.float32))
    delta = lax.optimization_barrier(jnp.sum(grad_out32 * output.astype(jnp.float32), axis=-1))
    grad_scores = (probs * (grad_probs - delta[..., None])).astype(jnp.bfloat16).astype(jnp.float32)
    grad_query = jnp.einsum('grs,sd->grd', grad_scores, keys.astype(jnp.float32)) * scale
    grad_keys = jnp.einsum('grs,grd->sd', grad_scores, query.astype(jnp.float32)) * scale
    return (grad_query, grad_keys, grad_values)

def reference(block_input, cotangent, gain_attn, w_query, w_key, w_value, qk_gain, w_out, gain_moe, w_gate, w_up, w_down, expert_ids, route_weight, pair_order):
    group = HEADS // KV_HEADS
    rows = 2 * BLOCK
    devices = N_FSDP * N_CP
    total = SEQS * SEQ
    all_pos = seq_positions(pair_order, BLOCK)
    cosine, sine = rope_tables(all_pos, HD)
    allowed = all_pos[None, :] <= all_pos[:, None]
    scale = 1.0 / math.sqrt(HD)
    attn_gain = gain_attn.astype(jnp.float32)
    moe_gain = gain_moe.astype(jnp.float32)
    gains32 = qk_gain.astype(jnp.float32)

    def attn_forward(seq_in):
        resid = seq_in.astype(jnp.float32)
        normed_in = rms_scale(resid, attn_gain).astype(jnp.bfloat16)
        q_pre = jnp.dot(normed_in, w_query, preferred_element_type=jnp.float32).reshape(SEQ, HEADS, HD)
        k_pre = jnp.dot(normed_in, w_key, preferred_element_type=jnp.float32).reshape(SEQ, KV_HEADS, HD)
        value_rows = jnp.dot(normed_in, w_value, preferred_element_type=jnp.float32).astype(jnp.bfloat16)
        query_rot = head_post(q_pre, gains32[0], cosine, sine).astype(jnp.bfloat16)
        key_rot = head_post(k_pre, gains32[1], cosine, sine).astype(jnp.bfloat16)
        query_heads = query_rot.reshape(SEQ, KV_HEADS, group, HD).transpose(1, 2, 0, 3)
        key_heads = key_rot.transpose(1, 0, 2)
        value_heads = value_rows.reshape(SEQ, KV_HEADS, HD).transpose(1, 0, 2)
        context_heads, lse = lax.map(lambda item: attend_head(item[0], item[1], item[2], allowed, scale), (query_heads, key_heads, value_heads))
        context = context_heads.transpose(2, 0, 1, 3).reshape(SEQ, HEADS * HD)
        hidden_res = resid + jnp.dot(context, w_out, preferred_element_type=jnp.float32)
        return (normed_in, q_pre, k_pre, query_heads, key_heads, value_heads, context_heads, lse, context, hidden_res)
    hidden_all = lax.map(lambda seq_in: attn_forward(seq_in)[-1], block_input)
    normed_mid = rms_scale(hidden_all, moe_gain).astype(jnp.bfloat16).reshape(total, D)
    ids_dev = expert_ids.reshape(devices, rows, TOPK)
    weight_dev = route_weight.reshape(devices, rows, TOPK)
    slots = jax.vmap(lambda ids: route_slots(ids, EXPERTS, CAP))(ids_dev)
    token_index = (jnp.arange(devices, dtype=jnp.int32)[:, None] * rows + jnp.arange(rows, dtype=jnp.int32)[None, :]).astype(jnp.int32)
    token_index = jnp.broadcast_to(token_index[:, :, None], (devices, rows, TOPK))

    def fill_table(slot_rows, tokens):
        return jnp.full((EXPERTS * CAP,), total, jnp.int32).at[slot_rows.reshape(-1)].set(tokens.reshape(-1))

    def fill_weights(slot_rows, weights):
        return jnp.zeros((EXPERTS * CAP,), jnp.bfloat16).at[slot_rows.reshape(-1)].set(weights.reshape(-1))
    table = jax.vmap(fill_table)(slots, token_index).reshape(devices, EXPERTS, CAP).transpose(1, 0, 2).reshape(EXPERTS, devices * CAP)
    wtable = jax.vmap(fill_weights)(slots, weight_dev).reshape(devices, EXPERTS, CAP).transpose(1, 0, 2).reshape(EXPERTS, devices * CAP)
    mid_pad = jnp.concatenate([normed_mid, jnp.zeros((1, D), jnp.bfloat16)], axis=0)
    top_pad = jnp.concatenate([cotangent.reshape(total, D).astype(jnp.bfloat16), jnp.zeros((1, D), jnp.bfloat16)], axis=0)

    def expert_step(carry, item):
        mixed_acc, grad_acc = carry
        gate_w, up_w, down_w, index, weights = item
        arrived = mid_pad[index]
        gate_pre = jnp.dot(arrived, gate_w, preferred_element_type=jnp.float32)
        up_pre = jnp.dot(arrived, up_w, preferred_element_type=jnp.float32)
        gate_sig = jax.nn.sigmoid(gate_pre)
        gate_act = gate_pre * gate_sig
        expert_hidden = (gate_act * up_pre).astype(jnp.bfloat16)
        expert_out = jnp.dot(expert_hidden, down_w, preferred_element_type=jnp.float32).astype(jnp.bfloat16)
        weights32 = weights.astype(jnp.float32)[:, None]
        mixed_acc = mixed_acc.at[index].add(weights32 * expert_out.astype(jnp.float32))
        grad_eo = (weights32 * top_pad[index].astype(jnp.float32)).astype(jnp.bfloat16)
        grad_hidden = jnp.dot(grad_eo, down_w.T, preferred_element_type=jnp.float32)
        grad_down = jnp.dot(expert_hidden.T, grad_eo, preferred_element_type=jnp.float32)
        grad_gate_pre = (grad_hidden * up_pre * gate_sig * (1.0 + gate_pre * (1.0 - gate_sig))).astype(jnp.bfloat16)
        grad_up_pre = (grad_hidden * gate_act).astype(jnp.bfloat16)
        grad_gate = jnp.dot(arrived.T, grad_gate_pre, preferred_element_type=jnp.float32)
        grad_up = jnp.dot(arrived.T, grad_up_pre, preferred_element_type=jnp.float32)
        grad_rows = (jnp.dot(grad_gate_pre, gate_w.T, preferred_element_type=jnp.float32) + jnp.dot(grad_up_pre, up_w.T, preferred_element_type=jnp.float32)).astype(jnp.bfloat16)
        grad_acc = grad_acc.at[index].add(grad_rows.astype(jnp.float32))
        return ((mixed_acc, grad_acc), (grad_gate, grad_up, grad_down))
    start = (jnp.zeros((total + 1, D), jnp.float32), jnp.zeros((total + 1, D), jnp.float32))
    (mixed_acc, grad_acc), (grad_w_gate, grad_w_up, grad_w_down) = lax.scan(expert_step, start, (w_gate, w_up, w_down, table, wtable))
    mixed = mixed_acc[:total].reshape(SEQS, SEQ, D)
    grad_mid_all = grad_acc[:total].reshape(SEQS, SEQ, D)
    block_output = (hidden_all + mixed).astype(jnp.bfloat16)

    def back_step(carry, item):
        seq_in, seq_top, hidden_res, grad_mid = item
        normed_in, q_pre, k_pre, query_heads, key_heads, value_heads, context_heads, lse, context, hidden_again = attn_forward(seq_in)
        _, mid_back = jax.vjp(rms_scale, hidden_res, moe_gain)
        grad_res_mid, grad_moe_gain = mid_back(grad_mid)
        grad_res = seq_top + grad_res_mid
        grad_res_b = grad_res.astype(jnp.bfloat16)
        grad_wo = jnp.dot(context.T, grad_res_b, preferred_element_type=jnp.float32)
        grad_context = jnp.dot(grad_res_b, w_out.T, preferred_element_type=jnp.float32).astype(jnp.bfloat16)
        grad_ctx_heads = grad_context.reshape(SEQ, KV_HEADS, group, HD).transpose(1, 2, 0, 3)
        grad_q_heads, grad_k_heads, grad_v_heads = lax.map(lambda it: attend_back(it[0], it[1], it[2], it[3], it[4], it[5], allowed, scale), (query_heads, key_heads, value_heads, context_heads, grad_ctx_heads, lse))
        grad_query_rot = grad_q_heads.transpose(2, 0, 1, 3).reshape(SEQ, HEADS, HD)
        grad_key_rot = grad_k_heads.transpose(1, 0, 2)
        grad_values = grad_v_heads.transpose(1, 0, 2).reshape(SEQ, KV_HEADS * HD)
        _, query_back = jax.vjp(lambda pre, gain: head_post(pre, gain, cosine, sine), q_pre, gains32[0])
        grad_q_pre, grad_q_gain = query_back(grad_query_rot)
        _, key_back = jax.vjp(lambda pre, gain: head_post(pre, gain, cosine, sine), k_pre, gains32[1])
        grad_k_pre, grad_k_gain = key_back(grad_key_rot)
        grad_q_b = grad_q_pre.reshape(SEQ, HEADS * HD).astype(jnp.bfloat16)
        grad_k_b = grad_k_pre.reshape(SEQ, KV_HEADS * HD).astype(jnp.bfloat16)
        grad_v_b = grad_values.astype(jnp.bfloat16)
        grad_wq = jnp.dot(normed_in.T, grad_q_b, preferred_element_type=jnp.float32)
        grad_wk = jnp.dot(normed_in.T, grad_k_b, preferred_element_type=jnp.float32)
        grad_wv = jnp.dot(normed_in.T, grad_v_b, preferred_element_type=jnp.float32)
        grad_in_norm = jnp.dot(grad_q_b, w_query.T, preferred_element_type=jnp.float32) + jnp.dot(grad_k_b, w_key.T, preferred_element_type=jnp.float32) + jnp.dot(grad_v_b, w_value.T, preferred_element_type=jnp.float32)
        _, in_back = jax.vjp(rms_scale, seq_in.astype(jnp.float32), attn_gain)
        grad_res_in, grad_attn_gain = in_back(grad_in_norm)
        grad_input = grad_res + grad_res_in
        sums = (grad_attn_gain, grad_wq, grad_wk, grad_wv, jnp.stack([grad_q_gain, grad_k_gain]), grad_wo, grad_moe_gain)
        carry = tuple((a + b for a, b in zip(carry, sums)))
        return (carry, grad_input)
    zero_sums = (jnp.zeros((D,), jnp.float32), jnp.zeros((D, HEADS * HD), jnp.float32), jnp.zeros((D, KV_HEADS * HD), jnp.float32), jnp.zeros((D, KV_HEADS * HD), jnp.float32), jnp.zeros((2, HD), jnp.float32), jnp.zeros((HEADS * HD, D), jnp.float32), jnp.zeros((D,), jnp.float32))
    sums, grad_input = lax.scan(back_step, zero_sums, (block_input, cotangent, hidden_all, grad_mid_all))
    grad_gain_attn, grad_w_query, grad_w_key, grad_w_value, grad_qk_gain, grad_w_out, grad_gain_moe = sums
    return (block_output, grad_input, grad_gain_attn, grad_w_query, grad_w_key, grad_w_value, grad_qk_gain, grad_w_out, grad_gain_moe, grad_w_gate, grad_w_up, grad_w_down)
```

```python
import functools
import math

import jax
import jax.numpy as jnp
from jax import lax
from jax.experimental import pallas as pl
from jax.experimental.pallas import tpu as pltpu
from jax.sharding import PartitionSpec as P

BLOCK = 64


EPSILON = 1e-06
THETA = 1000000.0


def rms_scale(values, gain):
    return values * lax.rsqrt(jnp.mean(values * values, axis=-1, keepdims=True) + EPSILON) * gain


def rotate_half(values):
    half = values.shape[-1] // 2
    return jnp.concatenate([-values[..., half:], values[..., :half]], axis=-1)


def head_post(pre, gain, cosine, sine):
    normed = rms_scale(pre, gain)
    return normed * cosine[:, None, :] + rotate_half(normed) * sine[:, None, :]


def rope_tables(positions, head_dim):
    freqs = THETA ** (-(jnp.arange(head_dim // 2, dtype=jnp.float32) * 2.0 / head_dim))
    angles = positions.astype(jnp.float32)[:, None] * freqs[None, :]
    angles = jnp.concatenate([angles, angles], axis=-1)
    return (jnp.cos(angles), jnp.sin(angles))


def seq_positions(pair_order, block):
    blocks = 2 * pair_order.shape[0]
    rows = jnp.arange(blocks * block, dtype=jnp.int32)
    owner = rows // (2 * block)
    first = pair_order[owner]
    which = jnp.where(rows // block % 2 == 0, first, blocks - 1 - first)
    return which * block + rows % block


def route_tables(ids, weights, experts, capacity):
    flat = ids.reshape(-1)
    onehot = (flat[:, None] == jnp.arange(experts, dtype=jnp.int32)[None, :]).astype(jnp.int32)
    before = jnp.cumsum(onehot, axis=0) - onehot
    rank = jnp.sum(before * onehot, axis=1)
    slots = (flat * capacity + rank).reshape(ids.shape)
    columns = jnp.arange(experts * capacity, dtype=jnp.int32)
    hits = slots[:, :, None] == columns[None, None, :]
    place = jnp.sum(hits.astype(jnp.float32), axis=1).astype(jnp.bfloat16)
    mixing = jnp.sum(jnp.where(hits, weights[:, :, None].astype(jnp.float32), 0.0), axis=1).astype(
        jnp.bfloat16
    )
    return (place, mixing)


def attend_head(query, keys, values, allowed, scale):
    scores = jnp.einsum("grd,sd->grs", query, keys, preferred_element_type=jnp.float32) * scale
    scores = jnp.where(allowed[None], scores, -jnp.inf)
    top = jnp.max(scores, axis=-1, keepdims=True)
    lse = top[..., 0] + jnp.log(jnp.sum(jnp.exp(scores - top), axis=-1))
    probs = jnp.exp(scores - lse[..., None]).astype(jnp.bfloat16)
    output = jnp.einsum("grs,sd->grd", probs, values, preferred_element_type=jnp.float32)
    return (output.astype(jnp.bfloat16), lse)


def attend_back(query, keys, values, output, grad_out, lse, allowed, scale):
    scores = jnp.einsum("grd,sd->grs", query, keys, preferred_element_type=jnp.float32) * scale
    scores = jnp.where(allowed[None], scores, -jnp.inf)
    probs = jnp.exp(scores - lse[..., None])
    grad_values = jnp.einsum(
        "grs,grd->sd", probs.astype(jnp.bfloat16), grad_out, preferred_element_type=jnp.float32
    )
    grad_probs = jnp.einsum("grd,sd->grs", grad_out, values, preferred_element_type=jnp.float32)
    delta = jnp.sum(grad_out.astype(jnp.float32) * output.astype(jnp.float32), axis=-1)
    grad_scores = (probs * (grad_probs - delta[..., None])).astype(jnp.bfloat16)
    grad_query = (
        jnp.einsum("grs,sd->grd", grad_scores, keys, preferred_element_type=jnp.float32) * scale
    )
    grad_keys = (
        jnp.einsum("grs,grd->sd", grad_scores, query, preferred_element_type=jnp.float32) * scale
    )
    return (grad_query, grad_keys, grad_values)


def contract_rows(left, right):
    return lax.dot_general(
        left, right, (((0,), (0,)), ((), ())), preferred_element_type=jnp.float32
    )


def contract_cols(left, right):
    return lax.dot_general(
        left, right, (((1,), (1,)), ((), ())), preferred_element_type=jnp.float32
    )


def wide_body(
    block_input,
    cotangent,
    gain_attn,
    w_query,
    w_key,
    w_value,
    qk_gain,
    w_out,
    gain_moe,
    w_gate,
    w_up,
    w_down,
    expert_ids,
    route_weight,
    pair_order,
):
    g_attn, wq_full, wk_full, wv_full, qk_full, wo_full, g_moe = (
        lax.all_gather(gain_attn, ("fsdp", "cp"), axis=0, tiled=True),
        lax.all_gather(w_query, ("fsdp", "cp"), axis=0, tiled=True),
        lax.all_gather(w_key, ("fsdp", "cp"), axis=0, tiled=True),
        lax.all_gather(w_value, ("fsdp", "cp"), axis=0, tiled=True),
        lax.all_gather(qk_gain, ("fsdp", "cp"), axis=1, tiled=True),
        lax.all_gather(w_out, ("fsdp", "cp"), axis=0, tiled=True),
        lax.all_gather(gain_moe, ("fsdp", "cp"), axis=0, tiled=True),
    )
    rows = block_input.shape[1]
    width = block_input.shape[2]
    head_dim = qk_full.shape[1]
    kv_heads = wk_full.shape[1] // head_dim
    heads = wq_full.shape[1] // head_dim
    group = heads // kv_heads
    experts = lax.axis_size(("fsdp", "cp"))
    capacity = max(2, 3 * BLOCK * expert_ids.shape[2] // experts)
    scale = 1.0 / math.sqrt(head_dim)
    resid = block_input[0].astype(jnp.float32)
    normed_in = rms_scale(resid, g_attn.astype(jnp.float32)).astype(jnp.bfloat16)
    q_pre = jnp.dot(normed_in, wq_full, preferred_element_type=jnp.float32).reshape(
        rows, heads, head_dim
    )
    k_pre = jnp.dot(normed_in, wk_full, preferred_element_type=jnp.float32).reshape(
        rows, kv_heads, head_dim
    )
    value_rows = jnp.dot(normed_in, wv_full, preferred_element_type=jnp.float32).astype(
        jnp.bfloat16
    )
    all_pos = seq_positions(pair_order, BLOCK)
    local_pos = lax.dynamic_slice_in_dim(all_pos, lax.axis_index("cp") * rows, rows)
    cosine, sine = rope_tables(local_pos, head_dim)
    gains32 = qk_full.astype(jnp.float32)
    query_rot = head_post(q_pre, gains32[0], cosine, sine).astype(jnp.bfloat16)
    key_rot = head_post(k_pre, gains32[1], cosine, sine).astype(jnp.bfloat16)
    keys_all, values_all = (
        lax.all_gather(key_rot.reshape(rows, kv_heads * head_dim), "cp", axis=0, tiled=True),
        lax.all_gather(value_rows, "cp", axis=0, tiled=True),
    )
    span = keys_all.shape[0]
    allowed = all_pos[None, :] <= local_pos[:, None]
    query_heads = query_rot.reshape(rows, kv_heads, group, head_dim).transpose(1, 2, 0, 3)
    key_heads = keys_all.reshape(span, kv_heads, head_dim).transpose(1, 0, 2)
    value_heads = values_all.reshape(span, kv_heads, head_dim).transpose(1, 0, 2)
    context_heads, lse = lax.map(
        lambda item: attend_head(item[0], item[1], item[2], allowed, scale),
        (query_heads, key_heads, value_heads),
    )
    context = context_heads.transpose(2, 0, 1, 3).reshape(rows, heads * head_dim)
    hidden_res = resid + jnp.dot(context, wo_full, preferred_element_type=jnp.float32)
    normed_mid = rms_scale(hidden_res, g_moe.astype(jnp.float32)).astype(jnp.bfloat16)
    place, mixing = route_tables(expert_ids[0], route_weight[0], experts, capacity)
    sent = contract_rows(place, normed_mid).astype(jnp.bfloat16)
    arrived = lax.all_to_all(
        sent.reshape(experts, capacity, width),
        ("fsdp", "cp"),
        split_axis=0,
        concat_axis=0,
        tiled=True,
    ).reshape(experts * capacity, width)
    gate_w = w_gate[0]
    up_w = w_up[0]
    down_w = w_down[0]
    gate_pre = jnp.dot(arrived, gate_w, preferred_element_type=jnp.float32)
    up_pre = jnp.dot(arrived, up_w, preferred_element_type=jnp.float32)
    gate_sig = jax.nn.sigmoid(gate_pre)
    gate_act = gate_pre * gate_sig
    expert_hidden = (gate_act * up_pre).astype(jnp.bfloat16)
    expert_out = jnp.dot(expert_hidden, down_w, preferred_element_type=jnp.float32).astype(
        jnp.bfloat16
    )
    returned = lax.all_to_all(
        expert_out.reshape(experts, capacity, width),
        ("fsdp", "cp"),
        split_axis=0,
        concat_axis=0,
        tiled=True,
    ).reshape(experts * capacity, width)
    mixed = jnp.dot(mixing, returned, preferred_element_type=jnp.float32)
    block_output = (hidden_res + mixed).astype(jnp.bfloat16)
    g_attn, wq_full, wk_full, wv_full, qk_full, wo_full, g_moe = (
        lax.all_gather(gain_attn, ("fsdp", "cp"), axis=0, tiled=True),
        lax.all_gather(w_query, ("fsdp", "cp"), axis=0, tiled=True),
        lax.all_gather(w_key, ("fsdp", "cp"), axis=0, tiled=True),
        lax.all_gather(w_value, ("fsdp", "cp"), axis=0, tiled=True),
        lax.all_gather(qk_gain, ("fsdp", "cp"), axis=1, tiled=True),
        lax.all_gather(w_out, ("fsdp", "cp"), axis=0, tiled=True),
        lax.all_gather(gain_moe, ("fsdp", "cp"), axis=0, tiled=True),
    )
    attn_gain = g_attn.astype(jnp.float32)
    moe_gain = g_moe.astype(jnp.float32)
    gains_back = qk_full.astype(jnp.float32)
    grad_top = cotangent[0]
    grad_top_b = grad_top.astype(jnp.bfloat16)
    grad_sent = contract_rows(mixing, grad_top_b).astype(jnp.bfloat16)
    grad_arrived = lax.all_to_all(
        grad_sent.reshape(experts, capacity, width),
        ("fsdp", "cp"),
        split_axis=0,
        concat_axis=0,
        tiled=True,
    ).reshape(experts * capacity, width)
    grad_hidden = contract_cols(grad_arrived, down_w)
    grad_down = contract_rows(expert_hidden, grad_arrived)
    grad_gate_pre = (grad_hidden * up_pre * gate_sig * (1.0 + gate_pre * (1.0 - gate_sig))).astype(
        jnp.bfloat16
    )
    grad_up_pre = (grad_hidden * gate_act).astype(jnp.bfloat16)
    grad_gate = contract_rows(arrived, grad_gate_pre)
    grad_up = contract_rows(arrived, grad_up_pre)
    grad_rows = (contract_cols(grad_gate_pre, gate_w) + contract_cols(grad_up_pre, up_w)).astype(
        jnp.bfloat16
    )
    grad_back = lax.all_to_all(
        grad_rows.reshape(experts, capacity, width),
        ("fsdp", "cp"),
        split_axis=0,
        concat_axis=0,
        tiled=True,
    ).reshape(experts * capacity, width)
    grad_mid = jnp.dot(place, grad_back, preferred_element_type=jnp.float32)
    _, mid_back = jax.vjp(rms_scale, hidden_res, moe_gain)
    grad_res_mid, grad_moe_gain = mid_back(grad_mid)
    grad_res = grad_top + grad_res_mid
    grad_res_b = grad_res.astype(jnp.bfloat16)
    grad_wo = contract_rows(context, grad_res_b)
    grad_context = contract_cols(grad_res_b, wo_full).astype(jnp.bfloat16)
    grad_ctx_heads = grad_context.reshape(rows, kv_heads, group, head_dim).transpose(1, 2, 0, 3)
    grad_q_heads, grad_k_heads, grad_v_heads = lax.map(
        lambda it: attend_back(it[0], it[1], it[2], it[3], it[4], it[5], allowed, scale),
        (query_heads, key_heads, value_heads, context_heads, grad_ctx_heads, lse),
    )
    grad_keys_all = grad_k_heads.transpose(1, 0, 2).reshape(span, kv_heads * head_dim)
    grad_values_all = grad_v_heads.transpose(1, 0, 2).reshape(span, kv_heads * head_dim)
    grad_key_rot, grad_values = (
        lax.psum_scatter(
            grad_keys_all.astype(jnp.bfloat16), "cp", scatter_dimension=0, tiled=True
        ).astype(jnp.float32),
        lax.psum_scatter(
            grad_values_all.astype(jnp.bfloat16), "cp", scatter_dimension=0, tiled=True
        ).astype(jnp.float32),
    )
    grad_query_rot = grad_q_heads.transpose(2, 0, 1, 3).reshape(rows, heads, head_dim)
    _, query_back = jax.vjp(
        lambda pre, gain: head_post(pre, gain, cosine, sine), q_pre, gains_back[0]
    )
    grad_q_pre, grad_q_gain = query_back(grad_query_rot)
    _, key_back = jax.vjp(
        lambda pre, gain: head_post(pre, gain, cosine, sine), k_pre, gains_back[1]
    )
    grad_k_pre, grad_k_gain = key_back(grad_key_rot.reshape(rows, kv_heads, head_dim))
    grad_q_b = grad_q_pre.reshape(rows, heads * head_dim).astype(jnp.bfloat16)
    grad_k_b = grad_k_pre.reshape(rows, kv_heads * head_dim).astype(jnp.bfloat16)
    grad_v_b = grad_values.astype(jnp.bfloat16)
    grad_wq = contract_rows(normed_in, grad_q_b)
    grad_wk = contract_rows(normed_in, grad_k_b)
    grad_wv = contract_rows(normed_in, grad_v_b)
    grad_in_norm = (
        contract_cols(grad_q_b, wq_full)
        + contract_cols(grad_k_b, wk_full)
        + contract_cols(grad_v_b, wv_full)
    )
    _, in_back = jax.vjp(rms_scale, resid, attn_gain)
    grad_res_in, grad_attn_gain = in_back(grad_in_norm)
    grad_input = grad_res + grad_res_in
    grad_qk = jnp.stack([grad_q_gain, grad_k_gain])
    owned_grads = (
        lax.psum_scatter(grad_attn_gain, ("fsdp", "cp"), scatter_dimension=0, tiled=True),
        lax.psum_scatter(grad_wq, ("fsdp", "cp"), scatter_dimension=0, tiled=True),
        lax.psum_scatter(grad_wk, ("fsdp", "cp"), scatter_dimension=0, tiled=True),
        lax.psum_scatter(grad_wv, ("fsdp", "cp"), scatter_dimension=0, tiled=True),
        lax.psum_scatter(grad_qk, ("fsdp", "cp"), scatter_dimension=1, tiled=True),
        lax.psum_scatter(grad_wo, ("fsdp", "cp"), scatter_dimension=0, tiled=True),
        lax.psum_scatter(grad_moe_gain, ("fsdp", "cp"), scatter_dimension=0, tiled=True),
    )
    return (
        block_output[None],
        grad_input[None],
        owned_grads[0],
        owned_grads[1],
        owned_grads[2],
        owned_grads[3],
        owned_grads[4],
        owned_grads[5],
        owned_grads[6],
        grad_gate[None],
        grad_up[None],
        grad_down[None],
    )


MESH = pl.DeviceIdType.MESH
ANY = pl.BlockSpec(memory_space=pl.ANY)
VM = pl.BlockSpec(memory_space=pltpu.VMEM)


def place_of():
    f = lax.axis_index("fsdp")
    c = lax.axis_index("cp")
    return f, c, c // 2, c % 2


def flip(f, bit):
    return f + bit - 2 * bit * ((f // bit) % 2)


class Wire:
    def __init__(self):
        self.sent = []

    def send(self, src, dst, ssem, rsem, dev, when=None):
        copy = pltpu.make_async_remote_copy(
            src_ref=src, dst_ref=dst, send_sem=ssem, recv_sem=rsem, device_id=dev, device_id_type=MESH
        )
        if when is None:
            copy.start()
        else:
            pl.when(when)(copy.start)
        self.sent.append((copy, when))

    def drain(self):
        for copy, when in self.sent:
            if when is None:
                copy.wait_send()
            else:
                pl.when(when)(copy.wait_send)


def got(dst, ssem, rsem, dev, when=None):
    copy = pltpu.make_async_remote_copy(
        src_ref=dst, dst_ref=dst, send_sem=ssem, recv_sem=rsem, device_id=dev, device_id_type=MESH
    )
    if when is None:
        copy.wait_recv()
    else:
        pl.when(when)(copy.wait_recv)


def greet(f, c, z, zs, planes):
    bar = pltpu.get_barrier_semaphore()
    k = c % 2
    sib = c + 1 - 2 * k
    near = [((f, sib), None), ((f, c + 2), z < zs - 1), ((f, c - 2), z > 0)]
    if planes:
        near += [((flip(f, 1), c), None), ((flip(f, 2), c), None)]
    for dev, when in near:
        def hello(dev=dev):
            pl.semaphore_signal(bar, inc=1, device_id=dev, device_id_type=MESH)
        if when is None:
            hello()
        else:
            pl.when(when)(hello)
    base = 3 if planes else 1
    inner = jnp.logical_and(z > 0, z < zs - 1)
    pl.semaphore_wait(bar, base + jnp.where(inner, 2, 1))


def ag_kernel(zs, planes, x_ref, o_ref, loc, sl, szr, szl, rz, sp1, rp1, sp2, rp2, ssib, rsib):
    f, c, z, k = place_of()
    half = x_ref.shape[1] // 2
    sib = (f, c + 1 - 2 * k)
    b1 = 1 + k
    b2 = 2 - k
    f1 = flip(f, b1)
    f2 = flip(f, b2)
    cols = [f, f1, f2, flip(f1, b2)] if planes else [0]
    cs = 2 * zs

    def chunk(col, zz):
        at = (cols[col] * cs if planes else 0) + 2 * zz
        return o_ref.at[pl.ds(at, 2), :, pl.ds(pl.multiple_of(k * half, 128), half)]

    def other(col, zz):
        at = (cols[col] * cs if planes else 0) + 2 * zz
        return o_ref.at[pl.ds(at, 2), :, pl.ds(pl.multiple_of((1 - k) * half, 128), half)]

    mine = (f * cs if planes else 0) + c
    theirs = (f * cs if planes else 0) + c + 1 - 2 * k
    own = pltpu.make_async_copy(x_ref, o_ref.at[mine], loc)
    own.start()
    greet(f, c, z, zs, planes)
    w = Wire()
    w.send(x_ref, o_ref.at[mine], sl.at[0], sl.at[1], sib)
    own.wait()
    got(o_ref.at[theirs], sl.at[0], sl.at[1], sib)

    def spread(zz, when):
        if planes:
            w.send(chunk(0, zz), chunk(0, zz), sp1.at[zz], rp1.at[zz], (f1, c), when)
            w.send(chunk(0, zz), chunk(0, zz), sp2.at[zz], rp2.at[zz], (f2, c), when)

    def relay(zz, when):
        if planes:
            got(chunk(1, zz), sp1.at[zz], rp1.at[zz], (f1, c), when)
            w.send(chunk(1, zz), chunk(1, zz), sp2.at[zs + zz], rp2.at[zs + zz], (f2, c), when)
            w.send(chunk(1, zz), chunk(1, zz), ssib.at[zs + zz], rsib.at[zs + zz], sib, when)

    w.send(chunk(0, z), chunk(0, z), szr.at[z], rz.at[z], (f, c + 2), z < zs - 1)
    w.send(chunk(0, z), chunk(0, z), szl.at[z], rz.at[z], (f, c - 2), z > 0)
    spread(z, None)
    order = []
    for h in range(1, zs):
        for zz, when, on, dz, sem in (
            (z - h, z - h >= 0, z < zs - 1, 2, szr),
            (z + h, z + h < zs, z > 0, -2, szl),
        ):
            got(chunk(0, zz), sem.at[zz], rz.at[zz], (f, c), when)
            w.send(chunk(0, zz), chunk(0, zz), sem.at[zz], rz.at[zz], (f, c + dz), jnp.logical_and(when, on))
            spread(zz, when)
            w.send(chunk(0, zz), chunk(0, zz), ssib.at[zz], rsib.at[zz], sib, when)
            order.append((zz, when))
        if h == 1:
            relay(z, None)
    for zz, when in order:
        relay(zz, when)
    if planes:
        for col, base in ((2, 0), (3, zs)):
            for zz, when in [(z, None)] + order:
                got(chunk(col, zz), sp2.at[base + zz], rp2.at[base + zz], (f2, c), when)
                w.send(chunk(col, zz), chunk(col, zz), ssib.at[col * zs + zz], rsib.at[col * zs + zz], sib, when)
    if planes:
        for mycol, theircol in ((0, 0), (1, 2), (2, 1), (3, 3)):
            for zz, when in ([(z, None)] if mycol else []) + order:
                got(other(mycol, zz), ssib.at[theircol * zs + zz], rsib.at[theircol * zs + zz], sib, when)
    else:
        for zz, when in order:
            got(other(0, zz), ssib.at[zz], rsib.at[zz], sib, when)
    w.drain()


def gather(x, zs, planes, cid, nf=4):
    rows, width = x.shape
    n = (nf if planes else 1) * 2 * zs
    D = pltpu.SemaphoreType.DMA
    return pl.pallas_call(
        functools.partial(ag_kernel, zs, planes),
        out_shape=jax.ShapeDtypeStruct((n, rows, width), x.dtype),
        in_specs=[VM],
        out_specs=ANY,
        scratch_shapes=[D(()), D((2,)), D((zs,)), D((zs,)), D((zs,)), D((zs,)), D((zs,)), D((2 * zs,)), D((2 * zs,)), D((4 * zs,)), D((4 * zs,))],
        compiler_params=pltpu.CompilerParams(collective_id=cid, has_side_effects=True),
        name="gather_all" if planes else "gather_seq",
    )(x)


def add_into(dst, src, rows=32):
    n, r, wd = dst.shape

    def step(i, _):
        a = pl.ds(pl.multiple_of(i % (r // rows) * rows, rows), rows)
        j = i // (r // rows)
        dst[j, a, :] = (dst[j, a, :].astype(jnp.float32) + src[j, a, :].astype(jnp.float32)).astype(dst.dtype)
        return 0

    lax.fori_loop(0, n * (r // rows), step, 0)


def rs_kernel(zs, planes, x_ref, o_ref, t, r0, r1, r2, ral, rar, fin, lsem, s0, q0, s1, q1, s2, q2, szr, szl, rzr, rzl, sf):
    f, c, z, k = place_of()
    half = o_ref.shape[1] // 2
    sib = (f, c + 1 - 2 * k)
    b1 = 2 - k
    b2 = 1 + k
    f1 = flip(f, b1)
    f2 = flip(f, b2)
    f3 = flip(f1, b2)
    cs = 2 * zs
    cols = [f3, f1, f2, f] if planes else [0]
    nc = len(cols)
    last = zs - 1
    low = z < zs // 2
    zord = []
    for i in range(zs - 1):
        far_low = jnp.where(i < zs - 1 - z, last - i, zs - 2 - i)
        far_high = jnp.where(i < z, i, i + 1)
        zord.append(jnp.where(low, far_low, far_high))
    zord.append(z)

    def src(col, zz, kk):
        at = (col * cs if planes else 0) + 2 * zz
        return x_ref.at[pl.ds(at, 2), :, pl.ds(pl.multiple_of(kk * half, 128), half)]

    greet(f, c, z, zs, planes)
    w = Wire()
    locals_ = []
    for ci in range(nc):
        for zi in range(zs):
            i = ci * zs + zi
            col = cols[ci]
            zz = zord[zi]
            slot = (ci if not planes else {0: 0, 1: 2, 2: 1, 3: 3}[ci]) * zs + zz
            w.send(src(col, zz, 1 - k), r0.at[slot], s0.at[slot], q0.at[slot], sib)
            cp = pltpu.make_async_copy(src(col, zz, k), t.at[ci * zs + zz], lsem.at[i])
            cp.start()
            locals_.append(cp)

    def first(ci, zi):
        zz = zord[zi]
        locals_[ci * zs + zi].wait()
        got(r0.at[ci * zs + zz], s0.at[ci * zs + zz], q0.at[ci * zs + zz], sib)
        add_into(t.at[ci * zs + zz], r0.at[ci * zs + zz])

    if planes:
        for ci in (0, 1):
            for zi in range(zs):
                zz = zord[zi]
                first(ci, zi)
                m = ci * zs + zz
                w.send(t.at[m], r1.at[m], s1.at[m], q1.at[m], (f1, c))
        for zi in range(zs):
            zz = zord[zi]
            first(2, zi)
            got(r1.at[zz], s1.at[zz], q1.at[zz], (f1, c))
            add_into(t.at[2 * zs + zz], r1.at[zz])
            w.send(t.at[2 * zs + zz], r2.at[zz], s2.at[zz], q2.at[zz], (f2, c))
        for zi in range(zs):
            first(3, zi)
        base = 3 * zs
    else:
        base = 0

    def complete(zi):
        zz = zord[zi]
        if planes:
            got(r1.at[zs + zz], s1.at[zs + zz], q1.at[zs + zz], (f1, c))
            add_into(t.at[base + zz], r1.at[zs + zz])
            got(r2.at[zz], s2.at[zz], q2.at[zz], (f2, c))
            add_into(t.at[base + zz], r2.at[zz])
        else:
            first(0, zi)

    for zi in range(zs - 1):
        zz = zord[zi]
        complete(zi)
        right = zz > z
        from_left = jnp.logical_and(right, z > 0)
        from_right = jnp.logical_and(jnp.logical_not(right), z < zs - 1)
        got(ral.at[zz], szr.at[zz], rzr.at[zz], (f, c), from_left)
        got(rar.at[zz], szl.at[zz], rzl.at[zz], (f, c), from_right)

        @pl.when(from_left)
        def _():
            add_into(t.at[base + zz], ral.at[zz])

        @pl.when(from_right)
        def _():
            add_into(t.at[base + zz], rar.at[zz])

        w.send(t.at[base + zz], ral.at[zz], szr.at[zz], rzr.at[zz], (f, c + 2), right)
        w.send(t.at[base + zz], rar.at[zz], szl.at[zz], rzl.at[zz], (f, c - 2), jnp.logical_not(right))
    complete(zs - 1)
    got(ral.at[z], szr.at[z], rzr.at[z], (f, c), z > 0)
    got(rar.at[z], szl.at[z], rzl.at[z], (f, c), z < zs - 1)

    @pl.when(z > 0)
    def _():
        add_into(t.at[base + z], ral.at[z])

    @pl.when(z < zs - 1)
    def _():
        add_into(t.at[base + z], rar.at[z])

    w.send(t.at[base + z, 1 - k], fin, sf.at[0], sf.at[1], sib)
    o_ref[:, pl.ds(pl.multiple_of(k * half, 128), half)] = t[base + z, k]
    got(fin, sf.at[0], sf.at[1], sib)
    o_ref[:, pl.ds(pl.multiple_of((1 - k) * half, 128), half)] = fin[...]
    w.drain()


def scatter(x, zs, planes, cid, nf=4):
    n, rows, width = x.shape
    D = pltpu.SemaphoreType.DMA
    half = width // 2
    nc = (nf if planes else 1) * zs
    V = lambda m: pltpu.VMEM((m, 2, rows, half), x.dtype)
    return pl.pallas_call(
        functools.partial(rs_kernel, zs, planes),
        out_shape=jax.ShapeDtypeStruct((rows, width), x.dtype),
        in_specs=[ANY],
        out_specs=VM,
        scratch_shapes=[V(nc), V(nc), V(2 * zs), V(zs), V(zs), V(zs), pltpu.VMEM((rows, half), x.dtype),
            D((nc,)), D((nc,)), D((nc,)), D((2 * zs,)), D((2 * zs,)), D((zs,)), D((zs,)), D((zs,)), D((zs,)), D((zs,)), D((zs,)), D((2,))],
        compiler_params=pltpu.CompilerParams(collective_id=cid, has_side_effects=True, vmem_limit_bytes=60 * 2**20),
        name="scatter_all" if planes else "scatter_seq",
    )(x)


def greet_all(f, c, nf, nc):
    bar = pltpu.get_barrier_semaphore()
    n = nf * nc
    me = f * nc + c

    def hello(i, _):
        j = (me + i) % n
        pl.semaphore_signal(bar, inc=1, device_id=(j // nc, j % nc), device_id_type=MESH)
        return 0

    lax.fori_loop(1, n, hello, 0)
    pl.semaphore_wait(bar, n - 1)


def deal_tiles(src, dst, ssem, rsem, f, c, nf, nc):
    n = nf * nc
    me = f * nc + c

    def go(i, _):
        j = (me + i) % n
        pltpu.make_async_remote_copy(
            src_ref=src.at[j], dst_ref=dst.at[me], send_sem=ssem, recv_sem=rsem,
            device_id=(j // nc, j % nc), device_id_type=MESH,
        ).start()
        return 0

    lax.fori_loop(1, n, go, 0)
    dst[me] = src[me]


def await_tiles(src, dst, ssem, rsem, f, c, nf, nc):
    n = nf * nc
    every = pltpu.make_async_remote_copy(
        src_ref=src.at[pl.ds(0, n - 1)], dst_ref=dst.at[pl.ds(0, n - 1)], send_sem=ssem, recv_sem=rsem,
        device_id=(f, c), device_id_type=MESH,
    )
    every.wait_send()
    every.wait_recv()


def front_kernel(nf, zs, x_ref, wp_ref, tl_ref, o_ref, w_ref, to_ref, loc, wloc, sl, szr, szl, rz, ssib, rsib, ts, tr, sw, rw, swx, swy):
    f, c, z, k = place_of()
    nc = 2 * zs
    half = x_ref.shape[1] // 2
    sib_c = c + 1 - 2 * k
    sib = (f, sib_c)
    fx, fy = flip(f, 1), flip(f, 2)
    fr = [f, fx, fy, flip(fx, 2)]

    def chunk(zz, kk):
        return o_ref.at[pl.ds(2 * zz, 2), :, pl.ds(pl.multiple_of(kk * half, 128), half)]

    def piece(rel, cc):
        return w_ref.at[fr[rel] * nc + cc]

    own = pltpu.make_async_copy(x_ref, o_ref.at[c], loc)
    own.start()
    wown = pltpu.make_async_copy(wp_ref.at[c], piece(0, c), wloc)
    wown.start()
    greet_all(f, c, nf, nc)
    w = Wire()
    w.send(x_ref, o_ref.at[c], sl.at[0], sl.at[1], sib)
    w.send(wp_ref.at[sib_c], piece(0, c), sw.at[sib_c], rw.at[c], sib)
    for h in range(1, zs):
        for zz, when in ((z - h, z - h >= 0), (z + h, z + h < zs)):
            for kk in (0, 1):
                cc = 2 * zz + kk
                w.send(wp_ref.at[cc], piece(0, c), sw.at[cc], rw.at[c], (f, cc), when)
    own.wait()
    got(o_ref.at[sib_c], sl.at[0], sl.at[1], sib)
    w.send(chunk(z, k), chunk(z, k), szr.at[z], rz.at[z], (f, c + 2), z < zs - 1)
    w.send(chunk(z, k), chunk(z, k), szl.at[z], rz.at[z], (f, c - 2), z > 0)
    deal_tiles(tl_ref, to_ref, ts, tr, f, c, nf, nc)

    def plane(cc, when):
        w.send(piece(0, cc), piece(0, cc), swx.at[cc], rw.at[nc + cc], (fx, c), when)
        w.send(piece(0, cc), piece(0, cc), swy.at[cc], rw.at[2 * nc + cc], (fy, c), when)

    def onward(cc, kk, when):
        if kk == 0:
            got(piece(1, cc), swx.at[cc], rw.at[nc + cc], (fx, c), when)
            w.send(piece(1, cc), piece(1, cc), swy.at[nc + cc], rw.at[3 * nc + cc], (fy, c), when)
        else:
            got(piece(2, cc), swy.at[cc], rw.at[2 * nc + cc], (fy, c), when)
            w.send(piece(2, cc), piece(2, cc), swx.at[nc + cc], rw.at[3 * nc + cc], (fx, c), when)

    wown.wait()
    plane(c, None)
    got(piece(0, sib_c), sw.at[sib_c], rw.at[sib_c], sib)
    plane(sib_c, None)
    far = []
    for h in range(1, zs):
        for zz, when, on, dz, sem in (
            (z - h, z - h >= 0, z < zs - 1, 2, szr),
            (z + h, z + h < zs, z > 0, -2, szl),
        ):
            for kk in (0, 1):
                cc = 2 * zz + kk
                got(piece(0, cc), sw.at[cc], rw.at[cc], (f, cc), when)
                plane(cc, when)
            far.append((zz, when))
        for zz, when, on, dz, sem in (
            (z - h, z - h >= 0, z < zs - 1, 2, szr),
            (z + h, z + h < zs, z > 0, -2, szl),
        ):
            got(chunk(zz, k), sem.at[zz], rz.at[zz], (f, c), when)
            w.send(chunk(zz, k), chunk(zz, k), sem.at[zz], rz.at[zz], (f, c + dz), jnp.logical_and(when, on))
            w.send(chunk(zz, k), chunk(zz, k), ssib.at[zz], rsib.at[zz], sib, when)
    everyone = [(z, None)] + far
    for zz, when in everyone:
        for kk in (0, 1):
            onward(2 * zz + kk, kk, when)
    for zz, when in everyone:
        e, o = 2 * zz, 2 * zz + 1
        got(piece(2, e), swy.at[e], rw.at[2 * nc + e], (fy, c), when)
        got(piece(1, o), swx.at[o], rw.at[nc + o], (fx, c), when)
        got(piece(3, e), swy.at[nc + e], rw.at[3 * nc + e], (fy, c), when)
        got(piece(3, o), swx.at[nc + o], rw.at[3 * nc + o], (fx, c), when)
    for zz, when in far:
        got(chunk(zz, 1 - k), ssib.at[zz], rsib.at[zz], sib, when)
    await_tiles(tl_ref, to_ref, ts, tr, f, c, nf, nc)
    w.drain()


def front(x, wp, tl, nf, zs, cid):
    rows, width = x.shape
    nc = 2 * zs
    D = pltpu.SemaphoreType.DMA
    return pl.pallas_call(
        functools.partial(front_kernel, nf, zs),
        out_shape=(
            jax.ShapeDtypeStruct((nc, rows, width), x.dtype),
            jax.ShapeDtypeStruct((nf * nc,) + wp.shape[1:], wp.dtype),
            jax.ShapeDtypeStruct(tl.shape, tl.dtype),
        ),
        in_specs=[VM, VM, VM],
        out_specs=(ANY, ANY, VM),
        scratch_shapes=[D(()), D(()), D((2,)), D((zs,)), D((zs,)), D((zs,)), D((zs,)), D((zs,)), D(()), D(()), D((nc,)), D((4 * nc,)), D((2 * nc,)), D((2 * nc,))],
        compiler_params=pltpu.CompilerParams(collective_id=cid, has_side_effects=True),
        name="front",
    )(x, wp, tl)


def tail_kernel(nf, zs, x_ref, g_ref, tl_ref, o_ref, go_ref, to_ref, t, r0, ral, rar, fin, gt, ga, gb, lsem, s0, q0, szr, szl, rzr, rzl, sf, ts, tr, gl, sg, rg, sa, ra):
    f, c, z, k = place_of()
    nc = 2 * zs
    half = o_ref.shape[1] // 2
    sib_c = c + 1 - 2 * k
    sib = (f, sib_c)
    low = z < zs // 2
    zord = []
    for i in range(zs - 1):
        far_low = jnp.where(i < zs - 1 - z, zs - 1 - i, zs - 2 - i)
        far_high = jnp.where(i < z, i, i + 1)
        zord.append(jnp.where(low, far_low, far_high))
    zord.append(z)

    def src(zz, kk):
        return x_ref.at[pl.ds(2 * zz, 2), :, pl.ds(pl.multiple_of(kk * half, 128), half)]

    hc = nc // 2
    parts = []
    for p in (0, 1):
        fa = flip(f, 1 + p)
        fb = flip(f, 2 - p)
        parts.append((fa, fb, flip(fa, 2 - p)))
    gcopies = []
    for p, (fa, fb, fc) in enumerate(parts):
        for i, col in enumerate((fb, f)):
            cp = pltpu.make_async_copy(g_ref.at[col, pl.ds(p * hc, hc)], gt.at[p, i], gl.at[2 * p + i])
            cp.start()
            gcopies.append(cp)
    greet_all(f, c, nf, nc)
    w = Wire()
    for p, (fa, fb, fc) in enumerate(parts):
        for i, col in enumerate((fc, fa)):
            w.send(g_ref.at[col, pl.ds(p * hc, hc)], ga.at[p, i], sg.at[2 * p + i], rg.at[2 * p + i], (fa, c))
    locals_ = []
    for zi in range(zs):
        zz = zord[zi]
        w.send(src(zz, 1 - k), r0.at[zz], s0.at[zz], q0.at[zz], sib)
        cp = pltpu.make_async_copy(src(zz, k), t.at[zz], lsem.at[zi])
        cp.start()
        locals_.append(cp)
    deal_tiles(tl_ref, to_ref, ts, tr, f, c, nf, nc)

    def complete(zi):
        zz = zord[zi]
        locals_[zi].wait()
        got(r0.at[zz], s0.at[zz], q0.at[zz], sib)
        add_into(t.at[zz], r0.at[zz])

    for zi in range(zs - 1):
        zz = zord[zi]
        complete(zi)
        right = zz > z
        from_left = jnp.logical_and(right, z > 0)
        from_right = jnp.logical_and(jnp.logical_not(right), z < zs - 1)
        got(ral.at[zz], szr.at[zz], rzr.at[zz], (f, c), from_left)
        got(rar.at[zz], szl.at[zz], rzl.at[zz], (f, c), from_right)

        @pl.when(from_left)
        def _():
            add_into(t.at[zz], ral.at[zz])

        @pl.when(from_right)
        def _():
            add_into(t.at[zz], rar.at[zz])

        w.send(t.at[zz], ral.at[zz], szr.at[zz], rzr.at[zz], (f, c + 2), right)
        w.send(t.at[zz], rar.at[zz], szl.at[zz], rzl.at[zz], (f, c - 2), jnp.logical_not(right))
        if zi == 0:
            for p, (fa, fb, fc) in enumerate(parts):
                for i in (0, 1):
                    gcopies[2 * p + i].wait()
                    got(ga.at[p, i], sg.at[2 * p + i], rg.at[2 * p + i], (fa, c))
                    add_into(gt.at[p, i], ga.at[p, i])
                    if i == 0:
                        w.send(gt.at[p, 0], gb.at[p], sg.at[4 + p], rg.at[4 + p], (fb, c))
        if zi == 1:
            for p, (fa, fb, fc) in enumerate(parts):
                got(gb.at[p], sg.at[4 + p], rg.at[4 + p], (fb, c))
                add_into(gt.at[p, 1], gb.at[p])
            for cc in range(nc):
                w.send(gt.at[cc // hc, 1, cc % hc], go_ref.at[c], sa.at[cc], ra.at[c], (f, cc), c != cc)

            def keep(cc):
                @pl.when(c == cc)
                def _():
                    go_ref[cc] = gt[cc // hc, 1, cc % hc]

            for cc in range(nc):
                keep(cc)
    complete(zs - 1)
    got(ral.at[z], szr.at[z], rzr.at[z], (f, c), z > 0)
    got(rar.at[z], szl.at[z], rzl.at[z], (f, c), z < zs - 1)

    @pl.when(z > 0)
    def _():
        add_into(t.at[z], ral.at[z])

    @pl.when(z < zs - 1)
    def _():
        add_into(t.at[z], rar.at[z])

    w.send(t.at[z, 1 - k], fin, sf.at[0], sf.at[1], sib)
    o_ref[:, pl.ds(pl.multiple_of(k * half, 128), half)] = t[z, k]
    for cc in range(nc):
        got(go_ref.at[cc], sa.at[cc], ra.at[cc], (f, c), c != cc)
    got(fin, sf.at[0], sf.at[1], sib)
    o_ref[:, pl.ds(pl.multiple_of((1 - k) * half, 128), half)] = fin[...]
    await_tiles(tl_ref, to_ref, ts, tr, f, c, nf, nc)
    w.drain()


def tail(x, g, tl, nf, zs, cid):
    n, rows, width = x.shape
    nc = 2 * zs
    D = pltpu.SemaphoreType.DMA
    half = width // 2
    V = lambda m: pltpu.VMEM((m, 2, rows, half), x.dtype)
    gs = g.shape[2:]
    G = lambda *lead: pltpu.VMEM(lead + (nc // 2,) + gs, g.dtype)
    return pl.pallas_call(
        functools.partial(tail_kernel, nf, zs),
        out_shape=(
            jax.ShapeDtypeStruct((rows, width), x.dtype),
            jax.ShapeDtypeStruct((nc,) + gs, g.dtype),
            jax.ShapeDtypeStruct(tl.shape, tl.dtype),
        ),
        in_specs=[ANY, ANY, VM],
        out_specs=(VM, VM, VM),
        scratch_shapes=[V(zs), V(zs), V(zs), V(zs), pltpu.VMEM((rows, half), x.dtype), G(2, 2), G(2, 2), G(2),
            D((zs,)), D((zs,)), D((zs,)), D((zs,)), D((zs,)), D((zs,)), D((zs,)), D((2,)), D(()), D(()), D((4,)), D((6,)), D((6,)), D((nc,)), D((nc,))],
        compiler_params=pltpu.CompilerParams(collective_id=cid, has_side_effects=True, vmem_limit_bytes=60 * 2**20),
        name="tail",
    )(x, g, tl)


def attend_kernel(scale, qb, q_ref, k_ref, v_ref, pr_ref, pc_ref, o_ref, l_ref):
    rows = q_ref.shape[0]
    keys = k_ref[...]
    values = v_ref[...]
    for i in range(rows // qb):
        at = pl.ds(i * qb, qb)
        s = lax.dot_general(q_ref[at, :], keys, (((1,), (1,)), ((), ())), preferred_element_type=jnp.float32) * scale
        s = jnp.where(pc_ref[...] <= pr_ref[at, :], s, -jnp.inf)
        top = jnp.max(s, axis=-1, keepdims=True)
        e = jnp.exp(s - top)
        total = jnp.sum(e, axis=-1, keepdims=True)
        p = (e * (1.0 / total)).astype(jnp.bfloat16)
        o_ref[at, :] = jnp.dot(p, values, preferred_element_type=jnp.float32).astype(jnp.bfloat16)
        l_ref[at, :] = jnp.broadcast_to(top + jnp.log(total), (qb, l_ref.shape[1]))


def attend(q, keys, values, pos, scale):
    rows, width = q.shape
    hd = keys.shape[1]
    col = pl.BlockSpec((rows, hd), lambda h: (0, h))
    full = pl.BlockSpec((rows, hd), lambda h: (0, 0))
    return pl.pallas_call(
        functools.partial(attend_kernel, scale, 256),
        grid=(width // hd,),
        out_shape=(jax.ShapeDtypeStruct((rows, width), jnp.bfloat16), jax.ShapeDtypeStruct((rows, width), jnp.float32)),
        in_specs=[col, full, full, pl.BlockSpec((rows, 1), lambda h: (0, 0)), pl.BlockSpec((1, rows), lambda h: (0, 0))],
        out_specs=(col, col),
        name="attend",
    )(q, keys, values, pos[:, None], pos[None, :])


def attend_grad_kernel(scale, qb, q_ref, k_ref, v_ref, c_ref, g_ref, l_ref, pr_ref, pc_ref, gq_ref, gk_ref, gv_ref):
    rows = q_ref.shape[0]
    keys = k_ref[...]
    values = v_ref[...]

    @pl.when(pl.program_id(0) == 0)
    def _():
        gk_ref[...] = jnp.zeros_like(gk_ref)
        gv_ref[...] = jnp.zeros_like(gv_ref)

    for i in range(rows // qb):
        at = pl.ds(i * qb, qb)
        q = q_ref[at, :]
        g = g_ref[at, :]
        s = lax.dot_general(q, keys, (((1,), (1,)), ((), ())), preferred_element_type=jnp.float32) * scale
        p = jnp.where(pc_ref[...] <= pr_ref[at, :], jnp.exp(s - l_ref[at, 0:1]), 0.0)
        gv_ref[...] += lax.dot_general(p.astype(jnp.bfloat16), g, (((0,), (0,)), ((), ())), preferred_element_type=jnp.float32)
        gp = lax.dot_general(g, values, (((1,), (1,)), ((), ())), preferred_element_type=jnp.float32)
        delta = jnp.sum(g.astype(jnp.float32) * c_ref[at, :].astype(jnp.float32), axis=-1, keepdims=True)
        ds = (p * (gp - delta)).astype(jnp.bfloat16)
        gq_ref[at, :] = jnp.dot(ds, keys, preferred_element_type=jnp.float32) * scale
        gk_ref[...] += lax.dot_general(ds, q, (((0,), (0,)), ((), ())), preferred_element_type=jnp.float32) * scale


def attend_grad(q, keys, values, ctx, grad, lse, pos, scale):
    rows, width = q.shape
    hd = keys.shape[1]
    col = pl.BlockSpec((rows, hd), lambda h: (0, h))
    full = pl.BlockSpec((rows, hd), lambda h: (0, 0))
    return pl.pallas_call(
        functools.partial(attend_grad_kernel, scale, 256),
        grid=(width // hd,),
        out_shape=(jax.ShapeDtypeStruct((rows, width), jnp.float32), jax.ShapeDtypeStruct((rows, hd), jnp.float32), jax.ShapeDtypeStruct((rows, hd), jnp.float32)),
        in_specs=[col, full, full, col, col, col, pl.BlockSpec((rows, 1), lambda h: (0, 0)), pl.BlockSpec((1, rows), lambda h: (0, 0))],
        out_specs=(col, full, full),
        name="attend_grad",
    )(q, keys, values, ctx, grad, lse, pos[:, None], pos[None, :])


def head_body(
    nf,
    nc,
    block_input,
    cotangent,
    gain_attn,
    w_query,
    w_key,
    w_value,
    qk_gain,
    w_out,
    gain_moe,
    w_gate,
    w_up,
    w_down,
    expert_ids,
    route_weight,
    pair_order,
):
    bf16, f32 = jnp.bfloat16, jnp.float32
    f, c, z, k = place_of()
    n = nf * nc
    zs = nc // 2
    rows, width = block_input.shape[1:]
    hd = qk_gain.shape[1] * n
    kv_heads = w_key.shape[1] // hd
    heads = w_query.shape[1] // hd
    hp = heads // nc
    shard = w_query.shape[0]
    topk = expert_ids.shape[2]
    capacity = max(2, 3 * BLOCK * topk // n)
    span = nc * rows
    scale = 1.0 / math.sqrt(hd)
    x_own = block_input[0]
    resid = x_own.astype(f32)

    ids, weights = expert_ids[0], route_weight[0].astype(f32)
    named = ids[None, :, :] == jnp.arange(n, dtype=jnp.int32)[:, None, None]
    to_expert = jnp.sum(jnp.where(named, weights[None], 0.0), axis=-1)
    gains = jnp.concatenate([gain_attn, gain_moe]).astype(f32)
    gains = jnp.pad(gains, (0, rows - gains.shape[0]))
    qk_row = jnp.pad(qk_gain.reshape(-1).astype(f32), (0, rows - qk_gain.size))
    tiles = jnp.concatenate(
        [to_expert[:, None], jnp.broadcast_to(jnp.stack([gains, qk_row]), (n, 2, rows)), jnp.zeros((n, 5, rows), f32)], axis=1
    )
    per = nc // kv_heads
    wq_p = w_query.reshape(shard, nc, hp * hd).transpose(1, 0, 2)
    wk_p = jnp.repeat(w_key.reshape(shard, kv_heads, hd).transpose(1, 0, 2), per, axis=0)
    wv_p = jnp.repeat(w_value.reshape(shard, kv_heads, hd).transpose(1, 0, 2), per, axis=0)
    packed = jnp.concatenate([wq_p, wk_p, wv_p], axis=2)
    x_seq, w_all, dealt = front(x_own, packed, tiles, nf, zs, 0)

    qw = hp * hd
    w_cat = w_all.reshape(n * shard, qw + 2 * hd)
    gs = gain_attn.shape[0]
    g_attn = dealt[:, 1, :gs].reshape(-1)
    g_moe = dealt[:, 1, gs : 2 * gs].reshape(-1)
    g_qk = dealt[:, 2, : qk_gain.size].reshape(n, 2, -1).transpose(1, 0, 2).reshape(2, hd)
    route_w = dealt[:, 0, :]

    top_own = cotangent[0]
    top_b = top_own.astype(bf16)
    wo_own, top_b_sent, x_seq = lax.optimization_barrier((w_out, top_b, x_seq))
    lin = lambda ff, cc: ff * nc + cc
    hops = [(h, lin(h % hp, h // hp)) for h in range(n)]
    wo_mine = lax.all_gather(lax.ppermute(wo_own, ("fsdp", "cp"), hops), "fsdp", axis=0, tiled=True)
    top_all = lax.all_gather(top_b_sent, ("fsdp", "cp"), axis=0, tiled=True)

    x32 = x_seq.reshape(span, width).astype(f32)
    inv_in = lax.rsqrt(jnp.mean(x32 * x32, axis=-1, keepdims=True) + EPSILON)
    normed_in = (x32 * inv_in * g_attn).astype(bf16)
    pre = jnp.dot(normed_in, w_cat, preferred_element_type=f32)
    q_pre = pre[:, :qw].reshape(span, hp, hd)
    k_pre = pre[:, qw : qw + hd].reshape(span, 1, hd)
    values = pre[:, qw + hd :].astype(bf16)
    pos = seq_positions(pair_order, BLOCK)
    cosine, sine = rope_tables(pos, hd)
    query_rot = head_post(q_pre, g_qk[0], cosine, sine).astype(bf16).reshape(span, qw)
    key_rot = head_post(k_pre, g_qk[1], cosine, sine).astype(bf16).reshape(span, hd)
    context, lse = attend(query_rot, key_rot, values, pos, scale)
    partial = jnp.dot(context, wo_mine, preferred_element_type=f32).astype(bf16)
    attn_out = scatter(partial.reshape(nc, rows, width), zs, False, 1)
    hidden_res = resid + attn_out.astype(f32)
    normed_mid = rms_scale(hidden_res, g_moe).astype(bf16)

    tokens = gather(normed_mid, zs, True, 2, nf)
    hit = route_w > 0.0
    below = (jnp.arange(rows)[:, None] < jnp.arange(rows)[None, :]).astype(f32)
    rank = jnp.dot(hit.astype(f32), below, preferred_element_type=f32).astype(jnp.int32)
    slot = (rank[:, None, :] == jnp.arange(capacity, dtype=jnp.int32)[None, :, None]) & hit[:, None, :]
    place = slot.astype(bf16)
    mixing = jnp.where(slot, route_w[:, None, :], 0.0).astype(bf16)
    gate_w, up_w, down_w = w_gate[0], w_up[0], w_down[0]
    pick = lambda table, rws: jnp.einsum("srt,std->srd", table, rws, preferred_element_type=f32).astype(bf16).reshape(n * capacity, width)
    back = lambda table, rws: jnp.einsum("srt,srd->std", table, rws.reshape(n, capacity, width), preferred_element_type=f32).astype(bf16)
    arrived = pick(place, tokens)
    gate_pre = jnp.dot(arrived, gate_w, preferred_element_type=f32)
    up_pre = jnp.dot(arrived, up_w, preferred_element_type=f32)
    gate_sig = jax.nn.sigmoid(gate_pre)
    gate_act = gate_pre * gate_sig
    expert_hidden = (gate_act * up_pre).astype(bf16)

    grad_arrived = pick(mixing, top_all.reshape(n, rows, width))
    grad_hidden = contract_cols(grad_arrived, down_w)
    grad_gate_pre = (grad_hidden * up_pre * gate_sig * (1.0 + gate_pre * (1.0 - gate_sig))).astype(bf16)
    grad_up_pre = (grad_hidden * gate_act).astype(bf16)
    grad_rows = (contract_cols(grad_gate_pre, gate_w) + contract_cols(grad_up_pre, up_w)).astype(bf16)
    grad_mid = scatter(back(place, grad_rows), zs, True, 3, nf).astype(f32)

    _, mid_back = jax.vjp(rms_scale, hidden_res, g_moe)
    grad_res_mid, grad_moe_gain = mid_back(grad_mid)
    grad_res = top_own + grad_res_mid
    res_all = gather(grad_res.astype(bf16), zs, False, 4).reshape(span, width)

    hidden_late, arrived_late, grad_arrived_late, _ = lax.optimization_barrier((expert_hidden, arrived, grad_arrived, grad_mid))
    expert_out = jnp.dot(hidden_late, down_w, preferred_element_type=f32).astype(bf16)
    mixed = lax.psum_scatter(back(mixing, expert_out).reshape(n * rows, width), ("fsdp", "cp"), scatter_dimension=0, tiled=True)
    block_output = (hidden_res + mixed.astype(f32)).astype(bf16)
    grad_down = contract_rows(hidden_late, grad_arrived_late)
    grad_gate = contract_rows(arrived_late, grad_gate_pre)
    grad_up = contract_rows(arrived_late, grad_up_pre)

    grad_wo_mine = contract_rows(context, res_all)
    hops_back = [(b, a) for a, b in hops]
    grad_wo = lax.ppermute(
        lax.psum_scatter(grad_wo_mine.astype(bf16), "fsdp", scatter_dimension=0, tiled=True), ("fsdp", "cp"), hops_back
    ).astype(f32)
    grad_context = contract_cols(res_all, wo_mine).astype(bf16)
    grad_query, grad_keys, grad_values = attend_grad(query_rot, key_rot, values, context, grad_context, lse, pos, scale)
    pairs = [(cc, cc + 1 - 2 * (cc % 2)) for cc in range(nc)]
    both = jnp.stack([grad_keys, grad_values])
    both = both + lax.ppermute(both, "cp", pairs)
    grad_keys, grad_values = both[0], both[1]
    _, query_back = jax.vjp(lambda pre, gain: head_post(pre, gain, cosine, sine), q_pre, g_qk[0])
    grad_q_pre, grad_q_gain = query_back(grad_query.reshape(span, hp, hd))
    _, key_back = jax.vjp(lambda pre, gain: head_post(pre, gain, cosine, sine), k_pre, g_qk[1])
    grad_k_pre, grad_k_gain = key_back(grad_keys.reshape(span, 1, hd))
    grad_q_b = grad_q_pre.reshape(span, qw).astype(bf16)
    first = k == 0
    grad_kv_b = jnp.where(first, grad_k_pre.reshape(span, hd), grad_values).astype(bf16)
    grad_cat = jnp.concatenate([grad_q_b, grad_kv_b], axis=1)
    w_kv = jnp.where(first, w_cat[:, qw : qw + hd], w_cat[:, qw + hd :])
    w_back = jnp.concatenate([w_cat[:, :qw], w_kv], axis=1)
    grad_w = contract_rows(normed_in, grad_cat).astype(bf16)
    grad_norm = contract_cols(grad_cat, w_back)
    grad_attn_gain = jnp.sum(grad_norm * (x32 * inv_in), axis=0)
    grad_k_gain = jnp.where(first, grad_k_gain, 0.0)
    share = lambda v: v.reshape(n, -1)
    qk_parts = jnp.stack([grad_q_gain, grad_k_gain]).reshape(2, n, -1).transpose(1, 0, 2).reshape(n, -1)
    line0 = jnp.concatenate([share(grad_attn_gain), share(grad_moe_gain)], axis=1)
    wide = lambda v: jnp.pad(v, ((0, 0), (0, rows - v.shape[1])))
    sums = jnp.concatenate([wide(line0)[:, None], wide(qk_parts)[:, None], jnp.zeros((n, 6, rows), f32)], axis=1)
    grad_in, grads, summed = tail(
        grad_norm.astype(bf16).reshape(nc, rows, width), grad_w.reshape(nf, nc, shard, qw + hd), sums, nf, zs, 5
    )
    total = jnp.sum(summed, axis=0)
    own_attn_gain = total[0, :gs]
    own_moe_gain = total[0, gs : 2 * gs]
    own_qk = total[1, : qk_gain.size].reshape(2, -1)
    grad_wq = grads[:, :, :qw].transpose(1, 0, 2).reshape(shard, heads * hd).astype(f32)
    grad_kv = grads[:, :, qw:].reshape(kv_heads, per, shard, hd)
    grad_wk = grad_kv[:, 0].transpose(1, 0, 2).reshape(shard, kv_heads * hd).astype(f32)
    grad_wv = grad_kv[:, 1].transpose(1, 0, 2).reshape(shard, kv_heads * hd).astype(f32)
    _, in_back = jax.vjp(rms_scale, resid, g_attn)
    grad_input = grad_res + in_back(grad_in.astype(f32))[0]
    return (
        block_output[None],
        grad_input[None],
        own_attn_gain,
        grad_wq,
        grad_wk,
        grad_wv,
        own_qk,
        grad_wo,
        own_moe_gain,
        grad_gate[None],
        grad_up[None],
        grad_down[None],
    )


def body(nf, nc, block_input, *rest):
    kv_heads = rest[3].shape[1] // (rest[5].shape[1] * nf * nc)
    fits = nf == 4 and nc == 2 * kv_heads and rest[4].shape[1] == rest[3].shape[1]
    return head_body(nf, nc, block_input, *rest) if fits else wide_body(block_input, *rest)


def solution(mesh):
    return jax.shard_map(
        functools.partial(body, mesh.shape["fsdp"], mesh.shape["cp"]),
        mesh=mesh,
        in_specs=(
            P("fsdp", "cp", None),
            P("fsdp", "cp", None),
            P(("fsdp", "cp")),
            P(("fsdp", "cp"), None),
            P(("fsdp", "cp"), None),
            P(("fsdp", "cp"), None),
            P(None, ("fsdp", "cp")),
            P(("fsdp", "cp"), None),
            P(("fsdp", "cp")),
            P(("fsdp", "cp"), None, None),
            P(("fsdp", "cp"), None, None),
            P(("fsdp", "cp"), None, None),
            P("fsdp", "cp", None),
            P("fsdp", "cp", None),
            P(),
        ),
        out_specs=(
            P("fsdp", "cp", None),
            P("fsdp", "cp", None),
            P(("fsdp", "cp")),
            P(("fsdp", "cp"), None),
            P(("fsdp", "cp"), None),
            P(("fsdp", "cp"), None),
            P(None, ("fsdp", "cp")),
            P(("fsdp", "cp"), None),
            P(("fsdp", "cp")),
            P(("fsdp", "cp"), None, None),
            P(("fsdp", "cp"), None, None),
            P(("fsdp", "cp"), None, None),
        ),
        check_vma=False,
    )
```

```python
import functools
import math

import jax
import jax.numpy as jnp
from jax import lax
from jax.experimental import pallas as pl
from jax.experimental.pallas import tpu as pltpu
from jax.sharding import PartitionSpec as P

BLOCK = 64


EPSILON = 1e-06
THETA = 1000000.0


def rms_scale(values, gain):
    return values * lax.rsqrt(jnp.mean(values * values, axis=-1, keepdims=True) + EPSILON) * gain


def rotate_half(values):
    half = values.shape[-1] // 2
    return jnp.concatenate([-values[..., half:], values[..., :half]], axis=-1)


def head_post(pre, gain, cosine, sine):
    normed = rms_scale(pre, gain)
    return normed * cosine[:, None, :] + rotate_half(normed) * sine[:, None, :]


def rope_tables(positions, head_dim):
    freqs = THETA ** (-(jnp.arange(head_dim // 2, dtype=jnp.float32) * 2.0 / head_dim))
    angles = positions.astype(jnp.float32)[:, None] * freqs[None, :]
    angles = jnp.concatenate([angles, angles], axis=-1)
    return (jnp.cos(angles), jnp.sin(angles))


def seq_positions(pair_order, block):
    blocks = 2 * pair_order.shape[0]
    rows = jnp.arange(blocks * block, dtype=jnp.int32)
    owner = rows // (2 * block)
    first = pair_order[owner]
    which = jnp.where(rows // block % 2 == 0, first, blocks - 1 - first)
    return which * block + rows % block


def route_tables(ids, weights, experts, capacity):
    flat = ids.reshape(-1)
    onehot = (flat[:, None] == jnp.arange(experts, dtype=jnp.int32)[None, :]).astype(jnp.int32)
    before = jnp.cumsum(onehot, axis=0) - onehot
    rank = jnp.sum(before * onehot, axis=1)
    slots = (flat * capacity + rank).reshape(ids.shape)
    columns = jnp.arange(experts * capacity, dtype=jnp.int32)
    hits = slots[:, :, None] == columns[None, None, :]
    place = jnp.sum(hits.astype(jnp.float32), axis=1).astype(jnp.bfloat16)
    mixing = jnp.sum(jnp.where(hits, weights[:, :, None].astype(jnp.float32), 0.0), axis=1).astype(
        jnp.bfloat16
    )
    return (place, mixing)


def attend_head(query, keys, values, allowed, scale):
    scores = jnp.einsum("grd,sd->grs", query, keys, preferred_element_type=jnp.float32) * scale
    scores = jnp.where(allowed[None], scores, -jnp.inf)
    top = jnp.max(scores, axis=-1, keepdims=True)
    lse = top[..., 0] + jnp.log(jnp.sum(jnp.exp(scores - top), axis=-1))
    probs = jnp.exp(scores - lse[..., None]).astype(jnp.bfloat16)
    output = jnp.einsum("grs,sd->grd", probs, values, preferred_element_type=jnp.float32)
    return (output.astype(jnp.bfloat16), lse)


def attend_back(query, keys, values, output, grad_out, lse, allowed, scale):
    scores = jnp.einsum("grd,sd->grs", query, keys, preferred_element_type=jnp.float32) * scale
    scores = jnp.where(allowed[None], scores, -jnp.inf)
    probs = jnp.exp(scores - lse[..., None])
    grad_values = jnp.einsum(
        "grs,grd->sd", probs.astype(jnp.bfloat16), grad_out, preferred_element_type=jnp.float32
    )
    grad_probs = jnp.einsum("grd,sd->grs", grad_out, values, preferred_element_type=jnp.float32)
    delta = jnp.sum(grad_out.astype(jnp.float32) * output.astype(jnp.float32), axis=-1)
    grad_scores = (probs * (grad_probs - delta[..., None])).astype(jnp.bfloat16)
    grad_query = (
        jnp.einsum("grs,sd->grd", grad_scores, keys, preferred_element_type=jnp.float32) * scale
    )
    grad_keys = (
        jnp.einsum("grs,grd->sd", grad_scores, query, preferred_element_type=jnp.float32) * scale
    )
    return (grad_query, grad_keys, grad_values)


def contract_rows(left, right):
    return lax.dot_general(
        left, right, (((0,), (0,)), ((), ())), preferred_element_type=jnp.float32
    )


def contract_cols(left, right):
    return lax.dot_general(
        left, right, (((1,), (1,)), ((), ())), preferred_element_type=jnp.float32
    )


def wide_body(
    block_input,
    cotangent,
    gain_attn,
    w_query,
    w_key,
    w_value,
    qk_gain,
    w_out,
    gain_moe,
    w_gate,
    w_up,
    w_down,
    expert_ids,
    route_weight,
    pair_order,
):
    g_attn, wq_full, wk_full, wv_full, qk_full, wo_full, g_moe = (
        lax.all_gather(gain_attn, ("fsdp", "cp"), axis=0, tiled=True),
        lax.all_gather(w_query, ("fsdp", "cp"), axis=0, tiled=True),
        lax.all_gather(w_key, ("fsdp", "cp"), axis=0, tiled=True),
        lax.all_gather(w_value, ("fsdp", "cp"), axis=0, tiled=True),
        lax.all_gather(qk_gain, ("fsdp", "cp"), axis=1, tiled=True),
        lax.all_gather(w_out, ("fsdp", "cp"), axis=0, tiled=True),
        lax.all_gather(gain_moe, ("fsdp", "cp"), axis=0, tiled=True),
    )
    rows = block_input.shape[1]
    width = block_input.shape[2]
    head_dim = qk_full.shape[1]
    kv_heads = wk_full.shape[1] // head_dim
    heads = wq_full.shape[1] // head_dim
    group = heads // kv_heads
    experts = lax.axis_size(("fsdp", "cp"))
    capacity = max(2, 3 * BLOCK * expert_ids.shape[2] // experts)
    scale = 1.0 / math.sqrt(head_dim)
    resid = block_input[0].astype(jnp.float32)
    normed_in = rms_scale(resid, g_attn.astype(jnp.float32)).astype(jnp.bfloat16)
    q_pre = jnp.dot(normed_in, wq_full, preferred_element_type=jnp.float32).reshape(
        rows, heads, head_dim
    )
    k_pre = jnp.dot(normed_in, wk_full, preferred_element_type=jnp.float32).reshape(
        rows, kv_heads, head_dim
    )
    value_rows = jnp.dot(normed_in, wv_full, preferred_element_type=jnp.float32).astype(
        jnp.bfloat16
    )
    all_pos = seq_positions(pair_order, BLOCK)
    local_pos = lax.dynamic_slice_in_dim(all_pos, lax.axis_index("cp") * rows, rows)
    cosine, sine = rope_tables(local_pos, head_dim)
    gains32 = qk_full.astype(jnp.float32)
    query_rot = head_post(q_pre, gains32[0], cosine, sine).astype(jnp.bfloat16)
    key_rot = head_post(k_pre, gains32[1], cosine, sine).astype(jnp.bfloat16)
    keys_all, values_all = (
        lax.all_gather(key_rot.reshape(rows, kv_heads * head_dim), "cp", axis=0, tiled=True),
        lax.all_gather(value_rows, "cp", axis=0, tiled=True),
    )
    span = keys_all.shape[0]
    allowed = all_pos[None, :] <= local_pos[:, None]
    query_heads = query_rot.reshape(rows, kv_heads, group, head_dim).transpose(1, 2, 0, 3)
    key_heads = keys_all.reshape(span, kv_heads, head_dim).transpose(1, 0, 2)
    value_heads = values_all.reshape(span, kv_heads, head_dim).transpose(1, 0, 2)
    context_heads, lse = lax.map(
        lambda item: attend_head(item[0], item[1], item[2], allowed, scale),
        (query_heads, key_heads, value_heads),
    )
    context = context_heads.transpose(2, 0, 1, 3).reshape(rows, heads * head_dim)
    hidden_res = resid + jnp.dot(context, wo_full, preferred_element_type=jnp.float32)
    normed_mid = rms_scale(hidden_res, g_moe.astype(jnp.float32)).astype(jnp.bfloat16)
    place, mixing = route_tables(expert_ids[0], route_weight[0], experts, capacity)
    sent = contract_rows(place, normed_mid).astype(jnp.bfloat16)
    arrived = lax.all_to_all(
        sent.reshape(experts, capacity, width),
        ("fsdp", "cp"),
        split_axis=0,
        concat_axis=0,
        tiled=True,
    ).reshape(experts * capacity, width)
    gate_w = w_gate[0]
    up_w = w_up[0]
    down_w = w_down[0]
    gate_pre = jnp.dot(arrived, gate_w, preferred_element_type=jnp.float32)
    up_pre = jnp.dot(arrived, up_w, preferred_element_type=jnp.float32)
    gate_sig = jax.nn.sigmoid(gate_pre)
    gate_act = gate_pre * gate_sig
    expert_hidden = (gate_act * up_pre).astype(jnp.bfloat16)
    expert_out = jnp.dot(expert_hidden, down_w, preferred_element_type=jnp.float32).astype(
        jnp.bfloat16
    )
    returned = lax.all_to_all(
        expert_out.reshape(experts, capacity, width),
        ("fsdp", "cp"),
        split_axis=0,
        concat_axis=0,
        tiled=True,
    ).reshape(experts * capacity, width)
    mixed = jnp.dot(mixing, returned, preferred_element_type=jnp.float32)
    block_output = (hidden_res + mixed).astype(jnp.bfloat16)
    g_attn, wq_full, wk_full, wv_full, qk_full, wo_full, g_moe = (
        lax.all_gather(gain_attn, ("fsdp", "cp"), axis=0, tiled=True),
        lax.all_gather(w_query, ("fsdp", "cp"), axis=0, tiled=True),
        lax.all_gather(w_key, ("fsdp", "cp"), axis=0, tiled=True),
        lax.all_gather(w_value, ("fsdp", "cp"), axis=0, tiled=True),
        lax.all_gather(qk_gain, ("fsdp", "cp"), axis=1, tiled=True),
        lax.all_gather(w_out, ("fsdp", "cp"), axis=0, tiled=True),
        lax.all_gather(gain_moe, ("fsdp", "cp"), axis=0, tiled=True),
    )
    attn_gain = g_attn.astype(jnp.float32)
    moe_gain = g_moe.astype(jnp.float32)
    gains_back = qk_full.astype(jnp.float32)
    grad_top = cotangent[0]
    grad_top_b = grad_top.astype(jnp.bfloat16)
    grad_sent = contract_rows(mixing, grad_top_b).astype(jnp.bfloat16)
    grad_arrived = lax.all_to_all(
        grad_sent.reshape(experts, capacity, width),
        ("fsdp", "cp"),
        split_axis=0,
        concat_axis=0,
        tiled=True,
    ).reshape(experts * capacity, width)
    grad_hidden = contract_cols(grad_arrived, down_w)
    grad_down = contract_rows(expert_hidden, grad_arrived)
    grad_gate_pre = (grad_hidden * up_pre * gate_sig * (1.0 + gate_pre * (1.0 - gate_sig))).astype(
        jnp.bfloat16
    )
    grad_up_pre = (grad_hidden * gate_act).astype(jnp.bfloat16)
    grad_gate = contract_rows(arrived, grad_gate_pre)
    grad_up = contract_rows(arrived, grad_up_pre)
    grad_rows = (contract_cols(grad_gate_pre, gate_w) + contract_cols(grad_up_pre, up_w)).astype(
        jnp.bfloat16
    )
    grad_back = lax.all_to_all(
        grad_rows.reshape(experts, capacity, width),
        ("fsdp", "cp"),
        split_axis=0,
        concat_axis=0,
        tiled=True,
    ).reshape(experts * capacity, width)
    grad_mid = jnp.dot(place, grad_back, preferred_element_type=jnp.float32)
    _, mid_back = jax.vjp(rms_scale, hidden_res, moe_gain)
    grad_res_mid, grad_moe_gain = mid_back(grad_mid)
    grad_res = grad_top + grad_res_mid
    grad_res_b = grad_res.astype(jnp.bfloat16)
    grad_wo = contract_rows(context, grad_res_b)
    grad_context = contract_cols(grad_res_b, wo_full).astype(jnp.bfloat16)
    grad_ctx_heads = grad_context.reshape(rows, kv_heads, group, head_dim).transpose(1, 2, 0, 3)
    grad_q_heads, grad_k_heads, grad_v_heads = lax.map(
        lambda it: attend_back(it[0], it[1], it[2], it[3], it[4], it[5], allowed, scale),
        (query_heads, key_heads, value_heads, context_heads, grad_ctx_heads, lse),
    )
    grad_keys_all = grad_k_heads.transpose(1, 0, 2).reshape(span, kv_heads * head_dim)
    grad_values_all = grad_v_heads.transpose(1, 0, 2).reshape(span, kv_heads * head_dim)
    grad_key_rot, grad_values = (
        lax.psum_scatter(
            grad_keys_all.astype(jnp.bfloat16), "cp", scatter_dimension=0, tiled=True
        ).astype(jnp.float32),
        lax.psum_scatter(
            grad_values_all.astype(jnp.bfloat16), "cp", scatter_dimension=0, tiled=True
        ).astype(jnp.float32),
    )
    grad_query_rot = grad_q_heads.transpose(2, 0, 1, 3).reshape(rows, heads, head_dim)
    _, query_back = jax.vjp(
        lambda pre, gain: head_post(pre, gain, cosine, sine), q_pre, gains_back[0]
    )
    grad_q_pre, grad_q_gain = query_back(grad_query_rot)
    _, key_back = jax.vjp(
        lambda pre, gain: head_post(pre, gain, cosine, sine), k_pre, gains_back[1]
    )
    grad_k_pre, grad_k_gain = key_back(grad_key_rot.reshape(rows, kv_heads, head_dim))
    grad_q_b = grad_q_pre.reshape(rows, heads * head_dim).astype(jnp.bfloat16)
    grad_k_b = grad_k_pre.reshape(rows, kv_heads * head_dim).astype(jnp.bfloat16)
    grad_v_b = grad_values.astype(jnp.bfloat16)
    grad_wq = contract_rows(normed_in, grad_q_b)
    grad_wk = contract_rows(normed_in, grad_k_b)
    grad_wv = contract_rows(normed_in, grad_v_b)
    grad_in_norm = (
        contract_cols(grad_q_b, wq_full)
        + contract_cols(grad_k_b, wk_full)
        + contract_cols(grad_v_b, wv_full)
    )
    _, in_back = jax.vjp(rms_scale, resid, attn_gain)
    grad_res_in, grad_attn_gain = in_back(grad_in_norm)
    grad_input = grad_res + grad_res_in
    grad_qk = jnp.stack([grad_q_gain, grad_k_gain])
    owned_grads = (
        lax.psum_scatter(grad_attn_gain, ("fsdp", "cp"), scatter_dimension=0, tiled=True),
        lax.psum_scatter(grad_wq, ("fsdp", "cp"), scatter_dimension=0, tiled=True),
        lax.psum_scatter(grad_wk, ("fsdp", "cp"), scatter_dimension=0, tiled=True),
        lax.psum_scatter(grad_wv, ("fsdp", "cp"), scatter_dimension=0, tiled=True),
        lax.psum_scatter(grad_qk, ("fsdp", "cp"), scatter_dimension=1, tiled=True),
        lax.psum_scatter(grad_wo, ("fsdp", "cp"), scatter_dimension=0, tiled=True),
        lax.psum_scatter(grad_moe_gain, ("fsdp", "cp"), scatter_dimension=0, tiled=True),
    )
    return (
        block_output[None],
        grad_input[None],
        owned_grads[0],
        owned_grads[1],
        owned_grads[2],
        owned_grads[3],
        owned_grads[4],
        owned_grads[5],
        owned_grads[6],
        grad_gate[None],
        grad_up[None],
        grad_down[None],
    )


MESH = pl.DeviceIdType.MESH
ANY = pl.BlockSpec(memory_space=pl.ANY)
VM = pl.BlockSpec(memory_space=pltpu.VMEM)


def place_of():
    f = lax.axis_index("fsdp")
    c = lax.axis_index("cp")
    return f, c, c // 2, c % 2


def flip(f, bit):
    return f + bit - 2 * bit * ((f // bit) % 2)


class Wire:
    def __init__(self):
        self.sent = []

    def send(self, src, dst, ssem, rsem, dev, when=None):
        copy = pltpu.make_async_remote_copy(
            src_ref=src, dst_ref=dst, send_sem=ssem, recv_sem=rsem, device_id=dev, device_id_type=MESH
        )
        if when is None:
            copy.start()
        else:
            pl.when(when)(copy.start)
        self.sent.append((copy, when))
        return self.sent[-1]

    def settle(self, entries):
        for entry in entries:
            self.sent = [e for e in self.sent if e is not entry]
            self.wait(*entry)

    def wait(self, copy, when):
        if when is None:
            copy.wait_send()
        else:
            pl.when(when)(copy.wait_send)

    def drain(self):
        for entry in self.sent:
            self.wait(*entry)


def got(dst, ssem, rsem, dev, when=None):
    copy = pltpu.make_async_remote_copy(
        src_ref=dst, dst_ref=dst, send_sem=ssem, recv_sem=rsem, device_id=dev, device_id_type=MESH
    )
    if when is None:
        copy.wait_recv()
    else:
        pl.when(when)(copy.wait_recv)


def greet(f, c, z, zs, planes):
    bar = pltpu.get_barrier_semaphore()
    k = c % 2
    sib = c + 1 - 2 * k
    near = [((f, sib), None), ((f, c + 2), z < zs - 1), ((f, c - 2), z > 0)]
    if planes:
        near += [((flip(f, 1), c), None), ((flip(f, 2), c), None)]
    for dev, when in near:
        def hello(dev=dev):
            pl.semaphore_signal(bar, inc=1, device_id=dev, device_id_type=MESH)
        if when is None:
            hello()
        else:
            pl.when(when)(hello)
    base = 3 if planes else 1
    inner = jnp.logical_and(z > 0, z < zs - 1)
    pl.semaphore_wait(bar, base + jnp.where(inner, 2, 1))


def ag_kernel(zs, planes, x_ref, o_ref, loc, sl, szr, szl, rz, sp1, rp1, sp2, rp2, ssib, rsib):
    f, c, z, k = place_of()
    half = x_ref.shape[1] // 2
    sib = (f, c + 1 - 2 * k)
    b1 = 1 + k
    b2 = 2 - k
    f1 = flip(f, b1)
    f2 = flip(f, b2)
    cols = [f, f1, f2, flip(f1, b2)] if planes else [0]
    cs = 2 * zs

    def chunk(col, zz):
        at = (cols[col] * cs if planes else 0) + 2 * zz
        return o_ref.at[pl.ds(at, 2), :, pl.ds(pl.multiple_of(k * half, 128), half)]

    def other(col, zz):
        at = (cols[col] * cs if planes else 0) + 2 * zz
        return o_ref.at[pl.ds(at, 2), :, pl.ds(pl.multiple_of((1 - k) * half, 128), half)]

    mine = (f * cs if planes else 0) + c
    theirs = (f * cs if planes else 0) + c + 1 - 2 * k
    own = pltpu.make_async_copy(x_ref, o_ref.at[mine], loc)
    own.start()
    greet(f, c, z, zs, planes)
    w = Wire()
    w.send(x_ref, o_ref.at[mine], sl.at[0], sl.at[1], sib)
    own.wait()
    got(o_ref.at[theirs], sl.at[0], sl.at[1], sib)

    def spread(zz, when):
        if planes:
            w.send(chunk(0, zz), chunk(0, zz), sp1.at[zz], rp1.at[zz], (f1, c), when)
            w.send(chunk(0, zz), chunk(0, zz), sp2.at[zz], rp2.at[zz], (f2, c), when)

    def relay(zz, when):
        if planes:
            got(chunk(1, zz), sp1.at[zz], rp1.at[zz], (f1, c), when)
            w.send(chunk(1, zz), chunk(1, zz), sp2.at[zs + zz], rp2.at[zs + zz], (f2, c), when)
            w.send(chunk(1, zz), chunk(1, zz), ssib.at[zs + zz], rsib.at[zs + zz], sib, when)

    w.send(chunk(0, z), chunk(0, z), szr.at[z], rz.at[z], (f, c + 2), z < zs - 1)
    w.send(chunk(0, z), chunk(0, z), szl.at[z], rz.at[z], (f, c - 2), z > 0)
    spread(z, None)
    order = []
    for h in range(1, zs):
        for zz, when, on, dz, sem in (
            (z - h, z - h >= 0, z < zs - 1, 2, szr),
            (z + h, z + h < zs, z > 0, -2, szl),
        ):
            got(chunk(0, zz), sem.at[zz], rz.at[zz], (f, c), when)
            w.send(chunk(0, zz), chunk(0, zz), sem.at[zz], rz.at[zz], (f, c + dz), jnp.logical_and(when, on))
            spread(zz, when)
            w.send(chunk(0, zz), chunk(0, zz), ssib.at[zz], rsib.at[zz], sib, when)
            order.append((zz, when))
        if h == 1:
            relay(z, None)
    for zz, when in order:
        relay(zz, when)
    if planes:
        for col, base in ((2, 0), (3, zs)):
            for zz, when in [(z, None)] + order:
                got(chunk(col, zz), sp2.at[base + zz], rp2.at[base + zz], (f2, c), when)
                w.send(chunk(col, zz), chunk(col, zz), ssib.at[col * zs + zz], rsib.at[col * zs + zz], sib, when)
    if planes:
        for mycol, theircol in ((0, 0), (1, 2), (2, 1), (3, 3)):
            for zz, when in ([(z, None)] if mycol else []) + order:
                got(other(mycol, zz), ssib.at[theircol * zs + zz], rsib.at[theircol * zs + zz], sib, when)
    else:
        for zz, when in order:
            got(other(0, zz), ssib.at[zz], rsib.at[zz], sib, when)
    w.drain()


def gather(x, zs, planes, cid, nf=4):
    rows, width = x.shape
    n = (nf if planes else 1) * 2 * zs
    D = pltpu.SemaphoreType.DMA
    return pl.pallas_call(
        functools.partial(ag_kernel, zs, planes),
        out_shape=jax.ShapeDtypeStruct((n, rows, width), x.dtype),
        in_specs=[VM],
        out_specs=ANY,
        scratch_shapes=[D(()), D((2,)), D((zs,)), D((zs,)), D((zs,)), D((zs,)), D((zs,)), D((2 * zs,)), D((2 * zs,)), D((4 * zs,)), D((4 * zs,))],
        compiler_params=pltpu.CompilerParams(collective_id=cid, has_side_effects=True),
        name="gather_all" if planes else "gather_seq",
    )(x)


def add_into(dst, src, rows=32):
    n, r, wd = dst.shape

    def step(i, _):
        a = pl.ds(pl.multiple_of(i % (r // rows) * rows, rows), rows)
        j = i // (r // rows)
        dst[j, a, :] = (dst[j, a, :].astype(jnp.float32) + src[j, a, :].astype(jnp.float32)).astype(dst.dtype)
        return 0

    lax.fori_loop(0, n * (r // rows), step, 0)


def rs_kernel(zs, planes, x_ref, o_ref, t, r0, r1, r2, ral, rar, fin, lsem, s0, q0, s1, q1, s2, q2, szr, szl, rzr, rzl, sf):
    f, c, z, k = place_of()
    half = o_ref.shape[1] // 2
    sib = (f, c + 1 - 2 * k)
    b1 = 2 - k
    b2 = 1 + k
    f1 = flip(f, b1)
    f2 = flip(f, b2)
    f3 = flip(f1, b2)
    cs = 2 * zs
    cols = [f3, f1, f2, f] if planes else [0]
    nc = len(cols)
    last = zs - 1
    low = z < zs // 2
    zord = []
    for i in range(zs - 1):
        far_low = jnp.where(i < zs - 1 - z, last - i, zs - 2 - i)
        far_high = jnp.where(i < z, i, i + 1)
        zord.append(jnp.where(low, far_low, far_high))
    zord.append(z)

    def src(col, zz, kk):
        at = (col * cs if planes else 0) + 2 * zz
        return x_ref.at[pl.ds(at, 2), :, pl.ds(pl.multiple_of(kk * half, 128), half)]

    greet(f, c, z, zs, planes)
    w = Wire()
    locals_ = []
    for ci in range(nc):
        for zi in range(zs):
            i = ci * zs + zi
            col = cols[ci]
            zz = zord[zi]
            slot = (ci if not planes else {0: 0, 1: 2, 2: 1, 3: 3}[ci]) * zs + zz
            w.send(src(col, zz, 1 - k), r0.at[slot], s0.at[slot], q0.at[slot], sib)
            cp = pltpu.make_async_copy(src(col, zz, k), t.at[ci * zs + zz], lsem.at[i])
            cp.start()
            locals_.append(cp)

    def first(ci, zi):
        zz = zord[zi]
        locals_[ci * zs + zi].wait()
        got(r0.at[ci * zs + zz], s0.at[ci * zs + zz], q0.at[ci * zs + zz], sib)
        add_into(t.at[ci * zs + zz], r0.at[ci * zs + zz])

    if planes:
        for ci in (0, 1):
            for zi in range(zs):
                zz = zord[zi]
                first(ci, zi)
                m = ci * zs + zz
                w.send(t.at[m], r1.at[m], s1.at[m], q1.at[m], (f1, c))
        for zi in range(zs):
            zz = zord[zi]
            first(2, zi)
            got(r1.at[zz], s1.at[zz], q1.at[zz], (f1, c))
            add_into(t.at[2 * zs + zz], r1.at[zz])
            w.send(t.at[2 * zs + zz], r2.at[zz], s2.at[zz], q2.at[zz], (f2, c))
        for zi in range(zs):
            first(3, zi)
        base = 3 * zs
    else:
        base = 0

    def complete(zi):
        zz = zord[zi]
        if planes:
            got(r1.at[zs + zz], s1.at[zs + zz], q1.at[zs + zz], (f1, c))
            add_into(t.at[base + zz], r1.at[zs + zz])
            got(r2.at[zz], s2.at[zz], q2.at[zz], (f2, c))
            add_into(t.at[base + zz], r2.at[zz])
        else:
            first(0, zi)

    for zi in range(zs - 1):
        zz = zord[zi]
        complete(zi)
        right = zz > z
        from_left = jnp.logical_and(right, z > 0)
        from_right = jnp.logical_and(jnp.logical_not(right), z < zs - 1)
        got(ral.at[zz], szr.at[zz], rzr.at[zz], (f, c), from_left)
        got(rar.at[zz], szl.at[zz], rzl.at[zz], (f, c), from_right)

        @pl.when(from_left)
        def _():
            add_into(t.at[base + zz], ral.at[zz])

        @pl.when(from_right)
        def _():
            add_into(t.at[base + zz], rar.at[zz])

        w.send(t.at[base + zz], ral.at[zz], szr.at[zz], rzr.at[zz], (f, c + 2), right)
        w.send(t.at[base + zz], rar.at[zz], szl.at[zz], rzl.at[zz], (f, c - 2), jnp.logical_not(right))
    complete(zs - 1)
    got(ral.at[z], szr.at[z], rzr.at[z], (f, c), z > 0)
    got(rar.at[z], szl.at[z], rzl.at[z], (f, c), z < zs - 1)

    @pl.when(z > 0)
    def _():
        add_into(t.at[base + z], ral.at[z])

    @pl.when(z < zs - 1)
    def _():
        add_into(t.at[base + z], rar.at[z])

    w.send(t.at[base + z, 1 - k], fin, sf.at[0], sf.at[1], sib)
    o_ref[:, pl.ds(pl.multiple_of(k * half, 128), half)] = t[base + z, k]
    got(fin, sf.at[0], sf.at[1], sib)
    o_ref[:, pl.ds(pl.multiple_of((1 - k) * half, 128), half)] = fin[...]
    w.drain()


def scatter(x, zs, planes, cid, nf=4):
    n, rows, width = x.shape
    D = pltpu.SemaphoreType.DMA
    half = width // 2
    nc = (nf if planes else 1) * zs
    V = lambda m: pltpu.VMEM((m, 2, rows, half), x.dtype)
    return pl.pallas_call(
        functools.partial(rs_kernel, zs, planes),
        out_shape=jax.ShapeDtypeStruct((rows, width), x.dtype),
        in_specs=[ANY],
        out_specs=VM,
        scratch_shapes=[V(nc), V(nc), V(2 * zs), V(zs), V(zs), V(zs), pltpu.VMEM((rows, half), x.dtype),
            D((nc,)), D((nc,)), D((nc,)), D((2 * zs,)), D((2 * zs,)), D((zs,)), D((zs,)), D((zs,)), D((zs,)), D((zs,)), D((zs,)), D((2,))],
        compiler_params=pltpu.CompilerParams(collective_id=cid, has_side_effects=True, vmem_limit_bytes=60 * 2**20),
        name="scatter_all" if planes else "scatter_seq",
    )(x)


def greet_cross(f, c, nf, nc):
    bar = pltpu.get_barrier_semaphore()
    for i in range(1, nc):
        pl.semaphore_signal(bar, inc=1, device_id=(f, (c + i) % nc), device_id_type=MESH)
    for i in range(1, nf):
        pl.semaphore_signal(bar, inc=1, device_id=((f + i) % nf, c), device_id_type=MESH)
    pl.semaphore_wait(bar, nc + nf - 2)


def tile_steps(w, nf, nc, src, dst, hub, ssem, rsem, sp, rp):
    f, c, z, k = place_of()

    def go(i, _):
        j = (c + i) % nc
        pltpu.make_async_remote_copy(
            src_ref=src.at[j], dst_ref=hub.at[c], send_sem=ssem, recv_sem=rsem, device_id=(f, j), device_id_type=MESH
        ).start()
        return 0

    lax.fori_loop(1, nc, go, 0)
    hub[c] = src[c]
    yield
    every = pltpu.make_async_remote_copy(
        src_ref=src.at[pl.ds(0, nc - 1)], dst_ref=hub.at[pl.ds(0, nc - 1)], send_sem=ssem, recv_sem=rsem,
        device_id=(f, c), device_id_type=MESH,
    )
    every.wait_send()
    every.wait_recv()
    mine = pl.ds(f * nc, nc)
    for i in range(1, nf):
        ff = (f + i) % nf
        w.send(hub.at[:, ff], dst.at[mine], sp.at[i], rp.at[i], (ff, c))
    dst[mine] = hub[:, f]
    yield
    for i in range(1, nf):
        ff = (f + nf - i) % nf
        got(dst.at[pl.ds(ff * nc, nc)], sp.at[i], rp.at[i], (f, c))
    yield


def tile_bufs(nf, nc, tile):
    D = pltpu.SemaphoreType.DMA
    return [pltpu.VMEM((nc, nf) + tile, jnp.float32), D(()), D(()), D((nf,)), D((nf,))]


def gather_steps(w, zs, planes, late, x_ref, o_ref, loc, sl, szr, szl, rz, sp1, rp1, sp2, rp2, ssib, rsib):
    f, c, z, k = place_of()
    half = x_ref.shape[1] // 2
    sib = (f, c + 1 - 2 * k)
    b1 = 1 + k
    b2 = 2 - k
    f1 = flip(f, b1)
    f2 = flip(f, b2)
    cols = [f, f1, f2, flip(f1, b2)] if planes else [0]
    cs = 2 * zs

    def chunk(col, zz, kk):
        at = (cols[col] * cs if planes else 0) + 2 * zz
        return o_ref.at[pl.ds(at, 2), :, pl.ds(pl.multiple_of(kk * half, 128), half)]

    mine = (f * cs if planes else 0) + c
    theirs = (f * cs if planes else 0) + c + 1 - 2 * k
    own = pltpu.make_async_copy(x_ref, o_ref.at[mine], loc)
    own.start()
    w.send(x_ref, o_ref.at[mine], sl.at[0], sl.at[1], sib)
    yield
    own.wait()
    got(o_ref.at[theirs], sl.at[0], sl.at[1], sib)

    def spread(zz, when):
        if planes:
            w.send(chunk(0, zz, k), chunk(0, zz, k), sp1.at[zz], rp1.at[zz], (f1, c), when)
            w.send(chunk(0, zz, k), chunk(0, zz, k), sp2.at[zz], rp2.at[zz], (f2, c), when)

    def relay(zz, when):
        if planes:
            got(chunk(1, zz, k), sp1.at[zz], rp1.at[zz], (f1, c), when)
            w.send(chunk(1, zz, k), chunk(1, zz, k), sp2.at[zs + zz], rp2.at[zs + zz], (f2, c), when)
            w.send(chunk(1, zz, k), chunk(1, zz, k), ssib.at[zs + zz], rsib.at[zs + zz], sib, when)

    if late:
        spread(z, None)
        yield
    w.send(chunk(0, z, k), chunk(0, z, k), szr.at[z], rz.at[z], (f, c + 2), z < zs - 1)
    w.send(chunk(0, z, k), chunk(0, z, k), szl.at[z], rz.at[z], (f, c - 2), z > 0)
    if not late:
        spread(z, None)
    yield
    if late:
        relay(z, None)
        yield
    order = []
    for h in range(1, zs):
        for zz, when, on, dz, sem in (
            (z - h, z - h >= 0, z < zs - 1, 2, szr),
            (z + h, z + h < zs, z > 0, -2, szl),
        ):
            got(chunk(0, zz, k), sem.at[zz], rz.at[zz], (f, c), when)
            w.send(chunk(0, zz, k), chunk(0, zz, k), sem.at[zz], rz.at[zz], (f, c + dz), jnp.logical_and(when, on))
            spread(zz, when)
            w.send(chunk(0, zz, k), chunk(0, zz, k), ssib.at[zz], rsib.at[zz], sib, when)
            order.append((zz, when))
        yield
        if h == 1 and not late:
            relay(z, None)
            yield
    for zz, when in order:
        relay(zz, when)
        yield
    if planes:
        for col, base in ((2, 0), (3, zs)):
            for zz, when in [(z, None)] + order:
                got(chunk(col, zz, k), sp2.at[base + zz], rp2.at[base + zz], (f2, c), when)
                w.send(chunk(col, zz, k), chunk(col, zz, k), ssib.at[col * zs + zz], rsib.at[col * zs + zz], sib, when)
            yield
        for mycol, theircol in ((0, 0), (1, 2), (2, 1), (3, 3)):
            for zz, when in ([(z, None)] if mycol else []) + order:
                got(chunk(mycol, zz, 1 - k), ssib.at[theircol * zs + zz], rsib.at[theircol * zs + zz], sib, when)
    else:
        for zz, when in order:
            got(chunk(0, zz, 1 - k), ssib.at[zz], rsib.at[zz], sib, when)
    yield


def gather_sems(zs):
    D = pltpu.SemaphoreType.DMA
    return [D(()), D((2,)), D((zs,)), D((zs,)), D((zs,)), D((zs,)), D((zs,)), D((2 * zs,)), D((2 * zs,)), D((4 * zs,)), D((4 * zs,))]


def advance(steps, name="step"):
    with jax.named_scope(name):
        return next(steps, steps) is not steps


def head_rows_steps(w, nf, nc, hp, wo_ref, wo_all, hub, loc, so, ro):
    f, c, z, k = place_of()
    fx, fy = flip(f, 1), flip(f, 2)
    fd = flip(fx, 2)
    hr = wo_ref.shape[0] // 2
    halves = []
    for p in (0, 1):
        j = c % hp
        m = f
        if p:
            j, m = flip(j, 2), flip(f, 2)
        halves.append((p, pl.ds(p * hr, hr), j, f == j, m))
    keeps = []
    for p, at, j, is_hub, m in halves:
        w.send(wo_ref.at[at], hub.at[f, at], so.at[p, 0], ro.at[p, f], (j, c), jnp.logical_not(is_hub))
        keep = pltpu.make_async_copy(wo_ref.at[at], hub.at[f, at], loc.at[p])
        pl.when(is_hub)(keep.start)
        keeps.append(keep)
    yield
    stays = []
    for p, at, j, is_hub, m in halves:
        for ff in range(nf):
            got(hub.at[ff, at], so.at[p, 0], ro.at[p, ff], (f, c), jnp.logical_and(is_hub, ff != f))
            pl.when(jnp.logical_and(is_hub, ff == f))(keeps[p].wait)
            dc = (ff * nc + c) // hp
            w.send(hub.at[ff, at], wo_all.at[m, at], so.at[p, 1 + ff], ro.at[p, nf], (f, dc), jnp.logical_and(is_hub, dc != c))
            stay = pltpu.make_async_copy(hub.at[ff, at], wo_all.at[m, at], loc.at[2 + p])
            pl.when(jnp.logical_and(is_hub, dc == c))(stay.start)
        stays.append(stay)
    yield
    for p, at, j, is_hub, m in halves:
        here = (hp * c + m) % nc == c
        got(wo_all.at[m, at], so.at[p, 1], ro.at[p, nf], (f, c), jnp.logical_not(here))
        pl.when(here)(stays[p].wait)
        w.send(wo_all.at[m, at], wo_all.at[m, at], so.at[p, nf + 1], ro.at[p, nf + 1], (fx, c))
        w.send(wo_all.at[m, at], wo_all.at[m, at], so.at[p, nf + 2], ro.at[p, nf + 2], (fy, c))
    yield
    for p, at, j, is_hub, m in halves:
        mx, my = flip(m, 1), flip(m, 2)
        got(wo_all.at[mx, at], so.at[p, nf + 1], ro.at[p, nf + 1], (fx, c))
        got(wo_all.at[my, at], so.at[p, nf + 2], ro.at[p, nf + 2], (fy, c))
        if p == 0:
            w.send(wo_all.at[mx, at], wo_all.at[mx, at], so.at[p, nf + 3], ro.at[p, nf + 3], (fy, c))
        else:
            w.send(wo_all.at[my, at], wo_all.at[my, at], so.at[p, nf + 3], ro.at[p, nf + 3], (fx, c))
    yield
    for p, at, j, is_hub, m in halves:
        got(wo_all.at[flip(flip(m, 1), 2), at], so.at[p, nf + 3], ro.at[p, nf + 3], (f, c))
    yield


def far_first(z, zs):
    last = zs - 1
    low = z < zs // 2
    order = []
    for i in range(zs - 1):
        far_low = jnp.where(i < zs - 1 - z, last - i, zs - 2 - i)
        far_high = jnp.where(i < z, i, i + 1)
        order.append(jnp.where(low, far_low, far_high))
    return order + [z]


def line_sum_steps(w, zs, make, o_ref, t, u, r0, ral, rar, fin, s0, q0, szr, szl, rzr, rzl, sf):
    f, c, z, k = place_of()
    half = o_ref.shape[1] // 2
    sib = (f, c + 1 - 2 * k)
    order = far_first(z, zs)

    def first(zz):
        make(zz)
        w.send(u.at[zz], r0.at[zz], s0.at[zz], q0.at[zz], sib)

    def complete(zz):
        got(r0.at[zz], s0.at[zz], q0.at[zz], sib)
        add_into(t.at[zz], r0.at[zz])

    def onward(zz):
        right = zz > z
        from_left = jnp.logical_and(right, z > 0)
        from_right = jnp.logical_and(jnp.logical_not(right), z < zs - 1)
        got(ral.at[zz], szr.at[zz], rzr.at[zz], (f, c), from_left)
        got(rar.at[zz], szl.at[zz], rzl.at[zz], (f, c), from_right)

        @pl.when(from_left)
        def _():
            add_into(t.at[zz], ral.at[zz])

        @pl.when(from_right)
        def _():
            add_into(t.at[zz], rar.at[zz])

        w.send(t.at[zz], ral.at[zz], szr.at[zz], rzr.at[zz], (f, c + 2), right)
        w.send(t.at[zz], rar.at[zz], szl.at[zz], rzl.at[zz], (f, c - 2), jnp.logical_not(right))

    first(order[0])
    yield
    for zi in range(zs - 1):
        first(order[zi + 1])
        complete(order[zi])
        yield
        onward(order[zi])
        yield
    complete(z)
    got(ral.at[z], szr.at[z], rzr.at[z], (f, c), z > 0)

    @pl.when(z > 0)
    def _():
        add_into(t.at[z], ral.at[z])

    yield
    got(rar.at[z], szl.at[z], rzl.at[z], (f, c), z < zs - 1)

    @pl.when(z < zs - 1)
    def _():
        add_into(t.at[z], rar.at[z])

    w.send(t.at[z, 1 - k], fin, sf.at[0], sf.at[1], sib)
    o_ref[:, pl.ds(pl.multiple_of(k * half, 128), half)] = t[z, k]
    yield
    got(fin, sf.at[0], sf.at[1], sib)
    o_ref[:, pl.ds(pl.multiple_of((1 - k) * half, 128), half)] = fin[...]
    yield


def line_sum_bufs(zs, rows, half, dtype):
    D = pltpu.SemaphoreType.DMA
    V = pltpu.VMEM((zs, 2, rows, half), dtype)
    return [V, V, V, V, V, pltpu.VMEM((rows, half), dtype)] + [D((zs,))] * 6 + [D((2,))]


def attn_kernel(nf, zs, hp, scale, refs):
    (x_ref, wp_ref, tl_ref, wo_ref, tb_ref, cos_ref, sin_ref, pr_ref, pc_ref,
     o_ref, nm_ref, w_ref, to_ref, wo_all, top_all, qp_ref, kp_ref, qr_ref, kr_ref, v_ref, ctx_ref, lse_ref, hid_ref, tok_all,
     gain, gain_mid, mid, out_ref, loc, wloc, sl, szr, szl, rz, ssib, rsib, sw, rw, swx, swy) = refs[:40]
    tile_b = refs[40:45]
    head_bufs = refs[45:49]
    top_sems = refs[49:60]
    tok_sems = refs[60:71]
    sum_bufs = refs[71:]
    f, c, z, k = place_of()
    nc = 2 * zs
    rows, width = x_ref.shape
    half = width // 2
    hd = kr_ref.shape[1]
    qw = hp * hd
    f32, bf16 = jnp.float32, jnp.bfloat16
    sib_c = c + 1 - 2 * k
    sib = (f, sib_c)
    fx, fy = flip(f, 1), flip(f, 2)
    fr = [f, fx, fy, flip(fx, 2)]

    def chunk(zz, kk):
        return o_ref.at[pl.ds(2 * zz, 2), :, pl.ds(pl.multiple_of(kk * half, 128), half)]

    def piece(rel, cc):
        return w_ref.at[fr[rel] * nc + cc]

    own = pltpu.make_async_copy(x_ref, o_ref.at[c], loc)
    own.start()
    wown = pltpu.make_async_copy(wp_ref.at[c], piece(0, c), wloc)
    wown.start()
    with jax.named_scope("greet"):
        greet_cross(f, c, nf, nc)
    w = Wire()
    head_steps = head_rows_steps(w, nf, nc, hp, wo_ref, wo_all, *head_bufs)
    top_steps = gather_steps(w, zs, True, True, tb_ref, top_all, *top_sems)
    small_steps = tile_steps(w, nf, nc, tl_ref, to_ref, *tile_b)
    advance(small_steps, "tiles")
    w.send(x_ref, o_ref.at[c], sl.at[0], sl.at[1], sib)
    w.send(wp_ref.at[sib_c], piece(0, c), sw.at[sib_c], rw.at[c], sib)
    for h in range(1, zs):
        for zz, when in ((z - h, z - h >= 0), (z + h, z + h < zs)):
            for kk in (0, 1):
                cc = 2 * zz + kk
                w.send(wp_ref.at[cc], piece(0, c), sw.at[cc], rw.at[c], (f, cc), when)
    own.wait()
    got(o_ref.at[sib_c], sl.at[0], sl.at[1], sib)
    on_line = [
        w.send(chunk(z, k), chunk(z, k), szr.at[z], rz.at[z], (f, c + 2), z < zs - 1),
        w.send(chunk(z, k), chunk(z, k), szl.at[z], rz.at[z], (f, c - 2), z > 0),
    ]
    advance(head_steps, "heads")
    advance(small_steps, "tiles")

    def plane(cc, when):
        w.send(piece(0, cc), piece(0, cc), swx.at[cc], rw.at[nc + cc], (fx, c), when)
        w.send(piece(0, cc), piece(0, cc), swy.at[cc], rw.at[2 * nc + cc], (fy, c), when)

    def onward(cc, kk, when):
        if kk == 0:
            got(piece(1, cc), swx.at[cc], rw.at[nc + cc], (fx, c), when)
            w.send(piece(1, cc), piece(1, cc), swy.at[nc + cc], rw.at[3 * nc + cc], (fy, c), when)
        else:
            got(piece(2, cc), swy.at[cc], rw.at[2 * nc + cc], (fy, c), when)
            w.send(piece(2, cc), piece(2, cc), swx.at[nc + cc], rw.at[3 * nc + cc], (fx, c), when)

    def norm(zz):
        nb = 32

        def block(i, _):
            j = i // (rows // nb)
            at = pl.ds(pl.multiple_of(i % (rows // nb) * nb, nb), nb)
            v = o_ref[2 * zz + j, at, :].astype(f32)
            inv = lax.rsqrt(jnp.mean(v * v, axis=-1, keepdims=True) + EPSILON)
            to = pl.ds(pl.multiple_of(2 * zz * rows + i * nb, nb), nb)
            nm_ref[to, :] = (v * inv * gain[...]).astype(bf16)
            return 0

        with jax.named_scope("norm"):
            lax.fori_loop(0, 2 * rows // nb, block, 0)

    sides = [
        (
            (z - h, z - h >= 0, z < zs - 1, 2, szr),
            (z + h, z + h < zs, z > 0, -2, szl),
        )
        for h in range(1, zs)
    ]
    far = [(zz, when) for pair in sides for zz, when, *_ in pair]
    wown.wait()
    plane(c, None)
    got(piece(0, sib_c), sw.at[sib_c], rw.at[sib_c], sib)
    plane(sib_c, None)
    for zz, when in far:
        for kk in (0, 1):
            cc = 2 * zz + kk
            with jax.named_scope("w1"):
                got(piece(0, cc), sw.at[cc], rw.at[cc], (f, cc), when)
            plane(cc, when)
    advance(small_steps, "tiles")
    advance(head_steps, "heads")
    for i in range(width // 128):
        gain[:, pl.ds(128 * i, 128)] = to_ref[2 * i, 1:2, :] + to_ref[2 * i + 1, 1:2, :]
        gain_mid[:, pl.ds(128 * i, 128)] = to_ref[2 * i, 4:5, :] + to_ref[2 * i + 1, 4:5, :]
    norm(z)
    with jax.named_scope("w2"):
        for zz, when in [(z, None)] + far[:2]:
            for kk in (0, 1):
                onward(2 * zz + kk, kk, when)
    waiting = []
    for h, pair in enumerate(sides):
        for zz, when, on, dz, sem in pair:
            with jax.named_scope("x"):
                got(chunk(zz, k), sem.at[zz], rz.at[zz], (f, c), when)
            on_line.append(w.send(chunk(zz, k), chunk(zz, k), sem.at[zz], rz.at[zz], (f, c + dz), jnp.logical_and(when, on)))
            w.send(chunk(zz, k), chunk(zz, k), ssib.at[zz], rsib.at[zz], sib, when)
        if h == 0:
            advance(head_steps, "heads")
            with jax.named_scope("w2"):
                for zz, when in far[2:]:
                    for kk in (0, 1):
                        onward(2 * zz + kk, kk, when)
        if h == zs - 3:
            advance(head_steps, "heads")
            advance(top_steps, "top")
        if h == zs - 2:
            with jax.named_scope("line"):
                w.settle(on_line)
            advance(top_steps, "top")
            advance(top_steps, "top")
        for zz, when in waiting:
            got(chunk(zz, 1 - k), ssib.at[zz], rsib.at[zz], sib, when)
            pl.when(when)(functools.partial(norm, zz))
        waiting = [(zz, when) for zz, when, *_ in pair]
    for zz, when in waiting:
        got(chunk(zz, 1 - k), ssib.at[zz], rsib.at[zz], sib, when)
        pl.when(when)(functools.partial(norm, zz))
    with jax.named_scope("wait_w"):
        for zz, when in [(z, None)] + far:
            e, o = 2 * zz, 2 * zz + 1
            got(piece(2, e), swy.at[e], rw.at[2 * nc + e], (fy, c), when)
            got(piece(1, o), swx.at[o], rw.at[nc + o], (fx, c), when)
            got(piece(3, e), swy.at[nc + e], rw.at[3 * nc + e], (fy, c), when)
            got(piece(3, o), swx.at[nc + o], rw.at[3 * nc + o], (fx, c), when)

    gq = jnp.sum(to_ref[:, 2, :], axis=0, keepdims=True)
    gk = jnp.sum(to_ref[:, 3, :], axis=0, keepdims=True)
    qb = 2 * rows
    span = nc * rows
    low_half = lax.broadcasted_iota(jnp.int32, (1, hd), 1) < hd // 2

    def turned(t, g, at):
        t = t * lax.rsqrt(jnp.mean(t * t, axis=-1, keepdims=True) + EPSILON) * g
        other = pltpu.roll(t, hd // 2, 1)
        return (t * cos_ref[at, :] + jnp.where(low_half, -other, other) * sin_ref[at, :]).astype(bf16)

    def project(i, _):
        at = pl.ds(pl.multiple_of(i * qb, qb), qb)
        a = nm_ref[at, :]
        for nb in range((qw + 2 * hd) // (2 * hd)):
            wide = pl.ds(nb * 2 * hd, 2 * hd)
            pre = jnp.dot(a, w_ref[:, :, wide].reshape(width, 2 * hd), preferred_element_type=f32)
            for s in (0, 1):
                part = pre[:, s * hd : (s + 1) * hd]
                h = 2 * nb + s
                if h < hp:
                    qp_ref[at, pl.ds(h * hd, hd)] = part
                    qr_ref[at, pl.ds(h * hd, hd)] = turned(part, gq, at)
                elif h == hp:
                    kp_ref[at, :] = part
                    kr_ref[at, :] = turned(part, gk, at)
                else:
                    v_ref[at, :] = part.astype(bf16)
        return 0

    for i in range(span // qb):
        with jax.named_scope("project"):
            project(i, 0)

    lane = lax.broadcasted_iota(jnp.int32, (1, hd), 1)

    def attend(i, h):
        at = pl.ds(pl.multiple_of(i * qb, qb), qb)
        hc = pl.ds(pl.multiple_of(h * hd, hd), hd)
        s = lax.dot_general(qr_ref[at, hc], kr_ref[...], (((1,), (1,)), ((), ())), preferred_element_type=f32) * scale
        s = jnp.where(pc_ref[...] <= pr_ref[at, :], s, -jnp.inf)
        top = jnp.max(s, axis=-1, keepdims=True)
        e = jnp.exp(s - top)
        total = jnp.sum(e, axis=-1, keepdims=True)
        p = (e * (1.0 / total)).astype(bf16)
        ctx_ref[at, hc] = jnp.dot(p, v_ref[...], preferred_element_type=f32).astype(bf16)
        lse_ref[at, :] = jnp.where(lane == h, top + jnp.log(total), lse_ref[at, :])

    lse_ref[...] = jnp.zeros_like(lse_ref)

    while advance(head_steps, "heads"):
        pass

    t, u = sum_bufs[0], sum_bufs[1]

    def make(zz):
        def heads(h, _):
            attend(zz, h)
            return 0

        with jax.named_scope("attend"):
            lax.fori_loop(0, hp, heads, 0)
        at = pl.ds(pl.multiple_of(2 * zz * rows, rows), 2 * rows)
        a = ctx_ref[at, :]
        for dst, kk in ((u, 1 - k), (t, k)):
            def block(j, _, dst=dst, kk=kk):
                cols = pl.ds(pl.multiple_of(kk * half + j * 512, 128), 512)
                o = jnp.dot(a, wo_all[:, :, cols].reshape(qw, 512), preferred_element_type=f32).astype(bf16)
                dst[zz, :, :, pl.ds(pl.multiple_of(j * 512, 512), 512)] = o.reshape(2, rows, 512)
                return 0

            lax.fori_loop(0, half // 512, block, 0)

    sum_steps = line_sum_steps(w, zs, make, out_ref, *sum_bufs)
    for turn in "sstsstssssst":
        if turn == "s":
            advance(sum_steps, "sum")
        else:
            advance(top_steps, "top")
    while advance(sum_steps, "sum"):
        pass

    def middle(i, _):
        at = pl.ds(pl.multiple_of(i * 32, 32), 32)
        v = x_ref[at, :].astype(f32) + out_ref[at, :].astype(f32)
        hid_ref[at, :] = v
        inv = lax.rsqrt(jnp.mean(v * v, axis=-1, keepdims=True) + EPSILON)
        mid[at, :] = (v * inv * gain_mid[...]).astype(bf16)
        return 0

    with jax.named_scope("middle"):
        lax.fori_loop(0, rows // 32, middle, 0)
    tok_steps = gather_steps(w, zs, True, False, mid, tok_all, *tok_sems)
    advance(tok_steps, "tok")
    advance(tok_steps, "tok")
    busy = True
    while busy:
        busy = advance(top_steps, "top")
        busy = advance(tok_steps, "tok") or busy
    w.drain()


def attention(x, wp, tl, wo, tb, cosine, sine, pos, nf, zs, hp, scale, cid):
    rows, width = x.shape
    nc = 2 * zs
    span = nc * rows
    hd = cosine.shape[1]
    bf16, f32 = jnp.bfloat16, jnp.float32
    D = pltpu.SemaphoreType.DMA
    S = jax.ShapeDtypeStruct
    outs = [
        (S((nc, rows, width), bf16), VM),
        (S((span, width), bf16), VM),
        (S((nf * nc,) + wp.shape[1:], bf16), VM),
        (S((nf * nc,) + tl.shape[2:], f32), VM),
        (S((hp,) + wo.shape, bf16), VM),
        (S((nf * nc, rows, width), bf16), ANY),
        (S((span, hp * hd), f32), VM),
        (S((span, hd), f32), VM),
        (S((span, hp * hd), bf16), VM),
        (S((span, hd), bf16), VM),
        (S((span, hd), bf16), VM),
        (S((span, hp * hd), bf16), VM),
        (S((span, hd), f32), VM),
        (S((rows, width), f32), VM),
        (S((nf * nc, rows, width), bf16), ANY),
    ]
    R = pltpu.VMEM((rows, width), bf16)
    scratch = [pltpu.VMEM((1, width), f32), pltpu.VMEM((1, width), f32), R, R, D(()), D(()), D((2,)), D((zs,)), D((zs,)), D((zs,)), D((zs,)), D((zs,)),
               D((nc,)), D((4 * nc,)), D((2 * nc,)), D((2 * nc,))]
    scratch += tile_bufs(nf, nc, tl.shape[2:])
    scratch += [pltpu.VMEM((nf,) + wo.shape, bf16), D((4,)), D((2, nf + 4)), D((2, nf + 4))] + gather_sems(zs) + gather_sems(zs) + line_sum_bufs(zs, rows, width // 2, bf16)
    return pl.pallas_call(
        lambda *refs: attn_kernel(nf, zs, hp, scale, refs),
        out_shape=[s for s, _ in outs],
        in_specs=[VM] * 9,
        out_specs=[b for _, b in outs],
        scratch_shapes=scratch,
        compiler_params=pltpu.CompilerParams(collective_id=cid, has_side_effects=True, vmem_limit_bytes=60 * 2**20),
        name="attention",
    )(x, wp, tl, wo, tb, cosine, sine, pos[:, None], pos[None, :])


def tail_kernel(nf, zs, x_ref, g_ref, tl_ref, o_ref, go_ref, to_ref, t, r0, ral, rar, fin, gt, ga, gb, lsem, s0, q0, szr, szl, rzr, rzl, sf, gl, sg, rg, sa, ra, *tile_b):
    f, c, z, k = place_of()
    nc = 2 * zs
    half = o_ref.shape[1] // 2
    sib_c = c + 1 - 2 * k
    sib = (f, sib_c)
    low = z < zs // 2
    zord = []
    for i in range(zs - 1):
        far_low = jnp.where(i < zs - 1 - z, zs - 1 - i, zs - 2 - i)
        far_high = jnp.where(i < z, i, i + 1)
        zord.append(jnp.where(low, far_low, far_high))
    zord.append(z)

    def src(zz, kk):
        return x_ref.at[pl.ds(2 * zz, 2), :, pl.ds(pl.multiple_of(kk * half, 128), half)]

    hc = nc // 2
    parts = []
    for p in (0, 1):
        fa = flip(f, 1 + p)
        fb = flip(f, 2 - p)
        parts.append((fa, fb, flip(fa, 2 - p)))
    gcopies = []
    for p, (fa, fb, fc) in enumerate(parts):
        for i, col in enumerate((fb, f)):
            cp = pltpu.make_async_copy(g_ref.at[col, pl.ds(p * hc, hc)], gt.at[p, i], gl.at[2 * p + i])
            cp.start()
            gcopies.append(cp)
    greet_cross(f, c, nf, nc)
    w = Wire()
    for p, (fa, fb, fc) in enumerate(parts):
        for i, col in enumerate((fc, fa)):
            w.send(g_ref.at[col, pl.ds(p * hc, hc)], ga.at[p, i], sg.at[2 * p + i], rg.at[2 * p + i], (fa, c))
    locals_ = []
    for zi in range(zs):
        zz = zord[zi]
        w.send(src(zz, 1 - k), r0.at[zz], s0.at[zz], q0.at[zz], sib)
        cp = pltpu.make_async_copy(src(zz, k), t.at[zz], lsem.at[zi])
        cp.start()
        locals_.append(cp)
    small_steps = tile_steps(w, nf, nc, tl_ref, to_ref, *tile_b)
    advance(small_steps)

    def complete(zi):
        zz = zord[zi]
        locals_[zi].wait()
        got(r0.at[zz], s0.at[zz], q0.at[zz], sib)
        add_into(t.at[zz], r0.at[zz])

    for zi in range(zs - 1):
        zz = zord[zi]
        complete(zi)
        right = zz > z
        from_left = jnp.logical_and(right, z > 0)
        from_right = jnp.logical_and(jnp.logical_not(right), z < zs - 1)
        got(ral.at[zz], szr.at[zz], rzr.at[zz], (f, c), from_left)
        got(rar.at[zz], szl.at[zz], rzl.at[zz], (f, c), from_right)

        @pl.when(from_left)
        def _():
            add_into(t.at[zz], ral.at[zz])

        @pl.when(from_right)
        def _():
            add_into(t.at[zz], rar.at[zz])

        w.send(t.at[zz], ral.at[zz], szr.at[zz], rzr.at[zz], (f, c + 2), right)
        w.send(t.at[zz], rar.at[zz], szl.at[zz], rzl.at[zz], (f, c - 2), jnp.logical_not(right))
        advance(small_steps)
        if zi == 0:
            for p, (fa, fb, fc) in enumerate(parts):
                for i in (0, 1):
                    gcopies[2 * p + i].wait()
                    got(ga.at[p, i], sg.at[2 * p + i], rg.at[2 * p + i], (fa, c))
                    add_into(gt.at[p, i], ga.at[p, i])
                    if i == 0:
                        w.send(gt.at[p, 0], gb.at[p], sg.at[4 + p], rg.at[4 + p], (fb, c))
        if zi == 1:
            for p, (fa, fb, fc) in enumerate(parts):
                got(gb.at[p], sg.at[4 + p], rg.at[4 + p], (fb, c))
                add_into(gt.at[p, 1], gb.at[p])
            for cc in range(nc):
                w.send(gt.at[cc // hc, 1, cc % hc], go_ref.at[c], sa.at[cc], ra.at[c], (f, cc), c != cc)

            def keep(cc):
                @pl.when(c == cc)
                def _():
                    go_ref[cc] = gt[cc // hc, 1, cc % hc]

            for cc in range(nc):
                keep(cc)
    complete(zs - 1)
    got(ral.at[z], szr.at[z], rzr.at[z], (f, c), z > 0)
    got(rar.at[z], szl.at[z], rzl.at[z], (f, c), z < zs - 1)

    @pl.when(z > 0)
    def _():
        add_into(t.at[z], ral.at[z])

    @pl.when(z < zs - 1)
    def _():
        add_into(t.at[z], rar.at[z])

    w.send(t.at[z, 1 - k], fin, sf.at[0], sf.at[1], sib)
    o_ref[:, pl.ds(pl.multiple_of(k * half, 128), half)] = t[z, k]
    for cc in range(nc):
        got(go_ref.at[cc], sa.at[cc], ra.at[cc], (f, c), c != cc)
    got(fin, sf.at[0], sf.at[1], sib)
    o_ref[:, pl.ds(pl.multiple_of((1 - k) * half, 128), half)] = fin[...]
    while advance(small_steps):
        pass
    w.drain()


def tail(x, g, tl, nf, zs, cid):
    n, rows, width = x.shape
    nc = 2 * zs
    D = pltpu.SemaphoreType.DMA
    half = width // 2
    V = lambda m: pltpu.VMEM((m, 2, rows, half), x.dtype)
    gs = g.shape[2:]
    G = lambda *lead: pltpu.VMEM(lead + (nc // 2,) + gs, g.dtype)
    return pl.pallas_call(
        functools.partial(tail_kernel, nf, zs),
        out_shape=(
            jax.ShapeDtypeStruct((rows, width), x.dtype),
            jax.ShapeDtypeStruct((nc,) + gs, g.dtype),
            jax.ShapeDtypeStruct((nf * nc,) + tl.shape[2:], tl.dtype),
        ),
        in_specs=[ANY, ANY, VM],
        out_specs=(VM, VM, VM),
        scratch_shapes=[V(zs), V(zs), V(zs), V(zs), pltpu.VMEM((rows, half), x.dtype), G(2, 2), G(2, 2), G(2),
            D((zs,)), D((zs,)), D((zs,)), D((zs,)), D((zs,)), D((zs,)), D((zs,)), D((2,)), D((4,)), D((6,)), D((6,)), D((nc,)), D((nc,))] + tile_bufs(nf, nc, tl.shape[2:]),
        compiler_params=pltpu.CompilerParams(collective_id=cid, has_side_effects=True, vmem_limit_bytes=60 * 2**20),
        name="tail",
    )(x, g, tl)


def attend_grad_kernel(scale, qb, q_ref, k_ref, v_ref, c_ref, g_ref, l_ref, pr_ref, pc_ref, gq_ref, gk_ref, gv_ref):
    rows = q_ref.shape[0]
    keys = k_ref[...]
    values = v_ref[...]

    @pl.when(pl.program_id(0) == 0)
    def _():
        gk_ref[...] = jnp.zeros_like(gk_ref)
        gv_ref[...] = jnp.zeros_like(gv_ref)

    lane = lax.broadcasted_iota(jnp.int32, (1, l_ref.shape[1]), 1)
    for i in range(rows // qb):
        at = pl.ds(i * qb, qb)
        q = q_ref[at, :]
        g = g_ref[at, :]
        s = lax.dot_general(q, keys, (((1,), (1,)), ((), ())), preferred_element_type=jnp.float32) * scale
        p = jnp.where(pc_ref[...] <= pr_ref[at, :], jnp.exp(s - jnp.sum(jnp.where(lane == pl.program_id(0), l_ref[at, :], 0.0), axis=-1, keepdims=True)), 0.0)
        gv_ref[...] += lax.dot_general(p.astype(jnp.bfloat16), g, (((0,), (0,)), ((), ())), preferred_element_type=jnp.float32)
        gp = lax.dot_general(g, values, (((1,), (1,)), ((), ())), preferred_element_type=jnp.float32)
        delta = jnp.sum(g.astype(jnp.float32) * c_ref[at, :].astype(jnp.float32), axis=-1, keepdims=True)
        ds = (p * (gp - delta)).astype(jnp.bfloat16)
        gq_ref[at, :] = jnp.dot(ds, keys, preferred_element_type=jnp.float32) * scale
        gk_ref[...] += lax.dot_general(ds, q, (((0,), (0,)), ((), ())), preferred_element_type=jnp.float32) * scale


def attend_grad(q, keys, values, ctx, grad, lse, pos, scale):
    rows, width = q.shape
    hd = keys.shape[1]
    col = pl.BlockSpec((rows, hd), lambda h: (0, h))
    full = pl.BlockSpec((rows, hd), lambda h: (0, 0))
    return pl.pallas_call(
        functools.partial(attend_grad_kernel, scale, 256),
        grid=(width // hd,),
        out_shape=(jax.ShapeDtypeStruct((rows, width), jnp.float32), jax.ShapeDtypeStruct((rows, hd), jnp.float32), jax.ShapeDtypeStruct((rows, hd), jnp.float32)),
        in_specs=[col, full, full, col, col, full, pl.BlockSpec((rows, 1), lambda h: (0, 0)), pl.BlockSpec((1, rows), lambda h: (0, 0))],
        out_specs=(col, full, full),
        name="attend_grad",
    )(q, keys, values, ctx, grad, lse, pos[:, None], pos[None, :])


def head_body(
    nf,
    nc,
    block_input,
    cotangent,
    gain_attn,
    w_query,
    w_key,
    w_value,
    qk_gain,
    w_out,
    gain_moe,
    w_gate,
    w_up,
    w_down,
    expert_ids,
    route_weight,
    pair_order,
):
    bf16, f32 = jnp.bfloat16, jnp.float32
    f, c, z, k = place_of()
    n = nf * nc
    zs = nc // 2
    rows, width = block_input.shape[1:]
    hd = qk_gain.shape[1] * n
    kv_heads = w_key.shape[1] // hd
    heads = w_query.shape[1] // hd
    hp = heads // nc
    shard = w_query.shape[0]
    topk = expert_ids.shape[2]
    capacity = max(2, 3 * BLOCK * topk // n)
    span = nc * rows
    scale = 1.0 / math.sqrt(hd)
    x_own = block_input[0]
    resid = x_own.astype(f32)

    ids, weights = expert_ids[0], route_weight[0].astype(f32)
    named = ids[None, :, :] == jnp.arange(n, dtype=jnp.int32)[:, None, None]
    to_expert = jnp.sum(jnp.where(named, weights[None], 0.0), axis=-1)
    lane = jnp.arange(rows)
    gs = gain_attn.shape[0]
    me = f * nc + c
    spots = lane // gs == me % (rows // gs)
    gain_row = lambda g: jnp.where(spots, jnp.tile(g.astype(f32), rows // gs), 0.0)
    qs = qk_gain.shape[1]
    qk_row = lambda g: jnp.where(lane // qs == me, jnp.tile(g.astype(f32), rows // qs), 0.0)
    small = jnp.stack([gain_row(gain_attn), qk_row(qk_gain[0]), qk_row(qk_gain[1]), gain_row(gain_moe)])
    tiles = jnp.concatenate([to_expert[:, None], jnp.broadcast_to(small, (n,) + small.shape), jnp.zeros((n, 3, rows), f32)], axis=1)
    by_place = lambda t: t.reshape((nf, nc) + t.shape[1:]).swapaxes(0, 1)
    per = nc // kv_heads
    wq_p = w_query.reshape(shard, nc, hp * hd).transpose(1, 0, 2)
    wk_p = jnp.repeat(w_key.reshape(shard, kv_heads, hd).transpose(1, 0, 2), per, axis=0)
    wv_p = jnp.repeat(w_value.reshape(shard, kv_heads, hd).transpose(1, 0, 2), per, axis=0)
    packed = jnp.concatenate([wq_p, wk_p, wv_p], axis=2)
    top_own = cotangent[0]
    pos = seq_positions(pair_order, BLOCK)
    cosine, sine = rope_tables(pos, hd)
    (x_seq, normed_in, w_all, dealt, wo_all, top_all, q_pre, k_pre, query_rot, key_rot, values, context, lse, hidden_res, tokens) = attention(
        x_own, packed, by_place(tiles), w_out, top_own.astype(bf16), cosine, sine, pos, nf, zs, hp, scale, 0
    )
    lin = lambda ff, cc: ff * nc + cc
    hops = [(h, lin(h % hp, h // hp)) for h in range(n)]
    qw = hp * hd
    w_cat = w_all.reshape(n * shard, qw + 2 * hd)
    wo_mine = wo_all.reshape(qw, width)
    full_row = lambda r: dealt[:, r].reshape(-1, rows // gs, rows).sum(axis=1).reshape(-1)
    g_attn, g_moe = full_row(1), full_row(4)
    g_qk = dealt[:, 2:4].sum(axis=0)
    route_w = dealt[:, 0, :]
    q_pre = q_pre.reshape(span, hp, hd)
    k_pre = k_pre.reshape(span, 1, hd)
    hit = route_w > 0.0
    below = (jnp.arange(rows)[:, None] < jnp.arange(rows)[None, :]).astype(f32)
    rank = jnp.dot(hit.astype(f32), below, preferred_element_type=f32).astype(jnp.int32)
    slot = (rank[:, None, :] == jnp.arange(capacity, dtype=jnp.int32)[None, :, None]) & hit[:, None, :]
    place = slot.astype(bf16)
    mixing = jnp.where(slot, route_w[:, None, :], 0.0).astype(bf16)
    gate_w, up_w, down_w = w_gate[0], w_up[0], w_down[0]
    pick = lambda table, rws: jnp.einsum("srt,std->srd", table, rws, preferred_element_type=f32).astype(bf16).reshape(n * capacity, width)
    back = lambda table, rws: jnp.einsum("srt,srd->std", table, rws.reshape(n, capacity, width), preferred_element_type=f32).astype(bf16)
    arrived = pick(place, tokens)
    gate_pre = jnp.dot(arrived, gate_w, preferred_element_type=f32)
    up_pre = jnp.dot(arrived, up_w, preferred_element_type=f32)
    gate_sig = jax.nn.sigmoid(gate_pre)
    gate_act = gate_pre * gate_sig
    expert_hidden = (gate_act * up_pre).astype(bf16)

    grad_arrived = pick(mixing, top_all.reshape(n, rows, width))
    grad_hidden = contract_cols(grad_arrived, down_w)
    grad_gate_pre = (grad_hidden * up_pre * gate_sig * (1.0 + gate_pre * (1.0 - gate_sig))).astype(bf16)
    grad_up_pre = (grad_hidden * gate_act).astype(bf16)
    grad_rows = (contract_cols(grad_gate_pre, gate_w) + contract_cols(grad_up_pre, up_w)).astype(bf16)
    grad_mid = scatter(back(place, grad_rows), zs, True, 3, nf).astype(f32)

    _, mid_back = jax.vjp(rms_scale, hidden_res, g_moe)
    grad_res_mid, grad_moe_gain = mid_back(grad_mid)
    grad_res = top_own + grad_res_mid
    res_all = gather(grad_res.astype(bf16), zs, False, 4).reshape(span, width)

    hidden_late, arrived_late, grad_arrived_late, _ = lax.optimization_barrier((expert_hidden, arrived, grad_arrived, grad_mid))
    expert_out = jnp.dot(hidden_late, down_w, preferred_element_type=f32).astype(bf16)
    mixed = lax.psum_scatter(back(mixing, expert_out).reshape(n * rows, width), ("fsdp", "cp"), scatter_dimension=0, tiled=True)
    block_output = (hidden_res + mixed.astype(f32)).astype(bf16)
    grad_down = contract_rows(hidden_late, grad_arrived_late)
    grad_gate = contract_rows(arrived_late, grad_gate_pre)
    grad_up = contract_rows(arrived_late, grad_up_pre)

    grad_wo_mine = contract_rows(context, res_all)
    hops_back = [(b, a) for a, b in hops]
    grad_wo = lax.ppermute(
        lax.psum_scatter(grad_wo_mine.astype(bf16), "fsdp", scatter_dimension=0, tiled=True), ("fsdp", "cp"), hops_back
    ).astype(f32)
    grad_context = contract_cols(res_all, wo_mine).astype(bf16)
    grad_query, grad_keys, grad_values = attend_grad(query_rot, key_rot, values, context, grad_context, lse, pos, scale)
    pairs = [(cc, cc + 1 - 2 * (cc % 2)) for cc in range(nc)]
    both = jnp.stack([grad_keys, grad_values])
    both = both + lax.ppermute(both, "cp", pairs)
    grad_keys, grad_values = both[0], both[1]
    _, query_back = jax.vjp(lambda pre, gain: head_post(pre, gain, cosine, sine), q_pre, g_qk[0])
    grad_q_pre, grad_q_gain = query_back(grad_query.reshape(span, hp, hd))
    _, key_back = jax.vjp(lambda pre, gain: head_post(pre, gain, cosine, sine), k_pre, g_qk[1])
    grad_k_pre, grad_k_gain = key_back(grad_keys.reshape(span, 1, hd))
    grad_q_b = grad_q_pre.reshape(span, qw).astype(bf16)
    x32 = x_seq.reshape(span, width).astype(f32)
    inv_in = lax.rsqrt(jnp.mean(x32 * x32, axis=-1, keepdims=True) + EPSILON)
    first = k == 0
    grad_kv_b = jnp.where(first, grad_k_pre.reshape(span, hd), grad_values).astype(bf16)
    grad_cat = jnp.concatenate([grad_q_b, grad_kv_b], axis=1)
    w_kv = jnp.where(first, w_cat[:, qw : qw + hd], w_cat[:, qw + hd :])
    w_back = jnp.concatenate([w_cat[:, :qw], w_kv], axis=1)
    grad_w = contract_rows(normed_in, grad_cat).astype(bf16)
    grad_norm = contract_cols(grad_cat, w_back)
    grad_attn_gain = jnp.sum(grad_norm * (x32 * inv_in), axis=0)
    grad_k_gain = jnp.where(first, grad_k_gain, 0.0)
    share = lambda v: v.reshape(n, -1)
    qk_parts = jnp.stack([grad_q_gain, grad_k_gain]).reshape(2, n, -1).transpose(1, 0, 2).reshape(n, -1)
    line0 = jnp.concatenate([share(grad_attn_gain), share(grad_moe_gain)], axis=1)
    wide = lambda v: jnp.pad(v, ((0, 0), (0, rows - v.shape[1])))
    sums = jnp.concatenate([wide(line0)[:, None], wide(qk_parts)[:, None], jnp.zeros((n, 6, rows), f32)], axis=1)
    grad_in, grads, summed = tail(
        grad_norm.astype(bf16).reshape(nc, rows, width), grad_w.reshape(nf, nc, shard, qw + hd), by_place(sums), nf, zs, 5
    )
    total = jnp.sum(summed, axis=0)
    own_attn_gain = total[0, :gs]
    own_moe_gain = total[0, gs : 2 * gs]
    own_qk = total[1, : qk_gain.size].reshape(2, -1)
    grad_wq = grads[:, :, :qw].transpose(1, 0, 2).reshape(shard, heads * hd).astype(f32)
    grad_kv = grads[:, :, qw:].reshape(kv_heads, per, shard, hd)
    grad_wk = grad_kv[:, 0].transpose(1, 0, 2).reshape(shard, kv_heads * hd).astype(f32)
    grad_wv = grad_kv[:, 1].transpose(1, 0, 2).reshape(shard, kv_heads * hd).astype(f32)
    _, in_back = jax.vjp(rms_scale, resid, g_attn)
    grad_input = grad_res + in_back(grad_in.astype(f32))[0]
    return (
        block_output[None],
        grad_input[None],
        own_attn_gain,
        grad_wq,
        grad_wk,
        grad_wv,
        own_qk,
        grad_wo,
        own_moe_gain,
        grad_gate[None],
        grad_up[None],
        grad_down[None],
    )


def body(nf, nc, block_input, *rest):
    kv_heads = rest[3].shape[1] // (rest[5].shape[1] * nf * nc)
    fits = nf == 4 and nc == 2 * kv_heads and rest[4].shape[1] == rest[3].shape[1]
    return head_body(nf, nc, block_input, *rest) if fits else wide_body(block_input, *rest)


def solution(mesh):
    return jax.shard_map(
        functools.partial(body, mesh.shape["fsdp"], mesh.shape["cp"]),
        mesh=mesh,
        in_specs=(
            P("fsdp", "cp", None),
            P("fsdp", "cp", None),
            P(("fsdp", "cp")),
            P(("fsdp", "cp"), None),
            P(("fsdp", "cp"), None),
            P(("fsdp", "cp"), None),
            P(None, ("fsdp", "cp")),
            P(("fsdp", "cp"), None),
            P(("fsdp", "cp")),
            P(("fsdp", "cp"), None, None),
            P(("fsdp", "cp"), None, None),
            P(("fsdp", "cp"), None, None),
            P("fsdp", "cp", None),
            P("fsdp", "cp", None),
            P(),
        ),
        out_specs=(
            P("fsdp", "cp", None),
            P("fsdp", "cp", None),
            P(("fsdp", "cp")),
            P(("fsdp", "cp"), None),
            P(("fsdp", "cp"), None),
            P(("fsdp", "cp"), None),
            P(None, ("fsdp", "cp")),
            P(("fsdp", "cp"), None),
            P(("fsdp", "cp")),
            P(("fsdp", "cp"), None, None),
            P(("fsdp", "cp"), None, None),
            P(("fsdp", "cp"), None, None),
        ),
        check_vma=False,
    )
```

```python
import functools
import math

import jax
import jax.numpy as jnp
from jax import lax
from jax.experimental import pallas as pl
from jax.experimental.pallas import tpu as pltpu
from jax.sharding import PartitionSpec as P

BLOCK = 64


EPSILON = 1e-06
THETA = 1000000.0


def rms_scale(values, gain):
    return values * lax.rsqrt(jnp.mean(values * values, axis=-1, keepdims=True) + EPSILON) * gain


def rotate_half(values):
    half = values.shape[-1] // 2
    return jnp.concatenate([-values[..., half:], values[..., :half]], axis=-1)


def head_post(pre, gain, cosine, sine):
    normed = rms_scale(pre, gain)
    return normed * cosine[:, None, :] + rotate_half(normed) * sine[:, None, :]


def rope_tables(positions, head_dim):
    freqs = THETA ** (-(jnp.arange(head_dim // 2, dtype=jnp.float32) * 2.0 / head_dim))
    angles = positions.astype(jnp.float32)[:, None] * freqs[None, :]
    angles = jnp.concatenate([angles, angles], axis=-1)
    return (jnp.cos(angles), jnp.sin(angles))


def seq_positions(pair_order, block):
    blocks = 2 * pair_order.shape[0]
    rows = jnp.arange(blocks * block, dtype=jnp.int32)
    owner = rows // (2 * block)
    first = pair_order[owner]
    which = jnp.where(rows // block % 2 == 0, first, blocks - 1 - first)
    return which * block + rows % block


def route_tables(ids, weights, experts, capacity):
    flat = ids.reshape(-1)
    onehot = (flat[:, None] == jnp.arange(experts, dtype=jnp.int32)[None, :]).astype(jnp.int32)
    before = jnp.cumsum(onehot, axis=0) - onehot
    rank = jnp.sum(before * onehot, axis=1)
    slots = (flat * capacity + rank).reshape(ids.shape)
    columns = jnp.arange(experts * capacity, dtype=jnp.int32)
    hits = slots[:, :, None] == columns[None, None, :]
    place = jnp.sum(hits.astype(jnp.float32), axis=1).astype(jnp.bfloat16)
    mixing = jnp.sum(jnp.where(hits, weights[:, :, None].astype(jnp.float32), 0.0), axis=1).astype(
        jnp.bfloat16
    )
    return (place, mixing)


def attend_head(query, keys, values, allowed, scale):
    scores = jnp.einsum("grd,sd->grs", query, keys, preferred_element_type=jnp.float32) * scale
    scores = jnp.where(allowed[None], scores, -jnp.inf)
    top = jnp.max(scores, axis=-1, keepdims=True)
    lse = top[..., 0] + jnp.log(jnp.sum(jnp.exp(scores - top), axis=-1))
    probs = jnp.exp(scores - lse[..., None]).astype(jnp.bfloat16)
    output = jnp.einsum("grs,sd->grd", probs, values, preferred_element_type=jnp.float32)
    return (output.astype(jnp.bfloat16), lse)


def attend_back(query, keys, values, output, grad_out, lse, allowed, scale):
    scores = jnp.einsum("grd,sd->grs", query, keys, preferred_element_type=jnp.float32) * scale
    scores = jnp.where(allowed[None], scores, -jnp.inf)
    probs = jnp.exp(scores - lse[..., None])
    grad_values = jnp.einsum(
        "grs,grd->sd", probs.astype(jnp.bfloat16), grad_out, preferred_element_type=jnp.float32
    )
    grad_probs = jnp.einsum("grd,sd->grs", grad_out, values, preferred_element_type=jnp.float32)
    delta = jnp.sum(grad_out.astype(jnp.float32) * output.astype(jnp.float32), axis=-1)
    grad_scores = (probs * (grad_probs - delta[..., None])).astype(jnp.bfloat16)
    grad_query = (
        jnp.einsum("grs,sd->grd", grad_scores, keys, preferred_element_type=jnp.float32) * scale
    )
    grad_keys = (
        jnp.einsum("grs,grd->sd", grad_scores, query, preferred_element_type=jnp.float32) * scale
    )
    return (grad_query, grad_keys, grad_values)


def contract_rows(left, right):
    return lax.dot_general(
        left, right, (((0,), (0,)), ((), ())), preferred_element_type=jnp.float32
    )


def contract_cols(left, right):
    return lax.dot_general(
        left, right, (((1,), (1,)), ((), ())), preferred_element_type=jnp.float32
    )


def wide_body(
    block_input,
    cotangent,
    gain_attn,
    w_query,
    w_key,
    w_value,
    qk_gain,
    w_out,
    gain_moe,
    w_gate,
    w_up,
    w_down,
    expert_ids,
    route_weight,
    pair_order,
):
    g_attn, wq_full, wk_full, wv_full, qk_full, wo_full, g_moe = (
        lax.all_gather(gain_attn, ("fsdp", "cp"), axis=0, tiled=True),
        lax.all_gather(w_query, ("fsdp", "cp"), axis=0, tiled=True),
        lax.all_gather(w_key, ("fsdp", "cp"), axis=0, tiled=True),
        lax.all_gather(w_value, ("fsdp", "cp"), axis=0, tiled=True),
        lax.all_gather(qk_gain, ("fsdp", "cp"), axis=1, tiled=True),
        lax.all_gather(w_out, ("fsdp", "cp"), axis=0, tiled=True),
        lax.all_gather(gain_moe, ("fsdp", "cp"), axis=0, tiled=True),
    )
    rows = block_input.shape[1]
    width = block_input.shape[2]
    head_dim = qk_full.shape[1]
    kv_heads = wk_full.shape[1] // head_dim
    heads = wq_full.shape[1] // head_dim
    group = heads // kv_heads
    experts = lax.axis_size(("fsdp", "cp"))
    capacity = max(2, 3 * BLOCK * expert_ids.shape[2] // experts)
    scale = 1.0 / math.sqrt(head_dim)
    resid = block_input[0].astype(jnp.float32)
    normed_in = rms_scale(resid, g_attn.astype(jnp.float32)).astype(jnp.bfloat16)
    q_pre = jnp.dot(normed_in, wq_full, preferred_element_type=jnp.float32).reshape(
        rows, heads, head_dim
    )
    k_pre = jnp.dot(normed_in, wk_full, preferred_element_type=jnp.float32).reshape(
        rows, kv_heads, head_dim
    )
    value_rows = jnp.dot(normed_in, wv_full, preferred_element_type=jnp.float32).astype(
        jnp.bfloat16
    )
    all_pos = seq_positions(pair_order, BLOCK)
    local_pos = lax.dynamic_slice_in_dim(all_pos, lax.axis_index("cp") * rows, rows)
    cosine, sine = rope_tables(local_pos, head_dim)
    gains32 = qk_full.astype(jnp.float32)
    query_rot = head_post(q_pre, gains32[0], cosine, sine).astype(jnp.bfloat16)
    key_rot = head_post(k_pre, gains32[1], cosine, sine).astype(jnp.bfloat16)
    keys_all, values_all = (
        lax.all_gather(key_rot.reshape(rows, kv_heads * head_dim), "cp", axis=0, tiled=True),
        lax.all_gather(value_rows, "cp", axis=0, tiled=True),
    )
    span = keys_all.shape[0]
    allowed = all_pos[None, :] <= local_pos[:, None]
    query_heads = query_rot.reshape(rows, kv_heads, group, head_dim).transpose(1, 2, 0, 3)
    key_heads = keys_all.reshape(span, kv_heads, head_dim).transpose(1, 0, 2)
    value_heads = values_all.reshape(span, kv_heads, head_dim).transpose(1, 0, 2)
    context_heads, lse = lax.map(
        lambda item: attend_head(item[0], item[1], item[2], allowed, scale),
        (query_heads, key_heads, value_heads),
    )
    context = context_heads.transpose(2, 0, 1, 3).reshape(rows, heads * head_dim)
    hidden_res = resid + jnp.dot(context, wo_full, preferred_element_type=jnp.float32)
    normed_mid = rms_scale(hidden_res, g_moe.astype(jnp.float32)).astype(jnp.bfloat16)
    place, mixing = route_tables(expert_ids[0], route_weight[0], experts, capacity)
    sent = contract_rows(place, normed_mid).astype(jnp.bfloat16)
    arrived = lax.all_to_all(
        sent.reshape(experts, capacity, width),
        ("fsdp", "cp"),
        split_axis=0,
        concat_axis=0,
        tiled=True,
    ).reshape(experts * capacity, width)
    gate_w = w_gate[0]
    up_w = w_up[0]
    down_w = w_down[0]
    gate_pre = jnp.dot(arrived, gate_w, preferred_element_type=jnp.float32)
    up_pre = jnp.dot(arrived, up_w, preferred_element_type=jnp.float32)
    gate_sig = jax.nn.sigmoid(gate_pre)
    gate_act = gate_pre * gate_sig
    expert_hidden = (gate_act * up_pre).astype(jnp.bfloat16)
    expert_out = jnp.dot(expert_hidden, down_w, preferred_element_type=jnp.float32).astype(
        jnp.bfloat16
    )
    returned = lax.all_to_all(
        expert_out.reshape(experts, capacity, width),
        ("fsdp", "cp"),
        split_axis=0,
        concat_axis=0,
        tiled=True,
    ).reshape(experts * capacity, width)
    mixed = jnp.dot(mixing, returned, preferred_element_type=jnp.float32)
    block_output = (hidden_res + mixed).astype(jnp.bfloat16)
    g_attn, wq_full, wk_full, wv_full, qk_full, wo_full, g_moe = (
        lax.all_gather(gain_attn, ("fsdp", "cp"), axis=0, tiled=True),
        lax.all_gather(w_query, ("fsdp", "cp"), axis=0, tiled=True),
        lax.all_gather(w_key, ("fsdp", "cp"), axis=0, tiled=True),
        lax.all_gather(w_value, ("fsdp", "cp"), axis=0, tiled=True),
        lax.all_gather(qk_gain, ("fsdp", "cp"), axis=1, tiled=True),
        lax.all_gather(w_out, ("fsdp", "cp"), axis=0, tiled=True),
        lax.all_gather(gain_moe, ("fsdp", "cp"), axis=0, tiled=True),
    )
    attn_gain = g_attn.astype(jnp.float32)
    moe_gain = g_moe.astype(jnp.float32)
    gains_back = qk_full.astype(jnp.float32)
    grad_top = cotangent[0]
    grad_top_b = grad_top.astype(jnp.bfloat16)
    grad_sent = contract_rows(mixing, grad_top_b).astype(jnp.bfloat16)
    grad_arrived = lax.all_to_all(
        grad_sent.reshape(experts, capacity, width),
        ("fsdp", "cp"),
        split_axis=0,
        concat_axis=0,
        tiled=True,
    ).reshape(experts * capacity, width)
    grad_hidden = contract_cols(grad_arrived, down_w)
    grad_down = contract_rows(expert_hidden, grad_arrived)
    grad_gate_pre = (grad_hidden * up_pre * gate_sig * (1.0 + gate_pre * (1.0 - gate_sig))).astype(
        jnp.bfloat16
    )
    grad_up_pre = (grad_hidden * gate_act).astype(jnp.bfloat16)
    grad_gate = contract_rows(arrived, grad_gate_pre)
    grad_up = contract_rows(arrived, grad_up_pre)
    grad_rows = (contract_cols(grad_gate_pre, gate_w) + contract_cols(grad_up_pre, up_w)).astype(
        jnp.bfloat16
    )
    grad_back = lax.all_to_all(
        grad_rows.reshape(experts, capacity, width),
        ("fsdp", "cp"),
        split_axis=0,
        concat_axis=0,
        tiled=True,
    ).reshape(experts * capacity, width)
    grad_mid = jnp.dot(place, grad_back, preferred_element_type=jnp.float32)
    _, mid_back = jax.vjp(rms_scale, hidden_res, moe_gain)
    grad_res_mid, grad_moe_gain = mid_back(grad_mid)
    grad_res = grad_top + grad_res_mid
    grad_res_b = grad_res.astype(jnp.bfloat16)
    grad_wo = contract_rows(context, grad_res_b)
    grad_context = contract_cols(grad_res_b, wo_full).astype(jnp.bfloat16)
    grad_ctx_heads = grad_context.reshape(rows, kv_heads, group, head_dim).transpose(1, 2, 0, 3)
    grad_q_heads, grad_k_heads, grad_v_heads = lax.map(
        lambda it: attend_back(it[0], it[1], it[2], it[3], it[4], it[5], allowed, scale),
        (query_heads, key_heads, value_heads, context_heads, grad_ctx_heads, lse),
    )
    grad_keys_all = grad_k_heads.transpose(1, 0, 2).reshape(span, kv_heads * head_dim)
    grad_values_all = grad_v_heads.transpose(1, 0, 2).reshape(span, kv_heads * head_dim)
    grad_key_rot, grad_values = (
        lax.psum_scatter(
            grad_keys_all.astype(jnp.bfloat16), "cp", scatter_dimension=0, tiled=True
        ).astype(jnp.float32),
        lax.psum_scatter(
            grad_values_all.astype(jnp.bfloat16), "cp", scatter_dimension=0, tiled=True
        ).astype(jnp.float32),
    )
    grad_query_rot = grad_q_heads.transpose(2, 0, 1, 3).reshape(rows, heads, head_dim)
    _, query_back = jax.vjp(
        lambda pre, gain: head_post(pre, gain, cosine, sine), q_pre, gains_back[0]
    )
    grad_q_pre, grad_q_gain = query_back(grad_query_rot)
    _, key_back = jax.vjp(
        lambda pre, gain: head_post(pre, gain, cosine, sine), k_pre, gains_back[1]
    )
    grad_k_pre, grad_k_gain = key_back(grad_key_rot.reshape(rows, kv_heads, head_dim))
    grad_q_b = grad_q_pre.reshape(rows, heads * head_dim).astype(jnp.bfloat16)
    grad_k_b = grad_k_pre.reshape(rows, kv_heads * head_dim).astype(jnp.bfloat16)
    grad_v_b = grad_values.astype(jnp.bfloat16)
    grad_wq = contract_rows(normed_in, grad_q_b)
    grad_wk = contract_rows(normed_in, grad_k_b)
    grad_wv = contract_rows(normed_in, grad_v_b)
    grad_in_norm = (
        contract_cols(grad_q_b, wq_full)
        + contract_cols(grad_k_b, wk_full)
        + contract_cols(grad_v_b, wv_full)
    )
    _, in_back = jax.vjp(rms_scale, resid, attn_gain)
    grad_res_in, grad_attn_gain = in_back(grad_in_norm)
    grad_input = grad_res + grad_res_in
    grad_qk = jnp.stack([grad_q_gain, grad_k_gain])
    owned_grads = (
        lax.psum_scatter(grad_attn_gain, ("fsdp", "cp"), scatter_dimension=0, tiled=True),
        lax.psum_scatter(grad_wq, ("fsdp", "cp"), scatter_dimension=0, tiled=True),
        lax.psum_scatter(grad_wk, ("fsdp", "cp"), scatter_dimension=0, tiled=True),
        lax.psum_scatter(grad_wv, ("fsdp", "cp"), scatter_dimension=0, tiled=True),
        lax.psum_scatter(grad_qk, ("fsdp", "cp"), scatter_dimension=1, tiled=True),
        lax.psum_scatter(grad_wo, ("fsdp", "cp"), scatter_dimension=0, tiled=True),
        lax.psum_scatter(grad_moe_gain, ("fsdp", "cp"), scatter_dimension=0, tiled=True),
    )
    return (
        block_output[None],
        grad_input[None],
        owned_grads[0],
        owned_grads[1],
        owned_grads[2],
        owned_grads[3],
        owned_grads[4],
        owned_grads[5],
        owned_grads[6],
        grad_gate[None],
        grad_up[None],
        grad_down[None],
    )


MESH = pl.DeviceIdType.MESH
ANY = pl.BlockSpec(memory_space=pl.ANY)
VM = pl.BlockSpec(memory_space=pltpu.VMEM)


def place_of():
    f = lax.axis_index("fsdp")
    c = lax.axis_index("cp")
    return f, c, c // 2, c % 2


def flip(f, bit):
    return f + bit - 2 * bit * ((f // bit) % 2)


class Wire:
    def __init__(self):
        self.sent = []

    def send(self, src, dst, ssem, rsem, dev, when=None):
        copy = pltpu.make_async_remote_copy(
            src_ref=src, dst_ref=dst, send_sem=ssem, recv_sem=rsem, device_id=dev, device_id_type=MESH
        )
        if when is None:
            copy.start()
        else:
            pl.when(when)(copy.start)
        self.sent.append((copy, when))
        return self.sent[-1]

    def settle(self, entries):
        for entry in entries:
            self.sent = [e for e in self.sent if e is not entry]
            self.wait(*entry)

    def wait(self, copy, when):
        if when is None:
            copy.wait_send()
        else:
            pl.when(when)(copy.wait_send)

    def drain(self):
        for entry in self.sent:
            self.wait(*entry)


def got(dst, ssem, rsem, dev, when=None):
    copy = pltpu.make_async_remote_copy(
        src_ref=dst, dst_ref=dst, send_sem=ssem, recv_sem=rsem, device_id=dev, device_id_type=MESH
    )
    if when is None:
        copy.wait_recv()
    else:
        pl.when(when)(copy.wait_recv)


def greet(f, c, z, zs, planes):
    bar = pltpu.get_barrier_semaphore()
    k = c % 2
    sib = c + 1 - 2 * k
    near = [((f, sib), None), ((f, c + 2), z < zs - 1), ((f, c - 2), z > 0)]
    if planes:
        near += [((flip(f, 1), c), None), ((flip(f, 2), c), None)]
    for dev, when in near:
        def hello(dev=dev):
            pl.semaphore_signal(bar, inc=1, device_id=dev, device_id_type=MESH)
        if when is None:
            hello()
        else:
            pl.when(when)(hello)
    base = 3 if planes else 1
    inner = jnp.logical_and(z > 0, z < zs - 1)
    pl.semaphore_wait(bar, base + jnp.where(inner, 2, 1))


def ag_kernel(zs, planes, x_ref, o_ref, loc, sl, szr, szl, rz, sp1, rp1, sp2, rp2, ssib, rsib):
    f, c, z, k = place_of()
    half = x_ref.shape[1] // 2
    sib = (f, c + 1 - 2 * k)
    b1 = 1 + k
    b2 = 2 - k
    f1 = flip(f, b1)
    f2 = flip(f, b2)
    cols = [f, f1, f2, flip(f1, b2)] if planes else [0]
    cs = 2 * zs

    def chunk(col, zz):
        at = (cols[col] * cs if planes else 0) + 2 * zz
        return o_ref.at[pl.ds(at, 2), :, pl.ds(pl.multiple_of(k * half, 128), half)]

    def other(col, zz):
        at = (cols[col] * cs if planes else 0) + 2 * zz
        return o_ref.at[pl.ds(at, 2), :, pl.ds(pl.multiple_of((1 - k) * half, 128), half)]

    mine = (f * cs if planes else 0) + c
    theirs = (f * cs if planes else 0) + c + 1 - 2 * k
    own = pltpu.make_async_copy(x_ref, o_ref.at[mine], loc)
    own.start()
    greet(f, c, z, zs, planes)
    w = Wire()
    w.send(x_ref, o_ref.at[mine], sl.at[0], sl.at[1], sib)
    own.wait()
    got(o_ref.at[theirs], sl.at[0], sl.at[1], sib)

    def spread(zz, when):
        if planes:
            w.send(chunk(0, zz), chunk(0, zz), sp1.at[zz], rp1.at[zz], (f1, c), when)
            w.send(chunk(0, zz), chunk(0, zz), sp2.at[zz], rp2.at[zz], (f2, c), when)

    def relay(zz, when):
        if planes:
            got(chunk(1, zz), sp1.at[zz], rp1.at[zz], (f1, c), when)
            w.send(chunk(1, zz), chunk(1, zz), sp2.at[zs + zz], rp2.at[zs + zz], (f2, c), when)
            w.send(chunk(1, zz), chunk(1, zz), ssib.at[zs + zz], rsib.at[zs + zz], sib, when)

    w.send(chunk(0, z), chunk(0, z), szr.at[z], rz.at[z], (f, c + 2), z < zs - 1)
    w.send(chunk(0, z), chunk(0, z), szl.at[z], rz.at[z], (f, c - 2), z > 0)
    spread(z, None)
    order = []
    for h in range(1, zs):
        for zz, when, on, dz, sem in (
            (z - h, z - h >= 0, z < zs - 1, 2, szr),
            (z + h, z + h < zs, z > 0, -2, szl),
        ):
            got(chunk(0, zz), sem.at[zz], rz.at[zz], (f, c), when)
            w.send(chunk(0, zz), chunk(0, zz), sem.at[zz], rz.at[zz], (f, c + dz), jnp.logical_and(when, on))
            spread(zz, when)
            w.send(chunk(0, zz), chunk(0, zz), ssib.at[zz], rsib.at[zz], sib, when)
            order.append((zz, when))
        if h == 1:
            relay(z, None)
    for zz, when in order:
        relay(zz, when)
    if planes:
        for col, base in ((2, 0), (3, zs)):
            for zz, when in [(z, None)] + order:
                got(chunk(col, zz), sp2.at[base + zz], rp2.at[base + zz], (f2, c), when)
                w.send(chunk(col, zz), chunk(col, zz), ssib.at[col * zs + zz], rsib.at[col * zs + zz], sib, when)
    if planes:
        for mycol, theircol in ((0, 0), (1, 2), (2, 1), (3, 3)):
            for zz, when in ([(z, None)] if mycol else []) + order:
                got(other(mycol, zz), ssib.at[theircol * zs + zz], rsib.at[theircol * zs + zz], sib, when)
    else:
        for zz, when in order:
            got(other(0, zz), ssib.at[zz], rsib.at[zz], sib, when)
    w.drain()


def gather(x, zs, planes, cid, nf=4):
    rows, width = x.shape
    n = (nf if planes else 1) * 2 * zs
    D = pltpu.SemaphoreType.DMA
    return pl.pallas_call(
        functools.partial(ag_kernel, zs, planes),
        out_shape=jax.ShapeDtypeStruct((n, rows, width), x.dtype),
        in_specs=[VM],
        out_specs=ANY,
        scratch_shapes=[D(()), D((2,)), D((zs,)), D((zs,)), D((zs,)), D((zs,)), D((zs,)), D((2 * zs,)), D((2 * zs,)), D((4 * zs,)), D((4 * zs,))],
        compiler_params=pltpu.CompilerParams(collective_id=cid, has_side_effects=True),
        name="gather_all" if planes else "gather_seq",
    )(x)


def add_into(dst, src, rows=32):
    n, r, wd = dst.shape

    def step(i, _):
        a = pl.ds(pl.multiple_of(i % (r // rows) * rows, rows), rows)
        j = i // (r // rows)
        dst[j, a, :] = (dst[j, a, :].astype(jnp.float32) + src[j, a, :].astype(jnp.float32)).astype(dst.dtype)
        return 0

    lax.fori_loop(0, n * (r // rows), step, 0)


def rs_kernel(zs, planes, x_ref, o_ref, t, r0, r1, r2, ral, rar, fin, lsem, s0, q0, s1, q1, s2, q2, szr, szl, rzr, rzl, sf):
    f, c, z, k = place_of()
    half = o_ref.shape[1] // 2
    sib = (f, c + 1 - 2 * k)
    b1 = 2 - k
    b2 = 1 + k
    f1 = flip(f, b1)
    f2 = flip(f, b2)
    f3 = flip(f1, b2)
    cs = 2 * zs
    cols = [f3, f1, f2, f] if planes else [0]
    nc = len(cols)
    last = zs - 1
    low = z < zs // 2
    zord = []
    for i in range(zs - 1):
        far_low = jnp.where(i < zs - 1 - z, last - i, zs - 2 - i)
        far_high = jnp.where(i < z, i, i + 1)
        zord.append(jnp.where(low, far_low, far_high))
    zord.append(z)

    def src(col, zz, kk):
        at = (col * cs if planes else 0) + 2 * zz
        return x_ref.at[pl.ds(at, 2), :, pl.ds(pl.multiple_of(kk * half, 128), half)]

    greet(f, c, z, zs, planes)
    w = Wire()
    locals_ = []
    for ci in range(nc):
        for zi in range(zs):
            i = ci * zs + zi
            col = cols[ci]
            zz = zord[zi]
            slot = (ci if not planes else {0: 0, 1: 2, 2: 1, 3: 3}[ci]) * zs + zz
            w.send(src(col, zz, 1 - k), r0.at[slot], s0.at[slot], q0.at[slot], sib)
            cp = pltpu.make_async_copy(src(col, zz, k), t.at[ci * zs + zz], lsem.at[i])
            cp.start()
            locals_.append(cp)

    def first(ci, zi):
        zz = zord[zi]
        locals_[ci * zs + zi].wait()
        got(r0.at[ci * zs + zz], s0.at[ci * zs + zz], q0.at[ci * zs + zz], sib)
        add_into(t.at[ci * zs + zz], r0.at[ci * zs + zz])

    if planes:
        for ci in (0, 1):
            for zi in range(zs):
                zz = zord[zi]
                first(ci, zi)
                m = ci * zs + zz
                w.send(t.at[m], r1.at[m], s1.at[m], q1.at[m], (f1, c))
        for zi in range(zs):
            zz = zord[zi]
            first(2, zi)
            got(r1.at[zz], s1.at[zz], q1.at[zz], (f1, c))
            add_into(t.at[2 * zs + zz], r1.at[zz])
            w.send(t.at[2 * zs + zz], r2.at[zz], s2.at[zz], q2.at[zz], (f2, c))
        for zi in range(zs):
            first(3, zi)
        base = 3 * zs
    else:
        base = 0

    def complete(zi):
        zz = zord[zi]
        if planes:
            got(r1.at[zs + zz], s1.at[zs + zz], q1.at[zs + zz], (f1, c))
            add_into(t.at[base + zz], r1.at[zs + zz])
            got(r2.at[zz], s2.at[zz], q2.at[zz], (f2, c))
            add_into(t.at[base + zz], r2.at[zz])
        else:
            first(0, zi)

    for zi in range(zs - 1):
        zz = zord[zi]
        complete(zi)
        right = zz > z
        from_left = jnp.logical_and(right, z > 0)
        from_right = jnp.logical_and(jnp.logical_not(right), z < zs - 1)
        got(ral.at[zz], szr.at[zz], rzr.at[zz], (f, c), from_left)
        got(rar.at[zz], szl.at[zz], rzl.at[zz], (f, c), from_right)

        @pl.when(from_left)
        def _():
            add_into(t.at[base + zz], ral.at[zz])

        @pl.when(from_right)
        def _():
            add_into(t.at[base + zz], rar.at[zz])

        w.send(t.at[base + zz], ral.at[zz], szr.at[zz], rzr.at[zz], (f, c + 2), right)
        w.send(t.at[base + zz], rar.at[zz], szl.at[zz], rzl.at[zz], (f, c - 2), jnp.logical_not(right))
    complete(zs - 1)
    got(ral.at[z], szr.at[z], rzr.at[z], (f, c), z > 0)
    got(rar.at[z], szl.at[z], rzl.at[z], (f, c), z < zs - 1)

    @pl.when(z > 0)
    def _():
        add_into(t.at[base + z], ral.at[z])

    @pl.when(z < zs - 1)
    def _():
        add_into(t.at[base + z], rar.at[z])

    w.send(t.at[base + z, 1 - k], fin, sf.at[0], sf.at[1], sib)
    o_ref[:, pl.ds(pl.multiple_of(k * half, 128), half)] = t[base + z, k]
    got(fin, sf.at[0], sf.at[1], sib)
    o_ref[:, pl.ds(pl.multiple_of((1 - k) * half, 128), half)] = fin[...]
    w.drain()


def scatter(x, zs, planes, cid, nf=4):
    n, rows, width = x.shape
    D = pltpu.SemaphoreType.DMA
    half = width // 2
    nc = (nf if planes else 1) * zs
    V = lambda m: pltpu.VMEM((m, 2, rows, half), x.dtype)
    return pl.pallas_call(
        functools.partial(rs_kernel, zs, planes),
        out_shape=jax.ShapeDtypeStruct((rows, width), x.dtype),
        in_specs=[ANY],
        out_specs=VM,
        scratch_shapes=[V(nc), V(nc), V(2 * zs), V(zs), V(zs), V(zs), pltpu.VMEM((rows, half), x.dtype),
            D((nc,)), D((nc,)), D((nc,)), D((2 * zs,)), D((2 * zs,)), D((zs,)), D((zs,)), D((zs,)), D((zs,)), D((zs,)), D((zs,)), D((2,))],
        compiler_params=pltpu.CompilerParams(collective_id=cid, has_side_effects=True, vmem_limit_bytes=60 * 2**20),
        name="scatter_all" if planes else "scatter_seq",
    )(x)


def greet_cross(f, c, nf, nc):
    bar = pltpu.get_barrier_semaphore()
    for i in range(1, nc):
        pl.semaphore_signal(bar, inc=1, device_id=(f, (c + i) % nc), device_id_type=MESH)
    for i in range(1, nf):
        pl.semaphore_signal(bar, inc=1, device_id=((f + i) % nf, c), device_id_type=MESH)
    pl.semaphore_wait(bar, nc + nf - 2)


def tile_steps(w, nf, nc, src, dst, hub, ssem, rsem, sp, rp):
    f, c, z, k = place_of()

    def go(i, _):
        j = (c + i) % nc
        pltpu.make_async_remote_copy(
            src_ref=src.at[j], dst_ref=hub.at[c], send_sem=ssem, recv_sem=rsem, device_id=(f, j), device_id_type=MESH
        ).start()
        return 0

    lax.fori_loop(1, nc, go, 0)
    hub[c] = src[c]
    yield
    every = pltpu.make_async_remote_copy(
        src_ref=src.at[pl.ds(0, nc - 1)], dst_ref=hub.at[pl.ds(0, nc - 1)], send_sem=ssem, recv_sem=rsem,
        device_id=(f, c), device_id_type=MESH,
    )
    every.wait_send()
    every.wait_recv()
    mine = pl.ds(f * nc, nc)
    for i in range(1, nf):
        ff = (f + i) % nf
        w.send(hub.at[:, ff], dst.at[mine], sp.at[i], rp.at[i], (ff, c))
    dst[mine] = hub[:, f]
    yield
    for i in range(1, nf):
        ff = (f + nf - i) % nf
        got(dst.at[pl.ds(ff * nc, nc)], sp.at[i], rp.at[i], (f, c))
    yield


def tile_bufs(nf, nc, tile):
    D = pltpu.SemaphoreType.DMA
    return [pltpu.VMEM((nc, nf) + tile, jnp.float32), D(()), D(()), D((nf,)), D((nf,))]


def gather_steps(w, zs, planes, late, x_ref, o_ref, loc, sl, szr, szl, rz, sp1, rp1, sp2, rp2, ssib, rsib):
    f, c, z, k = place_of()
    half = x_ref.shape[1] // 2
    sib = (f, c + 1 - 2 * k)
    b1 = 1 + k
    b2 = 2 - k
    f1 = flip(f, b1)
    f2 = flip(f, b2)
    cols = [f, f1, f2, flip(f1, b2)] if planes else [0]
    cs = 2 * zs

    def chunk(col, zz, kk):
        at = (cols[col] * cs if planes else 0) + 2 * zz
        return o_ref.at[pl.ds(at, 2), :, pl.ds(pl.multiple_of(kk * half, 128), half)]

    mine = (f * cs if planes else 0) + c
    theirs = (f * cs if planes else 0) + c + 1 - 2 * k
    own = pltpu.make_async_copy(x_ref, o_ref.at[mine], loc)
    own.start()
    w.send(x_ref, o_ref.at[mine], sl.at[0], sl.at[1], sib)
    yield
    own.wait()
    got(o_ref.at[theirs], sl.at[0], sl.at[1], sib)

    def spread(zz, when):
        if planes:
            w.send(chunk(0, zz, k), chunk(0, zz, k), sp1.at[zz], rp1.at[zz], (f1, c), when)
            w.send(chunk(0, zz, k), chunk(0, zz, k), sp2.at[zz], rp2.at[zz], (f2, c), when)

    def relay(zz, when):
        if planes:
            got(chunk(1, zz, k), sp1.at[zz], rp1.at[zz], (f1, c), when)
            w.send(chunk(1, zz, k), chunk(1, zz, k), sp2.at[zs + zz], rp2.at[zs + zz], (f2, c), when)
            w.send(chunk(1, zz, k), chunk(1, zz, k), ssib.at[zs + zz], rsib.at[zs + zz], sib, when)

    if late:
        spread(z, None)
        yield
    w.send(chunk(0, z, k), chunk(0, z, k), szr.at[z], rz.at[z], (f, c + 2), z < zs - 1)
    w.send(chunk(0, z, k), chunk(0, z, k), szl.at[z], rz.at[z], (f, c - 2), z > 0)
    if not late:
        spread(z, None)
    yield
    if late:
        relay(z, None)
        yield
    order = []
    for h in range(1, zs):
        for zz, when, on, dz, sem in (
            (z - h, z - h >= 0, z < zs - 1, 2, szr),
            (z + h, z + h < zs, z > 0, -2, szl),
        ):
            got(chunk(0, zz, k), sem.at[zz], rz.at[zz], (f, c), when)
            w.send(chunk(0, zz, k), chunk(0, zz, k), sem.at[zz], rz.at[zz], (f, c + dz), jnp.logical_and(when, on))
            spread(zz, when)
            w.send(chunk(0, zz, k), chunk(0, zz, k), ssib.at[zz], rsib.at[zz], sib, when)
            order.append((zz, when))
        yield
        if h == 1 and not late:
            relay(z, None)
            yield
    for zz, when in order:
        relay(zz, when)
        yield
    if planes:
        for col, base in ((2, 0), (3, zs)):
            for zz, when in [(z, None)] + order:
                got(chunk(col, zz, k), sp2.at[base + zz], rp2.at[base + zz], (f2, c), when)
                w.send(chunk(col, zz, k), chunk(col, zz, k), ssib.at[col * zs + zz], rsib.at[col * zs + zz], sib, when)
            yield
        for mycol, theircol in ((0, 0), (1, 2), (2, 1), (3, 3)):
            for zz, when in ([(z, None)] if mycol else []) + order:
                got(chunk(mycol, zz, 1 - k), ssib.at[theircol * zs + zz], rsib.at[theircol * zs + zz], sib, when)
    else:
        for zz, when in order:
            got(chunk(0, zz, 1 - k), ssib.at[zz], rsib.at[zz], sib, when)
    yield


def gather_sems(zs):
    D = pltpu.SemaphoreType.DMA
    return [D(()), D((2,)), D((zs,)), D((zs,)), D((zs,)), D((zs,)), D((zs,)), D((2 * zs,)), D((2 * zs,)), D((4 * zs,)), D((4 * zs,))]


def advance(steps, name="step"):
    with jax.named_scope(name):
        return next(steps, steps) is not steps


def head_rows_steps(w, nf, nc, hp, wo_ref, wo_all, hub, loc, so, ro):
    f, c, z, k = place_of()
    fx, fy = flip(f, 1), flip(f, 2)
    fd = flip(fx, 2)
    hr = wo_ref.shape[0] // 2
    halves = []
    for p in (0, 1):
        j = c % hp
        m = f
        if p:
            j, m = flip(j, 2), flip(f, 2)
        halves.append((p, pl.ds(p * hr, hr), j, f == j, m))
    keeps = []
    for p, at, j, is_hub, m in halves:
        w.send(wo_ref.at[at], hub.at[f, at], so.at[p, 0], ro.at[p, f], (j, c), jnp.logical_not(is_hub))
        keep = pltpu.make_async_copy(wo_ref.at[at], hub.at[f, at], loc.at[p])
        pl.when(is_hub)(keep.start)
        keeps.append(keep)
    yield
    stays = []
    for p, at, j, is_hub, m in halves:
        for ff in range(nf):
            got(hub.at[ff, at], so.at[p, 0], ro.at[p, ff], (f, c), jnp.logical_and(is_hub, ff != f))
            pl.when(jnp.logical_and(is_hub, ff == f))(keeps[p].wait)
            dc = (ff * nc + c) // hp
            w.send(hub.at[ff, at], wo_all.at[m, at], so.at[p, 1 + ff], ro.at[p, nf], (f, dc), jnp.logical_and(is_hub, dc != c))
            stay = pltpu.make_async_copy(hub.at[ff, at], wo_all.at[m, at], loc.at[2 + p])
            pl.when(jnp.logical_and(is_hub, dc == c))(stay.start)
        stays.append(stay)
    yield
    for p, at, j, is_hub, m in halves:
        here = (hp * c + m) % nc == c
        got(wo_all.at[m, at], so.at[p, 1], ro.at[p, nf], (f, c), jnp.logical_not(here))
        pl.when(here)(stays[p].wait)
        w.send(wo_all.at[m, at], wo_all.at[m, at], so.at[p, nf + 1], ro.at[p, nf + 1], (fx, c))
        w.send(wo_all.at[m, at], wo_all.at[m, at], so.at[p, nf + 2], ro.at[p, nf + 2], (fy, c))
    yield
    for p, at, j, is_hub, m in halves:
        mx, my = flip(m, 1), flip(m, 2)
        got(wo_all.at[mx, at], so.at[p, nf + 1], ro.at[p, nf + 1], (fx, c))
        got(wo_all.at[my, at], so.at[p, nf + 2], ro.at[p, nf + 2], (fy, c))
        if p == 0:
            w.send(wo_all.at[mx, at], wo_all.at[mx, at], so.at[p, nf + 3], ro.at[p, nf + 3], (fy, c))
        else:
            w.send(wo_all.at[my, at], wo_all.at[my, at], so.at[p, nf + 3], ro.at[p, nf + 3], (fx, c))
    yield
    for p, at, j, is_hub, m in halves:
        got(wo_all.at[flip(flip(m, 1), 2), at], so.at[p, nf + 3], ro.at[p, nf + 3], (f, c))
    yield


def far_first(z, zs):
    last = zs - 1
    low = z < zs // 2
    order = []
    for i in range(zs - 1):
        far_low = jnp.where(i < zs - 1 - z, last - i, zs - 2 - i)
        far_high = jnp.where(i < z, i, i + 1)
        order.append(jnp.where(low, far_low, far_high))
    return order + [z]


def line_sum_steps(w, zs, make, o_ref, t, u, r0, ral, rar, fin, s0, q0, szr, szl, rzr, rzl, sf):
    f, c, z, k = place_of()
    half = o_ref.shape[1] // 2
    sib = (f, c + 1 - 2 * k)
    order = far_first(z, zs)

    def first(zz):
        make(zz)
        w.send(u.at[zz], r0.at[zz], s0.at[zz], q0.at[zz], sib)

    def complete(zz):
        got(r0.at[zz], s0.at[zz], q0.at[zz], sib)
        add_into(t.at[zz], r0.at[zz])

    def onward(zz):
        right = zz > z
        from_left = jnp.logical_and(right, z > 0)
        from_right = jnp.logical_and(jnp.logical_not(right), z < zs - 1)
        got(ral.at[zz], szr.at[zz], rzr.at[zz], (f, c), from_left)
        got(rar.at[zz], szl.at[zz], rzl.at[zz], (f, c), from_right)

        @pl.when(from_left)
        def _():
            add_into(t.at[zz], ral.at[zz])

        @pl.when(from_right)
        def _():
            add_into(t.at[zz], rar.at[zz])

        w.send(t.at[zz], ral.at[zz], szr.at[zz], rzr.at[zz], (f, c + 2), right)
        w.send(t.at[zz], rar.at[zz], szl.at[zz], rzl.at[zz], (f, c - 2), jnp.logical_not(right))

    first(order[0])
    yield
    for zi in range(zs - 1):
        first(order[zi + 1])
        complete(order[zi])
        yield
        onward(order[zi])
        yield
    complete(z)
    got(ral.at[z], szr.at[z], rzr.at[z], (f, c), z > 0)

    @pl.when(z > 0)
    def _():
        add_into(t.at[z], ral.at[z])

    yield
    got(rar.at[z], szl.at[z], rzl.at[z], (f, c), z < zs - 1)

    @pl.when(z < zs - 1)
    def _():
        add_into(t.at[z], rar.at[z])

    w.send(t.at[z, 1 - k], fin, sf.at[0], sf.at[1], sib)
    o_ref[:, pl.ds(pl.multiple_of(k * half, 128), half)] = t[z, k]
    yield
    got(fin, sf.at[0], sf.at[1], sib)
    o_ref[:, pl.ds(pl.multiple_of((1 - k) * half, 128), half)] = fin[...]
    yield


def line_sum_bufs(zs, rows, half, dtype):
    D = pltpu.SemaphoreType.DMA
    V = pltpu.VMEM((zs, 2, rows, half), dtype)
    return [V, V, V, V, V, pltpu.VMEM((rows, half), dtype)] + [D((zs,))] * 6 + [D((2,))]


def attn_kernel(nf, zs, hp, scale, refs):
    (x_ref, wp_ref, tl_ref, wo_ref, tb_ref, cos_ref, sin_ref, pr_ref, pc_ref,
     o_ref, nm_ref, w_ref, to_ref, wo_all, top_all, qp_ref, kp_ref, qr_ref, kr_ref, v_ref, ctx_ref, lse_ref, hid_ref, tok_all,
     gain, gain_mid, mid, out_ref, loc, wloc, sl, szr, szl, rz, ssib, rsib, sw, rw, swx, swy) = refs[:40]
    tile_b = refs[40:45]
    head_bufs = refs[45:49]
    top_sems = refs[49:60]
    tok_sems = refs[60:71]
    sum_bufs = refs[71:]
    f, c, z, k = place_of()
    nc = 2 * zs
    rows, width = x_ref.shape
    half = width // 2
    hd = kr_ref.shape[1]
    qw = hp * hd
    f32, bf16 = jnp.float32, jnp.bfloat16
    sib_c = c + 1 - 2 * k
    sib = (f, sib_c)
    fx, fy = flip(f, 1), flip(f, 2)
    fr = [f, fx, fy, flip(fx, 2)]

    def chunk(zz, kk):
        return o_ref.at[pl.ds(2 * zz, 2), :, pl.ds(pl.multiple_of(kk * half, 128), half)]

    def piece(rel, cc):
        return w_ref.at[fr[rel] * nc + cc]

    own = pltpu.make_async_copy(x_ref, o_ref.at[c], loc)
    own.start()
    wown = pltpu.make_async_copy(wp_ref.at[c], piece(0, c), wloc)
    wown.start()
    with jax.named_scope("greet"):
        greet_cross(f, c, nf, nc)
    w = Wire()
    head_steps = head_rows_steps(w, nf, nc, hp, wo_ref, wo_all, *head_bufs)
    top_steps = gather_steps(w, zs, True, True, tb_ref, top_all, *top_sems)
    small_steps = tile_steps(w, nf, nc, tl_ref, to_ref, *tile_b)
    advance(small_steps, "tiles")
    w.send(x_ref, o_ref.at[c], sl.at[0], sl.at[1], sib)
    w.send(wp_ref.at[sib_c], piece(0, c), sw.at[sib_c], rw.at[c], sib)
    for h in range(1, zs):
        for zz, when in ((z - h, z - h >= 0), (z + h, z + h < zs)):
            for kk in (0, 1):
                cc = 2 * zz + kk
                w.send(wp_ref.at[cc], piece(0, c), sw.at[cc], rw.at[c], (f, cc), when)
    own.wait()
    got(o_ref.at[sib_c], sl.at[0], sl.at[1], sib)
    on_line = [
        w.send(chunk(z, k), chunk(z, k), szr.at[z], rz.at[z], (f, c + 2), z < zs - 1),
        w.send(chunk(z, k), chunk(z, k), szl.at[z], rz.at[z], (f, c - 2), z > 0),
    ]
    advance(head_steps, "heads")
    advance(small_steps, "tiles")

    def plane(cc, when):
        w.send(piece(0, cc), piece(0, cc), swx.at[cc], rw.at[nc + cc], (fx, c), when)
        w.send(piece(0, cc), piece(0, cc), swy.at[cc], rw.at[2 * nc + cc], (fy, c), when)

    def onward(cc, kk, when):
        if kk == 0:
            got(piece(1, cc), swx.at[cc], rw.at[nc + cc], (fx, c), when)
            w.send(piece(1, cc), piece(1, cc), swy.at[nc + cc], rw.at[3 * nc + cc], (fy, c), when)
        else:
            got(piece(2, cc), swy.at[cc], rw.at[2 * nc + cc], (fy, c), when)
            w.send(piece(2, cc), piece(2, cc), swx.at[nc + cc], rw.at[3 * nc + cc], (fx, c), when)

    def norm(zz):
        nb = 32

        def block(i, _):
            j = i // (rows // nb)
            at = pl.ds(pl.multiple_of(i % (rows // nb) * nb, nb), nb)
            v = o_ref[2 * zz + j, at, :].astype(f32)
            inv = lax.rsqrt(jnp.mean(v * v, axis=-1, keepdims=True) + EPSILON)
            to = pl.ds(pl.multiple_of(2 * zz * rows + i * nb, nb), nb)
            nm_ref[to, :] = (v * inv * gain[...]).astype(bf16)
            return 0

        with jax.named_scope("norm"):
            lax.fori_loop(0, 2 * rows // nb, block, 0)

    sides = [
        (
            (z - h, z - h >= 0, z < zs - 1, 2, szr),
            (z + h, z + h < zs, z > 0, -2, szl),
        )
        for h in range(1, zs)
    ]
    far = [(zz, when) for pair in sides for zz, when, *_ in pair]
    wown.wait()
    plane(c, None)
    got(piece(0, sib_c), sw.at[sib_c], rw.at[sib_c], sib)
    plane(sib_c, None)
    for zz, when in far:
        for kk in (0, 1):
            cc = 2 * zz + kk
            with jax.named_scope("w1"):
                got(piece(0, cc), sw.at[cc], rw.at[cc], (f, cc), when)
            plane(cc, when)
    advance(small_steps, "tiles")
    advance(head_steps, "heads")
    for i in range(width // 128):
        gain[:, pl.ds(128 * i, 128)] = to_ref[2 * i, 1:2, :] + to_ref[2 * i + 1, 1:2, :]
        gain_mid[:, pl.ds(128 * i, 128)] = to_ref[2 * i, 4:5, :] + to_ref[2 * i + 1, 4:5, :]
    norm(z)
    with jax.named_scope("w2"):
        for zz, when in [(z, None)] + far[:2]:
            for kk in (0, 1):
                onward(2 * zz + kk, kk, when)
    waiting = []
    for h, pair in enumerate(sides):
        for zz, when, on, dz, sem in pair:
            with jax.named_scope("x"):
                got(chunk(zz, k), sem.at[zz], rz.at[zz], (f, c), when)
            on_line.append(w.send(chunk(zz, k), chunk(zz, k), sem.at[zz], rz.at[zz], (f, c + dz), jnp.logical_and(when, on)))
            w.send(chunk(zz, k), chunk(zz, k), ssib.at[zz], rsib.at[zz], sib, when)
        if h == 0:
            advance(head_steps, "heads")
            with jax.named_scope("w2"):
                for zz, when in far[2:]:
                    for kk in (0, 1):
                        onward(2 * zz + kk, kk, when)
        if h == zs - 3:
            advance(head_steps, "heads")
            advance(top_steps, "top")
        if h == zs - 2:
            with jax.named_scope("line"):
                w.settle(on_line)
            advance(top_steps, "top")
            advance(top_steps, "top")
        for zz, when in waiting:
            got(chunk(zz, 1 - k), ssib.at[zz], rsib.at[zz], sib, when)
            pl.when(when)(functools.partial(norm, zz))
        waiting = [(zz, when) for zz, when, *_ in pair]
    for zz, when in waiting:
        got(chunk(zz, 1 - k), ssib.at[zz], rsib.at[zz], sib, when)
        pl.when(when)(functools.partial(norm, zz))
    with jax.named_scope("wait_w"):
        for zz, when in [(z, None)] + far:
            e, o = 2 * zz, 2 * zz + 1
            got(piece(2, e), swy.at[e], rw.at[2 * nc + e], (fy, c), when)
            got(piece(1, o), swx.at[o], rw.at[nc + o], (fx, c), when)
            got(piece(3, e), swy.at[nc + e], rw.at[3 * nc + e], (fy, c), when)
            got(piece(3, o), swx.at[nc + o], rw.at[3 * nc + o], (fx, c), when)

    gq = jnp.sum(to_ref[:, 2, :], axis=0, keepdims=True)
    gk = jnp.sum(to_ref[:, 3, :], axis=0, keepdims=True)
    qb = 2 * rows
    span = nc * rows
    low_half = lax.broadcasted_iota(jnp.int32, (1, hd), 1) < hd // 2

    def turned(t, g, at):
        t = t * lax.rsqrt(jnp.mean(t * t, axis=-1, keepdims=True) + EPSILON) * g
        other = pltpu.roll(t, hd // 2, 1)
        return (t * cos_ref[at, :] + jnp.where(low_half, -other, other) * sin_ref[at, :]).astype(bf16)

    def project(i, _):
        at = pl.ds(pl.multiple_of(i * qb, qb), qb)
        a = nm_ref[at, :]
        for nb in range((qw + 2 * hd) // (2 * hd)):
            wide = pl.ds(nb * 2 * hd, 2 * hd)
            pre = jnp.dot(a, w_ref[:, :, wide].reshape(width, 2 * hd), preferred_element_type=f32)
            for s in (0, 1):
                part = pre[:, s * hd : (s + 1) * hd]
                h = 2 * nb + s
                if h < hp:
                    qp_ref[at, pl.ds(h * hd, hd)] = part
                    qr_ref[at, pl.ds(h * hd, hd)] = turned(part, gq, at)
                elif h == hp:
                    kp_ref[at, :] = part
                    kr_ref[at, :] = turned(part, gk, at)
                else:
                    v_ref[at, :] = part.astype(bf16)
        return 0

    for i in range(span // qb):
        with jax.named_scope("project"):
            project(i, 0)

    lane = lax.broadcasted_iota(jnp.int32, (1, hd), 1)

    def attend(i, h):
        at = pl.ds(pl.multiple_of(i * qb, qb), qb)
        hc = pl.ds(pl.multiple_of(h * hd, hd), hd)
        s = lax.dot_general(qr_ref[at, hc], kr_ref[...], (((1,), (1,)), ((), ())), preferred_element_type=f32) * scale
        s = jnp.where(pc_ref[...] <= pr_ref[at, :], s, -jnp.inf)
        top = jnp.max(s, axis=-1, keepdims=True)
        e = jnp.exp(s - top)
        total = jnp.sum(e, axis=-1, keepdims=True)
        p = (e * (1.0 / total)).astype(bf16)
        ctx_ref[at, hc] = jnp.dot(p, v_ref[...], preferred_element_type=f32).astype(bf16)
        lse_ref[at, :] = jnp.where(lane == h, top + jnp.log(total), lse_ref[at, :])

    lse_ref[...] = jnp.zeros_like(lse_ref)

    while advance(head_steps, "heads"):
        pass

    t, u = sum_bufs[0], sum_bufs[1]

    def make(zz):
        def heads(h, _):
            attend(zz, h)
            return 0

        with jax.named_scope("attend"):
            lax.fori_loop(0, hp, heads, 0)
        at = pl.ds(pl.multiple_of(2 * zz * rows, rows), 2 * rows)
        a = ctx_ref[at, :]
        for dst, kk in ((u, 1 - k), (t, k)):
            def block(j, _, dst=dst, kk=kk):
                cols = pl.ds(pl.multiple_of(kk * half + j * 512, 128), 512)
                o = jnp.dot(a, wo_all[:, :, cols].reshape(qw, 512), preferred_element_type=f32).astype(bf16)
                dst[zz, :, :, pl.ds(pl.multiple_of(j * 512, 512), 512)] = o.reshape(2, rows, 512)
                return 0

            lax.fori_loop(0, half // 512, block, 0)

    sum_steps = line_sum_steps(w, zs, make, out_ref, *sum_bufs)
    for turn in "sstsstssssst":
        if turn == "s":
            advance(sum_steps, "sum")
        else:
            advance(top_steps, "top")
    while advance(sum_steps, "sum"):
        pass

    def middle(i, _):
        at = pl.ds(pl.multiple_of(i * 32, 32), 32)
        v = x_ref[at, :].astype(f32) + out_ref[at, :].astype(f32)
        hid_ref[at, :] = v
        inv = lax.rsqrt(jnp.mean(v * v, axis=-1, keepdims=True) + EPSILON)
        mid[at, :] = (v * inv * gain_mid[...]).astype(bf16)
        return 0

    with jax.named_scope("middle"):
        lax.fori_loop(0, rows // 32, middle, 0)
    tok_steps = gather_steps(w, zs, True, False, mid, tok_all, *tok_sems)
    advance(tok_steps, "tok")
    advance(tok_steps, "tok")
    busy = True
    while busy:
        busy = advance(top_steps, "top")
        busy = advance(tok_steps, "tok") or busy
    w.drain()


def attention(x, wp, tl, wo, tb, cosine, sine, pos, nf, zs, hp, scale, cid):
    rows, width = x.shape
    nc = 2 * zs
    span = nc * rows
    hd = cosine.shape[1]
    bf16, f32 = jnp.bfloat16, jnp.float32
    D = pltpu.SemaphoreType.DMA
    S = jax.ShapeDtypeStruct
    outs = [
        (S((nc, rows, width), bf16), VM),
        (S((span, width), bf16), VM),
        (S((nf * nc,) + wp.shape[1:], bf16), VM),
        (S((nf * nc,) + tl.shape[2:], f32), VM),
        (S((hp,) + wo.shape, bf16), VM),
        (S((nf * nc, rows, width), bf16), ANY),
        (S((span, hp * hd), f32), VM),
        (S((span, hd), f32), VM),
        (S((span, hp * hd), bf16), VM),
        (S((span, hd), bf16), VM),
        (S((span, hd), bf16), VM),
        (S((span, hp * hd), bf16), VM),
        (S((span, hd), f32), VM),
        (S((rows, width), f32), VM),
        (S((nf * nc, rows, width), bf16), ANY),
    ]
    R = pltpu.VMEM((rows, width), bf16)
    scratch = [pltpu.VMEM((1, width), f32), pltpu.VMEM((1, width), f32), R, R, D(()), D(()), D((2,)), D((zs,)), D((zs,)), D((zs,)), D((zs,)), D((zs,)),
               D((nc,)), D((4 * nc,)), D((2 * nc,)), D((2 * nc,))]
    scratch += tile_bufs(nf, nc, tl.shape[2:])
    scratch += [pltpu.VMEM((nf,) + wo.shape, bf16), D((4,)), D((2, nf + 4)), D((2, nf + 4))] + gather_sems(zs) + gather_sems(zs) + line_sum_bufs(zs, rows, width // 2, bf16)
    return pl.pallas_call(
        lambda *refs: attn_kernel(nf, zs, hp, scale, refs),
        out_shape=[s for s, _ in outs],
        in_specs=[VM] * 9,
        out_specs=[b for _, b in outs],
        scratch_shapes=scratch,
        compiler_params=pltpu.CompilerParams(collective_id=cid, has_side_effects=True, vmem_limit_bytes=60 * 2**20),
        name="attention",
    )(x, wp, tl, wo, tb, cosine, sine, pos[:, None], pos[None, :])


def sum_block(dst, srcs, rows=32):
    n, r, wd = dst.shape

    def step(i, _):
        a = pl.ds(pl.multiple_of(i % (r // rows) * rows, rows), rows)
        j = i // (r // rows)
        total = srcs[0][j, a, :].astype(jnp.float32)
        for s in srcs[1:]:
            total = total + s[j, a, :].astype(jnp.float32)
        dst[j, a, :] = total.astype(dst.dtype)
        return 0

    lax.fori_loop(0, n * (r // rows), step, 0)


def spill_sum_steps(w, zs, x_ref, o_ref, r0, r1, r2, ral, rar, stage, out, fin, ls, s0, q0, s1, q1, s2, q2, szr, szl, rzr, rzl, sf):
    f, c, z, k = place_of()
    half = o_ref.shape[1] // 2
    sib = (f, c + 1 - 2 * k)
    b1 = 2 - k
    b2 = 1 + k
    f1 = flip(f, b1)
    f2 = flip(f, b2)
    f3 = flip(f1, b2)
    cs = 2 * zs
    cols = [f3, f1, f2, f]
    order = far_first(z, zs)
    held = [None] * out.shape[0]
    count = [0]

    def src(col, zz, kk):
        return x_ref.at[pl.ds(col * cs + 2 * zz, 2), :, pl.ds(pl.multiple_of(kk * half, 128), half)]

    for ci in range(4):
        for zz in order:
            slot = {0: 0, 1: 2, 2: 1, 3: 3}[ci] * zs + zz
            w.send(src(cols[ci], zz, 1 - k), r0.at[slot], s0.at[slot], q0.at[slot], sib)
    yield

    def load(i, ref, when=None):
        copy = pltpu.make_async_copy(ref, stage.at[i], ls.at[i])
        if when is None:
            copy.start()
        else:
            pl.when(when)(copy.start)
        return copy

    def slot_for():
        i = count[0] % len(held)
        count[0] += 1
        if held[i] is not None:
            w.settle(held[i])
        return i

    def base(ci, zz):
        got(r0.at[ci * zs + zz], s0.at[ci * zs + zz], q0.at[ci * zs + zz], sib)
        loads = [load(0, src(cols[ci], zz, k)), load(1, r0.at[ci * zs + zz])]
        if ci >= 2:
            m = (ci - 2) * zs + zz
            got(r1.at[m], s1.at[m], q1.at[m], (f1, c))
            loads.append(load(2, r1.at[m]))
        if ci == 3:
            got(r2.at[zz], s2.at[zz], q2.at[zz], (f2, c))
            loads.append(load(3, r2.at[zz]))
        return loads

    def total(loads):
        i = slot_for()
        for copy in loads:
            copy.wait()
        sum_block(out.at[i], [stage.at[j] for j in range(len(loads))])
        return i

    for ci in (0, 1, 2):
        for zz in order:
            loads = base(ci, zz)
            yield
            i = total(loads)
            if ci < 2:
                m = ci * zs + zz
                held[i] = [w.send(out.at[i], r1.at[m], s1.at[m], q1.at[m], (f1, c))]
            else:
                held[i] = [w.send(out.at[i], r2.at[zz], s2.at[zz], q2.at[zz], (f2, c))]
            yield
    for zz in order[:-1]:
        loads = base(3, zz)
        right = zz > z
        from_left = jnp.logical_and(right, z > 0)
        from_right = jnp.logical_and(jnp.logical_not(right), z < zs - 1)
        got(ral.at[zz], szr.at[zz], rzr.at[zz], (f, c), from_left)
        got(rar.at[zz], szl.at[zz], rzl.at[zz], (f, c), from_right)
        more = [load(4, ral.at[zz], from_left), load(4, rar.at[zz], from_right)]
        yield
        i = total(loads)
        for copy, when in zip(more, (from_left, from_right)):
            pl.when(when)(copy.wait)

            @pl.when(when)
            def _(i=i):
                add_into(out.at[i], stage.at[4])

        held[i] = [
            w.send(out.at[i], ral.at[zz], szr.at[zz], rzr.at[zz], (f, c + 2), right),
            w.send(out.at[i], rar.at[zz], szl.at[zz], rzl.at[zz], (f, c - 2), jnp.logical_not(right)),
        ]
        yield
    loads = base(3, z)
    got(ral.at[z], szr.at[z], rzr.at[z], (f, c), z > 0)
    more = load(4, ral.at[z], z > 0)
    yield
    i = total(loads)
    pl.when(z > 0)(more.wait)

    @pl.when(z > 0)
    def _():
        add_into(out.at[i], stage.at[4])

    got(rar.at[z], szl.at[z], rzl.at[z], (f, c), z < zs - 1)
    more = load(4, rar.at[z], z < zs - 1)
    pl.when(z < zs - 1)(more.wait)

    @pl.when(z < zs - 1)
    def _():
        add_into(out.at[i], stage.at[4])

    w.send(out.at[i, 1 - k], fin, sf.at[0], sf.at[1], sib)
    o_ref[:, pl.ds(pl.multiple_of(k * half, 128), half)] = out[i, k]
    yield
    got(fin, sf.at[0], sf.at[1], sib)
    o_ref[:, pl.ds(pl.multiple_of((1 - k) * half, 128), half)] = fin[...]
    yield


def head_sum_steps(w, nf, nc, hp, g, o_ref, ga, gb, loc, sg, rg, so, ro):
    f, c, z, k = place_of()
    hr = g.shape[1] // 2
    parts = []
    for p in (0, 1):
        mm = (lambda d: flip(d, 2)) if p else (lambda d: d)
        fa = flip(f, 1 + p)
        fb = flip(f, 2 - p)
        parts.append((p, pl.ds(p * hr, hr), mm, fa, fb, flip(fa, 2 - p)))
    for p, at, mm, fa, fb, fc in parts:
        for i, d in enumerate((fc, fa)):
            w.send(g.at[mm(d), at], ga.at[p, i], sg.at[p, i], rg.at[p, i], (fa, c))
    yield
    for p, at, mm, fa, fb, fc in parts:
        for i, d in enumerate((fb, f)):
            got(ga.at[p, i], sg.at[p, i], rg.at[p, i], (fa, c))
            add_into(g.at[pl.ds(mm(d), 1), at], ga.at[p, pl.ds(i, 1)])
            if i == 0:
                w.send(g.at[mm(fb), at], gb.at[p], sg.at[p, 2], rg.at[p, 2], (fb, c))
    yield
    for p, at, mm, fa, fb, fc in parts:
        got(gb.at[p], sg.at[p, 2], rg.at[p, 2], (fb, c))
        add_into(g.at[pl.ds(mm(f), 1), at], gb.at[pl.ds(p, 1)])
        head = hp * c + mm(f)
        df, dc = head // nc, head % nc
        stay = jnp.logical_and(df == f, dc == c)
        w.send(g.at[mm(f), at], o_ref.at[at], so.at[p], ro.at[p], (df, dc), jnp.logical_not(stay))
        keep = pltpu.make_async_copy(g.at[mm(f), at], o_ref.at[at], loc.at[p])
        pl.when(stay)(keep.start)
        pl.when(stay)(keep.wait)
    yield
    for p, at, mm, fa, fb, fc in parts:
        head = f * nc + c
        here = jnp.logical_and(head // hp == c, mm(head % hp) == f)
        got(o_ref.at[at], so.at[p], ro.at[p], (f, c), jnp.logical_not(here))
    yield


def weight_sum_steps(w, nf, nc, g, o_ref, ga, gb, sg, rg, sa, ra):
    f, c, z, k = place_of()
    hc = nc // 2
    parts = []
    for p in (0, 1):
        fa = flip(f, 1 + p)
        fb = flip(f, 2 - p)
        parts.append((p, pl.ds(p * hc, hc), fa, fb, flip(fa, 2 - p)))
    for p, at, fa, fb, fc in parts:
        for i, col in enumerate((fc, fa)):
            w.send(g.at[col, at], ga.at[p, i], sg.at[2 * p + i], rg.at[2 * p + i], (fa, c))
    yield
    for p, at, fa, fb, fc in parts:
        for i, col in enumerate((fb, f)):
            got(ga.at[p, i], sg.at[2 * p + i], rg.at[2 * p + i], (fa, c))
            add_into(g.at[col, at], ga.at[p, i])
            if i == 0:
                w.send(g.at[fb, at], gb.at[p], sg.at[4 + p], rg.at[4 + p], (fb, c))
    yield
    for p, at, fa, fb, fc in parts:
        got(gb.at[p], sg.at[4 + p], rg.at[4 + p], (fb, c))
        add_into(g.at[f, at], gb.at[p])
    for i in range(1, nc):
        cc = (c + i) % nc
        w.send(g.at[f, cc], o_ref.at[c], sa.at[cc], ra.at[c], (f, cc))
    o_ref[c] = g[f, c]
    yield
    for i in range(1, nc):
        cc = (c + i) % nc
        got(o_ref.at[cc], sa.at[cc], ra.at[cc], (f, c))
    yield


def grad_kernel(nf, zs, hp, scale, refs):
    (res_ref, nm_ref, w_ref, wo_ref, qp_ref, kp_ref, qr_ref, kr_ref, v_ref, ctx_ref, lse_ref, cos_ref, sin_ref, pr_ref, pc_ref,
     gqk_ref, gat_ref, moe_ref, mix_ref,
     out_ref, go_ref, gwo_ref, to_ref, mixed_ref, h0, h1, h2, hl, hr,
     res, gkv, gkv2, gcat, gw, gwo, tl, gqk, gat, loc, sl, szr, szl, rz, ssib, rsib, sk) = refs[:46]
    rest = list(refs[46:])

    def take(n):
        part = rest[:n]
        del rest[:n]
        return part

    tile_b = take(5)
    sum_bufs = take(13)
    spill_bufs = take(15)
    head_b = take(7)
    weight_b = take(6)
    f, c, z, k = place_of()
    nc = 2 * zs
    rows, width = res_ref.shape
    half = width // 2
    hd = kr_ref.shape[1]
    qw = hp * hd
    span = nc * rows
    f32, bf16 = jnp.float32, jnp.bfloat16
    sib_c = c + 1 - 2 * k
    sib = (f, sib_c)
    first = k == 0

    def chunk(zz, kk):
        return res.at[pl.ds(2 * zz, 2), :, pl.ds(pl.multiple_of(kk * half, 128), half)]

    own = pltpu.make_async_copy(res_ref, res.at[c], loc)
    own.start()
    with jax.named_scope("greet"):
        greet_cross(f, c, nf, nc)
    w = Wire()
    w.send(res_ref, res.at[c], sl.at[0], sl.at[1], sib)
    mix_steps = spill_sum_steps(w, zs, mix_ref, mixed_ref, h0, h1, h2, hl, hr, *spill_bufs)
    own.wait()
    got(res.at[sib_c], sl.at[0], sl.at[1], sib)
    w.send(chunk(z, k), chunk(z, k), szr.at[z], rz.at[z], (f, c + 2), z < zs - 1)
    w.send(chunk(z, k), chunk(z, k), szl.at[z], rz.at[z], (f, c - 2), z > 0)
    advance(mix_steps, "mix")
    gkv[...] = jnp.zeros_like(gkv)
    gqk[...] = jnp.zeros_like(gqk)
    gat[...] = jnp.zeros_like(gat)
    gq, gk = gqk_ref[0:1, :], gqk_ref[1:2, :]
    low_half = lax.broadcasted_iota(jnp.int32, (1, hd), 1) < hd // 2
    lane = lax.broadcasted_iota(jnp.int32, (1, hd), 1)

    def turned_back(t, g, grad, at):
        u = grad * sin_ref[at, :]
        other = pltpu.roll(u, hd // 2, 1)
        gy = grad * cos_ref[at, :] + jnp.where(low_half, other, -other)
        r = lax.rsqrt(jnp.mean(t * t, axis=-1, keepdims=True) + EPSILON)
        n = t * r
        gn = gy * g
        back = r * (gn - n * jnp.mean(gn * n, axis=-1, keepdims=True))
        return back, jnp.sum(gy * n, axis=0, keepdims=True)

    def process(zz):
        at = pl.ds(pl.multiple_of(2 * zz * rows, 2 * rows), 2 * rows)
        rr = res[pl.ds(2 * zz, 2)].reshape(2 * rows, width)

        def head(h, _):
            hc = pl.ds(pl.multiple_of(h * hd, hd), hd)
            g = lax.dot_general(rr, wo_ref[h], (((1,), (1,)), ((), ())), preferred_element_type=f32).astype(bf16)
            q = qr_ref[at, hc]
            s = lax.dot_general(q, kr_ref[...], (((1,), (1,)), ((), ())), preferred_element_type=f32) * scale
            lse = jnp.sum(jnp.where(lane == h, lse_ref[at, :], 0.0), axis=-1, keepdims=True)
            p = jnp.where(pc_ref[...] <= pr_ref[at, :], jnp.exp(s - lse), 0.0)
            gkv[1] += lax.dot_general(p.astype(bf16), g, (((0,), (0,)), ((), ())), preferred_element_type=f32)
            gp = lax.dot_general(g, v_ref[...], (((1,), (1,)), ((), ())), preferred_element_type=f32)
            delta = jnp.sum(g.astype(f32) * ctx_ref[at, hc].astype(f32), axis=-1, keepdims=True)
            ds = (p * (gp - delta)).astype(bf16)
            gkv[0] += lax.dot_general(ds, q, (((0,), (0,)), ((), ())), preferred_element_type=f32) * scale
            gr = jnp.dot(ds, kr_ref[...], preferred_element_type=f32) * scale
            back, gain = turned_back(qp_ref[at, hc], gq, gr, at)
            gcat[at, hc] = back.astype(bf16)
            gqk[0:1, :] += gain
            return 0

        with jax.named_scope("process"):
            lax.fori_loop(0, hp, head, 0)

    def mix(count):
        for _ in range(count):
            advance(mix_steps, "mix")

    near = far_first(z, zs)[::-1]
    mix(2 * zs)
    process(near[0])
    for h in range(1, zs):
        sides = (
            (z - h, z - h >= 0, z < zs - 1, 2, szr),
            (z + h, z + h < zs, z > 0, -2, szl),
        )
        with jax.named_scope("hop"):
            for zz, when, on, dz, sem in sides:
                got(chunk(zz, k), sem.at[zz], rz.at[zz], (f, c), when)
                w.send(chunk(zz, k), chunk(zz, k), sem.at[zz], rz.at[zz], (f, c + dz), jnp.logical_and(when, on))
                w.send(chunk(zz, k), chunk(zz, k), ssib.at[zz], rsib.at[zz], sib, when)
        mix(zs - 1)
        with jax.named_scope("rest"):
            for zz, when, *_ in sides:
                got(chunk(zz, 1 - k), ssib.at[zz], rsib.at[zz], sib, when)
        process(near[h])
    w.send(gkv, gkv2, sk.at[0], sk.at[1], sib)
    mix(2)

    with jax.named_scope("gwo"):
        def gwo_block(j, _):
            cols = pl.ds(pl.multiple_of(j * 256, 256), 256)
            r = res[:, :, cols].reshape(span, 256)
            o = lax.dot_general(ctx_ref[...], r, (((0,), (0,)), ((), ())), preferred_element_type=f32).astype(bf16)
            gwo[:, :, cols] = o.reshape(hp, hd, 256)
            return 0

        lax.fori_loop(0, width // 256, gwo_block, 0)
    head_steps = head_sum_steps(w, nf, nc, hp, gwo, gwo_ref, *head_b)
    advance(head_steps, "heads")
    mix(2)
    with jax.named_scope("kv"):
        got(gkv2, sk.at[0], sk.at[1], sib)

        def keys(i, _):
            at = pl.ds(pl.multiple_of(i * 2 * rows, 2 * rows), 2 * rows)
            back, gain = turned_back(kp_ref[at, :], gk, gkv[0, at, :] + gkv2[0, at, :], at)
            gv = gkv[1, at, :] + gkv2[1, at, :]
            gcat[at, pl.ds(qw, hd)] = jnp.where(first, back, gv).astype(bf16)
            gqk[1:2, :] += jnp.where(first, gain, 0.0)
            return 0

        lax.fori_loop(0, zs, keys, 0)
    t, u = sum_bufs[0], sum_bufs[1]

    def make(zz):
        at = pl.ds(pl.multiple_of(2 * zz * rows, 2 * rows), 2 * rows)
        a = gcat[at, 0:qw]
        b = gcat[at, qw : qw + hd]
        for dst, kk in ((u, 1 - k), (t, k)):
            def block(j, _, dst=dst, kk=kk):
                slabs = pl.ds(kk * (half // 64) + j * 8, 8)
                wq = w_ref[slabs, :, 0:qw].reshape(512, qw)
                wk = w_ref[slabs, :, pl.ds(pl.multiple_of(qw + k * hd, hd), hd)].reshape(512, hd)
                o = lax.dot_general(a, wq, (((1,), (1,)), ((), ())), preferred_element_type=f32)
                o = o + lax.dot_general(b, wk, (((1,), (1,)), ((), ())), preferred_element_type=f32)
                cols = pl.ds(pl.multiple_of(kk * half + j * 512, 512), 512)
                gat[:, cols] += jnp.sum(o * nm_ref[at, cols].astype(f32), axis=0, keepdims=True)
                dst[zz, :, :, pl.ds(pl.multiple_of(j * 512, 512), 512)] = o.astype(bf16).reshape(2, rows, 512)
                return 0

            lax.fori_loop(0, half // 512, block, 0)

    sum_steps = line_sum_steps(w, zs, make, out_ref, *sum_bufs)
    for _ in range(2):
        advance(sum_steps, "sum")
    advance(head_steps, "heads")
    with jax.named_scope("gw"):
        def gw_block(j, _):
            cols = pl.ds(pl.multiple_of(j * 256, 256), 256)
            o = lax.dot_general(nm_ref[:, cols], gcat[...], (((0,), (0,)), ((), ())), preferred_element_type=f32).astype(bf16)
            gw[j // 2, pl.ds(j % 2 * 4, 4)] = o.reshape(4, 64, qw + hd)
            return 0

        lax.fori_loop(0, width // 256, gw_block, 0)
    weight_steps = weight_sum_steps(w, nf, nc, gw, go_ref, *weight_b)
    advance(weight_steps, "weights")
    for turn in "mmmssmmsmmwsmsmwhs":
        if turn == "s":
            advance(sum_steps, "sum")
        elif turn == "w":
            advance(weight_steps, "weights")
        elif turn == "h":
            advance(head_steps, "heads")
        else:
            mix(1)
    for cc in range(nc):
        for ff in range(nf):
            lanes = pl.ds(128 * ((ff * nc + cc) // 2), 128)
            tl[cc, ff, 0:1, :] = gat[:, lanes] / gat_ref[:, lanes]
            tl[cc, ff, 1:2, :] = moe_ref[:, lanes]
            tl[cc, ff, 2:4, :] = gqk[...]
            tl[cc, ff, 4:8, :] = jnp.zeros((4, hd), f32)
    small_steps = tile_steps(w, nf, nc, tl, to_ref, *tile_b)
    advance(small_steps, "tiles")
    for name, steps in (("sum", sum_steps), ("heads", head_steps), ("mix", mix_steps), ("weights", weight_steps), ("tiles", small_steps)):
        while advance(steps, name):
            pass
    w.drain()


def gradients(res, nm, wcat, wo, qp, kp, qr, kr, v, ctx, lse, cosine, sine, pos, gqk, gat, moe, mix, nf, zs, hp, scale, cid):
    rows, width = res.shape
    nc = 2 * zs
    span = nc * rows
    hd = cosine.shape[1]
    bf16, f32 = jnp.bfloat16, jnp.float32
    D = pltpu.SemaphoreType.DMA
    S = jax.ShapeDtypeStruct
    half = width // 2
    cols = hp * hd + hd
    shard = wcat.shape[1]
    spill = lambda n: (S((n, 2, rows, half), bf16), ANY)
    outs = [
        (S((rows, width), bf16), VM),
        (S((nc, shard, cols), bf16), VM),
        (S((hd, width), bf16), VM),
        (S((nf * nc, 8, hd), f32), VM),
        (S((rows, width), bf16), VM),
        spill(4 * zs), spill(2 * zs), spill(zs), spill(zs), spill(zs),
    ]
    V = pltpu.VMEM
    chunk = (2, rows, half)
    scratch = [V((nc, rows, width), bf16), V((2, span, hd), f32), V((2, span, hd), f32), V((span, cols), bf16),
               V((nf, nc, shard, cols), bf16), V((hp, hd, width), bf16), V((nc, nf, 8, hd), f32), V((2, hd), f32), V((1, width), f32),
               D(()), D((2,)), D((zs,)), D((zs,)), D((zs,)), D((zs,)), D((zs,)), D((2,))]
    scratch += tile_bufs(nf, nc, (8, hd)) + line_sum_bufs(zs, rows, half, bf16)
    scratch += [V((5,) + chunk, bf16), V((3,) + chunk, bf16), V((rows, half), bf16), D((5,)), D((4 * zs,)), D((4 * zs,)), D((2 * zs,)), D((2 * zs,)),
                D((zs,)), D((zs,)), D((zs,)), D((zs,)), D((zs,)), D((zs,)), D((2,))]
    scratch += [V((2, 2, hd // 2, width), bf16), V((2, hd // 2, width), bf16), D((2,)), D((2, 3)), D((2, 3)), D((2,)), D((2,))]
    scratch += [V((2, 2, nc // 2, shard, cols), bf16), V((2, nc // 2, shard, cols), bf16), D((6,)), D((6,)), D((nc,)), D((nc,))]
    return pl.pallas_call(
        lambda *refs: grad_kernel(nf, zs, hp, scale, refs),
        out_shape=[s for s, _ in outs],
        in_specs=[VM] * 18 + [ANY],
        out_specs=[b for _, b in outs],
        scratch_shapes=scratch,
        compiler_params=pltpu.CompilerParams(collective_id=cid, has_side_effects=True, vmem_limit_bytes=62 * 2**20),
        name="gradients",
    )(res, nm, wcat, wo, qp, kp, qr, kr, v, ctx, lse, cosine, sine, pos[:, None], pos[None, :], gqk, gat, moe, mix)


def expert_kernel(nf, zs, refs):
    (tok, top, place, mixing, wg, wu, wd,
     out_ref, shares, arr, garr, hid, ggp, gup,
     tb, cb, a, g, rows_b, t, u, r0, r1, r2, ral, rar, fin, sh,
     lt, lc, la, lg, ls, s0, q0, s1, q1, s2, q2, szr, szl, rzr, rzl, sf) = refs
    f, c, z, k = place_of()
    nc = 2 * zs
    rows, width = tb.shape[2:]
    half = width // 2
    cap = place.shape[1]
    per = zs * cap
    f32, bf16 = jnp.float32, jnp.bfloat16
    sib = (f, c + 1 - 2 * k)
    f1 = flip(f, 2 - k)
    f2 = flip(f, 1 + k)
    cols = [flip(flip(f, 1), 2), flip(f, 1), flip(f, 2), f]
    order = far_first(z, zs)
    with jax.named_scope("greet"):
        greet(f, c, z, zs, True)
    w = Wire()

    def fetch(col, s, slot):
        two = pl.ds(col * nc + 2 * s, 2)
        return (
            pltpu.make_async_copy(tok.at[two], tb.at[slot], lt.at[slot]),
            pltpu.make_async_copy(top.at[two], cb.at[slot], lc.at[slot]),
        )

    def compute(li):
        col = cols[li]
        base = pl.multiple_of(col * per, 16)
        for copy in fetch(col, 0, 0):
            copy.start()
        if li:
            for copy in keep:
                copy.wait()

        def pick(s, _):
            slot = s % 2

            @pl.when(s < zs - 1)
            def _():
                for copy in fetch(col, s + 1, 1 - slot):
                    copy.start()

            for copy in fetch(col, s, slot):
                copy.wait()
            at = pl.ds(pl.multiple_of(s * cap, 16), cap)
            a[at, :] = jnp.dot(place[col * zs + s], tb[slot].reshape(2 * rows, width), preferred_element_type=f32).astype(bf16)
            g[at, :] = jnp.dot(mixing[col * zs + s], cb[slot].reshape(2 * rows, width), preferred_element_type=f32).astype(bf16)
            return 0

        with jax.named_scope("pick"):
            lax.fori_loop(0, zs, pick, 0)
        mine = pl.ds(base, per)
        keep[:] = [pltpu.make_async_copy(a, arr.at[mine], la), pltpu.make_async_copy(g, garr.at[mine], lg)]
        for copy in keep:
            copy.start()

        def hidden(j, _):
            cc = pl.ds(pl.multiple_of(j * 256, 256), 256)
            gate = jnp.dot(a[...], wg[:, cc], preferred_element_type=f32)
            up = jnp.dot(a[...], wu[:, cc], preferred_element_type=f32)
            back = lax.dot_general(g[...], wd[cc, :], (((1,), (1,)), ((), ())), preferred_element_type=f32)
            sig = jax.nn.sigmoid(gate)
            act = gate * sig
            hid[mine, cc] = (act * up).astype(bf16)
            ggp[mine, cc] = (back * up * sig * (1.0 + gate * (1.0 - sig))).astype(bf16)
            gup[mine, cc] = (back * act).astype(bf16)
            return 0

        with jax.named_scope("hidden"):
            lax.fori_loop(0, wg.shape[1] // 256, hidden, 0)

        def rows_of(j, _):
            cc = pl.ds(pl.multiple_of(j * 256, 256), 256)
            o = lax.dot_general(ggp[mine, :], wg[cc, :], (((1,), (1,)), ((), ())), preferred_element_type=f32)
            o = o + lax.dot_general(gup[mine, :], wu[cc, :], (((1,), (1,)), ((), ())), preferred_element_type=f32)
            rows_b[:, cc] = o.astype(bf16)
            return 0

        with jax.named_scope("rows"):
            lax.fori_loop(0, width // 256, rows_of, 0)

        def spread(s, _):
            at = pl.ds(pl.multiple_of(s * cap, 16), cap)
            p = place[col * zs + s]
            for dst, kk in ((u.at[li % 2], 1 - k), (t.at[pl.ds(li * zs, zs)], k)):
                r = rows_b[at, pl.ds(pl.multiple_of(kk * half, 128), half)]
                o = lax.dot_general(p, r, (((0,), (0,)), ((), ())), preferred_element_type=f32)
                dst[s] = o.astype(bf16).reshape(2, rows, half)
            return 0

        if li >= 2:
            w.settle(passed[li - 2])
        with jax.named_scope("spread"):
            lax.fori_loop(0, zs, spread, 0)
        passed.append(
            [w.send(u.at[li % 2, zz], r0.at[li * zs + zz], s0.at[li * zs + zz], q0.at[li * zs + zz], sib) for zz in order]
        )

    def pair(li, zz):
        m = li * zs + zz
        got(r0.at[m], s0.at[m], q0.at[m], sib)
        add_into(t.at[m], r0.at[m])

    def second(li, zz, when):
        got(r1.at[zz], s1.at[zz], q1.at[zz], (f1, c), when)

        @pl.when(when)
        def _():
            add_into(t.at[li * zs + zz], r1.at[zz])

        w.send(t.at[li * zs + zz], r2.at[zz], s2.at[zz], q2.at[zz], (f2, c), when)

    keep, passed = [], []
    compute(0)
    for zz in order:
        pair(0, zz)
        w.send(t.at[zz], r1.at[zz], s1.at[zz], q1.at[zz], (f1, c))
    for li in (1, 2):
        compute(li)
        is_first = k == 2 - li
        for zz in order:
            pair(li, zz)
            w.send(t.at[li * zs + zz], r1.at[zs + zz], s1.at[zs + zz], q1.at[zs + zz], (f1, c), is_first)
        for zz in order:
            second(li, zz, jnp.logical_not(is_first))
    compute(3)
    for copy in keep:
        copy.wait()

    def give(i, _):
        at = pl.ds(pl.multiple_of(i * per, 16), per)

        def out_of(j, _):
            cc = pl.ds(pl.multiple_of(j * 256, 256), 256)
            rows_b[:, cc] = jnp.dot(hid[at, :], wd[:, cc], preferred_element_type=f32).astype(bf16)
            return 0

        lax.fori_loop(0, width // 256, out_of, 0)

        def one(s, _):
            slot = s % 2
            there = lambda ss: pltpu.make_async_copy(sh.at[slot], shares.at[pl.ds(i * nc + 2 * ss, 2)], ls.at[slot])

            @pl.when(s > 1)
            def _():
                there(s - 2).wait()

            e = rows_b[pl.ds(pl.multiple_of(s * cap, 16), cap), :]
            o = lax.dot_general(mixing[i * zs + s], e, (((0,), (0,)), ((), ())), preferred_element_type=f32)
            sh[slot] = o.astype(bf16).reshape(2, rows, width)
            there(s).start()
            return 0

        lax.fori_loop(0, zs, one, 0)
        for s in (zs - 2, zs - 1):
            pltpu.make_async_copy(sh.at[s % 2], shares.at[pl.ds(i * nc + 2 * s, 2)], ls.at[s % 2]).wait()
        return 0

    base = 3 * zs

    def complete(zz):
        pair(3, zz)
        got(r1.at[zs + zz], s1.at[zs + zz], q1.at[zs + zz], (f1, c))
        add_into(t.at[base + zz], r1.at[zs + zz])
        got(r2.at[zz], s2.at[zz], q2.at[zz], (f2, c))
        add_into(t.at[base + zz], r2.at[zz])

    for i, zz in enumerate(order[:-1]):
        with jax.named_scope("complete"):
            complete(zz)
        right = zz > z
        from_left = jnp.logical_and(right, z > 0)
        from_right = jnp.logical_and(jnp.logical_not(right), z < zs - 1)
        with jax.named_scope("line"):
            got(ral.at[zz], szr.at[zz], rzr.at[zz], (f, c), from_left)
            got(rar.at[zz], szl.at[zz], rzl.at[zz], (f, c), from_right)

        @pl.when(from_left)
        def _():
            add_into(t.at[base + zz], ral.at[zz])

        @pl.when(from_right)
        def _():
            add_into(t.at[base + zz], rar.at[zz])

        w.send(t.at[base + zz], ral.at[zz], szr.at[zz], rzr.at[zz], (f, c + 2), right)
        w.send(t.at[base + zz], rar.at[zz], szl.at[zz], rzl.at[zz], (f, c - 2), jnp.logical_not(right))
        with jax.named_scope("give"):
            give(i, 0)
    with jax.named_scope("complete"):
        complete(z)
    with jax.named_scope("give"):
        for i in range(zs - 1, nf):
            give(i, 0)
    with jax.named_scope("line"):
        got(ral.at[z], szr.at[z], rzr.at[z], (f, c), z > 0)
        got(rar.at[z], szl.at[z], rzl.at[z], (f, c), z < zs - 1)

    @pl.when(z > 0)
    def _():
        add_into(t.at[base + z], ral.at[z])

    @pl.when(z < zs - 1)
    def _():
        add_into(t.at[base + z], rar.at[z])

    w.send(t.at[base + z, 1 - k], fin, sf.at[0], sf.at[1], sib)
    out_ref[:, pl.ds(pl.multiple_of(k * half, 128), half)] = t[base + z, k]
    got(fin, sf.at[0], sf.at[1], sib)
    out_ref[:, pl.ds(pl.multiple_of((1 - k) * half, 128), half)] = fin[...]
    w.drain()


def experts_of(tokens, top, place, mixing, wg, wu, wd, nf, zs, cid):
    n, rows, width = tokens.shape
    slots = place.shape[0] * place.shape[1]
    per = slots // nf
    ff = wg.shape[1]
    half = width // 2
    bf16 = jnp.bfloat16
    S = jax.ShapeDtypeStruct
    D = pltpu.SemaphoreType.DMA
    V = lambda *s: pltpu.VMEM(s, bf16)
    C = lambda *m: pltpu.VMEM(m + (2, rows, half), bf16)
    outs = [
        (S((rows, width), bf16), VM),
        (S((n, rows, width), bf16), ANY),
        (S((slots, width), bf16), ANY),
        (S((slots, width), bf16), ANY),
        (S((slots, ff), bf16), VM),
        (S((slots, ff), bf16), VM),
        (S((slots, ff), bf16), VM),
    ]
    scratch = [V(2, 2, rows, width), V(2, 2, rows, width), V(per, width), V(per, width), V(per, width),
               C(nf * zs), C(2, zs), C(nf * zs), C(2 * zs), C(zs), C(zs), C(zs), V(rows, half), V(2, 2, rows, width),
               D((2,)), D((2,)), D(()), D(()), D((2,)), D((nf * zs,)), D((nf * zs,)), D((2 * zs,)), D((2 * zs,)), D((zs,)), D((zs,)),
               D((zs,)), D((zs,)), D((zs,)), D((zs,)), D((2,))]
    return pl.pallas_call(
        lambda *refs: expert_kernel(nf, zs, refs),
        out_shape=[s for s, _ in outs],
        in_specs=[ANY, ANY] + [VM] * 5,
        out_specs=[b for _, b in outs],
        scratch_shapes=scratch,
        compiler_params=pltpu.CompilerParams(collective_id=cid, has_side_effects=True, vmem_limit_bytes=62 * 2**20),
        name="experts",
    )(tokens, top, place, mixing, wg, wu, wd)


def head_body(
    nf,
    nc,
    block_input,
    cotangent,
    gain_attn,
    w_query,
    w_key,
    w_value,
    qk_gain,
    w_out,
    gain_moe,
    w_gate,
    w_up,
    w_down,
    expert_ids,
    route_weight,
    pair_order,
):
    bf16, f32 = jnp.bfloat16, jnp.float32
    f, c, z, k = place_of()
    n = nf * nc
    zs = nc // 2
    rows, width = block_input.shape[1:]
    hd = qk_gain.shape[1] * n
    kv_heads = w_key.shape[1] // hd
    heads = w_query.shape[1] // hd
    hp = heads // nc
    shard = w_query.shape[0]
    topk = expert_ids.shape[2]
    capacity = max(2, 3 * BLOCK * topk // n)
    span = nc * rows
    scale = 1.0 / math.sqrt(hd)
    x_own = block_input[0]
    resid = x_own.astype(f32)

    ids, weights = expert_ids[0], route_weight[0].astype(f32)
    named = ids[None, :, :] == jnp.arange(n, dtype=jnp.int32)[:, None, None]
    to_expert = jnp.sum(jnp.where(named, weights[None], 0.0), axis=-1)
    lane = jnp.arange(rows)
    gs = gain_attn.shape[0]
    me = f * nc + c
    spots = lane // gs == me % (rows // gs)
    gain_row = lambda g: jnp.where(spots, jnp.tile(g.astype(f32), rows // gs), 0.0)
    qs = qk_gain.shape[1]
    qk_row = lambda g: jnp.where(lane // qs == me, jnp.tile(g.astype(f32), rows // qs), 0.0)
    small = jnp.stack([gain_row(gain_attn), qk_row(qk_gain[0]), qk_row(qk_gain[1]), gain_row(gain_moe)])
    tiles = jnp.concatenate([to_expert[:, None], jnp.broadcast_to(small, (n,) + small.shape), jnp.zeros((n, 3, rows), f32)], axis=1)
    by_place = lambda t: t.reshape((nf, nc) + t.shape[1:]).swapaxes(0, 1)
    per = nc // kv_heads
    wq_p = w_query.reshape(shard, nc, hp * hd).transpose(1, 0, 2)
    wk_p = jnp.repeat(w_key.reshape(shard, kv_heads, hd).transpose(1, 0, 2), per, axis=0)
    wv_p = jnp.repeat(w_value.reshape(shard, kv_heads, hd).transpose(1, 0, 2), per, axis=0)
    packed = jnp.concatenate([wq_p, wk_p, wv_p], axis=2)
    top_own = cotangent[0]
    pos = seq_positions(pair_order, BLOCK)
    cosine, sine = rope_tables(pos, hd)
    (x_seq, normed_in, w_all, dealt, wo_all, top_all, q_pre, k_pre, query_rot, key_rot, values, context, lse, hidden_res, tokens) = attention(
        x_own, packed, by_place(tiles), w_out, top_own.astype(bf16), cosine, sine, pos, nf, zs, hp, scale, 0
    )
    qw = hp * hd
    full_row = lambda r: dealt[:, r].reshape(-1, rows // gs, rows).sum(axis=1).reshape(-1)
    g_attn, g_moe = full_row(1), full_row(4)
    g_qk = dealt[:, 2:4].sum(axis=0)
    route_w = dealt[:, 0, :]
    hit = route_w > 0.0
    below = (jnp.arange(rows)[:, None] < jnp.arange(rows)[None, :]).astype(f32)
    rank = jnp.dot(hit.astype(f32), below, preferred_element_type=f32).astype(jnp.int32)
    slot = (rank[:, None, :] == jnp.arange(capacity, dtype=jnp.int32)[None, :, None]) & hit[:, None, :]
    place = slot.astype(bf16)
    mixing = jnp.where(slot, route_w[:, None, :], 0.0).astype(bf16)
    gate_w, up_w, down_w = w_gate[0], w_up[0], w_down[0]
    def paired(table):
        two = table.reshape(n // 2, 2, capacity, rows)
        none = jnp.zeros((n // 2, capacity, rows), bf16)
        upper = jnp.concatenate([two[:, 0], none], axis=2)
        lower = jnp.concatenate([none, two[:, 1]], axis=2)
        return jnp.concatenate([upper, lower], axis=1)

    grad_mid, shares, arrived, grad_arrived, expert_hidden, grad_gate_pre, grad_up_pre = experts_of(
        tokens, top_all, paired(place), paired(mixing), gate_w, up_w, down_w, nf, zs, 3
    )
    grad_mid = grad_mid.astype(f32)

    _, mid_back = jax.vjp(rms_scale, hidden_res, g_moe)
    grad_res_mid, grad_moe_gain = mid_back(grad_mid)
    grad_res = top_own + grad_res_mid

    grad_down = contract_rows(expert_hidden, grad_arrived)
    grad_gate = contract_rows(arrived, grad_gate_pre)
    grad_up = contract_rows(arrived, grad_up_pre)

    grad_in, grads, grad_wo, summed, mixed, *_ = gradients(
        grad_res.astype(bf16), normed_in, w_all, wo_all, q_pre, k_pre, query_rot, key_rot, values, context, lse, cosine, sine, pos,
        g_qk, g_attn[None], grad_moe_gain[None], shares, nf, zs, hp, scale, 4
    )
    block_output = (hidden_res + mixed.astype(f32)).astype(bf16)
    total = jnp.sum(summed, axis=0)
    part = lambda row, size: lax.dynamic_slice_in_dim(row, me * size % rows, size)
    own_attn_gain = part(total[0], gs)
    own_moe_gain = part(total[1], gs)
    own_qk = jnp.stack([part(total[2], qs), part(total[3], qs)])
    grad_wo = grad_wo.astype(f32)
    grad_wq = grads[:, :, :qw].transpose(1, 0, 2).reshape(shard, heads * hd).astype(f32)
    grad_kv = grads[:, :, qw:].reshape(kv_heads, per, shard, hd)
    grad_wk = grad_kv[:, 0].transpose(1, 0, 2).reshape(shard, kv_heads * hd).astype(f32)
    grad_wv = grad_kv[:, 1].transpose(1, 0, 2).reshape(shard, kv_heads * hd).astype(f32)
    _, in_back = jax.vjp(rms_scale, resid, g_attn)
    grad_input = grad_res + in_back(grad_in.astype(f32))[0]
    return (
        block_output[None],
        grad_input[None],
        own_attn_gain,
        grad_wq,
        grad_wk,
        grad_wv,
        own_qk,
        grad_wo,
        own_moe_gain,
        grad_gate[None],
        grad_up[None],
        grad_down[None],
    )


def body(nf, nc, block_input, *rest):
    kv_heads = rest[3].shape[1] // (rest[5].shape[1] * nf * nc)
    fits = nf == 4 and nc == 2 * kv_heads and rest[4].shape[1] == rest[3].shape[1]
    return head_body(nf, nc, block_input, *rest) if fits else wide_body(block_input, *rest)


def solution(mesh):
    return jax.shard_map(
        functools.partial(body, mesh.shape["fsdp"], mesh.shape["cp"]),
        mesh=mesh,
        in_specs=(
            P("fsdp", "cp", None),
            P("fsdp", "cp", None),
            P(("fsdp", "cp")),
            P(("fsdp", "cp"), None),
            P(("fsdp", "cp"), None),
            P(("fsdp", "cp"), None),
            P(None, ("fsdp", "cp")),
            P(("fsdp", "cp"), None),
            P(("fsdp", "cp")),
            P(("fsdp", "cp"), None, None),
            P(("fsdp", "cp"), None, None),
            P(("fsdp", "cp"), None, None),
            P("fsdp", "cp", None),
            P("fsdp", "cp", None),
            P(),
        ),
        out_specs=(
            P("fsdp", "cp", None),
            P("fsdp", "cp", None),
            P(("fsdp", "cp")),
            P(("fsdp", "cp"), None),
            P(("fsdp", "cp"), None),
            P(("fsdp", "cp"), None),
            P(None, ("fsdp", "cp")),
            P(("fsdp", "cp"), None),
            P(("fsdp", "cp")),
            P(("fsdp", "cp"), None, None),
            P(("fsdp", "cp"), None, None),
            P(("fsdp", "cp"), None, None),
        ),
        check_vma=False,
    )
```

```python
import functools
import math

import jax
import jax.numpy as jnp
from jax import lax
from jax.experimental import pallas as pl
from jax.experimental.pallas import tpu as pltpu
from jax.sharding import PartitionSpec as P

BLOCK = 64


EPSILON = 1e-06
THETA = 1000000.0


def rms_scale(values, gain):
    return values * lax.rsqrt(jnp.mean(values * values, axis=-1, keepdims=True) + EPSILON) * gain


def rotate_half(values):
    half = values.shape[-1] // 2
    return jnp.concatenate([-values[..., half:], values[..., :half]], axis=-1)


def head_post(pre, gain, cosine, sine):
    normed = rms_scale(pre, gain)
    return normed * cosine[:, None, :] + rotate_half(normed) * sine[:, None, :]


def rope_tables(positions, head_dim):
    freqs = THETA ** (-(jnp.arange(head_dim // 2, dtype=jnp.float32) * 2.0 / head_dim))
    angles = positions.astype(jnp.float32)[:, None] * freqs[None, :]
    angles = jnp.concatenate([angles, angles], axis=-1)
    return (jnp.cos(angles), jnp.sin(angles))


def seq_positions(pair_order, block):
    blocks = 2 * pair_order.shape[0]
    rows = jnp.arange(blocks * block, dtype=jnp.int32)
    owner = rows // (2 * block)
    first = pair_order[owner]
    which = jnp.where(rows // block % 2 == 0, first, blocks - 1 - first)
    return which * block + rows % block


def route_tables(ids, weights, experts, capacity):
    flat = ids.reshape(-1)
    onehot = (flat[:, None] == jnp.arange(experts, dtype=jnp.int32)[None, :]).astype(jnp.int32)
    before = jnp.cumsum(onehot, axis=0) - onehot
    rank = jnp.sum(before * onehot, axis=1)
    slots = (flat * capacity + rank).reshape(ids.shape)
    columns = jnp.arange(experts * capacity, dtype=jnp.int32)
    hits = slots[:, :, None] == columns[None, None, :]
    place = jnp.sum(hits.astype(jnp.float32), axis=1).astype(jnp.bfloat16)
    mixing = jnp.sum(jnp.where(hits, weights[:, :, None].astype(jnp.float32), 0.0), axis=1).astype(
        jnp.bfloat16
    )
    return (place, mixing)


def attend_head(query, keys, values, allowed, scale):
    scores = jnp.einsum("grd,sd->grs", query, keys, preferred_element_type=jnp.float32) * scale
    scores = jnp.where(allowed[None], scores, -jnp.inf)
    top = jnp.max(scores, axis=-1, keepdims=True)
    lse = top[..., 0] + jnp.log(jnp.sum(jnp.exp(scores - top), axis=-1))
    probs = jnp.exp(scores - lse[..., None]).astype(jnp.bfloat16)
    output = jnp.einsum("grs,sd->grd", probs, values, preferred_element_type=jnp.float32)
    return (output.astype(jnp.bfloat16), lse)


def attend_back(query, keys, values, output, grad_out, lse, allowed, scale):
    scores = jnp.einsum("grd,sd->grs", query, keys, preferred_element_type=jnp.float32) * scale
    scores = jnp.where(allowed[None], scores, -jnp.inf)
    probs = jnp.exp(scores - lse[..., None])
    grad_values = jnp.einsum(
        "grs,grd->sd", probs.astype(jnp.bfloat16), grad_out, preferred_element_type=jnp.float32
    )
    grad_probs = jnp.einsum("grd,sd->grs", grad_out, values, preferred_element_type=jnp.float32)
    delta = jnp.sum(grad_out.astype(jnp.float32) * output.astype(jnp.float32), axis=-1)
    grad_scores = (probs * (grad_probs - delta[..., None])).astype(jnp.bfloat16)
    grad_query = (
        jnp.einsum("grs,sd->grd", grad_scores, keys, preferred_element_type=jnp.float32) * scale
    )
    grad_keys = (
        jnp.einsum("grs,grd->sd", grad_scores, query, preferred_element_type=jnp.float32) * scale
    )
    return (grad_query, grad_keys, grad_values)


def contract_rows(left, right):
    return lax.dot_general(
        left, right, (((0,), (0,)), ((), ())), preferred_element_type=jnp.float32
    )


def contract_cols(left, right):
    return lax.dot_general(
        left, right, (((1,), (1,)), ((), ())), preferred_element_type=jnp.float32
    )


def wide_body(
    block_input,
    cotangent,
    gain_attn,
    w_query,
    w_key,
    w_value,
    qk_gain,
    w_out,
    gain_moe,
    w_gate,
    w_up,
    w_down,
    expert_ids,
    route_weight,
    pair_order,
):
    g_attn, wq_full, wk_full, wv_full, qk_full, wo_full, g_moe = (
        lax.all_gather(gain_attn, ("fsdp", "cp"), axis=0, tiled=True),
        lax.all_gather(w_query, ("fsdp", "cp"), axis=0, tiled=True),
        lax.all_gather(w_key, ("fsdp", "cp"), axis=0, tiled=True),
        lax.all_gather(w_value, ("fsdp", "cp"), axis=0, tiled=True),
        lax.all_gather(qk_gain, ("fsdp", "cp"), axis=1, tiled=True),
        lax.all_gather(w_out, ("fsdp", "cp"), axis=0, tiled=True),
        lax.all_gather(gain_moe, ("fsdp", "cp"), axis=0, tiled=True),
    )
    rows = block_input.shape[1]
    width = block_input.shape[2]
    head_dim = qk_full.shape[1]
    kv_heads = wk_full.shape[1] // head_dim
    heads = wq_full.shape[1] // head_dim
    group = heads // kv_heads
    experts = lax.axis_size(("fsdp", "cp"))
    capacity = max(2, 3 * BLOCK * expert_ids.shape[2] // experts)
    scale = 1.0 / math.sqrt(head_dim)
    resid = block_input[0].astype(jnp.float32)
    normed_in = rms_scale(resid, g_attn.astype(jnp.float32)).astype(jnp.bfloat16)
    q_pre = jnp.dot(normed_in, wq_full, preferred_element_type=jnp.float32).reshape(
        rows, heads, head_dim
    )
    k_pre = jnp.dot(normed_in, wk_full, preferred_element_type=jnp.float32).reshape(
        rows, kv_heads, head_dim
    )
    value_rows = jnp.dot(normed_in, wv_full, preferred_element_type=jnp.float32).astype(
        jnp.bfloat16
    )
    all_pos = seq_positions(pair_order, BLOCK)
    local_pos = lax.dynamic_slice_in_dim(all_pos, lax.axis_index("cp") * rows, rows)
    cosine, sine = rope_tables(local_pos, head_dim)
    gains32 = qk_full.astype(jnp.float32)
    query_rot = head_post(q_pre, gains32[0], cosine, sine).astype(jnp.bfloat16)
    key_rot = head_post(k_pre, gains32[1], cosine, sine).astype(jnp.bfloat16)
    keys_all, values_all = (
        lax.all_gather(key_rot.reshape(rows, kv_heads * head_dim), "cp", axis=0, tiled=True),
        lax.all_gather(value_rows, "cp", axis=0, tiled=True),
    )
    span = keys_all.shape[0]
    allowed = all_pos[None, :] <= local_pos[:, None]
    query_heads = query_rot.reshape(rows, kv_heads, group, head_dim).transpose(1, 2, 0, 3)
    key_heads = keys_all.reshape(span, kv_heads, head_dim).transpose(1, 0, 2)
    value_heads = values_all.reshape(span, kv_heads, head_dim).transpose(1, 0, 2)
    context_heads, lse = lax.map(
        lambda item: attend_head(item[0], item[1], item[2], allowed, scale),
        (query_heads, key_heads, value_heads),
    )
    context = context_heads.transpose(2, 0, 1, 3).reshape(rows, heads * head_dim)
    hidden_res = resid + jnp.dot(context, wo_full, preferred_element_type=jnp.float32)
    normed_mid = rms_scale(hidden_res, g_moe.astype(jnp.float32)).astype(jnp.bfloat16)
    place, mixing = route_tables(expert_ids[0], route_weight[0], experts, capacity)
    sent = contract_rows(place, normed_mid).astype(jnp.bfloat16)
    arrived = lax.all_to_all(
        sent.reshape(experts, capacity, width),
        ("fsdp", "cp"),
        split_axis=0,
        concat_axis=0,
        tiled=True,
    ).reshape(experts * capacity, width)
    gate_w = w_gate[0]
    up_w = w_up[0]
    down_w = w_down[0]
    gate_pre = jnp.dot(arrived, gate_w, preferred_element_type=jnp.float32)
    up_pre = jnp.dot(arrived, up_w, preferred_element_type=jnp.float32)
    gate_sig = jax.nn.sigmoid(gate_pre)
    gate_act = gate_pre * gate_sig
    expert_hidden = (gate_act * up_pre).astype(jnp.bfloat16)
    expert_out = jnp.dot(expert_hidden, down_w, preferred_element_type=jnp.float32).astype(
        jnp.bfloat16
    )
    returned = lax.all_to_all(
        expert_out.reshape(experts, capacity, width),
        ("fsdp", "cp"),
        split_axis=0,
        concat_axis=0,
        tiled=True,
    ).reshape(experts * capacity, width)
    mixed = jnp.dot(mixing, returned, preferred_element_type=jnp.float32)
    block_output = (hidden_res + mixed).astype(jnp.bfloat16)
    g_attn, wq_full, wk_full, wv_full, qk_full, wo_full, g_moe = (
        lax.all_gather(gain_attn, ("fsdp", "cp"), axis=0, tiled=True),
        lax.all_gather(w_query, ("fsdp", "cp"), axis=0, tiled=True),
        lax.all_gather(w_key, ("fsdp", "cp"), axis=0, tiled=True),
        lax.all_gather(w_value, ("fsdp", "cp"), axis=0, tiled=True),
        lax.all_gather(qk_gain, ("fsdp", "cp"), axis=1, tiled=True),
        lax.all_gather(w_out, ("fsdp", "cp"), axis=0, tiled=True),
        lax.all_gather(gain_moe, ("fsdp", "cp"), axis=0, tiled=True),
    )
    attn_gain = g_attn.astype(jnp.float32)
    moe_gain = g_moe.astype(jnp.float32)
    gains_back = qk_full.astype(jnp.float32)
    grad_top = cotangent[0]
    grad_top_b = grad_top.astype(jnp.bfloat16)
    grad_sent = contract_rows(mixing, grad_top_b).astype(jnp.bfloat16)
    grad_arrived = lax.all_to_all(
        grad_sent.reshape(experts, capacity, width),
        ("fsdp", "cp"),
        split_axis=0,
        concat_axis=0,
        tiled=True,
    ).reshape(experts * capacity, width)
    grad_hidden = contract_cols(grad_arrived, down_w)
    grad_down = contract_rows(expert_hidden, grad_arrived)
    grad_gate_pre = (grad_hidden * up_pre * gate_sig * (1.0 + gate_pre * (1.0 - gate_sig))).astype(
        jnp.bfloat16
    )
    grad_up_pre = (grad_hidden * gate_act).astype(jnp.bfloat16)
    grad_gate = contract_rows(arrived, grad_gate_pre)
    grad_up = contract_rows(arrived, grad_up_pre)
    grad_rows = (contract_cols(grad_gate_pre, gate_w) + contract_cols(grad_up_pre, up_w)).astype(
        jnp.bfloat16
    )
    grad_back = lax.all_to_all(
        grad_rows.reshape(experts, capacity, width),
        ("fsdp", "cp"),
        split_axis=0,
        concat_axis=0,
        tiled=True,
    ).reshape(experts * capacity, width)
    grad_mid = jnp.dot(place, grad_back, preferred_element_type=jnp.float32)
    _, mid_back = jax.vjp(rms_scale, hidden_res, moe_gain)
    grad_res_mid, grad_moe_gain = mid_back(grad_mid)
    grad_res = grad_top + grad_res_mid
    grad_res_b = grad_res.astype(jnp.bfloat16)
    grad_wo = contract_rows(context, grad_res_b)
    grad_context = contract_cols(grad_res_b, wo_full).astype(jnp.bfloat16)
    grad_ctx_heads = grad_context.reshape(rows, kv_heads, group, head_dim).transpose(1, 2, 0, 3)
    grad_q_heads, grad_k_heads, grad_v_heads = lax.map(
        lambda it: attend_back(it[0], it[1], it[2], it[3], it[4], it[5], allowed, scale),
        (query_heads, key_heads, value_heads, context_heads, grad_ctx_heads, lse),
    )
    grad_keys_all = grad_k_heads.transpose(1, 0, 2).reshape(span, kv_heads * head_dim)
    grad_values_all = grad_v_heads.transpose(1, 0, 2).reshape(span, kv_heads * head_dim)
    grad_key_rot, grad_values = (
        lax.psum_scatter(
            grad_keys_all.astype(jnp.bfloat16), "cp", scatter_dimension=0, tiled=True
        ).astype(jnp.float32),
        lax.psum_scatter(
            grad_values_all.astype(jnp.bfloat16), "cp", scatter_dimension=0, tiled=True
        ).astype(jnp.float32),
    )
    grad_query_rot = grad_q_heads.transpose(2, 0, 1, 3).reshape(rows, heads, head_dim)
    _, query_back = jax.vjp(
        lambda pre, gain: head_post(pre, gain, cosine, sine), q_pre, gains_back[0]
    )
    grad_q_pre, grad_q_gain = query_back(grad_query_rot)
    _, key_back = jax.vjp(
        lambda pre, gain: head_post(pre, gain, cosine, sine), k_pre, gains_back[1]
    )
    grad_k_pre, grad_k_gain = key_back(grad_key_rot.reshape(rows, kv_heads, head_dim))
    grad_q_b = grad_q_pre.reshape(rows, heads * head_dim).astype(jnp.bfloat16)
    grad_k_b = grad_k_pre.reshape(rows, kv_heads * head_dim).astype(jnp.bfloat16)
    grad_v_b = grad_values.astype(jnp.bfloat16)
    grad_wq = contract_rows(normed_in, grad_q_b)
    grad_wk = contract_rows(normed_in, grad_k_b)
    grad_wv = contract_rows(normed_in, grad_v_b)
    grad_in_norm = (
        contract_cols(grad_q_b, wq_full)
        + contract_cols(grad_k_b, wk_full)
        + contract_cols(grad_v_b, wv_full)
    )
    _, in_back = jax.vjp(rms_scale, resid, attn_gain)
    grad_res_in, grad_attn_gain = in_back(grad_in_norm)
    grad_input = grad_res + grad_res_in
    grad_qk = jnp.stack([grad_q_gain, grad_k_gain])
    owned_grads = (
        lax.psum_scatter(grad_attn_gain, ("fsdp", "cp"), scatter_dimension=0, tiled=True),
        lax.psum_scatter(grad_wq, ("fsdp", "cp"), scatter_dimension=0, tiled=True),
        lax.psum_scatter(grad_wk, ("fsdp", "cp"), scatter_dimension=0, tiled=True),
        lax.psum_scatter(grad_wv, ("fsdp", "cp"), scatter_dimension=0, tiled=True),
        lax.psum_scatter(grad_qk, ("fsdp", "cp"), scatter_dimension=1, tiled=True),
        lax.psum_scatter(grad_wo, ("fsdp", "cp"), scatter_dimension=0, tiled=True),
        lax.psum_scatter(grad_moe_gain, ("fsdp", "cp"), scatter_dimension=0, tiled=True),
    )
    return (
        block_output[None],
        grad_input[None],
        owned_grads[0],
        owned_grads[1],
        owned_grads[2],
        owned_grads[3],
        owned_grads[4],
        owned_grads[5],
        owned_grads[6],
        grad_gate[None],
        grad_up[None],
        grad_down[None],
    )


MESH = pl.DeviceIdType.MESH
ANY = pl.BlockSpec(memory_space=pl.ANY)
VM = pl.BlockSpec(memory_space=pltpu.VMEM)


def place_of():
    f = lax.axis_index("fsdp")
    c = lax.axis_index("cp")
    return f, c, c // 2, c % 2


def flip(f, bit):
    return f + bit - 2 * bit * ((f // bit) % 2)


class Wire:
    def __init__(self):
        self.sent = []

    def send(self, src, dst, ssem, rsem, dev, when=None):
        copy = pltpu.make_async_remote_copy(
            src_ref=src, dst_ref=dst, send_sem=ssem, recv_sem=rsem, device_id=dev, device_id_type=MESH
        )
        if when is None:
            copy.start()
        else:
            pl.when(when)(copy.start)
        self.sent.append((copy, when))
        return self.sent[-1]

    def settle(self, entries):
        for entry in entries:
            self.sent = [e for e in self.sent if e is not entry]
            self.wait(*entry)

    def wait(self, copy, when):
        if when is None:
            copy.wait_send()
        else:
            pl.when(when)(copy.wait_send)

    def drain(self):
        for entry in self.sent:
            self.wait(*entry)


def got(dst, ssem, rsem, dev, when=None):
    copy = pltpu.make_async_remote_copy(
        src_ref=dst, dst_ref=dst, send_sem=ssem, recv_sem=rsem, device_id=dev, device_id_type=MESH
    )
    if when is None:
        copy.wait_recv()
    else:
        pl.when(when)(copy.wait_recv)


def greet(f, c, z, zs, planes):
    bar = pltpu.get_barrier_semaphore()
    k = c % 2
    sib = c + 1 - 2 * k
    near = [((f, sib), None), ((f, c + 2), z < zs - 1), ((f, c - 2), z > 0)]
    if planes:
        near += [((flip(f, 1), c), None), ((flip(f, 2), c), None)]
    for dev, when in near:
        def hello(dev=dev):
            pl.semaphore_signal(bar, inc=1, device_id=dev, device_id_type=MESH)
        if when is None:
            hello()
        else:
            pl.when(when)(hello)
    base = 3 if planes else 1
    inner = jnp.logical_and(z > 0, z < zs - 1)
    pl.semaphore_wait(bar, base + jnp.where(inner, 2, 1))


def ag_kernel(zs, planes, x_ref, o_ref, loc, sl, szr, szl, rz, sp1, rp1, sp2, rp2, ssib, rsib):
    f, c, z, k = place_of()
    half = x_ref.shape[1] // 2
    sib = (f, c + 1 - 2 * k)
    b1 = 1 + k
    b2 = 2 - k
    f1 = flip(f, b1)
    f2 = flip(f, b2)
    cols = [f, f1, f2, flip(f1, b2)] if planes else [0]
    cs = 2 * zs

    def chunk(col, zz):
        at = (cols[col] * cs if planes else 0) + 2 * zz
        return o_ref.at[pl.ds(at, 2), :, pl.ds(pl.multiple_of(k * half, 128), half)]

    def other(col, zz):
        at = (cols[col] * cs if planes else 0) + 2 * zz
        return o_ref.at[pl.ds(at, 2), :, pl.ds(pl.multiple_of((1 - k) * half, 128), half)]

    mine = (f * cs if planes else 0) + c
    theirs = (f * cs if planes else 0) + c + 1 - 2 * k
    own = pltpu.make_async_copy(x_ref, o_ref.at[mine], loc)
    own.start()
    greet(f, c, z, zs, planes)
    w = Wire()
    w.send(x_ref, o_ref.at[mine], sl.at[0], sl.at[1], sib)
    own.wait()
    got(o_ref.at[theirs], sl.at[0], sl.at[1], sib)

    def spread(zz, when):
        if planes:
            w.send(chunk(0, zz), chunk(0, zz), sp1.at[zz], rp1.at[zz], (f1, c), when)
            w.send(chunk(0, zz), chunk(0, zz), sp2.at[zz], rp2.at[zz], (f2, c), when)

    def relay(zz, when):
        if planes:
            got(chunk(1, zz), sp1.at[zz], rp1.at[zz], (f1, c), when)
            w.send(chunk(1, zz), chunk(1, zz), sp2.at[zs + zz], rp2.at[zs + zz], (f2, c), when)
            w.send(chunk(1, zz), chunk(1, zz), ssib.at[zs + zz], rsib.at[zs + zz], sib, when)

    w.send(chunk(0, z), chunk(0, z), szr.at[z], rz.at[z], (f, c + 2), z < zs - 1)
    w.send(chunk(0, z), chunk(0, z), szl.at[z], rz.at[z], (f, c - 2), z > 0)
    spread(z, None)
    order = []
    for h in range(1, zs):
        for zz, when, on, dz, sem in (
            (z - h, z - h >= 0, z < zs - 1, 2, szr),
            (z + h, z + h < zs, z > 0, -2, szl),
        ):
            got(chunk(0, zz), sem.at[zz], rz.at[zz], (f, c), when)
            w.send(chunk(0, zz), chunk(0, zz), sem.at[zz], rz.at[zz], (f, c + dz), jnp.logical_and(when, on))
            spread(zz, when)
            w.send(chunk(0, zz), chunk(0, zz), ssib.at[zz], rsib.at[zz], sib, when)
            order.append((zz, when))
        if h == 1:
            relay(z, None)
    for zz, when in order:
        relay(zz, when)
    if planes:
        for col, base in ((2, 0), (3, zs)):
            for zz, when in [(z, None)] + order:
                got(chunk(col, zz), sp2.at[base + zz], rp2.at[base + zz], (f2, c), when)
                w.send(chunk(col, zz), chunk(col, zz), ssib.at[col * zs + zz], rsib.at[col * zs + zz], sib, when)
    if planes:
        for mycol, theircol in ((0, 0), (1, 2), (2, 1), (3, 3)):
            for zz, when in ([(z, None)] if mycol else []) + order:
                got(other(mycol, zz), ssib.at[theircol * zs + zz], rsib.at[theircol * zs + zz], sib, when)
    else:
        for zz, when in order:
            got(other(0, zz), ssib.at[zz], rsib.at[zz], sib, when)
    w.drain()


def gather(x, zs, planes, cid, nf=4):
    rows, width = x.shape
    n = (nf if planes else 1) * 2 * zs
    D = pltpu.SemaphoreType.DMA
    return pl.pallas_call(
        functools.partial(ag_kernel, zs, planes),
        out_shape=jax.ShapeDtypeStruct((n, rows, width), x.dtype),
        in_specs=[VM],
        out_specs=ANY,
        scratch_shapes=[D(()), D((2,)), D((zs,)), D((zs,)), D((zs,)), D((zs,)), D((zs,)), D((2 * zs,)), D((2 * zs,)), D((4 * zs,)), D((4 * zs,))],
        compiler_params=pltpu.CompilerParams(collective_id=cid, has_side_effects=True),
        name="gather_all" if planes else "gather_seq",
    )(x)


def add_into(dst, src, rows=32):
    n, r, wd = dst.shape

    def step(i, _):
        a = pl.ds(pl.multiple_of(i % (r // rows) * rows, rows), rows)
        j = i // (r // rows)
        dst[j, a, :] = (dst[j, a, :].astype(jnp.float32) + src[j, a, :].astype(jnp.float32)).astype(dst.dtype)
        return 0

    lax.fori_loop(0, n * (r // rows), step, 0)


def rs_kernel(zs, planes, x_ref, o_ref, t, r0, r1, r2, ral, rar, fin, lsem, s0, q0, s1, q1, s2, q2, szr, szl, rzr, rzl, sf):
    f, c, z, k = place_of()
    half = o_ref.shape[1] // 2
    sib = (f, c + 1 - 2 * k)
    b1 = 2 - k
    b2 = 1 + k
    f1 = flip(f, b1)
    f2 = flip(f, b2)
    f3 = flip(f1, b2)
    cs = 2 * zs
    cols = [f3, f1, f2, f] if planes else [0]
    nc = len(cols)
    last = zs - 1
    low = z < zs // 2
    zord = []
    for i in range(zs - 1):
        far_low = jnp.where(i < zs - 1 - z, last - i, zs - 2 - i)
        far_high = jnp.where(i < z, i, i + 1)
        zord.append(jnp.where(low, far_low, far_high))
    zord.append(z)

    def src(col, zz, kk):
        at = (col * cs if planes else 0) + 2 * zz
        return x_ref.at[pl.ds(at, 2), :, pl.ds(pl.multiple_of(kk * half, 128), half)]

    greet(f, c, z, zs, planes)
    w = Wire()
    locals_ = []
    for ci in range(nc):
        for zi in range(zs):
            i = ci * zs + zi
            col = cols[ci]
            zz = zord[zi]
            slot = (ci if not planes else {0: 0, 1: 2, 2: 1, 3: 3}[ci]) * zs + zz
            w.send(src(col, zz, 1 - k), r0.at[slot], s0.at[slot], q0.at[slot], sib)
            cp = pltpu.make_async_copy(src(col, zz, k), t.at[ci * zs + zz], lsem.at[i])
            cp.start()
            locals_.append(cp)

    def first(ci, zi):
        zz = zord[zi]
        locals_[ci * zs + zi].wait()
        got(r0.at[ci * zs + zz], s0.at[ci * zs + zz], q0.at[ci * zs + zz], sib)
        add_into(t.at[ci * zs + zz], r0.at[ci * zs + zz])

    if planes:
        for ci in (0, 1):
            for zi in range(zs):
                zz = zord[zi]
                first(ci, zi)
                m = ci * zs + zz
                w.send(t.at[m], r1.at[m], s1.at[m], q1.at[m], (f1, c))
        for zi in range(zs):
            zz = zord[zi]
            first(2, zi)
            got(r1.at[zz], s1.at[zz], q1.at[zz], (f1, c))
            add_into(t.at[2 * zs + zz], r1.at[zz])
            w.send(t.at[2 * zs + zz], r2.at[zz], s2.at[zz], q2.at[zz], (f2, c))
        for zi in range(zs):
            first(3, zi)
        base = 3 * zs
    else:
        base = 0

    def complete(zi):
        zz = zord[zi]
        if planes:
            got(r1.at[zs + zz], s1.at[zs + zz], q1.at[zs + zz], (f1, c))
            add_into(t.at[base + zz], r1.at[zs + zz])
            got(r2.at[zz], s2.at[zz], q2.at[zz], (f2, c))
            add_into(t.at[base + zz], r2.at[zz])
        else:
            first(0, zi)

    for zi in range(zs - 1):
        zz = zord[zi]
        complete(zi)
        right = zz > z
        from_left = jnp.logical_and(right, z > 0)
        from_right = jnp.logical_and(jnp.logical_not(right), z < zs - 1)
        got(ral.at[zz], szr.at[zz], rzr.at[zz], (f, c), from_left)
        got(rar.at[zz], szl.at[zz], rzl.at[zz], (f, c), from_right)

        @pl.when(from_left)
        def _():
            add_into(t.at[base + zz], ral.at[zz])

        @pl.when(from_right)
        def _():
            add_into(t.at[base + zz], rar.at[zz])

        w.send(t.at[base + zz], ral.at[zz], szr.at[zz], rzr.at[zz], (f, c + 2), right)
        w.send(t.at[base + zz], rar.at[zz], szl.at[zz], rzl.at[zz], (f, c - 2), jnp.logical_not(right))
    complete(zs - 1)
    got(ral.at[z], szr.at[z], rzr.at[z], (f, c), z > 0)
    got(rar.at[z], szl.at[z], rzl.at[z], (f, c), z < zs - 1)

    @pl.when(z > 0)
    def _():
        add_into(t.at[base + z], ral.at[z])

    @pl.when(z < zs - 1)
    def _():
        add_into(t.at[base + z], rar.at[z])

    w.send(t.at[base + z, 1 - k], fin, sf.at[0], sf.at[1], sib)
    o_ref[:, pl.ds(pl.multiple_of(k * half, 128), half)] = t[base + z, k]
    got(fin, sf.at[0], sf.at[1], sib)
    o_ref[:, pl.ds(pl.multiple_of((1 - k) * half, 128), half)] = fin[...]
    w.drain()


def scatter(x, zs, planes, cid, nf=4):
    n, rows, width = x.shape
    D = pltpu.SemaphoreType.DMA
    half = width // 2
    nc = (nf if planes else 1) * zs
    V = lambda m: pltpu.VMEM((m, 2, rows, half), x.dtype)
    return pl.pallas_call(
        functools.partial(rs_kernel, zs, planes),
        out_shape=jax.ShapeDtypeStruct((rows, width), x.dtype),
        in_specs=[ANY],
        out_specs=VM,
        scratch_shapes=[V(nc), V(nc), V(2 * zs), V(zs), V(zs), V(zs), pltpu.VMEM((rows, half), x.dtype),
            D((nc,)), D((nc,)), D((nc,)), D((2 * zs,)), D((2 * zs,)), D((zs,)), D((zs,)), D((zs,)), D((zs,)), D((zs,)), D((zs,)), D((2,))],
        compiler_params=pltpu.CompilerParams(collective_id=cid, has_side_effects=True, vmem_limit_bytes=60 * 2**20),
        name="scatter_all" if planes else "scatter_seq",
    )(x)


def greet_cross(f, c, nf, nc):
    bar = pltpu.get_barrier_semaphore()
    for i in range(1, nc):
        pl.semaphore_signal(bar, inc=1, device_id=(f, (c + i) % nc), device_id_type=MESH)
    for i in range(1, nf):
        pl.semaphore_signal(bar, inc=1, device_id=((f + i) % nf, c), device_id_type=MESH)
    pl.semaphore_wait(bar, nc + nf - 2)


def tile_steps(w, nf, nc, src, dst, hub, ssem, rsem, sp, rp):
    f, c, z, k = place_of()

    def go(i, _):
        j = (c + i) % nc
        pltpu.make_async_remote_copy(
            src_ref=src.at[j], dst_ref=hub.at[c], send_sem=ssem, recv_sem=rsem, device_id=(f, j), device_id_type=MESH
        ).start()
        return 0

    lax.fori_loop(1, nc, go, 0)
    hub[c] = src[c]
    yield
    every = pltpu.make_async_remote_copy(
        src_ref=src.at[pl.ds(0, nc - 1)], dst_ref=hub.at[pl.ds(0, nc - 1)], send_sem=ssem, recv_sem=rsem,
        device_id=(f, c), device_id_type=MESH,
    )
    every.wait_send()
    every.wait_recv()
    mine = pl.ds(f * nc, nc)
    for i in range(1, nf):
        ff = (f + i) % nf
        w.send(hub.at[:, ff], dst.at[mine], sp.at[i], rp.at[i], (ff, c))
    dst[mine] = hub[:, f]
    yield
    for i in range(1, nf):
        ff = (f + nf - i) % nf
        got(dst.at[pl.ds(ff * nc, nc)], sp.at[i], rp.at[i], (f, c))
    yield


def tile_bufs(nf, nc, tile):
    D = pltpu.SemaphoreType.DMA
    return [pltpu.VMEM((nc, nf) + tile, jnp.float32), D(()), D(()), D((nf,)), D((nf,))]


def gather_steps(w, zs, planes, late, x_ref, o_ref, loc, sl, szr, szl, rz, sp1, rp1, sp2, rp2, ssib, rsib):
    f, c, z, k = place_of()
    half = x_ref.shape[1] // 2
    sib = (f, c + 1 - 2 * k)
    b1 = 1 + k
    b2 = 2 - k
    f1 = flip(f, b1)
    f2 = flip(f, b2)
    cols = [f, f1, f2, flip(f1, b2)] if planes else [0]
    cs = 2 * zs

    def chunk(col, zz, kk):
        at = (cols[col] * cs if planes else 0) + 2 * zz
        return o_ref.at[pl.ds(at, 2), :, pl.ds(pl.multiple_of(kk * half, 128), half)]

    mine = (f * cs if planes else 0) + c
    theirs = (f * cs if planes else 0) + c + 1 - 2 * k
    own = pltpu.make_async_copy(x_ref, o_ref.at[mine], loc)
    own.start()
    w.send(x_ref, o_ref.at[mine], sl.at[0], sl.at[1], sib)
    yield
    own.wait()
    got(o_ref.at[theirs], sl.at[0], sl.at[1], sib)

    def spread(zz, when):
        if planes:
            w.send(chunk(0, zz, k), chunk(0, zz, k), sp1.at[zz], rp1.at[zz], (f1, c), when)
            w.send(chunk(0, zz, k), chunk(0, zz, k), sp2.at[zz], rp2.at[zz], (f2, c), when)

    def relay(zz, when):
        if planes:
            got(chunk(1, zz, k), sp1.at[zz], rp1.at[zz], (f1, c), when)
            w.send(chunk(1, zz, k), chunk(1, zz, k), sp2.at[zs + zz], rp2.at[zs + zz], (f2, c), when)
            w.send(chunk(1, zz, k), chunk(1, zz, k), ssib.at[zs + zz], rsib.at[zs + zz], sib, when)

    if late:
        spread(z, None)
        yield
    w.send(chunk(0, z, k), chunk(0, z, k), szr.at[z], rz.at[z], (f, c + 2), z < zs - 1)
    w.send(chunk(0, z, k), chunk(0, z, k), szl.at[z], rz.at[z], (f, c - 2), z > 0)
    if not late:
        spread(z, None)
    yield
    if late:
        relay(z, None)
        yield
    order = []
    for h in range(1, zs):
        for zz, when, on, dz, sem in (
            (z - h, z - h >= 0, z < zs - 1, 2, szr),
            (z + h, z + h < zs, z > 0, -2, szl),
        ):
            got(chunk(0, zz, k), sem.at[zz], rz.at[zz], (f, c), when)
            w.send(chunk(0, zz, k), chunk(0, zz, k), sem.at[zz], rz.at[zz], (f, c + dz), jnp.logical_and(when, on))
            spread(zz, when)
            w.send(chunk(0, zz, k), chunk(0, zz, k), ssib.at[zz], rsib.at[zz], sib, when)
            order.append((zz, when))
        yield
        if h == 1 and not late:
            relay(z, None)
            yield
    for zz, when in order:
        relay(zz, when)
        yield
    if planes:
        for col, base in ((2, 0), (3, zs)):
            for zz, when in [(z, None)] + order:
                got(chunk(col, zz, k), sp2.at[base + zz], rp2.at[base + zz], (f2, c), when)
                w.send(chunk(col, zz, k), chunk(col, zz, k), ssib.at[col * zs + zz], rsib.at[col * zs + zz], sib, when)
            yield
        for mycol, theircol in ((0, 0), (1, 2), (2, 1), (3, 3)):
            for zz, when in ([(z, None)] if mycol else []) + order:
                got(chunk(mycol, zz, 1 - k), ssib.at[theircol * zs + zz], rsib.at[theircol * zs + zz], sib, when)
    else:
        for zz, when in order:
            got(chunk(0, zz, 1 - k), ssib.at[zz], rsib.at[zz], sib, when)
    yield


def gather_sems(zs):
    D = pltpu.SemaphoreType.DMA
    return [D(()), D((2,)), D((zs,)), D((zs,)), D((zs,)), D((zs,)), D((zs,)), D((2 * zs,)), D((2 * zs,)), D((4 * zs,)), D((4 * zs,))]


def advance(steps, name="step"):
    with jax.named_scope(name):
        return next(steps, steps) is not steps


def head_rows_steps(w, nf, nc, hp, wo_ref, wo_all, hub, loc, so, ro):
    f, c, z, k = place_of()
    fx, fy = flip(f, 1), flip(f, 2)
    fd = flip(fx, 2)
    hr = wo_ref.shape[0] // 2
    halves = []
    for p in (0, 1):
        j = c % hp
        m = f
        if p:
            j, m = flip(j, 2), flip(f, 2)
        halves.append((p, pl.ds(p * hr, hr), j, f == j, m))
    keeps = []
    for p, at, j, is_hub, m in halves:
        w.send(wo_ref.at[at], hub.at[f, at], so.at[p, 0], ro.at[p, f], (j, c), jnp.logical_not(is_hub))
        keep = pltpu.make_async_copy(wo_ref.at[at], hub.at[f, at], loc.at[p])
        pl.when(is_hub)(keep.start)
        keeps.append(keep)
    yield
    stays = []
    for p, at, j, is_hub, m in halves:
        for ff in range(nf):
            got(hub.at[ff, at], so.at[p, 0], ro.at[p, ff], (f, c), jnp.logical_and(is_hub, ff != f))
            pl.when(jnp.logical_and(is_hub, ff == f))(keeps[p].wait)
            dc = (ff * nc + c) // hp
            w.send(hub.at[ff, at], wo_all.at[m, at], so.at[p, 1 + ff], ro.at[p, nf], (f, dc), jnp.logical_and(is_hub, dc != c))
            stay = pltpu.make_async_copy(hub.at[ff, at], wo_all.at[m, at], loc.at[2 + p])
            pl.when(jnp.logical_and(is_hub, dc == c))(stay.start)
        stays.append(stay)
    yield
    for p, at, j, is_hub, m in halves:
        here = (hp * c + m) % nc == c
        got(wo_all.at[m, at], so.at[p, 1], ro.at[p, nf], (f, c), jnp.logical_not(here))
        pl.when(here)(stays[p].wait)
        w.send(wo_all.at[m, at], wo_all.at[m, at], so.at[p, nf + 1], ro.at[p, nf + 1], (fx, c))
        w.send(wo_all.at[m, at], wo_all.at[m, at], so.at[p, nf + 2], ro.at[p, nf + 2], (fy, c))
    yield
    for p, at, j, is_hub, m in halves:
        mx, my = flip(m, 1), flip(m, 2)
        got(wo_all.at[mx, at], so.at[p, nf + 1], ro.at[p, nf + 1], (fx, c))
        got(wo_all.at[my, at], so.at[p, nf + 2], ro.at[p, nf + 2], (fy, c))
        if p == 0:
            w.send(wo_all.at[mx, at], wo_all.at[mx, at], so.at[p, nf + 3], ro.at[p, nf + 3], (fy, c))
        else:
            w.send(wo_all.at[my, at], wo_all.at[my, at], so.at[p, nf + 3], ro.at[p, nf + 3], (fx, c))
    yield
    for p, at, j, is_hub, m in halves:
        got(wo_all.at[flip(flip(m, 1), 2), at], so.at[p, nf + 3], ro.at[p, nf + 3], (f, c))
    yield


def far_first(z, zs):
    last = zs - 1
    low = z < zs // 2
    order = []
    for i in range(zs - 1):
        far_low = jnp.where(i < zs - 1 - z, last - i, zs - 2 - i)
        far_high = jnp.where(i < z, i, i + 1)
        order.append(jnp.where(low, far_low, far_high))
    return order + [z]


def line_sum_steps(w, zs, make, o_ref, t, u, r0, ral, rar, fin, s0, q0, szr, szl, rzr, rzl, sf):
    f, c, z, k = place_of()
    half = o_ref.shape[1] // 2
    sib = (f, c + 1 - 2 * k)
    order = far_first(z, zs)

    def first(zz):
        make(zz)
        w.send(u.at[zz], r0.at[zz], s0.at[zz], q0.at[zz], sib)

    def complete(zz):
        got(r0.at[zz], s0.at[zz], q0.at[zz], sib)
        add_into(t.at[zz], r0.at[zz])

    def onward(zz):
        right = zz > z
        from_left = jnp.logical_and(right, z > 0)
        from_right = jnp.logical_and(jnp.logical_not(right), z < zs - 1)
        got(ral.at[zz], szr.at[zz], rzr.at[zz], (f, c), from_left)
        got(rar.at[zz], szl.at[zz], rzl.at[zz], (f, c), from_right)

        @pl.when(from_left)
        def _():
            add_into(t.at[zz], ral.at[zz])

        @pl.when(from_right)
        def _():
            add_into(t.at[zz], rar.at[zz])

        w.send(t.at[zz], ral.at[zz], szr.at[zz], rzr.at[zz], (f, c + 2), right)
        w.send(t.at[zz], rar.at[zz], szl.at[zz], rzl.at[zz], (f, c - 2), jnp.logical_not(right))

    first(order[0])
    yield
    for zi in range(zs - 1):
        first(order[zi + 1])
        complete(order[zi])
        yield
        onward(order[zi])
        yield
    complete(z)
    got(ral.at[z], szr.at[z], rzr.at[z], (f, c), z > 0)

    @pl.when(z > 0)
    def _():
        add_into(t.at[z], ral.at[z])

    yield
    got(rar.at[z], szl.at[z], rzl.at[z], (f, c), z < zs - 1)

    @pl.when(z < zs - 1)
    def _():
        add_into(t.at[z], rar.at[z])

    w.send(t.at[z, 1 - k], fin, sf.at[0], sf.at[1], sib)
    o_ref[:, pl.ds(pl.multiple_of(k * half, 128), half)] = t[z, k]
    yield
    got(fin, sf.at[0], sf.at[1], sib)
    o_ref[:, pl.ds(pl.multiple_of((1 - k) * half, 128), half)] = fin[...]
    yield


def line_sum_bufs(zs, rows, half, dtype):
    D = pltpu.SemaphoreType.DMA
    V = pltpu.VMEM((zs, 2, rows, half), dtype)
    return [V, V, V, V, V, pltpu.VMEM((rows, half), dtype)] + [D((zs,))] * 6 + [D((2,))]


def attn_kernel(nf, zs, hp, scale, refs):
    (x_ref, wp_ref, tl_ref, wo_ref, tb_ref, cos_ref, sin_ref, pr_ref, pc_ref,
     o_ref, nm_ref, w_ref, to_ref, wo_all, top_all, qp_ref, kp_ref, qr_ref, kr_ref, v_ref, ctx_ref, lse_ref, hid_ref, tok_all,
     gain, gain_mid, mid, out_ref, loc, wloc, sl, szr, szl, rz, ssib, rsib, sw, rw, swx, swy) = refs[:40]
    tile_b = refs[40:45]
    head_bufs = refs[45:49]
    top_sems = refs[49:60]
    tok_sems = refs[60:71]
    sum_bufs = refs[71:]
    f, c, z, k = place_of()
    nc = 2 * zs
    rows, width = x_ref.shape
    half = width // 2
    hd = kr_ref.shape[1]
    qw = hp * hd
    f32, bf16 = jnp.float32, jnp.bfloat16
    sib_c = c + 1 - 2 * k
    sib = (f, sib_c)
    fx, fy = flip(f, 1), flip(f, 2)
    fr = [f, fx, fy, flip(fx, 2)]

    def chunk(zz, kk):
        return o_ref.at[pl.ds(2 * zz, 2), :, pl.ds(pl.multiple_of(kk * half, 128), half)]

    def piece(rel, cc):
        return w_ref.at[fr[rel] * nc + cc]

    own = pltpu.make_async_copy(x_ref, o_ref.at[c], loc)
    own.start()
    wown = pltpu.make_async_copy(wp_ref.at[c], piece(0, c), wloc)
    wown.start()
    with jax.named_scope("greet"):
        greet_cross(f, c, nf, nc)
    w = Wire()
    head_steps = head_rows_steps(w, nf, nc, hp, wo_ref, wo_all, *head_bufs)
    top_steps = gather_steps(w, zs, True, True, tb_ref, top_all, *top_sems)
    small_steps = tile_steps(w, nf, nc, tl_ref, to_ref, *tile_b)
    advance(small_steps, "tiles")
    w.send(x_ref, o_ref.at[c], sl.at[0], sl.at[1], sib)
    w.send(wp_ref.at[sib_c], piece(0, c), sw.at[sib_c], rw.at[c], sib)
    for h in range(1, zs):
        for zz, when in ((z - h, z - h >= 0), (z + h, z + h < zs)):
            for kk in (0, 1):
                cc = 2 * zz + kk
                w.send(wp_ref.at[cc], piece(0, c), sw.at[cc], rw.at[c], (f, cc), when)
    own.wait()
    got(o_ref.at[sib_c], sl.at[0], sl.at[1], sib)
    on_line = [
        w.send(chunk(z, k), chunk(z, k), szr.at[z], rz.at[z], (f, c + 2), z < zs - 1),
        w.send(chunk(z, k), chunk(z, k), szl.at[z], rz.at[z], (f, c - 2), z > 0),
    ]
    advance(head_steps, "heads")
    advance(small_steps, "tiles")

    def plane(cc, when):
        w.send(piece(0, cc), piece(0, cc), swx.at[cc], rw.at[nc + cc], (fx, c), when)
        w.send(piece(0, cc), piece(0, cc), swy.at[cc], rw.at[2 * nc + cc], (fy, c), when)

    def onward(cc, kk, when):
        if kk == 0:
            got(piece(1, cc), swx.at[cc], rw.at[nc + cc], (fx, c), when)
            w.send(piece(1, cc), piece(1, cc), swy.at[nc + cc], rw.at[3 * nc + cc], (fy, c), when)
        else:
            got(piece(2, cc), swy.at[cc], rw.at[2 * nc + cc], (fy, c), when)
            w.send(piece(2, cc), piece(2, cc), swx.at[nc + cc], rw.at[3 * nc + cc], (fx, c), when)

    def norm(zz):
        nb = 32

        def block(i, _):
            j = i // (rows // nb)
            at = pl.ds(pl.multiple_of(i % (rows // nb) * nb, nb), nb)
            v = o_ref[2 * zz + j, at, :].astype(f32)
            inv = lax.rsqrt(jnp.mean(v * v, axis=-1, keepdims=True) + EPSILON)
            to = pl.ds(pl.multiple_of(2 * zz * rows + i * nb, nb), nb)
            nm_ref[to, :] = (v * inv * gain[...]).astype(bf16)
            return 0

        with jax.named_scope("norm"):
            lax.fori_loop(0, 2 * rows // nb, block, 0)

    sides = [
        (
            (z - h, z - h >= 0, z < zs - 1, 2, szr),
            (z + h, z + h < zs, z > 0, -2, szl),
        )
        for h in range(1, zs)
    ]
    far = [(zz, when) for pair in sides for zz, when, *_ in pair]
    wown.wait()
    plane(c, None)
    got(piece(0, sib_c), sw.at[sib_c], rw.at[sib_c], sib)
    plane(sib_c, None)
    for zz, when in far:
        for kk in (0, 1):
            cc = 2 * zz + kk
            with jax.named_scope("w1"):
                got(piece(0, cc), sw.at[cc], rw.at[cc], (f, cc), when)
            plane(cc, when)
    advance(small_steps, "tiles")
    advance(head_steps, "heads")
    for i in range(width // 128):
        gain[:, pl.ds(128 * i, 128)] = to_ref[2 * i, 1:2, :] + to_ref[2 * i + 1, 1:2, :]
        gain_mid[:, pl.ds(128 * i, 128)] = to_ref[2 * i, 4:5, :] + to_ref[2 * i + 1, 4:5, :]
    norm(z)
    with jax.named_scope("w2"):
        for zz, when in [(z, None)] + far[:2]:
            for kk in (0, 1):
                onward(2 * zz + kk, kk, when)
    waiting = []
    for h, pair in enumerate(sides):
        for zz, when, on, dz, sem in pair:
            with jax.named_scope("x"):
                got(chunk(zz, k), sem.at[zz], rz.at[zz], (f, c), when)
            on_line.append(w.send(chunk(zz, k), chunk(zz, k), sem.at[zz], rz.at[zz], (f, c + dz), jnp.logical_and(when, on)))
            w.send(chunk(zz, k), chunk(zz, k), ssib.at[zz], rsib.at[zz], sib, when)
        if h == 0:
            advance(head_steps, "heads")
            with jax.named_scope("w2"):
                for zz, when in far[2:]:
                    for kk in (0, 1):
                        onward(2 * zz + kk, kk, when)
        if h == zs - 3:
            advance(head_steps, "heads")
            advance(top_steps, "top")
        if h == zs - 2:
            with jax.named_scope("line"):
                w.settle(on_line)
            advance(top_steps, "top")
            advance(top_steps, "top")
        for zz, when in waiting:
            got(chunk(zz, 1 - k), ssib.at[zz], rsib.at[zz], sib, when)
            pl.when(when)(functools.partial(norm, zz))
        waiting = [(zz, when) for zz, when, *_ in pair]
    for zz, when in waiting:
        got(chunk(zz, 1 - k), ssib.at[zz], rsib.at[zz], sib, when)
        pl.when(when)(functools.partial(norm, zz))
    with jax.named_scope("wait_w"):
        for zz, when in [(z, None)] + far:
            e, o = 2 * zz, 2 * zz + 1
            got(piece(2, e), swy.at[e], rw.at[2 * nc + e], (fy, c), when)
            got(piece(1, o), swx.at[o], rw.at[nc + o], (fx, c), when)
            got(piece(3, e), swy.at[nc + e], rw.at[3 * nc + e], (fy, c), when)
            got(piece(3, o), swx.at[nc + o], rw.at[3 * nc + o], (fx, c), when)

    gq = jnp.sum(to_ref[:, 2, :], axis=0, keepdims=True)
    gk = jnp.sum(to_ref[:, 3, :], axis=0, keepdims=True)
    qb = 2 * rows
    span = nc * rows
    low_half = lax.broadcasted_iota(jnp.int32, (1, hd), 1) < hd // 2

    def turned(t, g, at):
        t = t * lax.rsqrt(jnp.mean(t * t, axis=-1, keepdims=True) + EPSILON) * g
        other = pltpu.roll(t, hd // 2, 1)
        return (t * cos_ref[at, :] + jnp.where(low_half, -other, other) * sin_ref[at, :]).astype(bf16)

    def project(i, _):
        at = pl.ds(pl.multiple_of(i * qb, qb), qb)
        a = nm_ref[at, :]
        for nb in range((qw + 2 * hd) // (2 * hd)):
            wide = pl.ds(nb * 2 * hd, 2 * hd)
            pre = jnp.dot(a, w_ref[:, :, wide].reshape(width, 2 * hd), preferred_element_type=f32)
            for s in (0, 1):
                part = pre[:, s * hd : (s + 1) * hd]
                h = 2 * nb + s
                if h < hp:
                    qp_ref[at, pl.ds(h * hd, hd)] = part
                    qr_ref[at, pl.ds(h * hd, hd)] = turned(part, gq, at)
                elif h == hp:
                    kp_ref[at, :] = part
                    kr_ref[at, :] = turned(part, gk, at)
                else:
                    v_ref[at, :] = part.astype(bf16)
        return 0

    for i in range(span // qb):
        with jax.named_scope("project"):
            project(i, 0)

    lane = lax.broadcasted_iota(jnp.int32, (1, hd), 1)

    def attend(i, h):
        at = pl.ds(pl.multiple_of(i * qb, qb), qb)
        hc = pl.ds(pl.multiple_of(h * hd, hd), hd)
        s = lax.dot_general(qr_ref[at, hc], kr_ref[...], (((1,), (1,)), ((), ())), preferred_element_type=f32) * scale
        s = jnp.where(pc_ref[...] <= pr_ref[at, :], s, -jnp.inf)
        top = jnp.max(s, axis=-1, keepdims=True)
        e = jnp.exp(s - top)
        total = jnp.sum(e, axis=-1, keepdims=True)
        p = (e * (1.0 / total)).astype(bf16)
        ctx_ref[at, hc] = jnp.dot(p, v_ref[...], preferred_element_type=f32).astype(bf16)
        lse_ref[at, :] = jnp.where(lane == h, top + jnp.log(total), lse_ref[at, :])

    lse_ref[...] = jnp.zeros_like(lse_ref)

    while advance(head_steps, "heads"):
        pass

    t, u = sum_bufs[0], sum_bufs[1]

    def make(zz):
        def heads(h, _):
            attend(zz, h)
            return 0

        with jax.named_scope("attend"):
            lax.fori_loop(0, hp, heads, 0)
        at = pl.ds(pl.multiple_of(2 * zz * rows, rows), 2 * rows)
        a = ctx_ref[at, :]
        for dst, kk in ((u, 1 - k), (t, k)):
            def block(j, _, dst=dst, kk=kk):
                cols = pl.ds(pl.multiple_of(kk * half + j * 512, 128), 512)
                o = jnp.dot(a, wo_all[:, :, cols].reshape(qw, 512), preferred_element_type=f32).astype(bf16)
                dst[zz, :, :, pl.ds(pl.multiple_of(j * 512, 512), 512)] = o.reshape(2, rows, 512)
                return 0

            lax.fori_loop(0, half // 512, block, 0)

    sum_steps = line_sum_steps(w, zs, make, out_ref, *sum_bufs)
    for turn in "sstsstssssst":
        if turn == "s":
            advance(sum_steps, "sum")
        else:
            advance(top_steps, "top")
    while advance(sum_steps, "sum"):
        pass

    def middle(i, _):
        at = pl.ds(pl.multiple_of(i * 32, 32), 32)
        v = x_ref[at, :].astype(f32) + out_ref[at, :].astype(f32)
        hid_ref[at, :] = v
        inv = lax.rsqrt(jnp.mean(v * v, axis=-1, keepdims=True) + EPSILON)
        mid[at, :] = (v * inv * gain_mid[...]).astype(bf16)
        return 0

    with jax.named_scope("middle"):
        lax.fori_loop(0, rows // 32, middle, 0)
    tok_steps = gather_steps(w, zs, True, False, mid, tok_all, *tok_sems)
    advance(tok_steps, "tok")
    advance(tok_steps, "tok")
    busy = True
    while busy:
        busy = advance(top_steps, "top")
        busy = advance(tok_steps, "tok") or busy
    w.drain()


def attention(x, wp, tl, wo, tb, cosine, sine, pos, nf, zs, hp, scale, cid):
    rows, width = x.shape
    nc = 2 * zs
    span = nc * rows
    hd = cosine.shape[1]
    bf16, f32 = jnp.bfloat16, jnp.float32
    D = pltpu.SemaphoreType.DMA
    S = jax.ShapeDtypeStruct
    outs = [
        (S((nc, rows, width), bf16), VM),
        (S((span, width), bf16), VM),
        (S((nf * nc,) + wp.shape[1:], bf16), VM),
        (S((nf * nc,) + tl.shape[2:], f32), VM),
        (S((hp,) + wo.shape, bf16), VM),
        (S((nf * nc, rows, width), bf16), ANY),
        (S((span, hp * hd), f32), VM),
        (S((span, hd), f32), VM),
        (S((span, hp * hd), bf16), VM),
        (S((span, hd), bf16), VM),
        (S((span, hd), bf16), VM),
        (S((span, hp * hd), bf16), VM),
        (S((span, hd), f32), VM),
        (S((rows, width), f32), VM),
        (S((nf * nc, rows, width), bf16), ANY),
    ]
    R = pltpu.VMEM((rows, width), bf16)
    scratch = [pltpu.VMEM((1, width), f32), pltpu.VMEM((1, width), f32), R, R, D(()), D(()), D((2,)), D((zs,)), D((zs,)), D((zs,)), D((zs,)), D((zs,)),
               D((nc,)), D((4 * nc,)), D((2 * nc,)), D((2 * nc,))]
    scratch += tile_bufs(nf, nc, tl.shape[2:])
    scratch += [pltpu.VMEM((nf,) + wo.shape, bf16), D((4,)), D((2, nf + 4)), D((2, nf + 4))] + gather_sems(zs) + gather_sems(zs) + line_sum_bufs(zs, rows, width // 2, bf16)
    return pl.pallas_call(
        lambda *refs: attn_kernel(nf, zs, hp, scale, refs),
        out_shape=[s for s, _ in outs],
        in_specs=[VM] * 9,
        out_specs=[b for _, b in outs],
        scratch_shapes=scratch,
        compiler_params=pltpu.CompilerParams(collective_id=cid, has_side_effects=True, vmem_limit_bytes=60 * 2**20),
        name="attention",
    )(x, wp, tl, wo, tb, cosine, sine, pos[:, None], pos[None, :])


def sum_block(dst, srcs, rows=32):
    n, r, wd = dst.shape

    def step(i, _):
        a = pl.ds(pl.multiple_of(i % (r // rows) * rows, rows), rows)
        j = i // (r // rows)
        total = srcs[0][j, a, :].astype(jnp.float32)
        for s in srcs[1:]:
            total = total + s[j, a, :].astype(jnp.float32)
        dst[j, a, :] = total.astype(dst.dtype)
        return 0

    lax.fori_loop(0, n * (r // rows), step, 0)


def spill_sum_steps(w, zs, x_ref, o_ref, r0, r1, r2, ral, rar, stage, out, fin, ls, s0, q0, s1, q1, s2, q2, szr, szl, rzr, rzl, sf):
    f, c, z, k = place_of()
    half = o_ref.shape[1] // 2
    sib = (f, c + 1 - 2 * k)
    b1 = 2 - k
    b2 = 1 + k
    f1 = flip(f, b1)
    f2 = flip(f, b2)
    f3 = flip(f1, b2)
    cs = 2 * zs
    cols = [f3, f1, f2, f]
    order = far_first(z, zs)
    held = [None] * out.shape[0]
    count = [0]

    def src(col, zz, kk):
        return x_ref.at[pl.ds(col * cs + 2 * zz, 2), :, pl.ds(pl.multiple_of(kk * half, 128), half)]

    for zz in order:
        for ci in range(4):
            slot = {0: 0, 1: 2, 2: 1, 3: 3}[ci] * zs + zz
            w.send(src(cols[ci], zz, 1 - k), r0.at[slot], s0.at[slot], q0.at[slot], sib)
    yield

    def load(i, ref, when=None):
        copy = pltpu.make_async_copy(ref, stage.at[i], ls.at[i])
        if when is None:
            copy.start()
        else:
            pl.when(when)(copy.start)
        return copy

    def slot_for():
        i = count[0] % len(held)
        count[0] += 1
        if held[i] is not None:
            w.settle(held[i])
        return i

    def base(ci, zz):
        got(r0.at[ci * zs + zz], s0.at[ci * zs + zz], q0.at[ci * zs + zz], sib)
        loads = [load(0, src(cols[ci], zz, k)), load(1, r0.at[ci * zs + zz])]
        if ci >= 2:
            m = (ci - 2) * zs + zz
            got(r1.at[m], s1.at[m], q1.at[m], (f1, c))
            loads.append(load(2, r1.at[m]))
        if ci == 3:
            got(r2.at[zz], s2.at[zz], q2.at[zz], (f2, c))
            loads.append(load(3, r2.at[zz]))
        return loads

    def total(loads):
        i = slot_for()
        for copy in loads:
            copy.wait()
        sum_block(out.at[i], [stage.at[j] for j in range(len(loads))])
        return i

    def plane(ci, zz):
        loads = base(ci, zz)
        yield
        i = total(loads)
        if ci < 2:
            m = ci * zs + zz
            held[i] = [w.send(out.at[i], r1.at[m], s1.at[m], q1.at[m], (f1, c))]
        else:
            held[i] = [w.send(out.at[i], r2.at[zz], s2.at[zz], q2.at[zz], (f2, c))]
        yield

    def line(zz):
        loads = base(3, zz)
        right = zz > z
        from_left = jnp.logical_and(right, z > 0)
        from_right = jnp.logical_and(jnp.logical_not(right), z < zs - 1)
        got(ral.at[zz], szr.at[zz], rzr.at[zz], (f, c), from_left)
        got(rar.at[zz], szl.at[zz], rzl.at[zz], (f, c), from_right)
        more = [load(4, ral.at[zz], from_left), load(4, rar.at[zz], from_right)]
        yield
        i = total(loads)
        for copy, when in zip(more, (from_left, from_right)):
            pl.when(when)(copy.wait)

            @pl.when(when)
            def _(i=i):
                add_into(out.at[i], stage.at[4])

        held[i] = [
            w.send(out.at[i], ral.at[zz], szr.at[zz], rzr.at[zz], (f, c + 2), right),
            w.send(out.at[i], rar.at[zz], szl.at[zz], rzl.at[zz], (f, c - 2), jnp.logical_not(right)),
        ]
        yield

    for i in range(zs + 2):
        if i < zs:
            for ci in (0, 1):
                yield from plane(ci, order[i])
        if 1 <= i <= zs:
            yield from plane(2, order[i - 1])
        if 2 <= i <= zs:
            yield from line(order[i - 2])
    loads = base(3, z)
    got(ral.at[z], szr.at[z], rzr.at[z], (f, c), z > 0)
    more = load(4, ral.at[z], z > 0)
    yield
    i = total(loads)
    pl.when(z > 0)(more.wait)

    @pl.when(z > 0)
    def _():
        add_into(out.at[i], stage.at[4])

    got(rar.at[z], szl.at[z], rzl.at[z], (f, c), z < zs - 1)
    more = load(4, rar.at[z], z < zs - 1)
    pl.when(z < zs - 1)(more.wait)

    @pl.when(z < zs - 1)
    def _():
        add_into(out.at[i], stage.at[4])

    w.send(out.at[i, 1 - k], fin, sf.at[0], sf.at[1], sib)
    o_ref[:, pl.ds(pl.multiple_of(k * half, 128), half)] = out[i, k]
    yield
    got(fin, sf.at[0], sf.at[1], sib)
    o_ref[:, pl.ds(pl.multiple_of((1 - k) * half, 128), half)] = fin[...]
    yield


def head_sum_steps(w, nf, nc, hp, g, o_ref, ga, gb, loc, sg, rg, so, ro):
    f, c, z, k = place_of()
    hr = g.shape[1] // 2
    parts = []
    for p in (0, 1):
        mm = (lambda d: flip(d, 2)) if p else (lambda d: d)
        fa = flip(f, 1 + p)
        fb = flip(f, 2 - p)
        parts.append((p, pl.ds(p * hr, hr), mm, fa, fb, flip(fa, 2 - p)))
    for p, at, mm, fa, fb, fc in parts:
        for i, d in enumerate((fc, fa)):
            w.send(g.at[mm(d), at], ga.at[p, i], sg.at[p, i], rg.at[p, i], (fa, c))
    yield
    for p, at, mm, fa, fb, fc in parts:
        for i, d in enumerate((fb, f)):
            got(ga.at[p, i], sg.at[p, i], rg.at[p, i], (fa, c))
            add_into(g.at[pl.ds(mm(d), 1), at], ga.at[p, pl.ds(i, 1)])
            if i == 0:
                w.send(g.at[mm(fb), at], gb.at[p], sg.at[p, 2], rg.at[p, 2], (fb, c))
    yield
    for p, at, mm, fa, fb, fc in parts:
        got(gb.at[p], sg.at[p, 2], rg.at[p, 2], (fb, c))
        add_into(g.at[pl.ds(mm(f), 1), at], gb.at[pl.ds(p, 1)])
        head = hp * c + mm(f)
        df, dc = head // nc, head % nc
        stay = jnp.logical_and(df == f, dc == c)
        w.send(g.at[mm(f), at], o_ref.at[at], so.at[p], ro.at[p], (df, dc), jnp.logical_not(stay))
        keep = pltpu.make_async_copy(g.at[mm(f), at], o_ref.at[at], loc.at[p])
        pl.when(stay)(keep.start)
        pl.when(stay)(keep.wait)
    yield
    for p, at, mm, fa, fb, fc in parts:
        head = f * nc + c
        here = jnp.logical_and(head // hp == c, mm(head % hp) == f)
        got(o_ref.at[at], so.at[p], ro.at[p], (f, c), jnp.logical_not(here))
    yield


def weight_sum_steps(w, nf, nc, g, o_ref, ga, gb, sg, rg, sa, ra):
    f, c, z, k = place_of()
    hc = nc // 2
    parts = []
    for p in (0, 1):
        fa = flip(f, 1 + p)
        fb = flip(f, 2 - p)
        parts.append((p, pl.ds(p * hc, hc), fa, fb, flip(fa, 2 - p)))
    for p, at, fa, fb, fc in parts:
        for i, col in enumerate((fc, fa)):
            w.send(g.at[col, at], ga.at[p, i], sg.at[2 * p + i], rg.at[2 * p + i], (fa, c))
    yield
    for p, at, fa, fb, fc in parts:
        for i, col in enumerate((fb, f)):
            got(ga.at[p, i], sg.at[2 * p + i], rg.at[2 * p + i], (fa, c))
            add_into(g.at[col, at], ga.at[p, i])
            if i == 0:
                w.send(g.at[fb, at], gb.at[p], sg.at[4 + p], rg.at[4 + p], (fb, c))
    yield
    for p, at, fa, fb, fc in parts:
        got(gb.at[p], sg.at[4 + p], rg.at[4 + p], (fb, c))
        add_into(g.at[f, at], gb.at[p])
    for i in range(1, nc):
        cc = (c + i) % nc
        w.send(g.at[f, cc], o_ref.at[c], sa.at[cc], ra.at[c], (f, cc))
    o_ref[c] = g[f, c]
    yield
    for i in range(1, nc):
        cc = (c + i) % nc
        got(o_ref.at[cc], sa.at[cc], ra.at[cc], (f, c))
    yield


def expert_grad_steps(arr, garr, hid, ggp, gup, ogate, oup, odown, big, blk, flat, tall, lbig, lblk, lout):
    width = arr.shape[1]
    nb = width // 256
    f32 = jnp.float32

    def job(whole, src, dst, down):
        fill = pltpu.make_async_copy(whole, big, lbig)
        cols = lambda j: pl.ds(pl.multiple_of(j * 256, 256), 256)
        block = lambda j: pltpu.make_async_copy(src.at[:, cols(j)], blk.at[j % 2], lblk.at[j % 2])
        held = tall if down else flat
        put = lambda j: pltpu.make_async_copy(held.at[j % 2], dst.at[:, cols(j)] if down else dst.at[cols(j)], lout.at[j % 2])

        def step(j, _):
            @pl.when(j + 1 < nb)
            def _():
                block(j + 1).start()

            block(j).wait()

            @pl.when(j > 1)
            def _():
                put(j - 2).wait()

            left, right = (big[...], blk[j % 2]) if down else (blk[j % 2], big[...])
            held[j % 2] = lax.dot_general(left, right, (((0,), (0,)), ((), ())), preferred_element_type=f32).astype(held.dtype)
            put(j).start()
            return 0

        fill.start()
        block(0).start()
        fill.wait()
        lax.fori_loop(0, nb // 2, step, 0)
        yield
        lax.fori_loop(nb // 2, nb, step, 0)
        for j in (nb - 2, nb - 1):
            put(j).wait()
        yield

    yield from job(ggp, arr, ogate, False)
    yield from job(gup, arr, oup, False)
    yield from job(hid, garr, odown, True)


def grad_kernel(nf, zs, hp, scale, refs):
    (res_ref, nm_ref, w_ref, wo_ref, qp_ref, kp_ref, qr_ref, kr_ref, v_ref, ctx_ref, lse_ref, cos_ref, sin_ref, pr_ref, pc_ref,
     gqk_ref, gat_ref, moe_ref, mix_ref, arr, garr, hid, ggp, gup,
     out_ref, go_ref, gwo_ref, to_ref, mixed_ref, ogate, oup, odown, h0, h1, h2, hl, hr,
     res, gkv, gkv2, gcat, gw, gwo, tl, gqk, gat, loc, sl, szr, szl, rz, ssib, rsib, sk) = refs[:54]
    rest = list(refs[54:])

    def take(n):
        part = rest[:n]
        del rest[:n]
        return part

    tile_b = take(5)
    sum_bufs = take(13)
    spill_bufs = take(15)
    head_b = take(7)
    weight_b = take(6)
    expert_b = take(7)
    expert_steps = expert_grad_steps(arr, garr, hid, ggp, gup, ogate, oup, odown, *expert_b)
    f, c, z, k = place_of()
    nc = 2 * zs
    rows, width = res_ref.shape
    half = width // 2
    hd = kr_ref.shape[1]
    qw = hp * hd
    span = nc * rows
    f32, bf16 = jnp.float32, jnp.bfloat16
    sib_c = c + 1 - 2 * k
    sib = (f, sib_c)
    first = k == 0

    def chunk(zz, kk):
        return res.at[pl.ds(2 * zz, 2), :, pl.ds(pl.multiple_of(kk * half, 128), half)]

    own = pltpu.make_async_copy(res_ref, res.at[c], loc)
    own.start()
    with jax.named_scope("greet"):
        greet_cross(f, c, nf, nc)
    w = Wire()
    w.send(res_ref, res.at[c], sl.at[0], sl.at[1], sib)
    mix_steps = spill_sum_steps(w, zs, mix_ref, mixed_ref, h0, h1, h2, hl, hr, *spill_bufs)
    own.wait()
    got(res.at[sib_c], sl.at[0], sl.at[1], sib)
    w.send(chunk(z, k), chunk(z, k), szr.at[z], rz.at[z], (f, c + 2), z < zs - 1)
    w.send(chunk(z, k), chunk(z, k), szl.at[z], rz.at[z], (f, c - 2), z > 0)
    advance(mix_steps, "mix")
    gkv[...] = jnp.zeros_like(gkv)
    gqk[...] = jnp.zeros_like(gqk)
    gat[...] = jnp.zeros_like(gat)
    gq, gk = gqk_ref[0:1, :], gqk_ref[1:2, :]
    low_half = lax.broadcasted_iota(jnp.int32, (1, hd), 1) < hd // 2
    lane = lax.broadcasted_iota(jnp.int32, (1, hd), 1)

    def turned_back(t, g, grad, at):
        u = grad * sin_ref[at, :]
        other = pltpu.roll(u, hd // 2, 1)
        gy = grad * cos_ref[at, :] + jnp.where(low_half, other, -other)
        r = lax.rsqrt(jnp.mean(t * t, axis=-1, keepdims=True) + EPSILON)
        n = t * r
        gn = gy * g
        back = r * (gn - n * jnp.mean(gn * n, axis=-1, keepdims=True))
        return back, jnp.sum(gy * n, axis=0, keepdims=True)

    def process(zz):
        at = pl.ds(pl.multiple_of(2 * zz * rows, 2 * rows), 2 * rows)
        rr = res[pl.ds(2 * zz, 2)].reshape(2 * rows, width)

        def head(h, _):
            hc = pl.ds(pl.multiple_of(h * hd, hd), hd)
            g = lax.dot_general(rr, wo_ref[h], (((1,), (1,)), ((), ())), preferred_element_type=f32).astype(bf16)
            q = qr_ref[at, hc]
            s = lax.dot_general(q, kr_ref[...], (((1,), (1,)), ((), ())), preferred_element_type=f32) * scale
            lse = jnp.sum(jnp.where(lane == h, lse_ref[at, :], 0.0), axis=-1, keepdims=True)
            p = jnp.where(pc_ref[...] <= pr_ref[at, :], jnp.exp(s - lse), 0.0)
            gkv[1] += lax.dot_general(p.astype(bf16), g, (((0,), (0,)), ((), ())), preferred_element_type=f32)
            gp = lax.dot_general(g, v_ref[...], (((1,), (1,)), ((), ())), preferred_element_type=f32)
            delta = jnp.sum(g.astype(f32) * ctx_ref[at, hc].astype(f32), axis=-1, keepdims=True)
            ds = (p * (gp - delta)).astype(bf16)
            gkv[0] += lax.dot_general(ds, q, (((0,), (0,)), ((), ())), preferred_element_type=f32) * scale
            gr = jnp.dot(ds, kr_ref[...], preferred_element_type=f32) * scale
            back, gain = turned_back(qp_ref[at, hc], gq, gr, at)
            gcat[at, hc] = back.astype(bf16)
            gqk[0:1, :] += gain
            return 0

        with jax.named_scope("process"):
            lax.fori_loop(0, hp, head, 0)

    def mix(count):
        for _ in range(count):
            advance(mix_steps, "mix")

    near = far_first(z, zs)[::-1]
    mix(8)
    process(near[0])
    counts = [(2, 4)] + [(2, 2)] * (zs - 3) + [(4, 2)]
    for h in range(1, zs):
        sides = (
            (z - h, z - h >= 0, z < zs - 1, 2, szr),
            (z + h, z + h < zs, z > 0, -2, szl),
        )
        with jax.named_scope("hop"):
            for zz, when, on, dz, sem in sides:
                got(chunk(zz, k), sem.at[zz], rz.at[zz], (f, c), when)
                w.send(chunk(zz, k), chunk(zz, k), sem.at[zz], rz.at[zz], (f, c + dz), jnp.logical_and(when, on))
                w.send(chunk(zz, k), chunk(zz, k), ssib.at[zz], rsib.at[zz], sib, when)
        mix(counts[h - 1][0])
        with jax.named_scope("rest"):
            for zz, when, *_ in sides:
                got(chunk(zz, 1 - k), ssib.at[zz], rsib.at[zz], sib, when)
        process(near[h])
        mix(counts[h - 1][1])
    w.send(gkv, gkv2, sk.at[0], sk.at[1], sib)

    with jax.named_scope("gwo"):
        def gwo_block(j, _):
            cols = pl.ds(pl.multiple_of(j * 256, 256), 256)
            r = res[:, :, cols].reshape(span, 256)
            o = lax.dot_general(ctx_ref[...], r, (((0,), (0,)), ((), ())), preferred_element_type=f32).astype(bf16)
            gwo[:, :, cols] = o.reshape(hp, hd, 256)
            return 0

        lax.fori_loop(0, width // 256, gwo_block, 0)
    head_steps = head_sum_steps(w, nf, nc, hp, gwo, gwo_ref, *head_b)
    advance(head_steps, "heads")
    advance(expert_steps, "expert")
    with jax.named_scope("kv"):
        got(gkv2, sk.at[0], sk.at[1], sib)

        def keys(i, _):
            at = pl.ds(pl.multiple_of(i * 2 * rows, 2 * rows), 2 * rows)
            back, gain = turned_back(kp_ref[at, :], gk, gkv[0, at, :] + gkv2[0, at, :], at)
            gv = gkv[1, at, :] + gkv2[1, at, :]
            gcat[at, pl.ds(qw, hd)] = jnp.where(first, back, gv).astype(bf16)
            gqk[1:2, :] += jnp.where(first, gain, 0.0)
            return 0

        lax.fori_loop(0, zs, keys, 0)
    t, u = sum_bufs[0], sum_bufs[1]

    def make(zz):
        at = pl.ds(pl.multiple_of(2 * zz * rows, 2 * rows), 2 * rows)
        a = gcat[at, 0:qw]
        b = gcat[at, qw : qw + hd]
        for dst, kk in ((u, 1 - k), (t, k)):
            def block(j, _, dst=dst, kk=kk):
                slabs = pl.ds(kk * (half // 64) + j * 8, 8)
                wq = w_ref[slabs, :, 0:qw].reshape(512, qw)
                wk = w_ref[slabs, :, pl.ds(pl.multiple_of(qw + k * hd, hd), hd)].reshape(512, hd)
                o = lax.dot_general(a, wq, (((1,), (1,)), ((), ())), preferred_element_type=f32)
                o = o + lax.dot_general(b, wk, (((1,), (1,)), ((), ())), preferred_element_type=f32)
                cols = pl.ds(pl.multiple_of(kk * half + j * 512, 512), 512)
                gat[:, cols] += jnp.sum(o * nm_ref[at, cols].astype(f32), axis=0, keepdims=True)
                dst[zz, :, :, pl.ds(pl.multiple_of(j * 512, 512), 512)] = o.astype(bf16).reshape(2, rows, 512)
                return 0

            lax.fori_loop(0, half // 512, block, 0)

    sum_steps = line_sum_steps(w, zs, make, out_ref, *sum_bufs)
    for _ in range(2):
        advance(sum_steps, "sum")
    advance(expert_steps, "expert")
    advance(head_steps, "heads")
    with jax.named_scope("gw"):
        def gw_block(j, _):
            cols = pl.ds(pl.multiple_of(j * 256, 256), 256)
            o = lax.dot_general(nm_ref[:, cols], gcat[...], (((0,), (0,)), ((), ())), preferred_element_type=f32).astype(bf16)
            gw[j // 2, pl.ds(j % 2 * 4, 4)] = o.reshape(4, 64, qw + hd)
            return 0

        lax.fori_loop(0, width // 256, gw_block, 0)
    weight_steps = weight_sum_steps(w, nf, nc, gw, go_ref, *weight_b)
    advance(weight_steps, "weights")
    small_steps = None
    for turn in "smsmsmsm+smgwmgmghmgwmsmtm":
        if turn == "+":
            for cc in range(nc):
                for ff in range(nf):
                    lanes = pl.ds(128 * ((ff * nc + cc) // 2), 128)
                    tl[cc, ff, 0:1, :] = gat[:, lanes] / gat_ref[:, lanes]
                    tl[cc, ff, 1:2, :] = moe_ref[:, lanes]
                    tl[cc, ff, 2:4, :] = gqk[...]
                    tl[cc, ff, 4:8, :] = jnp.zeros((4, hd), f32)
            small_steps = tile_steps(w, nf, nc, tl, to_ref, *tile_b)
            advance(small_steps, "tiles")
        else:
            name = {"s": "sum", "w": "weights", "h": "heads", "m": "mix", "t": "tiles", "g": "expert"}[turn]
            steps = {"s": sum_steps, "w": weight_steps, "h": head_steps, "m": mix_steps, "t": small_steps, "g": expert_steps}
            advance(steps[turn], name)
    for name, steps in (("sum", sum_steps), ("heads", head_steps), ("mix", mix_steps), ("weights", weight_steps), ("tiles", small_steps), ("expert", expert_steps)):
        while advance(steps, name):
            pass
    w.drain()


def gradients(res, nm, wcat, wo, qp, kp, qr, kr, v, ctx, lse, cosine, sine, pos, gqk, gat, moe, mix, experts, nf, zs, hp, scale, cid):
    rows, width = res.shape
    nc = 2 * zs
    span = nc * rows
    hd = cosine.shape[1]
    bf16, f32 = jnp.bfloat16, jnp.float32
    D = pltpu.SemaphoreType.DMA
    S = jax.ShapeDtypeStruct
    half = width // 2
    cols = hp * hd + hd
    shard = wcat.shape[1]
    slots, ff = experts[2].shape
    spill = lambda n: (S((n, 2, rows, half), bf16), ANY)
    outs = [
        (S((rows, width), bf16), VM),
        (S((nc, shard, cols), bf16), VM),
        (S((hd, width), bf16), VM),
        (S((nf * nc, 8, hd), f32), VM),
        (S((rows, width), bf16), VM),
        (S((width, ff), bf16), ANY),
        (S((width, ff), bf16), ANY),
        (S((ff, width), bf16), ANY),
        spill(4 * zs), spill(2 * zs), spill(zs), spill(zs), spill(zs),
    ]
    V = pltpu.VMEM
    chunk = (2, rows, half)
    scratch = [V((nc, rows, width), bf16), V((2, span, hd), f32), V((2, span, hd), f32), V((span, cols), bf16),
               V((nf, nc, shard, cols), bf16), V((hp, hd, width), bf16), V((nc, nf, 8, hd), f32), V((2, hd), f32), V((1, width), f32),
               D(()), D((2,)), D((zs,)), D((zs,)), D((zs,)), D((zs,)), D((zs,)), D((2,))]
    scratch += tile_bufs(nf, nc, (8, hd)) + line_sum_bufs(zs, rows, half, bf16)
    scratch += [V((5,) + chunk, bf16), V((3,) + chunk, bf16), V((rows, half), bf16), D((5,)), D((4 * zs,)), D((4 * zs,)), D((2 * zs,)), D((2 * zs,)),
                D((zs,)), D((zs,)), D((zs,)), D((zs,)), D((zs,)), D((zs,)), D((2,))]
    scratch += [V((2, 2, hd // 2, width), bf16), V((2, hd // 2, width), bf16), D((2,)), D((2, 3)), D((2, 3)), D((2,)), D((2,))]
    scratch += [V((2, 2, nc // 2, shard, cols), bf16), V((2, nc // 2, shard, cols), bf16), D((6,)), D((6,)), D((nc,)), D((nc,))]
    scratch += [V((slots, ff), bf16), V((2, slots, 256), bf16), V((2, 256, ff), bf16), V((2, ff, 256), bf16), D(()), D((2,)), D((2,))]
    return pl.pallas_call(
        lambda *refs: grad_kernel(nf, zs, hp, scale, refs),
        out_shape=[s for s, _ in outs],
        in_specs=[VM] * 18 + [ANY] * 6,
        out_specs=[b for _, b in outs],
        scratch_shapes=scratch,
        compiler_params=pltpu.CompilerParams(collective_id=cid, has_side_effects=True, vmem_limit_bytes=62 * 2**20),
        name="gradients",
    )(res, nm, wcat, wo, qp, kp, qr, kr, v, ctx, lse, cosine, sine, pos[:, None], pos[None, :], gqk, gat, moe, mix, *experts)


def flip_if(f, bit, when):
    return jnp.where(when, flip(f, bit), f)


def expert_kernel(nf, zs, refs):
    (tok, top, place, mixing, wg, wu, wd,
     out_ref, shares, arr, garr, hid, ggp, gup,
     tb, cb, a, g, rows_b, t, u, r0, r1, r2, ral, rar, fin, sh,
     lt, lc, la, lg, ls, s0, q0, s1, q1, s2, q2, szr, szl, rzr, rzl, sf) = refs
    f, c, z, k = place_of()
    nc = 2 * zs
    rows, width = tb.shape[2:]
    half = width // 2
    cap = place.shape[1]
    per = nf * cap
    f32, bf16 = jnp.float32, jnp.bfloat16
    sib = (f, c + 1 - 2 * k)
    f1 = flip(f, 2 - k)
    f2 = flip(f, 1 + k)
    order = far_first(z, zs)
    with jax.named_scope("greet"):
        greet(f, c, z, zs, True)
    w = Wire()

    def col_of(ci):
        return flip_if(flip_if(f, 1, ci < 2), 2, (ci % 2) == 0)

    def fetch(zz, ci, slot):
        two = pl.ds(col_of(ci) * nc + 2 * zz, 2)
        return (
            pltpu.make_async_copy(tok.at[two], tb.at[slot], lt.at[slot]),
            pltpu.make_async_copy(top.at[two], cb.at[slot], lc.at[slot]),
        )

    def compute(gi):
        zz = order[gi]
        for copy in fetch(zz, 0, 0):
            copy.start()
        if gi:
            for copy in keep:
                copy.wait()

        def pick(ci, _):
            slot = ci % 2

            @pl.when(ci < nf - 1)
            def _():
                for copy in fetch(zz, ci + 1, 1 - slot):
                    copy.start()

            for copy in fetch(zz, ci, slot):
                copy.wait()
            at = pl.ds(pl.multiple_of(ci * cap, 16), cap)
            chip = col_of(ci) * zs + zz
            a[at, :] = jnp.dot(place[chip], tb[slot].reshape(2 * rows, width), preferred_element_type=f32).astype(bf16)
            g[at, :] = jnp.dot(mixing[chip], cb[slot].reshape(2 * rows, width), preferred_element_type=f32).astype(bf16)
            return 0

        with jax.named_scope("pick"):
            lax.fori_loop(0, nf, pick, 0)
        mine = pl.ds(gi * per, per)
        keep[:] = [pltpu.make_async_copy(a, arr.at[mine], la), pltpu.make_async_copy(g, garr.at[mine], lg)]
        for copy in keep:
            copy.start()

        def hidden(j, _):
            cc = pl.ds(pl.multiple_of(j * 256, 256), 256)
            gate = jnp.dot(a[...], wg[:, cc], preferred_element_type=f32)
            up = jnp.dot(a[...], wu[:, cc], preferred_element_type=f32)
            back = lax.dot_general(g[...], wd[cc, :], (((1,), (1,)), ((), ())), preferred_element_type=f32)
            sig = jax.nn.sigmoid(gate)
            act = gate * sig
            hid[mine, cc] = (act * up).astype(bf16)
            ggp[mine, cc] = (back * up * sig * (1.0 + gate * (1.0 - sig))).astype(bf16)
            gup[mine, cc] = (back * act).astype(bf16)
            return 0

        with jax.named_scope("hidden"):
            lax.fori_loop(0, wg.shape[1] // 256, hidden, 0)

        def rows_of(j, _):
            cc = pl.ds(pl.multiple_of(j * 256, 256), 256)
            o = lax.dot_general(ggp[mine, :], wg[cc, :], (((1,), (1,)), ((), ())), preferred_element_type=f32)
            o = o + lax.dot_general(gup[mine, :], wu[cc, :], (((1,), (1,)), ((), ())), preferred_element_type=f32)
            rows_b[:, cc] = o.astype(bf16)
            return 0

        with jax.named_scope("rows"):
            lax.fori_loop(0, width // 256, rows_of, 0)

        def spread(ci, _):
            at = pl.ds(pl.multiple_of(ci * cap, 16), cap)
            p = place[col_of(ci) * zs + zz]
            for dst, kk in ((u.at[gi % 2, ci], 1 - k), (t.at[ci * zs + zz], k)):
                r = rows_b[at, pl.ds(pl.multiple_of(kk * half, 128), half)]
                o = lax.dot_general(p, r, (((0,), (0,)), ((), ())), preferred_element_type=f32)
                dst[...] = o.astype(bf16).reshape(2, rows, half)
            return 0

        if gi >= 2:
            w.settle(passed[gi - 2])
        with jax.named_scope("spread"):
            lax.fori_loop(0, nf, spread, 0)
        passed.append([])
        for ci in range(nf):
            m = ci * zs + zz
            passed[gi].append(w.send(u.at[gi % 2, ci], r0.at[m], s0.at[m], q0.at[m], sib))

    def pair(m):
        got(r0.at[m], s0.at[m], q0.at[m], sib)
        add_into(t.at[m], r0.at[m])

    def stage_one(zz):
        for i, m in ((0, zz), (1, (2 - k) * zs + zz)):
            pair(m)
            w.send(t.at[m], r1.at[i * zs + zz], s1.at[i * zs + zz], q1.at[i * zs + zz], (f1, c))

    def stage_two(zz):
        m = (1 + k) * zs + zz
        pair(m)
        got(r1.at[zz], s1.at[zz], q1.at[zz], (f1, c))
        add_into(t.at[m], r1.at[zz])
        w.send(t.at[m], r2.at[zz], s2.at[zz], q2.at[zz], (f2, c))

    def give(gi):
        zz = order[gi]
        at = pl.ds(gi * per, per)

        def out_of(j, _):
            cc = pl.ds(pl.multiple_of(j * 256, 256), 256)
            rows_b[:, cc] = jnp.dot(hid[at, :], wd[:, cc], preferred_element_type=f32).astype(bf16)
            return 0

        lax.fori_loop(0, width // 256, out_of, 0)

        def one(ci, _):
            slot = ci % 2
            there = lambda cj: pltpu.make_async_copy(sh.at[slot], shares.at[pl.ds(col_of(cj) * nc + 2 * zz, 2)], ls.at[slot])

            @pl.when(ci > 1)
            def _():
                there(ci - 2).wait()

            e = rows_b[pl.ds(pl.multiple_of(ci * cap, 16), cap), :]
            o = lax.dot_general(mixing[col_of(ci) * zs + zz], e, (((0,), (0,)), ((), ())), preferred_element_type=f32)
            sh[slot] = o.astype(bf16).reshape(2, rows, width)
            there(ci).start()
            return 0

        lax.fori_loop(0, nf, one, 0)
        for ci in (nf - 2, nf - 1):
            pltpu.make_async_copy(sh.at[ci % 2], shares.at[pl.ds(col_of(ci) * nc + 2 * zz, 2)], ls.at[ci % 2]).wait()

    base = 3 * zs

    def complete(zz):
        pair(base + zz)
        got(r1.at[zs + zz], s1.at[zs + zz], q1.at[zs + zz], (f1, c))
        add_into(t.at[base + zz], r1.at[zs + zz])
        got(r2.at[zz], s2.at[zz], q2.at[zz], (f2, c))
        add_into(t.at[base + zz], r2.at[zz])

    edge = jnp.logical_or(z == 0, z == zs - 1)

    def onward(zz, when):
        right = zz > z
        w.send(t.at[base + zz], ral.at[zz], szr.at[zz], rzr.at[zz], (f, c + 2), jnp.logical_and(when, right))
        w.send(t.at[base + zz], rar.at[zz], szl.at[zz], rzl.at[zz], (f, c - 2), jnp.logical_and(when, jnp.logical_not(right)))

    def stage_line(zz):
        complete(zz)
        onward(zz, edge)

    def stage_relay(zz):
        inner = jnp.logical_not(edge)
        from_left = jnp.logical_and(inner, zz > z)
        from_right = jnp.logical_and(inner, zz < z)
        with jax.named_scope("line"):
            got(ral.at[zz], szr.at[zz], rzr.at[zz], (f, c), from_left)
            got(rar.at[zz], szl.at[zz], rzl.at[zz], (f, c), from_right)

        @pl.when(from_left)
        def _():
            add_into(t.at[base + zz], ral.at[zz])

        @pl.when(from_right)
        def _():
            add_into(t.at[base + zz], rar.at[zz])

        onward(zz, inner)

    keep, passed = [], []
    for gi in range(zs):
        compute(gi)
        with jax.named_scope("one"):
            stage_one(order[gi])
        if gi >= 1:
            with jax.named_scope("two"):
                stage_two(order[gi - 1])
        if gi >= 3:
            stage_relay(order[gi - 3])
        if gi >= 2:
            with jax.named_scope("three"):
                stage_line(order[gi - 2])
    for copy in keep:
        copy.wait()
    with jax.named_scope("give"):
        give(0)
    with jax.named_scope("two"):
        stage_two(z)
    stage_relay(order[zs - 3])
    with jax.named_scope("three"):
        stage_line(order[zs - 2])
    for gi in range(1, zs):
        with jax.named_scope("give"):
            give(gi)
        if gi == 1:
            stage_relay(order[zs - 2])
            with jax.named_scope("complete"):
                complete(z)
    with jax.named_scope("line"):
        got(ral.at[z], szr.at[z], rzr.at[z], (f, c), z > 0)
        got(rar.at[z], szl.at[z], rzl.at[z], (f, c), z < zs - 1)

    @pl.when(z > 0)
    def _():
        add_into(t.at[base + z], ral.at[z])

    @pl.when(z < zs - 1)
    def _():
        add_into(t.at[base + z], rar.at[z])

    w.send(t.at[base + z, 1 - k], fin, sf.at[0], sf.at[1], sib)
    out_ref[:, pl.ds(pl.multiple_of(k * half, 128), half)] = t[base + z, k]
    got(fin, sf.at[0], sf.at[1], sib)
    out_ref[:, pl.ds(pl.multiple_of((1 - k) * half, 128), half)] = fin[...]
    w.drain()


def experts_of(tokens, top, place, mixing, wg, wu, wd, nf, zs, cid):
    n, rows, width = tokens.shape
    slots = place.shape[0] * place.shape[1]
    per = slots // zs
    ff = wg.shape[1]
    half = width // 2
    bf16 = jnp.bfloat16
    S = jax.ShapeDtypeStruct
    D = pltpu.SemaphoreType.DMA
    V = lambda *s: pltpu.VMEM(s, bf16)
    C = lambda *m: pltpu.VMEM(m + (2, rows, half), bf16)
    outs = [
        (S((rows, width), bf16), VM),
        (S((n, rows, width), bf16), ANY),
        (S((slots, width), bf16), ANY),
        (S((slots, width), bf16), ANY),
        (S((slots, ff), bf16), VM),
        (S((slots, ff), bf16), VM),
        (S((slots, ff), bf16), VM),
    ]
    scratch = [V(2, 2, rows, width), V(2, 2, rows, width), V(per, width), V(per, width), V(per, width),
               C(nf * zs), C(2, nf), C(nf * zs), C(2 * zs), C(zs), C(zs), C(zs), V(rows, half), V(2, 2, rows, width),
               D((2,)), D((2,)), D(()), D(()), D((2,)), D((nf * zs,)), D((nf * zs,)), D((2 * zs,)), D((2 * zs,)), D((zs,)), D((zs,)),
               D((zs,)), D((zs,)), D((zs,)), D((zs,)), D((2,))]
    return pl.pallas_call(
        lambda *refs: expert_kernel(nf, zs, refs),
        out_shape=[s for s, _ in outs],
        in_specs=[ANY, ANY] + [VM] * 5,
        out_specs=[b for _, b in outs],
        scratch_shapes=scratch,
        compiler_params=pltpu.CompilerParams(collective_id=cid, has_side_effects=True, vmem_limit_bytes=62 * 2**20),
        name="experts",
    )(tokens, top, place, mixing, wg, wu, wd)


def head_body(
    nf,
    nc,
    block_input,
    cotangent,
    gain_attn,
    w_query,
    w_key,
    w_value,
    qk_gain,
    w_out,
    gain_moe,
    w_gate,
    w_up,
    w_down,
    expert_ids,
    route_weight,
    pair_order,
):
    bf16, f32 = jnp.bfloat16, jnp.float32
    f, c, z, k = place_of()
    n = nf * nc
    zs = nc // 2
    rows, width = block_input.shape[1:]
    hd = qk_gain.shape[1] * n
    kv_heads = w_key.shape[1] // hd
    heads = w_query.shape[1] // hd
    hp = heads // nc
    shard = w_query.shape[0]
    topk = expert_ids.shape[2]
    capacity = max(2, 3 * BLOCK * topk // n)
    span = nc * rows
    scale = 1.0 / math.sqrt(hd)
    x_own = block_input[0]
    resid = x_own.astype(f32)

    ids, weights = expert_ids[0], route_weight[0].astype(f32)
    named = ids[None, :, :] == jnp.arange(n, dtype=jnp.int32)[:, None, None]
    to_expert = jnp.sum(jnp.where(named, weights[None], 0.0), axis=-1)
    lane = jnp.arange(rows)
    gs = gain_attn.shape[0]
    me = f * nc + c
    spots = lane // gs == me % (rows // gs)
    gain_row = lambda g: jnp.where(spots, jnp.tile(g.astype(f32), rows // gs), 0.0)
    qs = qk_gain.shape[1]
    qk_row = lambda g: jnp.where(lane // qs == me, jnp.tile(g.astype(f32), rows // qs), 0.0)
    small = jnp.stack([gain_row(gain_attn), qk_row(qk_gain[0]), qk_row(qk_gain[1]), gain_row(gain_moe)])
    tiles = jnp.concatenate([to_expert[:, None], jnp.broadcast_to(small, (n,) + small.shape), jnp.zeros((n, 3, rows), f32)], axis=1)
    by_place = lambda t: t.reshape((nf, nc) + t.shape[1:]).swapaxes(0, 1)
    per = nc // kv_heads
    wq_p = w_query.reshape(shard, nc, hp * hd).transpose(1, 0, 2)
    wk_p = jnp.repeat(w_key.reshape(shard, kv_heads, hd).transpose(1, 0, 2), per, axis=0)
    wv_p = jnp.repeat(w_value.reshape(shard, kv_heads, hd).transpose(1, 0, 2), per, axis=0)
    packed = jnp.concatenate([wq_p, wk_p, wv_p], axis=2)
    top_own = cotangent[0]
    pair = pair_order[:, None, None]
    both = jnp.concatenate([pair, 2 * pair_order.shape[0] - 1 - pair], axis=1)
    pos = (both * BLOCK + jnp.arange(BLOCK, dtype=jnp.int32)).reshape(-1)
    freqs = THETA ** (-(jnp.arange(hd // 2, dtype=f32) * 2.0 / hd))
    angles = pos.astype(f32)[:, None] * freqs[None, :]
    cosine, sine = jnp.tile(jnp.cos(angles), (1, 2)), jnp.tile(jnp.sin(angles), (1, 2))
    (x_seq, normed_in, w_all, dealt, wo_all, top_all, q_pre, k_pre, query_rot, key_rot, values, context, lse, hidden_res, tokens) = attention(
        x_own, packed, by_place(tiles), w_out, top_own.astype(bf16), cosine, sine, pos, nf, zs, hp, scale, 0
    )
    qw = hp * hd
    full_row = lambda r: dealt[:, r].reshape(-1, rows // gs, rows).sum(axis=1).reshape(-1)
    g_attn, g_moe = full_row(1), full_row(4)
    g_qk = dealt[:, 2:4].sum(axis=0)
    route_w = dealt[:, 0, :]
    hit = route_w > 0.0
    below = (jnp.arange(rows)[:, None] < jnp.arange(rows)[None, :]).astype(f32)
    rank = jnp.dot(hit.astype(f32), below, preferred_element_type=f32).astype(jnp.int32)
    slot = (rank[:, None, :] == jnp.arange(capacity, dtype=jnp.int32)[None, :, None]) & hit[:, None, :]
    place = slot.astype(bf16)
    mixing = jnp.where(slot, route_w[:, None, :], 0.0).astype(bf16)
    gate_w, up_w, down_w = w_gate[0], w_up[0], w_down[0]
    def paired(table):
        two = table.reshape(n // 2, 2, capacity, rows)
        none = jnp.zeros((n // 2, capacity, rows), bf16)
        upper = jnp.concatenate([two[:, 0], none], axis=2)
        lower = jnp.concatenate([none, two[:, 1]], axis=2)
        return jnp.concatenate([upper, lower], axis=1)

    grad_mid, shares, arrived, grad_arrived, expert_hidden, grad_gate_pre, grad_up_pre = experts_of(
        tokens, top_all, paired(place), paired(mixing), gate_w, up_w, down_w, nf, zs, 3
    )
    grad_mid = grad_mid.astype(f32)

    _, mid_back = jax.vjp(rms_scale, hidden_res, g_moe)
    grad_res_mid, grad_moe_gain = mid_back(grad_mid)
    grad_res = top_own + grad_res_mid

    grad_in, grads, grad_wo, summed, mixed, grad_gate, grad_up, grad_down, *_ = gradients(
        grad_res.astype(bf16), normed_in, w_all, wo_all, q_pre, k_pre, query_rot, key_rot, values, context, lse, cosine, sine, pos,
        g_qk, g_attn[None], grad_moe_gain[None], shares, (arrived, grad_arrived, expert_hidden, grad_gate_pre, grad_up_pre),
        nf, zs, hp, scale, 4
    )
    block_output = (hidden_res + mixed.astype(f32)).astype(bf16)
    total = jnp.sum(summed, axis=0)
    part = lambda row, size: lax.dynamic_slice_in_dim(row, me * size % rows, size)
    own_attn_gain = part(total[0], gs)
    own_moe_gain = part(total[1], gs)
    own_qk = jnp.stack([part(total[2], qs), part(total[3], qs)])
    grad_wo = grad_wo.astype(f32)
    grad_wq = grads[:, :, :qw].transpose(1, 0, 2).reshape(shard, heads * hd).astype(f32)
    grad_kv = grads[:, :, qw:].reshape(kv_heads, per, shard, hd)
    grad_wk = grad_kv[:, 0].transpose(1, 0, 2).reshape(shard, kv_heads * hd).astype(f32)
    grad_wv = grad_kv[:, 1].transpose(1, 0, 2).reshape(shard, kv_heads * hd).astype(f32)
    _, in_back = jax.vjp(rms_scale, resid, g_attn)
    grad_input = grad_res + in_back(grad_in.astype(f32))[0]
    return (
        block_output[None],
        grad_input[None],
        own_attn_gain,
        grad_wq,
        grad_wk,
        grad_wv,
        own_qk,
        grad_wo,
        own_moe_gain,
        grad_gate[None].astype(f32),
        grad_up[None].astype(f32),
        grad_down[None].astype(f32),
    )


def body(nf, nc, block_input, *rest):
    kv_heads = rest[3].shape[1] // (rest[5].shape[1] * nf * nc)
    fits = nf == 4 and nc == 2 * kv_heads and rest[4].shape[1] == rest[3].shape[1]
    return head_body(nf, nc, block_input, *rest) if fits else wide_body(block_input, *rest)


def solution(mesh):
    return jax.shard_map(
        functools.partial(body, mesh.shape["fsdp"], mesh.shape["cp"]),
        mesh=mesh,
        in_specs=(
            P("fsdp", "cp", None),
            P("fsdp", "cp", None),
            P(("fsdp", "cp")),
            P(("fsdp", "cp"), None),
            P(("fsdp", "cp"), None),
            P(("fsdp", "cp"), None),
            P(None, ("fsdp", "cp")),
            P(("fsdp", "cp"), None),
            P(("fsdp", "cp")),
            P(("fsdp", "cp"), None, None),
            P(("fsdp", "cp"), None, None),
            P(("fsdp", "cp"), None, None),
            P("fsdp", "cp", None),
            P("fsdp", "cp", None),
            P(),
        ),
        out_specs=(
            P("fsdp", "cp", None),
            P("fsdp", "cp", None),
            P(("fsdp", "cp")),
            P(("fsdp", "cp"), None),
            P(("fsdp", "cp"), None),
            P(("fsdp", "cp"), None),
            P(None, ("fsdp", "cp")),
            P(("fsdp", "cp"), None),
            P(("fsdp", "cp")),
            P(("fsdp", "cp"), None, None),
            P(("fsdp", "cp"), None, None),
            P(("fsdp", "cp"), None, None),
        ),
        check_vma=False,
    )
```

```python
import functools
import math

import jax
import jax.numpy as jnp
from jax import lax
from jax.experimental import pallas as pl
from jax.experimental.pallas import tpu as pltpu
from jax.sharding import PartitionSpec as P

BLOCK = 64


EPSILON = 1e-06
THETA = 1000000.0


def rms_scale(values, gain):
    return values * lax.rsqrt(jnp.mean(values * values, axis=-1, keepdims=True) + EPSILON) * gain


def rotate_half(values):
    half = values.shape[-1] // 2
    return jnp.concatenate([-values[..., half:], values[..., :half]], axis=-1)


def head_post(pre, gain, cosine, sine):
    normed = rms_scale(pre, gain)
    return normed * cosine[:, None, :] + rotate_half(normed) * sine[:, None, :]


def rope_tables(positions, head_dim):
    freqs = THETA ** (-(jnp.arange(head_dim // 2, dtype=jnp.float32) * 2.0 / head_dim))
    angles = positions.astype(jnp.float32)[:, None] * freqs[None, :]
    angles = jnp.concatenate([angles, angles], axis=-1)
    return (jnp.cos(angles), jnp.sin(angles))


def seq_positions(pair_order, block):
    blocks = 2 * pair_order.shape[0]
    rows = jnp.arange(blocks * block, dtype=jnp.int32)
    owner = rows // (2 * block)
    first = pair_order[owner]
    which = jnp.where(rows // block % 2 == 0, first, blocks - 1 - first)
    return which * block + rows % block


def route_tables(ids, weights, experts, capacity):
    flat = ids.reshape(-1)
    onehot = (flat[:, None] == jnp.arange(experts, dtype=jnp.int32)[None, :]).astype(jnp.int32)
    before = jnp.cumsum(onehot, axis=0) - onehot
    rank = jnp.sum(before * onehot, axis=1)
    slots = (flat * capacity + rank).reshape(ids.shape)
    columns = jnp.arange(experts * capacity, dtype=jnp.int32)
    hits = slots[:, :, None] == columns[None, None, :]
    place = jnp.sum(hits.astype(jnp.float32), axis=1).astype(jnp.bfloat16)
    mixing = jnp.sum(jnp.where(hits, weights[:, :, None].astype(jnp.float32), 0.0), axis=1).astype(
        jnp.bfloat16
    )
    return (place, mixing)


def attend_head(query, keys, values, allowed, scale):
    scores = jnp.einsum("grd,sd->grs", query, keys, preferred_element_type=jnp.float32) * scale
    scores = jnp.where(allowed[None], scores, -jnp.inf)
    top = jnp.max(scores, axis=-1, keepdims=True)
    lse = top[..., 0] + jnp.log(jnp.sum(jnp.exp(scores - top), axis=-1))
    probs = jnp.exp(scores - lse[..., None]).astype(jnp.bfloat16)
    output = jnp.einsum("grs,sd->grd", probs, values, preferred_element_type=jnp.float32)
    return (output.astype(jnp.bfloat16), lse)


def attend_back(query, keys, values, output, grad_out, lse, allowed, scale):
    scores = jnp.einsum("grd,sd->grs", query, keys, preferred_element_type=jnp.float32) * scale
    scores = jnp.where(allowed[None], scores, -jnp.inf)
    probs = jnp.exp(scores - lse[..., None])
    grad_values = jnp.einsum(
        "grs,grd->sd", probs.astype(jnp.bfloat16), grad_out, preferred_element_type=jnp.float32
    )
    grad_probs = jnp.einsum("grd,sd->grs", grad_out, values, preferred_element_type=jnp.float32)
    delta = jnp.sum(grad_out.astype(jnp.float32) * output.astype(jnp.float32), axis=-1)
    grad_scores = (probs * (grad_probs - delta[..., None])).astype(jnp.bfloat16)
    grad_query = (
        jnp.einsum("grs,sd->grd", grad_scores, keys, preferred_element_type=jnp.float32) * scale
    )
    grad_keys = (
        jnp.einsum("grs,grd->sd", grad_scores, query, preferred_element_type=jnp.float32) * scale
    )
    return (grad_query, grad_keys, grad_values)


def contract_rows(left, right):
    return lax.dot_general(
        left, right, (((0,), (0,)), ((), ())), preferred_element_type=jnp.float32
    )


def contract_cols(left, right):
    return lax.dot_general(
        left, right, (((1,), (1,)), ((), ())), preferred_element_type=jnp.float32
    )


def wide_body(
    block_input,
    cotangent,
    gain_attn,
    w_query,
    w_key,
    w_value,
    qk_gain,
    w_out,
    gain_moe,
    w_gate,
    w_up,
    w_down,
    expert_ids,
    route_weight,
    pair_order,
):
    g_attn, wq_full, wk_full, wv_full, qk_full, wo_full, g_moe = (
        lax.all_gather(gain_attn, ("fsdp", "cp"), axis=0, tiled=True),
        lax.all_gather(w_query, ("fsdp", "cp"), axis=0, tiled=True),
        lax.all_gather(w_key, ("fsdp", "cp"), axis=0, tiled=True),
        lax.all_gather(w_value, ("fsdp", "cp"), axis=0, tiled=True),
        lax.all_gather(qk_gain, ("fsdp", "cp"), axis=1, tiled=True),
        lax.all_gather(w_out, ("fsdp", "cp"), axis=0, tiled=True),
        lax.all_gather(gain_moe, ("fsdp", "cp"), axis=0, tiled=True),
    )
    rows = block_input.shape[1]
    width = block_input.shape[2]
    head_dim = qk_full.shape[1]
    kv_heads = wk_full.shape[1] // head_dim
    heads = wq_full.shape[1] // head_dim
    group = heads // kv_heads
    experts = lax.axis_size(("fsdp", "cp"))
    capacity = max(2, 3 * BLOCK * expert_ids.shape[2] // experts)
    scale = 1.0 / math.sqrt(head_dim)
    resid = block_input[0].astype(jnp.float32)
    normed_in = rms_scale(resid, g_attn.astype(jnp.float32)).astype(jnp.bfloat16)
    q_pre = jnp.dot(normed_in, wq_full, preferred_element_type=jnp.float32).reshape(
        rows, heads, head_dim
    )
    k_pre = jnp.dot(normed_in, wk_full, preferred_element_type=jnp.float32).reshape(
        rows, kv_heads, head_dim
    )
    value_rows = jnp.dot(normed_in, wv_full, preferred_element_type=jnp.float32).astype(
        jnp.bfloat16
    )
    all_pos = seq_positions(pair_order, BLOCK)
    local_pos = lax.dynamic_slice_in_dim(all_pos, lax.axis_index("cp") * rows, rows)
    cosine, sine = rope_tables(local_pos, head_dim)
    gains32 = qk_full.astype(jnp.float32)
    query_rot = head_post(q_pre, gains32[0], cosine, sine).astype(jnp.bfloat16)
    key_rot = head_post(k_pre, gains32[1], cosine, sine).astype(jnp.bfloat16)
    keys_all, values_all = (
        lax.all_gather(key_rot.reshape(rows, kv_heads * head_dim), "cp", axis=0, tiled=True),
        lax.all_gather(value_rows, "cp", axis=0, tiled=True),
    )
    span = keys_all.shape[0]
    allowed = all_pos[None, :] <= local_pos[:, None]
    query_heads = query_rot.reshape(rows, kv_heads, group, head_dim).transpose(1, 2, 0, 3)
    key_heads = keys_all.reshape(span, kv_heads, head_dim).transpose(1, 0, 2)
    value_heads = values_all.reshape(span, kv_heads, head_dim).transpose(1, 0, 2)
    context_heads, lse = lax.map(
        lambda item: attend_head(item[0], item[1], item[2], allowed, scale),
        (query_heads, key_heads, value_heads),
    )
    context = context_heads.transpose(2, 0, 1, 3).reshape(rows, heads * head_dim)
    hidden_res = resid + jnp.dot(context, wo_full, preferred_element_type=jnp.float32)
    normed_mid = rms_scale(hidden_res, g_moe.astype(jnp.float32)).astype(jnp.bfloat16)
    place, mixing = route_tables(expert_ids[0], route_weight[0], experts, capacity)
    sent = contract_rows(place, normed_mid).astype(jnp.bfloat16)
    arrived = lax.all_to_all(
        sent.reshape(experts, capacity, width),
        ("fsdp", "cp"),
        split_axis=0,
        concat_axis=0,
        tiled=True,
    ).reshape(experts * capacity, width)
    gate_w = w_gate[0]
    up_w = w_up[0]
    down_w = w_down[0]
    gate_pre = jnp.dot(arrived, gate_w, preferred_element_type=jnp.float32)
    up_pre = jnp.dot(arrived, up_w, preferred_element_type=jnp.float32)
    gate_sig = jax.nn.sigmoid(gate_pre)
    gate_act = gate_pre * gate_sig
    expert_hidden = (gate_act * up_pre).astype(jnp.bfloat16)
    expert_out = jnp.dot(expert_hidden, down_w, preferred_element_type=jnp.float32).astype(
        jnp.bfloat16
    )
    returned = lax.all_to_all(
        expert_out.reshape(experts, capacity, width),
        ("fsdp", "cp"),
        split_axis=0,
        concat_axis=0,
        tiled=True,
    ).reshape(experts * capacity, width)
    mixed = jnp.dot(mixing, returned, preferred_element_type=jnp.float32)
    block_output = (hidden_res + mixed).astype(jnp.bfloat16)
    g_attn, wq_full, wk_full, wv_full, qk_full, wo_full, g_moe = (
        lax.all_gather(gain_attn, ("fsdp", "cp"), axis=0, tiled=True),
        lax.all_gather(w_query, ("fsdp", "cp"), axis=0, tiled=True),
        lax.all_gather(w_key, ("fsdp", "cp"), axis=0, tiled=True),
        lax.all_gather(w_value, ("fsdp", "cp"), axis=0, tiled=True),
        lax.all_gather(qk_gain, ("fsdp", "cp"), axis=1, tiled=True),
        lax.all_gather(w_out, ("fsdp", "cp"), axis=0, tiled=True),
        lax.all_gather(gain_moe, ("fsdp", "cp"), axis=0, tiled=True),
    )
    attn_gain = g_attn.astype(jnp.float32)
    moe_gain = g_moe.astype(jnp.float32)
    gains_back = qk_full.astype(jnp.float32)
    grad_top = cotangent[0]
    grad_top_b = grad_top.astype(jnp.bfloat16)
    grad_sent = contract_rows(mixing, grad_top_b).astype(jnp.bfloat16)
    grad_arrived = lax.all_to_all(
        grad_sent.reshape(experts, capacity, width),
        ("fsdp", "cp"),
        split_axis=0,
        concat_axis=0,
        tiled=True,
    ).reshape(experts * capacity, width)
    grad_hidden = contract_cols(grad_arrived, down_w)
    grad_down = contract_rows(expert_hidden, grad_arrived)
    grad_gate_pre = (grad_hidden * up_pre * gate_sig * (1.0 + gate_pre * (1.0 - gate_sig))).astype(
        jnp.bfloat16
    )
    grad_up_pre = (grad_hidden * gate_act).astype(jnp.bfloat16)
    grad_gate = contract_rows(arrived, grad_gate_pre)
    grad_up = contract_rows(arrived, grad_up_pre)
    grad_rows = (contract_cols(grad_gate_pre, gate_w) + contract_cols(grad_up_pre, up_w)).astype(
        jnp.bfloat16
    )
    grad_back = lax.all_to_all(
        grad_rows.reshape(experts, capacity, width),
        ("fsdp", "cp"),
        split_axis=0,
        concat_axis=0,
        tiled=True,
    ).reshape(experts * capacity, width)
    grad_mid = jnp.dot(place, grad_back, preferred_element_type=jnp.float32)
    _, mid_back = jax.vjp(rms_scale, hidden_res, moe_gain)
    grad_res_mid, grad_moe_gain = mid_back(grad_mid)
    grad_res = grad_top + grad_res_mid
    grad_res_b = grad_res.astype(jnp.bfloat16)
    grad_wo = contract_rows(context, grad_res_b)
    grad_context = contract_cols(grad_res_b, wo_full).astype(jnp.bfloat16)
    grad_ctx_heads = grad_context.reshape(rows, kv_heads, group, head_dim).transpose(1, 2, 0, 3)
    grad_q_heads, grad_k_heads, grad_v_heads = lax.map(
        lambda it: attend_back(it[0], it[1], it[2], it[3], it[4], it[5], allowed, scale),
        (query_heads, key_heads, value_heads, context_heads, grad_ctx_heads, lse),
    )
    grad_keys_all = grad_k_heads.transpose(1, 0, 2).reshape(span, kv_heads * head_dim)
    grad_values_all = grad_v_heads.transpose(1, 0, 2).reshape(span, kv_heads * head_dim)
    grad_key_rot, grad_values = (
        lax.psum_scatter(
            grad_keys_all.astype(jnp.bfloat16), "cp", scatter_dimension=0, tiled=True
        ).astype(jnp.float32),
        lax.psum_scatter(
            grad_values_all.astype(jnp.bfloat16), "cp", scatter_dimension=0, tiled=True
        ).astype(jnp.float32),
    )
    grad_query_rot = grad_q_heads.transpose(2, 0, 1, 3).reshape(rows, heads, head_dim)
    _, query_back = jax.vjp(
        lambda pre, gain: head_post(pre, gain, cosine, sine), q_pre, gains_back[0]
    )
    grad_q_pre, grad_q_gain = query_back(grad_query_rot)
    _, key_back = jax.vjp(
        lambda pre, gain: head_post(pre, gain, cosine, sine), k_pre, gains_back[1]
    )
    grad_k_pre, grad_k_gain = key_back(grad_key_rot.reshape(rows, kv_heads, head_dim))
    grad_q_b = grad_q_pre.reshape(rows, heads * head_dim).astype(jnp.bfloat16)
    grad_k_b = grad_k_pre.reshape(rows, kv_heads * head_dim).astype(jnp.bfloat16)
    grad_v_b = grad_values.astype(jnp.bfloat16)
    grad_wq = contract_rows(normed_in, grad_q_b)
    grad_wk = contract_rows(normed_in, grad_k_b)
    grad_wv = contract_rows(normed_in, grad_v_b)
    grad_in_norm = (
        contract_cols(grad_q_b, wq_full)
        + contract_cols(grad_k_b, wk_full)
        + contract_cols(grad_v_b, wv_full)
    )
    _, in_back = jax.vjp(rms_scale, resid, attn_gain)
    grad_res_in, grad_attn_gain = in_back(grad_in_norm)
    grad_input = grad_res + grad_res_in
    grad_qk = jnp.stack([grad_q_gain, grad_k_gain])
    owned_grads = (
        lax.psum_scatter(grad_attn_gain, ("fsdp", "cp"), scatter_dimension=0, tiled=True),
        lax.psum_scatter(grad_wq, ("fsdp", "cp"), scatter_dimension=0, tiled=True),
        lax.psum_scatter(grad_wk, ("fsdp", "cp"), scatter_dimension=0, tiled=True),
        lax.psum_scatter(grad_wv, ("fsdp", "cp"), scatter_dimension=0, tiled=True),
        lax.psum_scatter(grad_qk, ("fsdp", "cp"), scatter_dimension=1, tiled=True),
        lax.psum_scatter(grad_wo, ("fsdp", "cp"), scatter_dimension=0, tiled=True),
        lax.psum_scatter(grad_moe_gain, ("fsdp", "cp"), scatter_dimension=0, tiled=True),
    )
    return (
        block_output[None],
        grad_input[None],
        owned_grads[0],
        owned_grads[1],
        owned_grads[2],
        owned_grads[3],
        owned_grads[4],
        owned_grads[5],
        owned_grads[6],
        grad_gate[None],
        grad_up[None],
        grad_down[None],
    )


MESH = pl.DeviceIdType.MESH
ANY = pl.BlockSpec(memory_space=pl.ANY)
VM = pl.BlockSpec(memory_space=pltpu.VMEM)


def place_of():
    f = lax.axis_index("fsdp")
    c = lax.axis_index("cp")
    return f, c, c // 2, c % 2


def flip(f, bit):
    return f + bit - 2 * bit * ((f // bit) % 2)


class Wire:
    def __init__(self):
        self.sent = []

    def send(self, src, dst, ssem, rsem, dev, when=None):
        copy = pltpu.make_async_remote_copy(
            src_ref=src, dst_ref=dst, send_sem=ssem, recv_sem=rsem, device_id=dev, device_id_type=MESH
        )
        if when is None:
            copy.start()
        else:
            pl.when(when)(copy.start)
        self.sent.append((copy, when))
        return self.sent[-1]

    def settle(self, entries):
        for entry in entries:
            self.sent = [e for e in self.sent if e is not entry]
            self.wait(*entry)

    def wait(self, copy, when):
        if when is None:
            copy.wait_send()
        else:
            pl.when(when)(copy.wait_send)

    def drain(self):
        for entry in self.sent:
            self.wait(*entry)


def got(dst, ssem, rsem, dev, when=None):
    copy = pltpu.make_async_remote_copy(
        src_ref=dst, dst_ref=dst, send_sem=ssem, recv_sem=rsem, device_id=dev, device_id_type=MESH
    )
    if when is None:
        copy.wait_recv()
    else:
        pl.when(when)(copy.wait_recv)


def greet(f, c, z, zs, planes):
    bar = pltpu.get_barrier_semaphore()
    k = c % 2
    sib = c + 1 - 2 * k
    near = [((f, sib), None), ((f, c + 2), z < zs - 1), ((f, c - 2), z > 0)]
    if planes:
        near += [((flip(f, 1), c), None), ((flip(f, 2), c), None)]
    for dev, when in near:
        def hello(dev=dev):
            pl.semaphore_signal(bar, inc=1, device_id=dev, device_id_type=MESH)
        if when is None:
            hello()
        else:
            pl.when(when)(hello)
    base = 3 if planes else 1
    inner = jnp.logical_and(z > 0, z < zs - 1)
    pl.semaphore_wait(bar, base + jnp.where(inner, 2, 1))


def ag_kernel(zs, planes, x_ref, o_ref, loc, sl, szr, szl, rz, sp1, rp1, sp2, rp2, ssib, rsib):
    f, c, z, k = place_of()
    half = x_ref.shape[1] // 2
    sib = (f, c + 1 - 2 * k)
    b1 = 1 + k
    b2 = 2 - k
    f1 = flip(f, b1)
    f2 = flip(f, b2)
    cols = [f, f1, f2, flip(f1, b2)] if planes else [0]
    cs = 2 * zs

    def chunk(col, zz):
        at = (cols[col] * cs if planes else 0) + 2 * zz
        return o_ref.at[pl.ds(at, 2), :, pl.ds(pl.multiple_of(k * half, 128), half)]

    def other(col, zz):
        at = (cols[col] * cs if planes else 0) + 2 * zz
        return o_ref.at[pl.ds(at, 2), :, pl.ds(pl.multiple_of((1 - k) * half, 128), half)]

    mine = (f * cs if planes else 0) + c
    theirs = (f * cs if planes else 0) + c + 1 - 2 * k
    own = pltpu.make_async_copy(x_ref, o_ref.at[mine], loc)
    own.start()
    greet(f, c, z, zs, planes)
    w = Wire()
    w.send(x_ref, o_ref.at[mine], sl.at[0], sl.at[1], sib)
    own.wait()
    got(o_ref.at[theirs], sl.at[0], sl.at[1], sib)

    def spread(zz, when):
        if planes:
            w.send(chunk(0, zz), chunk(0, zz), sp1.at[zz], rp1.at[zz], (f1, c), when)
            w.send(chunk(0, zz), chunk(0, zz), sp2.at[zz], rp2.at[zz], (f2, c), when)

    def relay(zz, when):
        if planes:
            got(chunk(1, zz), sp1.at[zz], rp1.at[zz], (f1, c), when)
            w.send(chunk(1, zz), chunk(1, zz), sp2.at[zs + zz], rp2.at[zs + zz], (f2, c), when)
            w.send(chunk(1, zz), chunk(1, zz), ssib.at[zs + zz], rsib.at[zs + zz], sib, when)

    w.send(chunk(0, z), chunk(0, z), szr.at[z], rz.at[z], (f, c + 2), z < zs - 1)
    w.send(chunk(0, z), chunk(0, z), szl.at[z], rz.at[z], (f, c - 2), z > 0)
    spread(z, None)
    order = []
    for h in range(1, zs):
        for zz, when, on, dz, sem in (
            (z - h, z - h >= 0, z < zs - 1, 2, szr),
            (z + h, z + h < zs, z > 0, -2, szl),
        ):
            got(chunk(0, zz), sem.at[zz], rz.at[zz], (f, c), when)
            w.send(chunk(0, zz), chunk(0, zz), sem.at[zz], rz.at[zz], (f, c + dz), jnp.logical_and(when, on))
            spread(zz, when)
            w.send(chunk(0, zz), chunk(0, zz), ssib.at[zz], rsib.at[zz], sib, when)
            order.append((zz, when))
        if h == 1:
            relay(z, None)
    for zz, when in order:
        relay(zz, when)
    if planes:
        for col, base in ((2, 0), (3, zs)):
            for zz, when in [(z, None)] + order:
                got(chunk(col, zz), sp2.at[base + zz], rp2.at[base + zz], (f2, c), when)
                w.send(chunk(col, zz), chunk(col, zz), ssib.at[col * zs + zz], rsib.at[col * zs + zz], sib, when)
    if planes:
        for mycol, theircol in ((0, 0), (1, 2), (2, 1), (3, 3)):
            for zz, when in ([(z, None)] if mycol else []) + order:
                got(other(mycol, zz), ssib.at[theircol * zs + zz], rsib.at[theircol * zs + zz], sib, when)
    else:
        for zz, when in order:
            got(other(0, zz), ssib.at[zz], rsib.at[zz], sib, when)
    w.drain()


def gather(x, zs, planes, cid, nf=4):
    rows, width = x.shape
    n = (nf if planes else 1) * 2 * zs
    D = pltpu.SemaphoreType.DMA
    return pl.pallas_call(
        functools.partial(ag_kernel, zs, planes),
        out_shape=jax.ShapeDtypeStruct((n, rows, width), x.dtype),
        in_specs=[VM],
        out_specs=ANY,
        scratch_shapes=[D(()), D((2,)), D((zs,)), D((zs,)), D((zs,)), D((zs,)), D((zs,)), D((2 * zs,)), D((2 * zs,)), D((4 * zs,)), D((4 * zs,))],
        compiler_params=pltpu.CompilerParams(collective_id=cid, has_side_effects=True),
        name="gather_all" if planes else "gather_seq",
    )(x)


def add_into(dst, src, rows=32):
    n, r, wd = dst.shape

    def step(i, _):
        a = pl.ds(pl.multiple_of(i % (r // rows) * rows, rows), rows)
        j = i // (r // rows)
        dst[j, a, :] = (dst[j, a, :].astype(jnp.float32) + src[j, a, :].astype(jnp.float32)).astype(dst.dtype)
        return 0

    lax.fori_loop(0, n * (r // rows), step, 0)


def rs_kernel(zs, planes, x_ref, o_ref, t, r0, r1, r2, ral, rar, fin, lsem, s0, q0, s1, q1, s2, q2, szr, szl, rzr, rzl, sf):
    f, c, z, k = place_of()
    half = o_ref.shape[1] // 2
    sib = (f, c + 1 - 2 * k)
    b1 = 2 - k
    b2 = 1 + k
    f1 = flip(f, b1)
    f2 = flip(f, b2)
    f3 = flip(f1, b2)
    cs = 2 * zs
    cols = [f3, f1, f2, f] if planes else [0]
    nc = len(cols)
    last = zs - 1
    low = z < zs // 2
    zord = []
    for i in range(zs - 1):
        far_low = jnp.where(i < zs - 1 - z, last - i, zs - 2 - i)
        far_high = jnp.where(i < z, i, i + 1)
        zord.append(jnp.where(low, far_low, far_high))
    zord.append(z)

    def src(col, zz, kk):
        at = (col * cs if planes else 0) + 2 * zz
        return x_ref.at[pl.ds(at, 2), :, pl.ds(pl.multiple_of(kk * half, 128), half)]

    greet(f, c, z, zs, planes)
    w = Wire()
    locals_ = []
    for ci in range(nc):
        for zi in range(zs):
            i = ci * zs + zi
            col = cols[ci]
            zz = zord[zi]
            slot = (ci if not planes else {0: 0, 1: 2, 2: 1, 3: 3}[ci]) * zs + zz
            w.send(src(col, zz, 1 - k), r0.at[slot], s0.at[slot], q0.at[slot], sib)
            cp = pltpu.make_async_copy(src(col, zz, k), t.at[ci * zs + zz], lsem.at[i])
            cp.start()
            locals_.append(cp)

    def first(ci, zi):
        zz = zord[zi]
        locals_[ci * zs + zi].wait()
        got(r0.at[ci * zs + zz], s0.at[ci * zs + zz], q0.at[ci * zs + zz], sib)
        add_into(t.at[ci * zs + zz], r0.at[ci * zs + zz])

    if planes:
        for ci in (0, 1):
            for zi in range(zs):
                zz = zord[zi]
                first(ci, zi)
                m = ci * zs + zz
                w.send(t.at[m], r1.at[m], s1.at[m], q1.at[m], (f1, c))
        for zi in range(zs):
            zz = zord[zi]
            first(2, zi)
            got(r1.at[zz], s1.at[zz], q1.at[zz], (f1, c))
            add_into(t.at[2 * zs + zz], r1.at[zz])
            w.send(t.at[2 * zs + zz], r2.at[zz], s2.at[zz], q2.at[zz], (f2, c))
        for zi in range(zs):
            first(3, zi)
        base = 3 * zs
    else:
        base = 0

    def complete(zi):
        zz = zord[zi]
        if planes:
            got(r1.at[zs + zz], s1.at[zs + zz], q1.at[zs + zz], (f1, c))
            add_into(t.at[base + zz], r1.at[zs + zz])
            got(r2.at[zz], s2.at[zz], q2.at[zz], (f2, c))
            add_into(t.at[base + zz], r2.at[zz])
        else:
            first(0, zi)

    for zi in range(zs - 1):
        zz = zord[zi]
        complete(zi)
        right = zz > z
        from_left = jnp.logical_and(right, z > 0)
        from_right = jnp.logical_and(jnp.logical_not(right), z < zs - 1)
        got(ral.at[zz], szr.at[zz], rzr.at[zz], (f, c), from_left)
        got(rar.at[zz], szl.at[zz], rzl.at[zz], (f, c), from_right)

        @pl.when(from_left)
        def _():
            add_into(t.at[base + zz], ral.at[zz])

        @pl.when(from_right)
        def _():
            add_into(t.at[base + zz], rar.at[zz])

        w.send(t.at[base + zz], ral.at[zz], szr.at[zz], rzr.at[zz], (f, c + 2), right)
        w.send(t.at[base + zz], rar.at[zz], szl.at[zz], rzl.at[zz], (f, c - 2), jnp.logical_not(right))
    complete(zs - 1)
    got(ral.at[z], szr.at[z], rzr.at[z], (f, c), z > 0)
    got(rar.at[z], szl.at[z], rzl.at[z], (f, c), z < zs - 1)

    @pl.when(z > 0)
    def _():
        add_into(t.at[base + z], ral.at[z])

    @pl.when(z < zs - 1)
    def _():
        add_into(t.at[base + z], rar.at[z])

    w.send(t.at[base + z, 1 - k], fin, sf.at[0], sf.at[1], sib)
    o_ref[:, pl.ds(pl.multiple_of(k * half, 128), half)] = t[base + z, k]
    got(fin, sf.at[0], sf.at[1], sib)
    o_ref[:, pl.ds(pl.multiple_of((1 - k) * half, 128), half)] = fin[...]
    w.drain()


def scatter(x, zs, planes, cid, nf=4):
    n, rows, width = x.shape
    D = pltpu.SemaphoreType.DMA
    half = width // 2
    nc = (nf if planes else 1) * zs
    V = lambda m: pltpu.VMEM((m, 2, rows, half), x.dtype)
    return pl.pallas_call(
        functools.partial(rs_kernel, zs, planes),
        out_shape=jax.ShapeDtypeStruct((rows, width), x.dtype),
        in_specs=[ANY],
        out_specs=VM,
        scratch_shapes=[V(nc), V(nc), V(2 * zs), V(zs), V(zs), V(zs), pltpu.VMEM((rows, half), x.dtype),
            D((nc,)), D((nc,)), D((nc,)), D((2 * zs,)), D((2 * zs,)), D((zs,)), D((zs,)), D((zs,)), D((zs,)), D((zs,)), D((zs,)), D((2,))],
        compiler_params=pltpu.CompilerParams(collective_id=cid, has_side_effects=True, vmem_limit_bytes=60 * 2**20),
        name="scatter_all" if planes else "scatter_seq",
    )(x)


def greet_cross(f, c, nf, nc):
    bar = pltpu.get_barrier_semaphore()
    for i in range(1, nc):
        pl.semaphore_signal(bar, inc=1, device_id=(f, (c + i) % nc), device_id_type=MESH)
    for i in range(1, nf):
        pl.semaphore_signal(bar, inc=1, device_id=((f + i) % nf, c), device_id_type=MESH)
    pl.semaphore_wait(bar, nc + nf - 2)


def tile_steps(w, nf, nc, src, dst, hub, ssem, rsem, sp, rp):
    f, c, z, k = place_of()

    def go(i, _):
        j = (c + i) % nc
        pltpu.make_async_remote_copy(
            src_ref=src.at[j], dst_ref=hub.at[c], send_sem=ssem, recv_sem=rsem, device_id=(f, j), device_id_type=MESH
        ).start()
        return 0

    lax.fori_loop(1, nc, go, 0)
    hub[c] = src[c]
    yield
    every = pltpu.make_async_remote_copy(
        src_ref=src.at[pl.ds(0, nc - 1)], dst_ref=hub.at[pl.ds(0, nc - 1)], send_sem=ssem, recv_sem=rsem,
        device_id=(f, c), device_id_type=MESH,
    )
    every.wait_send()
    every.wait_recv()
    mine = pl.ds(f * nc, nc)
    for i in range(1, nf):
        ff = (f + i) % nf
        w.send(hub.at[:, ff], dst.at[mine], sp.at[i], rp.at[i], (ff, c))
    dst[mine] = hub[:, f]
    yield
    for i in range(1, nf):
        ff = (f + nf - i) % nf
        got(dst.at[pl.ds(ff * nc, nc)], sp.at[i], rp.at[i], (f, c))
    yield


def tile_bufs(nf, nc, tile):
    D = pltpu.SemaphoreType.DMA
    return [pltpu.VMEM((nc, nf) + tile, jnp.float32), D(()), D(()), D((nf,)), D((nf,))]


def gather_steps(w, zs, planes, late, x_ref, o_ref, loc, sl, szr, szl, rz, sp1, rp1, sp2, rp2, ssib, rsib):
    f, c, z, k = place_of()
    half = x_ref.shape[1] // 2
    sib = (f, c + 1 - 2 * k)
    b1 = 1 + k
    b2 = 2 - k
    f1 = flip(f, b1)
    f2 = flip(f, b2)
    cols = [f, f1, f2, flip(f1, b2)] if planes else [0]
    cs = 2 * zs

    def chunk(col, zz, kk):
        at = (cols[col] * cs if planes else 0) + 2 * zz
        return o_ref.at[pl.ds(at, 2), :, pl.ds(pl.multiple_of(kk * half, 128), half)]

    mine = (f * cs if planes else 0) + c
    theirs = (f * cs if planes else 0) + c + 1 - 2 * k
    own = pltpu.make_async_copy(x_ref, o_ref.at[mine], loc)
    own.start()
    w.send(x_ref, o_ref.at[mine], sl.at[0], sl.at[1], sib)
    yield
    own.wait()
    got(o_ref.at[theirs], sl.at[0], sl.at[1], sib)

    def spread(zz, when):
        if planes:
            w.send(chunk(0, zz, k), chunk(0, zz, k), sp1.at[zz], rp1.at[zz], (f1, c), when)
            w.send(chunk(0, zz, k), chunk(0, zz, k), sp2.at[zz], rp2.at[zz], (f2, c), when)

    def relay(zz, when):
        if planes:
            got(chunk(1, zz, k), sp1.at[zz], rp1.at[zz], (f1, c), when)
            w.send(chunk(1, zz, k), chunk(1, zz, k), sp2.at[zs + zz], rp2.at[zs + zz], (f2, c), when)
            w.send(chunk(1, zz, k), chunk(1, zz, k), ssib.at[zs + zz], rsib.at[zs + zz], sib, when)

    if late:
        spread(z, None)
        yield
    w.send(chunk(0, z, k), chunk(0, z, k), szr.at[z], rz.at[z], (f, c + 2), z < zs - 1)
    w.send(chunk(0, z, k), chunk(0, z, k), szl.at[z], rz.at[z], (f, c - 2), z > 0)
    if not late:
        spread(z, None)
    yield
    if late:
        relay(z, None)
        yield
    order = []
    for h in range(1, zs):
        for zz, when, on, dz, sem in (
            (z - h, z - h >= 0, z < zs - 1, 2, szr),
            (z + h, z + h < zs, z > 0, -2, szl),
        ):
            got(chunk(0, zz, k), sem.at[zz], rz.at[zz], (f, c), when)
            w.send(chunk(0, zz, k), chunk(0, zz, k), sem.at[zz], rz.at[zz], (f, c + dz), jnp.logical_and(when, on))
            spread(zz, when)
            w.send(chunk(0, zz, k), chunk(0, zz, k), ssib.at[zz], rsib.at[zz], sib, when)
            order.append((zz, when))
        yield
        if h == 1 and not late:
            relay(z, None)
            yield
    for zz, when in order:
        relay(zz, when)
        yield
    if planes:
        for col, base in ((2, 0), (3, zs)):
            for zz, when in [(z, None)] + order:
                got(chunk(col, zz, k), sp2.at[base + zz], rp2.at[base + zz], (f2, c), when)
                w.send(chunk(col, zz, k), chunk(col, zz, k), ssib.at[col * zs + zz], rsib.at[col * zs + zz], sib, when)
            yield
        for mycol, theircol in ((0, 0), (1, 2), (2, 1), (3, 3)):
            for zz, when in ([(z, None)] if mycol else []) + order:
                got(chunk(mycol, zz, 1 - k), ssib.at[theircol * zs + zz], rsib.at[theircol * zs + zz], sib, when)
    else:
        for zz, when in order:
            got(chunk(0, zz, 1 - k), ssib.at[zz], rsib.at[zz], sib, when)
    yield


def gather_sems(zs):
    D = pltpu.SemaphoreType.DMA
    return [D(()), D((2,)), D((zs,)), D((zs,)), D((zs,)), D((zs,)), D((zs,)), D((2 * zs,)), D((2 * zs,)), D((4 * zs,)), D((4 * zs,))]


def advance(steps, name="step"):
    with jax.named_scope(name):
        return next(steps, steps) is not steps


def head_rows_steps(w, nf, nc, hp, wo_ref, wo_all, hub, loc, so, ro):
    f, c, z, k = place_of()
    fx, fy = flip(f, 1), flip(f, 2)
    fd = flip(fx, 2)
    hr = wo_ref.shape[0] // 2
    halves = []
    for p in (0, 1):
        j = c % hp
        m = f
        if p:
            j, m = flip(j, 2), flip(f, 2)
        halves.append((p, pl.ds(p * hr, hr), j, f == j, m))
    keeps = []
    for p, at, j, is_hub, m in halves:
        w.send(wo_ref.at[at], hub.at[f, at], so.at[p, 0], ro.at[p, f], (j, c), jnp.logical_not(is_hub))
        keep = pltpu.make_async_copy(wo_ref.at[at], hub.at[f, at], loc.at[p])
        pl.when(is_hub)(keep.start)
        keeps.append(keep)
    yield
    stays = []
    for p, at, j, is_hub, m in halves:
        for ff in range(nf):
            got(hub.at[ff, at], so.at[p, 0], ro.at[p, ff], (f, c), jnp.logical_and(is_hub, ff != f))
            pl.when(jnp.logical_and(is_hub, ff == f))(keeps[p].wait)
            dc = (ff * nc + c) // hp
            w.send(hub.at[ff, at], wo_all.at[m, at], so.at[p, 1 + ff], ro.at[p, nf], (f, dc), jnp.logical_and(is_hub, dc != c))
            stay = pltpu.make_async_copy(hub.at[ff, at], wo_all.at[m, at], loc.at[2 + p])
            pl.when(jnp.logical_and(is_hub, dc == c))(stay.start)
        stays.append(stay)
    yield
    for p, at, j, is_hub, m in halves:
        here = (hp * c + m) % nc == c
        got(wo_all.at[m, at], so.at[p, 1], ro.at[p, nf], (f, c), jnp.logical_not(here))
        pl.when(here)(stays[p].wait)
        w.send(wo_all.at[m, at], wo_all.at[m, at], so.at[p, nf + 1], ro.at[p, nf + 1], (fx, c))
        w.send(wo_all.at[m, at], wo_all.at[m, at], so.at[p, nf + 2], ro.at[p, nf + 2], (fy, c))
    yield
    for p, at, j, is_hub, m in halves:
        mx, my = flip(m, 1), flip(m, 2)
        got(wo_all.at[mx, at], so.at[p, nf + 1], ro.at[p, nf + 1], (fx, c))
        got(wo_all.at[my, at], so.at[p, nf + 2], ro.at[p, nf + 2], (fy, c))
        if p == 0:
            w.send(wo_all.at[mx, at], wo_all.at[mx, at], so.at[p, nf + 3], ro.at[p, nf + 3], (fy, c))
        else:
            w.send(wo_all.at[my, at], wo_all.at[my, at], so.at[p, nf + 3], ro.at[p, nf + 3], (fx, c))
    yield
    for p, at, j, is_hub, m in halves:
        got(wo_all.at[flip(flip(m, 1), 2), at], so.at[p, nf + 3], ro.at[p, nf + 3], (f, c))
    yield


def far_first(z, zs):
    last = zs - 1
    low = z < zs // 2
    order = []
    for i in range(zs - 1):
        far_low = jnp.where(i < zs - 1 - z, last - i, zs - 2 - i)
        far_high = jnp.where(i < z, i, i + 1)
        order.append(jnp.where(low, far_low, far_high))
    return order + [z]


def line_sum_steps(w, zs, make, o_ref, t, u, r0, ral, rar, fin, s0, q0, szr, szl, rzr, rzl, sf):
    f, c, z, k = place_of()
    half = o_ref.shape[1] // 2
    sib = (f, c + 1 - 2 * k)
    order = far_first(z, zs)

    def first(zz):
        make(zz)
        w.send(u.at[zz], r0.at[zz], s0.at[zz], q0.at[zz], sib)

    def complete(zz):
        got(r0.at[zz], s0.at[zz], q0.at[zz], sib)
        add_into(t.at[zz], r0.at[zz])

    def onward(zz):
        right = zz > z
        from_left = jnp.logical_and(right, z > 0)
        from_right = jnp.logical_and(jnp.logical_not(right), z < zs - 1)
        got(ral.at[zz], szr.at[zz], rzr.at[zz], (f, c), from_left)
        got(rar.at[zz], szl.at[zz], rzl.at[zz], (f, c), from_right)

        @pl.when(from_left)
        def _():
            add_into(t.at[zz], ral.at[zz])

        @pl.when(from_right)
        def _():
            add_into(t.at[zz], rar.at[zz])

        w.send(t.at[zz], ral.at[zz], szr.at[zz], rzr.at[zz], (f, c + 2), right)
        w.send(t.at[zz], rar.at[zz], szl.at[zz], rzl.at[zz], (f, c - 2), jnp.logical_not(right))

    first(order[0])
    yield
    for zi in range(zs - 1):
        first(order[zi + 1])
        complete(order[zi])
        yield
        onward(order[zi])
        yield
    complete(z)
    got(ral.at[z], szr.at[z], rzr.at[z], (f, c), z > 0)

    @pl.when(z > 0)
    def _():
        add_into(t.at[z], ral.at[z])

    yield
    got(rar.at[z], szl.at[z], rzl.at[z], (f, c), z < zs - 1)

    @pl.when(z < zs - 1)
    def _():
        add_into(t.at[z], rar.at[z])

    w.send(t.at[z, 1 - k], fin, sf.at[0], sf.at[1], sib)
    o_ref[:, pl.ds(pl.multiple_of(k * half, 128), half)] = t[z, k]
    yield
    got(fin, sf.at[0], sf.at[1], sib)
    o_ref[:, pl.ds(pl.multiple_of((1 - k) * half, 128), half)] = fin[...]
    yield


def line_sum_bufs(zs, rows, half, dtype):
    D = pltpu.SemaphoreType.DMA
    V = pltpu.VMEM((zs, 2, rows, half), dtype)
    return [V, V, V, V, V, pltpu.VMEM((rows, half), dtype)] + [D((zs,))] * 6 + [D((2,))]


def attn_kernel(nf, zs, hp, scale, refs):
    (x_ref, wp_ref, tl_ref, wo_ref, tb_ref, cos_ref, sin_ref, pr_ref, pc_ref,
     o_ref, nm_ref, w_ref, to_ref, wo_all, top_all, qp_ref, kp_ref, qr_ref, kr_ref, v_ref, ctx_ref, lse_ref, hid_ref, tok_all,
     gain, gain_mid, mid, out_ref, loc, wloc, sl, szr, szl, rz, ssib, rsib, sw, rw, swx, swy) = refs[:40]
    tile_b = refs[40:45]
    head_bufs = refs[45:49]
    top_sems = refs[49:60]
    tok_sems = refs[60:71]
    sum_bufs = refs[71:]
    f, c, z, k = place_of()
    nc = 2 * zs
    rows, width = x_ref.shape
    half = width // 2
    hd = kr_ref.shape[1]
    qw = hp * hd
    f32, bf16 = jnp.float32, jnp.bfloat16
    sib_c = c + 1 - 2 * k
    sib = (f, sib_c)
    fx, fy = flip(f, 1), flip(f, 2)
    fr = [f, fx, fy, flip(fx, 2)]

    def chunk(zz, kk):
        return o_ref.at[pl.ds(2 * zz, 2), :, pl.ds(pl.multiple_of(kk * half, 128), half)]

    def piece(rel, cc):
        return w_ref.at[fr[rel] * nc + cc]

    own = pltpu.make_async_copy(x_ref, o_ref.at[c], loc)
    own.start()
    wown = pltpu.make_async_copy(wp_ref.at[c], piece(0, c), wloc)
    wown.start()
    with jax.named_scope("greet"):
        greet_cross(f, c, nf, nc)
    w = Wire()
    head_steps = head_rows_steps(w, nf, nc, hp, wo_ref, wo_all, *head_bufs)
    top_steps = gather_steps(w, zs, True, True, tb_ref, top_all, *top_sems)
    small_steps = tile_steps(w, nf, nc, tl_ref, to_ref, *tile_b)
    advance(small_steps, "tiles")
    w.send(x_ref, o_ref.at[c], sl.at[0], sl.at[1], sib)
    w.send(wp_ref.at[sib_c], piece(0, c), sw.at[sib_c], rw.at[c], sib)
    for h in range(1, zs):
        for zz, when in ((z - h, z - h >= 0), (z + h, z + h < zs)):
            for kk in (0, 1):
                cc = 2 * zz + kk
                w.send(wp_ref.at[cc], piece(0, c), sw.at[cc], rw.at[c], (f, cc), when)
    own.wait()
    got(o_ref.at[sib_c], sl.at[0], sl.at[1], sib)
    on_line = [
        w.send(chunk(z, k), chunk(z, k), szr.at[z], rz.at[z], (f, c + 2), z < zs - 1),
        w.send(chunk(z, k), chunk(z, k), szl.at[z], rz.at[z], (f, c - 2), z > 0),
    ]
    advance(head_steps, "heads")
    advance(small_steps, "tiles")

    def plane(cc, when):
        w.send(piece(0, cc), piece(0, cc), swx.at[cc], rw.at[nc + cc], (fx, c), when)
        w.send(piece(0, cc), piece(0, cc), swy.at[cc], rw.at[2 * nc + cc], (fy, c), when)

    def onward(cc, kk, when):
        if kk == 0:
            got(piece(1, cc), swx.at[cc], rw.at[nc + cc], (fx, c), when)
            w.send(piece(1, cc), piece(1, cc), swy.at[nc + cc], rw.at[3 * nc + cc], (fy, c), when)
        else:
            got(piece(2, cc), swy.at[cc], rw.at[2 * nc + cc], (fy, c), when)
            w.send(piece(2, cc), piece(2, cc), swx.at[nc + cc], rw.at[3 * nc + cc], (fx, c), when)

    def norm(zz):
        nb = 32

        def block(i, _):
            j = i // (rows // nb)
            at = pl.ds(pl.multiple_of(i % (rows // nb) * nb, nb), nb)
            v = o_ref[2 * zz + j, at, :].astype(f32)
            inv = lax.rsqrt(jnp.mean(v * v, axis=-1, keepdims=True) + EPSILON)
            to = pl.ds(pl.multiple_of(2 * zz * rows + i * nb, nb), nb)
            nm_ref[to, :] = (v * inv * gain[...]).astype(bf16)
            return 0

        with jax.named_scope("norm"):
            lax.fori_loop(0, 2 * rows // nb, block, 0)

    sides = [
        (
            (z - h, z - h >= 0, z < zs - 1, 2, szr),
            (z + h, z + h < zs, z > 0, -2, szl),
        )
        for h in range(1, zs)
    ]
    far = [(zz, when) for pair in sides for zz, when, *_ in pair]
    wown.wait()
    plane(c, None)
    got(piece(0, sib_c), sw.at[sib_c], rw.at[sib_c], sib)
    plane(sib_c, None)
    for zz, when in far:
        for kk in (0, 1):
            cc = 2 * zz + kk
            with jax.named_scope("w1"):
                got(piece(0, cc), sw.at[cc], rw.at[cc], (f, cc), when)
            plane(cc, when)
    advance(small_steps, "tiles")
    advance(head_steps, "heads")
    for i in range(width // 128):
        gain[:, pl.ds(128 * i, 128)] = to_ref[2 * i, 1:2, :] + to_ref[2 * i + 1, 1:2, :]
        gain_mid[:, pl.ds(128 * i, 128)] = to_ref[2 * i, 4:5, :] + to_ref[2 * i + 1, 4:5, :]
    norm(z)
    with jax.named_scope("w2"):
        for zz, when in [(z, None)] + far[:2]:
            for kk in (0, 1):
                onward(2 * zz + kk, kk, when)
    waiting = []
    for h, pair in enumerate(sides):
        for zz, when, on, dz, sem in pair:
            with jax.named_scope("x"):
                got(chunk(zz, k), sem.at[zz], rz.at[zz], (f, c), when)
            on_line.append(w.send(chunk(zz, k), chunk(zz, k), sem.at[zz], rz.at[zz], (f, c + dz), jnp.logical_and(when, on)))
            w.send(chunk(zz, k), chunk(zz, k), ssib.at[zz], rsib.at[zz], sib, when)
        if h == 0:
            advance(head_steps, "heads")
            with jax.named_scope("w2"):
                for zz, when in far[2:]:
                    for kk in (0, 1):
                        onward(2 * zz + kk, kk, when)
        if h == zs - 3:
            advance(head_steps, "heads")
            advance(top_steps, "top")
        if h == zs - 2:
            with jax.named_scope("line"):
                w.settle(on_line)
            advance(top_steps, "top")
            advance(top_steps, "top")
        for zz, when in waiting:
            got(chunk(zz, 1 - k), ssib.at[zz], rsib.at[zz], sib, when)
            pl.when(when)(functools.partial(norm, zz))
        waiting = [(zz, when) for zz, when, *_ in pair]
    for zz, when in waiting:
        got(chunk(zz, 1 - k), ssib.at[zz], rsib.at[zz], sib, when)
        pl.when(when)(functools.partial(norm, zz))
    with jax.named_scope("wait_w"):
        for zz, when in [(z, None)] + far:
            e, o = 2 * zz, 2 * zz + 1
            got(piece(2, e), swy.at[e], rw.at[2 * nc + e], (fy, c), when)
            got(piece(1, o), swx.at[o], rw.at[nc + o], (fx, c), when)
            got(piece(3, e), swy.at[nc + e], rw.at[3 * nc + e], (fy, c), when)
            got(piece(3, o), swx.at[nc + o], rw.at[3 * nc + o], (fx, c), when)

    gq = jnp.sum(to_ref[:, 2, :], axis=0, keepdims=True)
    gk = jnp.sum(to_ref[:, 3, :], axis=0, keepdims=True)
    qb = 2 * rows
    span = nc * rows
    low_half = lax.broadcasted_iota(jnp.int32, (1, hd), 1) < hd // 2

    def turned(t, g, at):
        t = t * lax.rsqrt(jnp.mean(t * t, axis=-1, keepdims=True) + EPSILON) * g
        other = pltpu.roll(t, hd // 2, 1)
        return (t * cos_ref[at, :] + jnp.where(low_half, -other, other) * sin_ref[at, :]).astype(bf16)

    def project(i, _):
        at = pl.ds(pl.multiple_of(i * qb, qb), qb)
        a = nm_ref[at, :]
        for nb in range((qw + 2 * hd) // (2 * hd)):
            wide = pl.ds(nb * 2 * hd, 2 * hd)
            pre = jnp.dot(a, w_ref[:, :, wide].reshape(width, 2 * hd), preferred_element_type=f32)
            for s in (0, 1):
                part = pre[:, s * hd : (s + 1) * hd]
                h = 2 * nb + s
                if h < hp:
                    qp_ref[at, pl.ds(h * hd, hd)] = part
                    qr_ref[at, pl.ds(h * hd, hd)] = turned(part, gq, at)
                elif h == hp:
                    kp_ref[at, :] = part
                    kr_ref[at, :] = turned(part, gk, at)
                else:
                    v_ref[at, :] = part.astype(bf16)
        return 0

    with jax.named_scope("project"):
        lax.fori_loop(0, span // qb, project, 0)

    lane = lax.broadcasted_iota(jnp.int32, (1, hd), 1)

    def attend(i, h):
        at = pl.ds(pl.multiple_of(i * qb, qb), qb)
        hc = pl.ds(pl.multiple_of(h * hd, hd), hd)
        s = lax.dot_general(qr_ref[at, hc], kr_ref[...], (((1,), (1,)), ((), ())), preferred_element_type=f32) * scale
        s = jnp.where(pc_ref[...] <= pr_ref[at, :], s, -jnp.inf)
        top = jnp.max(s, axis=-1, keepdims=True)
        e = jnp.exp(s - top)
        total = jnp.sum(e, axis=-1, keepdims=True)
        p = (e * (1.0 / total)).astype(bf16)
        ctx_ref[at, hc] = jnp.dot(p, v_ref[...], preferred_element_type=f32).astype(bf16)
        lse_ref[at, :] = jnp.where(lane == h, top + jnp.log(total), lse_ref[at, :])

    lse_ref[...] = jnp.zeros_like(lse_ref)

    while advance(head_steps, "heads"):
        pass

    t, u = sum_bufs[0], sum_bufs[1]

    def make(zz):
        def heads(h, _):
            attend(zz, h)
            return 0

        with jax.named_scope("attend"):
            lax.fori_loop(0, hp, heads, 0)
        at = pl.ds(pl.multiple_of(2 * zz * rows, rows), 2 * rows)
        a = ctx_ref[at, :]
        for dst, kk in ((u, 1 - k), (t, k)):
            def block(j, _, dst=dst, kk=kk):
                cols = pl.ds(pl.multiple_of(kk * half + j * 512, 128), 512)
                o = jnp.dot(a, wo_all[:, :, cols].reshape(qw, 512), preferred_element_type=f32).astype(bf16)
                dst[zz, :, :, pl.ds(pl.multiple_of(j * 512, 512), 512)] = o.reshape(2, rows, 512)
                return 0

            lax.fori_loop(0, half // 512, block, 0)

    sum_steps = line_sum_steps(w, zs, make, out_ref, *sum_bufs)
    for turn in "sstsstssssst":
        if turn == "s":
            advance(sum_steps, "sum")
        else:
            advance(top_steps, "top")
    while advance(sum_steps, "sum"):
        pass

    def middle(i, _):
        at = pl.ds(pl.multiple_of(i * 32, 32), 32)
        v = x_ref[at, :].astype(f32) + out_ref[at, :].astype(f32)
        hid_ref[at, :] = v
        inv = lax.rsqrt(jnp.mean(v * v, axis=-1, keepdims=True) + EPSILON)
        mid[at, :] = (v * inv * gain_mid[...]).astype(bf16)
        return 0

    with jax.named_scope("middle"):
        lax.fori_loop(0, rows // 32, middle, 0)
    tok_steps = gather_steps(w, zs, True, False, mid, tok_all, *tok_sems)
    advance(tok_steps, "tok")
    advance(tok_steps, "tok")
    busy = True
    while busy:
        busy = advance(top_steps, "top")
        busy = advance(tok_steps, "tok") or busy
    w.drain()


def attention(x, wp, tl, wo, tb, cosine, sine, pos, nf, zs, hp, scale, cid):
    rows, width = x.shape
    nc = 2 * zs
    span = nc * rows
    hd = cosine.shape[1]
    bf16, f32 = jnp.bfloat16, jnp.float32
    D = pltpu.SemaphoreType.DMA
    S = jax.ShapeDtypeStruct
    outs = [
        (S((nc, rows, width), bf16), VM),
        (S((span, width), bf16), VM),
        (S((nf * nc,) + wp.shape[1:], bf16), VM),
        (S((nf * nc,) + tl.shape[2:], f32), VM),
        (S((hp,) + wo.shape, bf16), VM),
        (S((nf * nc, rows, width), bf16), ANY),
        (S((span, hp * hd), f32), VM),
        (S((span, hd), f32), VM),
        (S((span, hp * hd), bf16), VM),
        (S((span, hd), bf16), VM),
        (S((span, hd), bf16), VM),
        (S((span, hp * hd), bf16), VM),
        (S((span, hd), f32), VM),
        (S((rows, width), f32), VM),
        (S((nf * nc, rows, width), bf16), ANY),
    ]
    R = pltpu.VMEM((rows, width), bf16)
    scratch = [pltpu.VMEM((1, width), f32), pltpu.VMEM((1, width), f32), R, R, D(()), D(()), D((2,)), D((zs,)), D((zs,)), D((zs,)), D((zs,)), D((zs,)),
               D((nc,)), D((4 * nc,)), D((2 * nc,)), D((2 * nc,))]
    scratch += tile_bufs(nf, nc, tl.shape[2:])
    scratch += [pltpu.VMEM((nf,) + wo.shape, bf16), D((4,)), D((2, nf + 4)), D((2, nf + 4))] + gather_sems(zs) + gather_sems(zs) + line_sum_bufs(zs, rows, width // 2, bf16)
    return pl.pallas_call(
        lambda *refs: attn_kernel(nf, zs, hp, scale, refs),
        out_shape=[s for s, _ in outs],
        in_specs=[VM] * 9,
        out_specs=[b for _, b in outs],
        scratch_shapes=scratch,
        compiler_params=pltpu.CompilerParams(collective_id=cid, has_side_effects=True, vmem_limit_bytes=60 * 2**20),
        name="attention",
    )(x, wp, tl, wo, tb, cosine, sine, pos[:, None], pos[None, :])


def sum_block(dst, srcs, rows=32):
    n, r, wd = dst.shape

    def step(i, _):
        a = pl.ds(pl.multiple_of(i % (r // rows) * rows, rows), rows)
        j = i // (r // rows)
        total = srcs[0][j, a, :].astype(jnp.float32)
        for s in srcs[1:]:
            total = total + s[j, a, :].astype(jnp.float32)
        dst[j, a, :] = total.astype(dst.dtype)
        return 0

    lax.fori_loop(0, n * (r // rows), step, 0)


def spill_sum_steps(w, zs, x_ref, o_ref, r0, r1, r2, ral, rar, stage, out, fin, ls, s0, q0, s1, q1, s2, q2, szr, szl, rzr, rzl, sf):
    f, c, z, k = place_of()
    half = o_ref.shape[1] // 2
    sib = (f, c + 1 - 2 * k)
    b1 = 2 - k
    b2 = 1 + k
    f1 = flip(f, b1)
    f2 = flip(f, b2)
    f3 = flip(f1, b2)
    cs = 2 * zs
    cols = [f3, f1, f2, f]
    order = far_first(z, zs)
    held = [None] * out.shape[0]
    count = [0]

    def src(col, zz, kk):
        return x_ref.at[pl.ds(col * cs + 2 * zz, 2), :, pl.ds(pl.multiple_of(kk * half, 128), half)]

    for zz in order:
        for ci in range(4):
            slot = {0: 0, 1: 2, 2: 1, 3: 3}[ci] * zs + zz
            w.send(src(cols[ci], zz, 1 - k), r0.at[slot], s0.at[slot], q0.at[slot], sib)
    yield

    def load(i, ref, when=None):
        copy = pltpu.make_async_copy(ref, stage.at[i], ls.at[i])
        if when is None:
            copy.start()
        else:
            pl.when(when)(copy.start)
        return copy

    def slot_for():
        i = count[0] % len(held)
        count[0] += 1
        if held[i] is not None:
            w.settle(held[i])
        return i

    def base(ci, zz):
        got(r0.at[ci * zs + zz], s0.at[ci * zs + zz], q0.at[ci * zs + zz], sib)
        loads = [load(0, src(cols[ci], zz, k)), load(1, r0.at[ci * zs + zz])]
        if ci >= 2:
            m = (ci - 2) * zs + zz
            got(r1.at[m], s1.at[m], q1.at[m], (f1, c))
            loads.append(load(2, r1.at[m]))
        if ci == 3:
            got(r2.at[zz], s2.at[zz], q2.at[zz], (f2, c))
            loads.append(load(3, r2.at[zz]))
        return loads

    def total(loads):
        i = slot_for()
        for copy in loads:
            copy.wait()
        sum_block(out.at[i], [stage.at[j] for j in range(len(loads))])
        return i

    def plane(ci, zz):
        loads = base(ci, zz)
        yield
        i = total(loads)
        if ci < 2:
            m = ci * zs + zz
            held[i] = [w.send(out.at[i], r1.at[m], s1.at[m], q1.at[m], (f1, c))]
        else:
            held[i] = [w.send(out.at[i], r2.at[zz], s2.at[zz], q2.at[zz], (f2, c))]
        yield

    def line(zz):
        loads = base(3, zz)
        right = zz > z
        from_left = jnp.logical_and(right, z > 0)
        from_right = jnp.logical_and(jnp.logical_not(right), z < zs - 1)
        got(ral.at[zz], szr.at[zz], rzr.at[zz], (f, c), from_left)
        got(rar.at[zz], szl.at[zz], rzl.at[zz], (f, c), from_right)
        more = [load(4, ral.at[zz], from_left), load(4, rar.at[zz], from_right)]
        yield
        i = total(loads)
        for copy, when in zip(more, (from_left, from_right)):
            pl.when(when)(copy.wait)

            @pl.when(when)
            def _(i=i):
                add_into(out.at[i], stage.at[4])

        held[i] = [
            w.send(out.at[i], ral.at[zz], szr.at[zz], rzr.at[zz], (f, c + 2), right),
            w.send(out.at[i], rar.at[zz], szl.at[zz], rzl.at[zz], (f, c - 2), jnp.logical_not(right)),
        ]
        yield

    for i in range(zs + 2):
        if i < zs:
            for ci in (0, 1):
                yield from plane(ci, order[i])
        if 1 <= i <= zs:
            yield from plane(2, order[i - 1])
        if 2 <= i <= zs:
            yield from line(order[i - 2])
    loads = base(3, z)
    got(ral.at[z], szr.at[z], rzr.at[z], (f, c), z > 0)
    more = load(4, ral.at[z], z > 0)
    yield
    i = total(loads)
    pl.when(z > 0)(more.wait)

    @pl.when(z > 0)
    def _():
        add_into(out.at[i], stage.at[4])

    got(rar.at[z], szl.at[z], rzl.at[z], (f, c), z < zs - 1)
    more = load(4, rar.at[z], z < zs - 1)
    pl.when(z < zs - 1)(more.wait)

    @pl.when(z < zs - 1)
    def _():
        add_into(out.at[i], stage.at[4])

    w.send(out.at[i, 1 - k], fin, sf.at[0], sf.at[1], sib)
    o_ref[:, pl.ds(pl.multiple_of(k * half, 128), half)] = out[i, k]
    yield
    got(fin, sf.at[0], sf.at[1], sib)
    o_ref[:, pl.ds(pl.multiple_of((1 - k) * half, 128), half)] = fin[...]
    yield


def head_sum_steps(w, nf, nc, hp, g, o_ref, ga, gb, loc, sg, rg, so, ro):
    f, c, z, k = place_of()
    hr = g.shape[1] // 2
    parts = []
    for p in (0, 1):
        mm = (lambda d: flip(d, 2)) if p else (lambda d: d)
        fa = flip(f, 1 + p)
        fb = flip(f, 2 - p)
        parts.append((p, pl.ds(p * hr, hr), mm, fa, fb, flip(fa, 2 - p)))
    for p, at, mm, fa, fb, fc in parts:
        for i, d in enumerate((fc, fa)):
            w.send(g.at[mm(d), at], ga.at[p, i], sg.at[p, i], rg.at[p, i], (fa, c))
    yield
    for p, at, mm, fa, fb, fc in parts:
        for i, d in enumerate((fb, f)):
            got(ga.at[p, i], sg.at[p, i], rg.at[p, i], (fa, c))
            add_into(g.at[pl.ds(mm(d), 1), at], ga.at[p, pl.ds(i, 1)])
            if i == 0:
                w.send(g.at[mm(fb), at], gb.at[p], sg.at[p, 2], rg.at[p, 2], (fb, c))
    yield
    for p, at, mm, fa, fb, fc in parts:
        got(gb.at[p], sg.at[p, 2], rg.at[p, 2], (fb, c))
        add_into(g.at[pl.ds(mm(f), 1), at], gb.at[pl.ds(p, 1)])
        head = hp * c + mm(f)
        df, dc = head // nc, head % nc
        stay = jnp.logical_and(df == f, dc == c)
        w.send(g.at[mm(f), at], o_ref.at[at], so.at[p], ro.at[p], (df, dc), jnp.logical_not(stay))
        keep = pltpu.make_async_copy(g.at[mm(f), at], o_ref.at[at], loc.at[p])
        pl.when(stay)(keep.start)
        pl.when(stay)(keep.wait)
    yield
    for p, at, mm, fa, fb, fc in parts:
        head = f * nc + c
        here = jnp.logical_and(head // hp == c, mm(head % hp) == f)
        got(o_ref.at[at], so.at[p], ro.at[p], (f, c), jnp.logical_not(here))
    yield


def weight_sum_steps(w, nf, nc, g, o_ref, ga, gb, sg, rg, sa, ra):
    f, c, z, k = place_of()
    hc = nc // 2
    parts = []
    for p in (0, 1):
        fa = flip(f, 1 + p)
        fb = flip(f, 2 - p)
        parts.append((p, pl.ds(p * hc, hc), fa, fb, flip(fa, 2 - p)))
    for p, at, fa, fb, fc in parts:
        for i, col in enumerate((fc, fa)):
            w.send(g.at[col, at], ga.at[p, i], sg.at[2 * p + i], rg.at[2 * p + i], (fa, c))
    yield
    for p, at, fa, fb, fc in parts:
        for i, col in enumerate((fb, f)):
            got(ga.at[p, i], sg.at[2 * p + i], rg.at[2 * p + i], (fa, c))
            add_into(g.at[col, at], ga.at[p, i])
            if i == 0:
                w.send(g.at[fb, at], gb.at[p], sg.at[4 + p], rg.at[4 + p], (fb, c))
    yield
    for p, at, fa, fb, fc in parts:
        got(gb.at[p], sg.at[4 + p], rg.at[4 + p], (fb, c))
        add_into(g.at[f, at], gb.at[p])
    for i in range(1, nc):
        cc = (c + i) % nc
        w.send(g.at[f, cc], o_ref.at[c], sa.at[cc], ra.at[c], (f, cc))
    o_ref[c] = g[f, c]
    yield
    for i in range(1, nc):
        cc = (c + i) % nc
        got(o_ref.at[cc], sa.at[cc], ra.at[cc], (f, c))
    yield


def expert_grad_steps(arr, garr, hid, ggp, gup, ogate, oup, odown, big, blk, flat, tall, lbig, lblk, lout):
    width = arr.shape[1]
    nb = width // 256
    f32 = jnp.float32

    def job(whole, src, dst, down):
        fill = pltpu.make_async_copy(whole, big, lbig)
        cols = lambda j: pl.ds(pl.multiple_of(j * 256, 256), 256)
        block = lambda j: pltpu.make_async_copy(src.at[:, cols(j)], blk.at[j % 2], lblk.at[j % 2])
        held = tall if down else flat
        put = lambda j: pltpu.make_async_copy(held.at[j % 2], dst.at[:, cols(j)] if down else dst.at[cols(j)], lout.at[j % 2])

        def step(j, _):
            @pl.when(j + 1 < nb)
            def _():
                block(j + 1).start()

            block(j).wait()

            @pl.when(j > 1)
            def _():
                put(j - 2).wait()

            left, right = (big[...], blk[j % 2]) if down else (blk[j % 2], big[...])
            held[j % 2] = lax.dot_general(left, right, (((0,), (0,)), ((), ())), preferred_element_type=f32).astype(held.dtype)
            put(j).start()
            return 0

        fill.start()
        block(0).start()
        fill.wait()
        lax.fori_loop(0, nb, step, 0)
        for j in (nb - 2, nb - 1):
            put(j).wait()
        yield

    yield from job(ggp, arr, ogate, False)
    yield from job(gup, arr, oup, False)
    yield from job(hid, garr, odown, True)


def grad_kernel(nf, zs, hp, scale, refs):
    (res_ref, nm_ref, w_ref, wo_ref, qp_ref, kp_ref, qr_ref, kr_ref, v_ref, ctx_ref, lse_ref, cos_ref, sin_ref, pr_ref, pc_ref,
     gqk_ref, gat_ref, moe_ref, mix_ref, arr, garr, hid, ggp, gup,
     out_ref, go_ref, gwo_ref, to_ref, mixed_ref, ogate, oup, odown, h0, h1, h2, hl, hr,
     res, gkv, gkv2, gcat, gw, gwo, tl, gqk, gat, loc, sl, szr, szl, rz, ssib, rsib, sk) = refs[:54]
    rest = list(refs[54:])

    def take(n):
        part = rest[:n]
        del rest[:n]
        return part

    tile_b = take(5)
    sum_bufs = take(13)
    spill_bufs = take(15)
    head_b = take(7)
    weight_b = take(6)
    expert_b = take(7)
    expert_steps = expert_grad_steps(arr, garr, hid, ggp, gup, ogate, oup, odown, *expert_b)
    f, c, z, k = place_of()
    nc = 2 * zs
    rows, width = res_ref.shape
    half = width // 2
    hd = kr_ref.shape[1]
    qw = hp * hd
    span = nc * rows
    f32, bf16 = jnp.float32, jnp.bfloat16
    sib_c = c + 1 - 2 * k
    sib = (f, sib_c)
    first = k == 0

    def chunk(zz, kk):
        return res.at[pl.ds(2 * zz, 2), :, pl.ds(pl.multiple_of(kk * half, 128), half)]

    own = pltpu.make_async_copy(res_ref, res.at[c], loc)
    own.start()
    with jax.named_scope("greet"):
        greet_cross(f, c, nf, nc)
    w = Wire()
    w.send(res_ref, res.at[c], sl.at[0], sl.at[1], sib)
    mix_steps = spill_sum_steps(w, zs, mix_ref, mixed_ref, h0, h1, h2, hl, hr, *spill_bufs)
    own.wait()
    got(res.at[sib_c], sl.at[0], sl.at[1], sib)
    w.send(chunk(z, k), chunk(z, k), szr.at[z], rz.at[z], (f, c + 2), z < zs - 1)
    w.send(chunk(z, k), chunk(z, k), szl.at[z], rz.at[z], (f, c - 2), z > 0)
    advance(mix_steps, "mix")
    gkv[...] = jnp.zeros_like(gkv)
    gqk[...] = jnp.zeros_like(gqk)
    gat[...] = jnp.zeros_like(gat)
    gq, gk = gqk_ref[0:1, :], gqk_ref[1:2, :]
    low_half = lax.broadcasted_iota(jnp.int32, (1, hd), 1) < hd // 2
    lane = lax.broadcasted_iota(jnp.int32, (1, hd), 1)

    def turned_back(t, g, grad, at):
        u = grad * sin_ref[at, :]
        other = pltpu.roll(u, hd // 2, 1)
        gy = grad * cos_ref[at, :] + jnp.where(low_half, other, -other)
        r = lax.rsqrt(jnp.mean(t * t, axis=-1, keepdims=True) + EPSILON)
        n = t * r
        gn = gy * g
        back = r * (gn - n * jnp.mean(gn * n, axis=-1, keepdims=True))
        return back, jnp.sum(gy * n, axis=0, keepdims=True)

    def process(zz):
        at = pl.ds(pl.multiple_of(2 * zz * rows, 2 * rows), 2 * rows)
        rr = res[pl.ds(2 * zz, 2)].reshape(2 * rows, width)

        def head(h, _):
            hc = pl.ds(pl.multiple_of(h * hd, hd), hd)
            g = lax.dot_general(rr, wo_ref[h], (((1,), (1,)), ((), ())), preferred_element_type=f32).astype(bf16)
            q = qr_ref[at, hc]
            s = lax.dot_general(q, kr_ref[...], (((1,), (1,)), ((), ())), preferred_element_type=f32) * scale
            lse = jnp.sum(jnp.where(lane == h, lse_ref[at, :], 0.0), axis=-1, keepdims=True)
            p = jnp.where(pc_ref[...] <= pr_ref[at, :], jnp.exp(s - lse), 0.0)
            gkv[1] += lax.dot_general(p.astype(bf16), g, (((0,), (0,)), ((), ())), preferred_element_type=f32)
            gp = lax.dot_general(g, v_ref[...], (((1,), (1,)), ((), ())), preferred_element_type=f32)
            delta = jnp.sum(g.astype(f32) * ctx_ref[at, hc].astype(f32), axis=-1, keepdims=True)
            ds = (p * (gp - delta)).astype(bf16)
            gkv[0] += lax.dot_general(ds, q, (((0,), (0,)), ((), ())), preferred_element_type=f32) * scale
            gr = jnp.dot(ds, kr_ref[...], preferred_element_type=f32) * scale
            back, gain = turned_back(qp_ref[at, hc], gq, gr, at)
            gcat[at, hc] = back.astype(bf16)
            gqk[0:1, :] += gain
            return 0

        with jax.named_scope("process"):
            lax.fori_loop(0, hp, head, 0)

    def mix(count):
        for _ in range(count):
            advance(mix_steps, "mix")

    near = far_first(z, zs)[::-1]
    mix(8)
    process(near[0])
    counts = [(2, 4)] + [(2, 2)] * (zs - 3) + [(4, 2)]
    for h in range(1, zs):
        sides = (
            (z - h, z - h >= 0, z < zs - 1, 2, szr),
            (z + h, z + h < zs, z > 0, -2, szl),
        )
        with jax.named_scope("hop"):
            for zz, when, on, dz, sem in sides:
                got(chunk(zz, k), sem.at[zz], rz.at[zz], (f, c), when)
                w.send(chunk(zz, k), chunk(zz, k), sem.at[zz], rz.at[zz], (f, c + dz), jnp.logical_and(when, on))
                w.send(chunk(zz, k), chunk(zz, k), ssib.at[zz], rsib.at[zz], sib, when)
        mix(counts[h - 1][0])
        with jax.named_scope("rest"):
            for zz, when, *_ in sides:
                got(chunk(zz, 1 - k), ssib.at[zz], rsib.at[zz], sib, when)
        process(near[h])
        mix(counts[h - 1][1])
    w.send(gkv, gkv2, sk.at[0], sk.at[1], sib)

    with jax.named_scope("gwo"):
        def gwo_block(j, _):
            cols = pl.ds(pl.multiple_of(j * 256, 256), 256)
            r = res[:, :, cols].reshape(span, 256)
            o = lax.dot_general(ctx_ref[...], r, (((0,), (0,)), ((), ())), preferred_element_type=f32).astype(bf16)
            gwo[:, :, cols] = o.reshape(hp, hd, 256)
            return 0

        lax.fori_loop(0, width // 256, gwo_block, 0)
    head_steps = head_sum_steps(w, nf, nc, hp, gwo, gwo_ref, *head_b)
    advance(head_steps, "heads")
    advance(expert_steps, "expert")
    with jax.named_scope("kv"):
        got(gkv2, sk.at[0], sk.at[1], sib)

        def keys(i, _):
            at = pl.ds(pl.multiple_of(i * 2 * rows, 2 * rows), 2 * rows)
            back, gain = turned_back(kp_ref[at, :], gk, gkv[0, at, :] + gkv2[0, at, :], at)
            gv = gkv[1, at, :] + gkv2[1, at, :]
            gcat[at, pl.ds(qw, hd)] = jnp.where(first, back, gv).astype(bf16)
            gqk[1:2, :] += jnp.where(first, gain, 0.0)
            return 0

        lax.fori_loop(0, zs, keys, 0)
    t, u = sum_bufs[0], sum_bufs[1]

    def make(zz):
        at = pl.ds(pl.multiple_of(2 * zz * rows, 2 * rows), 2 * rows)
        a = gcat[at, 0:qw]
        b = gcat[at, qw : qw + hd]
        for dst, kk in ((u, 1 - k), (t, k)):
            def block(j, _, dst=dst, kk=kk):
                slabs = pl.ds(kk * (half // 64) + j * 8, 8)
                wq = w_ref[slabs, :, 0:qw].reshape(512, qw)
                wk = w_ref[slabs, :, pl.ds(pl.multiple_of(qw + k * hd, hd), hd)].reshape(512, hd)
                o = lax.dot_general(a, wq, (((1,), (1,)), ((), ())), preferred_element_type=f32)
                o = o + lax.dot_general(b, wk, (((1,), (1,)), ((), ())), preferred_element_type=f32)
                cols = pl.ds(pl.multiple_of(kk * half + j * 512, 512), 512)
                gat[:, cols] += jnp.sum(o * nm_ref[at, cols].astype(f32), axis=0, keepdims=True)
                dst[zz, :, :, pl.ds(pl.multiple_of(j * 512, 512), 512)] = o.astype(bf16).reshape(2, rows, 512)
                return 0

            lax.fori_loop(0, half // 512, block, 0)

    sum_steps = line_sum_steps(w, zs, make, out_ref, *sum_bufs)
    for _ in range(2):
        advance(sum_steps, "sum")
    advance(expert_steps, "expert")
    advance(head_steps, "heads")
    with jax.named_scope("gw"):
        def gw_block(j, _):
            cols = pl.ds(pl.multiple_of(j * 256, 256), 256)
            o = lax.dot_general(nm_ref[:, cols], gcat[...], (((0,), (0,)), ((), ())), preferred_element_type=f32).astype(bf16)
            gw[j // 2, pl.ds(j % 2 * 4, 4)] = o.reshape(4, 64, qw + hd)
            return 0

        lax.fori_loop(0, width // 256, gw_block, 0)
    weight_steps = weight_sum_steps(w, nf, nc, gw, go_ref, *weight_b)
    advance(weight_steps, "weights")
    small_steps = None
    for turn in "smsmsmsm+smgwmgmghmgwmsmtm":
        if turn == "+":
            for cc in range(nc):
                for ff in range(nf):
                    lanes = pl.ds(128 * ((ff * nc + cc) // 2), 128)
                    tl[cc, ff, 0:1, :] = gat[:, lanes] / gat_ref[:, lanes]
                    tl[cc, ff, 1:2, :] = moe_ref[:, lanes]
                    tl[cc, ff, 2:4, :] = gqk[...]
                    tl[cc, ff, 4:8, :] = jnp.zeros((4, hd), f32)
            small_steps = tile_steps(w, nf, nc, tl, to_ref, *tile_b)
            advance(small_steps, "tiles")
        else:
            name = {"s": "sum", "w": "weights", "h": "heads", "m": "mix", "t": "tiles", "g": "expert"}[turn]
            steps = {"s": sum_steps, "w": weight_steps, "h": head_steps, "m": mix_steps, "t": small_steps, "g": expert_steps}
            advance(steps[turn], name)
    for name, steps in (("sum", sum_steps), ("heads", head_steps), ("mix", mix_steps), ("weights", weight_steps), ("tiles", small_steps), ("expert", expert_steps)):
        while advance(steps, name):
            pass
    w.drain()


def gradients(res, nm, wcat, wo, qp, kp, qr, kr, v, ctx, lse, cosine, sine, pos, gqk, gat, moe, mix, experts, nf, zs, hp, scale, cid):
    rows, width = res.shape
    nc = 2 * zs
    span = nc * rows
    hd = cosine.shape[1]
    bf16, f32 = jnp.bfloat16, jnp.float32
    D = pltpu.SemaphoreType.DMA
    S = jax.ShapeDtypeStruct
    half = width // 2
    cols = hp * hd + hd
    shard = wcat.shape[1]
    slots, ff = experts[2].shape
    spill = lambda n: (S((n, 2, rows, half), bf16), ANY)
    outs = [
        (S((rows, width), bf16), VM),
        (S((nc, shard, cols), bf16), VM),
        (S((hd, width), bf16), VM),
        (S((nf * nc, 8, hd), f32), VM),
        (S((rows, width), bf16), VM),
        (S((width, ff), bf16), ANY),
        (S((width, ff), bf16), ANY),
        (S((ff, width), bf16), ANY),
        spill(4 * zs), spill(2 * zs), spill(zs), spill(zs), spill(zs),
    ]
    V = pltpu.VMEM
    chunk = (2, rows, half)
    scratch = [V((nc, rows, width), bf16), V((2, span, hd), f32), V((2, span, hd), f32), V((span, cols), bf16),
               V((nf, nc, shard, cols), bf16), V((hp, hd, width), bf16), V((nc, nf, 8, hd), f32), V((2, hd), f32), V((1, width), f32),
               D(()), D((2,)), D((zs,)), D((zs,)), D((zs,)), D((zs,)), D((zs,)), D((2,))]
    scratch += tile_bufs(nf, nc, (8, hd)) + line_sum_bufs(zs, rows, half, bf16)
    scratch += [V((5,) + chunk, bf16), V((3,) + chunk, bf16), V((rows, half), bf16), D((5,)), D((4 * zs,)), D((4 * zs,)), D((2 * zs,)), D((2 * zs,)),
                D((zs,)), D((zs,)), D((zs,)), D((zs,)), D((zs,)), D((zs,)), D((2,))]
    scratch += [V((2, 2, hd // 2, width), bf16), V((2, hd // 2, width), bf16), D((2,)), D((2, 3)), D((2, 3)), D((2,)), D((2,))]
    scratch += [V((2, 2, nc // 2, shard, cols), bf16), V((2, nc // 2, shard, cols), bf16), D((6,)), D((6,)), D((nc,)), D((nc,))]
    scratch += [V((slots, ff), bf16), V((2, slots, 256), bf16), V((2, 256, ff), bf16), V((2, ff, 256), bf16), D(()), D((2,)), D((2,))]
    return pl.pallas_call(
        lambda *refs: grad_kernel(nf, zs, hp, scale, refs),
        out_shape=[s for s, _ in outs],
        in_specs=[VM] * 18 + [ANY] * 6,
        out_specs=[b for _, b in outs],
        scratch_shapes=scratch,
        compiler_params=pltpu.CompilerParams(collective_id=cid, has_side_effects=True, vmem_limit_bytes=62 * 2**20),
        name="gradients",
    )(res, nm, wcat, wo, qp, kp, qr, kr, v, ctx, lse, cosine, sine, pos[:, None], pos[None, :], gqk, gat, moe, mix, *experts)


def flip_if(f, bit, when):
    return jnp.where(when, flip(f, bit), f)


def expert_kernel(nf, zs, refs):
    (tok, top, place, mixing, wg, wu, wd,
     out_ref, shares, arr, garr, hid, ggp, gup,
     tb, cb, a, g, rows_b, t, u, r0, r1, r2, ral, rar, fin, sh,
     lt, lc, la, lg, ls, s0, q0, s1, q1, s2, q2, szr, szl, rzr, rzl, sf) = refs
    f, c, z, k = place_of()
    nc = 2 * zs
    rows, width = tb.shape[2:]
    half = width // 2
    cap = place.shape[1]
    per = nf * cap
    f32, bf16 = jnp.float32, jnp.bfloat16
    sib = (f, c + 1 - 2 * k)
    f1 = flip(f, 2 - k)
    f2 = flip(f, 1 + k)
    order = far_first(z, zs)
    with jax.named_scope("greet"):
        greet(f, c, z, zs, True)
    w = Wire()

    def col_of(ci):
        return flip_if(flip_if(f, 1, ci < 2), 2, (ci % 2) == 0)

    def fetch(zz, ci, slot):
        two = pl.ds(col_of(ci) * nc + 2 * zz, 2)
        return (
            pltpu.make_async_copy(tok.at[two], tb.at[slot], lt.at[slot]),
            pltpu.make_async_copy(top.at[two], cb.at[slot], lc.at[slot]),
        )

    def compute(gi):
        zz = order[gi]
        for copy in fetch(zz, 0, 0):
            copy.start()
        if gi:
            for copy in keep:
                copy.wait()

        def pick(ci, _):
            slot = ci % 2

            @pl.when(ci < nf - 1)
            def _():
                for copy in fetch(zz, ci + 1, 1 - slot):
                    copy.start()

            for copy in fetch(zz, ci, slot):
                copy.wait()
            at = pl.ds(pl.multiple_of(ci * cap, 16), cap)
            chip = col_of(ci) * zs + zz
            a[at, :] = jnp.dot(place[chip], tb[slot].reshape(2 * rows, width), preferred_element_type=f32).astype(bf16)
            g[at, :] = jnp.dot(mixing[chip], cb[slot].reshape(2 * rows, width), preferred_element_type=f32).astype(bf16)
            return 0

        with jax.named_scope("pick"):
            lax.fori_loop(0, nf, pick, 0)
        mine = pl.ds(gi * per, per)
        keep[:] = [pltpu.make_async_copy(a, arr.at[mine], la), pltpu.make_async_copy(g, garr.at[mine], lg)]
        for copy in keep:
            copy.start()

        def hidden(j, _):
            cc = pl.ds(pl.multiple_of(j * 256, 256), 256)
            gate = jnp.dot(a[...], wg[:, cc], preferred_element_type=f32)
            up = jnp.dot(a[...], wu[:, cc], preferred_element_type=f32)
            back = lax.dot_general(g[...], wd[cc, :], (((1,), (1,)), ((), ())), preferred_element_type=f32)
            sig = jax.nn.sigmoid(gate)
            act = gate * sig
            hid[mine, cc] = (act * up).astype(bf16)
            ggp[mine, cc] = (back * up * sig * (1.0 + gate * (1.0 - sig))).astype(bf16)
            gup[mine, cc] = (back * act).astype(bf16)
            return 0

        with jax.named_scope("hidden"):
            lax.fori_loop(0, wg.shape[1] // 256, hidden, 0)

        def rows_of(j, _):
            cc = pl.ds(pl.multiple_of(j * 256, 256), 256)
            o = lax.dot_general(ggp[mine, :], wg[cc, :], (((1,), (1,)), ((), ())), preferred_element_type=f32)
            o = o + lax.dot_general(gup[mine, :], wu[cc, :], (((1,), (1,)), ((), ())), preferred_element_type=f32)
            rows_b[:, cc] = o.astype(bf16)
            return 0

        with jax.named_scope("rows"):
            lax.fori_loop(0, width // 256, rows_of, 0)

        def spread(ci, _):
            at = pl.ds(pl.multiple_of(ci * cap, 16), cap)
            p = place[col_of(ci) * zs + zz]
            for dst, kk in ((u.at[gi % 2, ci], 1 - k), (t.at[ci * zs + zz], k)):
                r = rows_b[at, pl.ds(pl.multiple_of(kk * half, 128), half)]
                o = lax.dot_general(p, r, (((0,), (0,)), ((), ())), preferred_element_type=f32)
                dst[...] = o.astype(bf16).reshape(2, rows, half)
            return 0

        if gi >= 2:
            w.settle(passed[gi - 2])
        with jax.named_scope("spread"):
            lax.fori_loop(0, nf, spread, 0)
        passed.append([])
        for ci in range(nf):
            m = ci * zs + zz
            passed[gi].append(w.send(u.at[gi % 2, ci], r0.at[m], s0.at[m], q0.at[m], sib))

    def pair(m):
        got(r0.at[m], s0.at[m], q0.at[m], sib)
        add_into(t.at[m], r0.at[m])

    def stage_one(zz):
        for i, m in ((0, zz), (1, (2 - k) * zs + zz)):
            pair(m)
            w.send(t.at[m], r1.at[i * zs + zz], s1.at[i * zs + zz], q1.at[i * zs + zz], (f1, c))

    def stage_two(zz):
        m = (1 + k) * zs + zz
        pair(m)
        got(r1.at[zz], s1.at[zz], q1.at[zz], (f1, c))
        add_into(t.at[m], r1.at[zz])
        w.send(t.at[m], r2.at[zz], s2.at[zz], q2.at[zz], (f2, c))

    def give(gi, zz):
        at = pl.ds(pl.multiple_of(gi * per, 16), per)

        def out_of(j, _):
            cc = pl.ds(pl.multiple_of(j * 256, 256), 256)
            rows_b[:, cc] = jnp.dot(hid[at, :], wd[:, cc], preferred_element_type=f32).astype(bf16)
            return 0

        lax.fori_loop(0, width // 256, out_of, 0)

        def one(ci, _):
            slot = ci % 2
            there = lambda cj: pltpu.make_async_copy(sh.at[slot], shares.at[pl.ds(col_of(cj) * nc + 2 * zz, 2)], ls.at[slot])

            @pl.when(ci > 1)
            def _():
                there(ci - 2).wait()

            e = rows_b[pl.ds(pl.multiple_of(ci * cap, 16), cap), :]
            o = lax.dot_general(mixing[col_of(ci) * zs + zz], e, (((0,), (0,)), ((), ())), preferred_element_type=f32)
            sh[slot] = o.astype(bf16).reshape(2, rows, width)
            there(ci).start()
            return 0

        lax.fori_loop(0, nf, one, 0)
        for ci in (nf - 2, nf - 1):
            pltpu.make_async_copy(sh.at[ci % 2], shares.at[pl.ds(col_of(ci) * nc + 2 * zz, 2)], ls.at[ci % 2]).wait()

    base = 3 * zs

    def complete(zz):
        pair(base + zz)
        got(r1.at[zs + zz], s1.at[zs + zz], q1.at[zs + zz], (f1, c))
        add_into(t.at[base + zz], r1.at[zs + zz])
        got(r2.at[zz], s2.at[zz], q2.at[zz], (f2, c))
        add_into(t.at[base + zz], r2.at[zz])

    edge = jnp.logical_or(z == 0, z == zs - 1)

    def onward(zz, when):
        right = zz > z
        w.send(t.at[base + zz], ral.at[zz], szr.at[zz], rzr.at[zz], (f, c + 2), jnp.logical_and(when, right))
        w.send(t.at[base + zz], rar.at[zz], szl.at[zz], rzl.at[zz], (f, c - 2), jnp.logical_and(when, jnp.logical_not(right)))

    def stage_line(zz):
        complete(zz)
        onward(zz, edge)

    def stage_relay(zz):
        inner = jnp.logical_not(edge)
        from_left = jnp.logical_and(inner, zz > z)
        from_right = jnp.logical_and(inner, zz < z)
        with jax.named_scope("line"):
            got(ral.at[zz], szr.at[zz], rzr.at[zz], (f, c), from_left)
            got(rar.at[zz], szl.at[zz], rzl.at[zz], (f, c), from_right)

        @pl.when(from_left)
        def _():
            add_into(t.at[base + zz], ral.at[zz])

        @pl.when(from_right)
        def _():
            add_into(t.at[base + zz], rar.at[zz])

        onward(zz, inner)

    keep, passed = [], []
    for gi in range(zs):
        compute(gi)
        with jax.named_scope("one"):
            stage_one(order[gi])
        if gi >= 1:
            with jax.named_scope("two"):
                stage_two(order[gi - 1])
        if gi >= 3:
            stage_relay(order[gi - 3])
        if gi >= 2:
            with jax.named_scope("three"):
                stage_line(order[gi - 2])
    for copy in keep:
        copy.wait()
    with jax.named_scope("give"):
        give(0, order[0])
    with jax.named_scope("two"):
        stage_two(z)
    stage_relay(order[zs - 3])
    with jax.named_scope("three"):
        stage_line(order[zs - 2])
    with jax.named_scope("give"):
        give(1, order[1])
    stage_relay(order[zs - 2])
    with jax.named_scope("complete"):
        complete(z)

    def give_late(gi, _):
        zz = order[-1]
        for i in range(2, zs - 1):
            zz = jnp.where(gi == i, order[i], zz)
        give(gi, zz)
        return 0

    with jax.named_scope("give"):
        lax.fori_loop(2, zs, give_late, 0)
    with jax.named_scope("line"):
        got(ral.at[z], szr.at[z], rzr.at[z], (f, c), z > 0)
        got(rar.at[z], szl.at[z], rzl.at[z], (f, c), z < zs - 1)

    @pl.when(z > 0)
    def _():
        add_into(t.at[base + z], ral.at[z])

    @pl.when(z < zs - 1)
    def _():
        add_into(t.at[base + z], rar.at[z])

    w.send(t.at[base + z, 1 - k], fin, sf.at[0], sf.at[1], sib)
    out_ref[:, pl.ds(pl.multiple_of(k * half, 128), half)] = t[base + z, k]
    got(fin, sf.at[0], sf.at[1], sib)
    out_ref[:, pl.ds(pl.multiple_of((1 - k) * half, 128), half)] = fin[...]
    w.drain()


def experts_of(tokens, top, place, mixing, wg, wu, wd, nf, zs, cid):
    n, rows, width = tokens.shape
    slots = place.shape[0] * place.shape[1]
    per = slots // zs
    ff = wg.shape[1]
    half = width // 2
    bf16 = jnp.bfloat16
    S = jax.ShapeDtypeStruct
    D = pltpu.SemaphoreType.DMA
    V = lambda *s: pltpu.VMEM(s, bf16)
    C = lambda *m: pltpu.VMEM(m + (2, rows, half), bf16)
    outs = [
        (S((rows, width), bf16), VM),
        (S((n, rows, width), bf16), ANY),
        (S((slots, width), bf16), ANY),
        (S((slots, width), bf16), ANY),
        (S((slots, ff), bf16), VM),
        (S((slots, ff), bf16), VM),
        (S((slots, ff), bf16), VM),
    ]
    scratch = [V(2, 2, rows, width), V(2, 2, rows, width), V(per, width), V(per, width), V(per, width),
               C(nf * zs), C(2, nf), C(nf * zs), C(2 * zs), C(zs), C(zs), C(zs), V(rows, half), V(2, 2, rows, width),
               D((2,)), D((2,)), D(()), D(()), D((2,)), D((nf * zs,)), D((nf * zs,)), D((2 * zs,)), D((2 * zs,)), D((zs,)), D((zs,)),
               D((zs,)), D((zs,)), D((zs,)), D((zs,)), D((2,))]
    return pl.pallas_call(
        lambda *refs: expert_kernel(nf, zs, refs),
        out_shape=[s for s, _ in outs],
        in_specs=[ANY, ANY] + [VM] * 5,
        out_specs=[b for _, b in outs],
        scratch_shapes=scratch,
        compiler_params=pltpu.CompilerParams(collective_id=cid, has_side_effects=True, vmem_limit_bytes=62 * 2**20),
        name="experts",
    )(tokens, top, place, mixing, wg, wu, wd)


def head_body(
    nf,
    nc,
    block_input,
    cotangent,
    gain_attn,
    w_query,
    w_key,
    w_value,
    qk_gain,
    w_out,
    gain_moe,
    w_gate,
    w_up,
    w_down,
    expert_ids,
    route_weight,
    pair_order,
):
    bf16, f32 = jnp.bfloat16, jnp.float32
    f, c, z, k = place_of()
    n = nf * nc
    zs = nc // 2
    rows, width = block_input.shape[1:]
    hd = qk_gain.shape[1] * n
    kv_heads = w_key.shape[1] // hd
    heads = w_query.shape[1] // hd
    hp = heads // nc
    shard = w_query.shape[0]
    topk = expert_ids.shape[2]
    capacity = max(2, 3 * BLOCK * topk // n)
    span = nc * rows
    scale = 1.0 / math.sqrt(hd)
    x_own = block_input[0]
    resid = x_own.astype(f32)

    ids, weights = expert_ids[0], route_weight[0].astype(f32)
    named = ids[None, :, :] == jnp.arange(n, dtype=jnp.int32)[:, None, None]
    to_expert = jnp.sum(jnp.where(named, weights[None], 0.0), axis=-1)
    lane = jnp.arange(rows)
    gs = gain_attn.shape[0]
    me = f * nc + c
    spots = lane // gs == me % (rows // gs)
    gain_row = lambda g: jnp.where(spots, jnp.tile(g.astype(f32), rows // gs), 0.0)
    qs = qk_gain.shape[1]
    qk_row = lambda g: jnp.where(lane // qs == me, jnp.tile(g.astype(f32), rows // qs), 0.0)
    small = jnp.stack([gain_row(gain_attn), qk_row(qk_gain[0]), qk_row(qk_gain[1]), gain_row(gain_moe)])
    tiles = jnp.concatenate([to_expert[:, None], jnp.broadcast_to(small, (n,) + small.shape), jnp.zeros((n, 3, rows), f32)], axis=1)
    by_place = lambda t: t.reshape((nf, nc) + t.shape[1:]).swapaxes(0, 1)
    per = nc // kv_heads
    wq_p = w_query.reshape(shard, nc, hp * hd).transpose(1, 0, 2)
    wk_p = jnp.repeat(w_key.reshape(shard, kv_heads, hd).transpose(1, 0, 2), per, axis=0)
    wv_p = jnp.repeat(w_value.reshape(shard, kv_heads, hd).transpose(1, 0, 2), per, axis=0)
    packed = jnp.concatenate([wq_p, wk_p, wv_p], axis=2)
    top_own = cotangent[0]
    pair = pair_order[:, None, None]
    both = jnp.concatenate([pair, 2 * pair_order.shape[0] - 1 - pair], axis=1)
    pos = (both * BLOCK + jnp.arange(BLOCK, dtype=jnp.int32)).reshape(-1)
    freqs = THETA ** (-(jnp.arange(hd // 2, dtype=f32) * 2.0 / hd))
    angles = pos.astype(f32)[:, None] * freqs[None, :]
    cosine, sine = jnp.tile(jnp.cos(angles), (1, 2)), jnp.tile(jnp.sin(angles), (1, 2))
    (x_seq, normed_in, w_all, dealt, wo_all, top_all, q_pre, k_pre, query_rot, key_rot, values, context, lse, hidden_res, tokens) = attention(
        x_own, packed, by_place(tiles), w_out, top_own.astype(bf16), cosine, sine, pos, nf, zs, hp, scale, 0
    )
    qw = hp * hd
    full_row = lambda r: dealt[:, r].reshape(-1, rows // gs, rows).sum(axis=1).reshape(-1)
    g_attn, g_moe = full_row(1), full_row(4)
    g_qk = dealt[:, 2:4].sum(axis=0)
    route_w = dealt[:, 0, :]
    hit = route_w > 0.0
    below = (jnp.arange(rows)[:, None] < jnp.arange(rows)[None, :]).astype(f32)
    rank = jnp.dot(hit.astype(f32), below, preferred_element_type=f32).astype(jnp.int32)
    slot = (rank[:, None, :] == jnp.arange(capacity, dtype=jnp.int32)[None, :, None]) & hit[:, None, :]
    place = slot.astype(bf16)
    mixing = jnp.where(slot, route_w[:, None, :], 0.0).astype(bf16)
    gate_w, up_w, down_w = w_gate[0], w_up[0], w_down[0]
    def paired(table):
        two = table.reshape(n // 2, 2, capacity, rows)
        none = jnp.zeros((n // 2, capacity, rows), bf16)
        upper = jnp.concatenate([two[:, 0], none], axis=2)
        lower = jnp.concatenate([none, two[:, 1]], axis=2)
        return jnp.concatenate([upper, lower], axis=1)

    grad_mid, shares, arrived, grad_arrived, expert_hidden, grad_gate_pre, grad_up_pre = experts_of(
        tokens, top_all, paired(place), paired(mixing), gate_w, up_w, down_w, nf, zs, 3
    )
    grad_mid = grad_mid.astype(f32)

    _, mid_back = jax.vjp(rms_scale, hidden_res, g_moe)
    grad_res_mid, grad_moe_gain = mid_back(grad_mid)
    grad_res = top_own + grad_res_mid

    grad_in, grads, grad_wo, summed, mixed, grad_gate, grad_up, grad_down, *_ = gradients(
        grad_res.astype(bf16), normed_in, w_all, wo_all, q_pre, k_pre, query_rot, key_rot, values, context, lse, cosine, sine, pos,
        g_qk, g_attn[None], grad_moe_gain[None], shares, (arrived, grad_arrived, expert_hidden, grad_gate_pre, grad_up_pre),
        nf, zs, hp, scale, 4
    )
    block_output = (hidden_res + mixed.astype(f32)).astype(bf16)
    total = jnp.sum(summed, axis=0)
    part = lambda row, size: lax.dynamic_slice_in_dim(row, me * size % rows, size)
    own_attn_gain = part(total[0], gs)
    own_moe_gain = part(total[1], gs)
    own_qk = jnp.stack([part(total[2], qs), part(total[3], qs)])
    grad_wo = grad_wo.astype(f32)
    grad_wq = grads[:, :, :qw].transpose(1, 0, 2).reshape(shard, heads * hd).astype(f32)
    grad_kv = grads[:, :, qw:].reshape(kv_heads, per, shard, hd)
    grad_wk = grad_kv[:, 0].transpose(1, 0, 2).reshape(shard, kv_heads * hd).astype(f32)
    grad_wv = grad_kv[:, 1].transpose(1, 0, 2).reshape(shard, kv_heads * hd).astype(f32)
    _, in_back = jax.vjp(rms_scale, resid, g_attn)
    grad_input = grad_res + in_back(grad_in.astype(f32))[0]
    return (
        block_output[None],
        grad_input[None],
        own_attn_gain,
        grad_wq,
        grad_wk,
        grad_wv,
        own_qk,
        grad_wo,
        own_moe_gain,
        grad_gate[None].astype(f32),
        grad_up[None].astype(f32),
        grad_down[None].astype(f32),
    )


def body(nf, nc, block_input, *rest):
    kv_heads = rest[3].shape[1] // (rest[5].shape[1] * nf * nc)
    fits = nf == 4 and nc == 2 * kv_heads and rest[4].shape[1] == rest[3].shape[1]
    return head_body(nf, nc, block_input, *rest) if fits else wide_body(block_input, *rest)


def solution(mesh):
    return jax.shard_map(
        functools.partial(body, mesh.shape["fsdp"], mesh.shape["cp"]),
        mesh=mesh,
        in_specs=(
            P("fsdp", "cp", None),
            P("fsdp", "cp", None),
            P(("fsdp", "cp")),
            P(("fsdp", "cp"), None),
            P(("fsdp", "cp"), None),
            P(("fsdp", "cp"), None),
            P(None, ("fsdp", "cp")),
            P(("fsdp", "cp"), None),
            P(("fsdp", "cp")),
            P(("fsdp", "cp"), None, None),
            P(("fsdp", "cp"), None, None),
            P(("fsdp", "cp"), None, None),
            P("fsdp", "cp", None),
            P("fsdp", "cp", None),
            P(),
        ),
        out_specs=(
            P("fsdp", "cp", None),
            P("fsdp", "cp", None),
            P(("fsdp", "cp")),
            P(("fsdp", "cp"), None),
            P(("fsdp", "cp"), None),
            P(("fsdp", "cp"), None),
            P(None, ("fsdp", "cp")),
            P(("fsdp", "cp"), None),
            P(("fsdp", "cp")),
            P(("fsdp", "cp"), None, None),
            P(("fsdp", "cp"), None, None),
            P(("fsdp", "cp"), None, None),
        ),
        check_vma=False,
    )
```
